128 devices in a mesh: ens: 1, slab: 2 (over core), feat: 64 (over z, y, x).
Axes of the slice: x: 4, y: 4, z: 4, core: 2. Of those that a mesh axis runs over, the one named last changes fastest.
Arguments:
- particles: float32 [2048, 65536], P('ens', ('slab', 'feat'))
- prec_diag: float32 [65536], P(('ens', 'slab', 'feat'))
- mean_vec: float32 [65536], P(('ens', 'slab', 'feat'))
- low_rank: bfloat16 [65536, 128], P(('ens', 'slab', 'feat'))
Outputs:
- output: float32 [2048, 65536], P('ens', ('slab', 'feat'))
All inputs are finite; a program needn't handle non-finite values.
Results may differ from the reference program's by a relative error of at most 0.001.
Values are sent between devices in bfloat16 or wider.
A program may use at most 1 GiB of HBM per device.

```python
import jax
import jax.numpy as jnp
from jax import lax

N = 2048
D = 65536
R = 128
NUM_STEPS = 3
BANDWIDTH = 4.0 * D
STEP_SIZE = 0.4 * D


def setup_inputs(seed: int = 0, part: int = 0) -> dict:
    base_key = jax.random.fold_in(jax.random.key(seed), part)
    key_mean, key_shift, key_noise, key_prec, key_fac, key_coef, key_cmean = jax.random.split(base_key, 7)
    mean_vec = jax.random.normal(key_mean, (D,), jnp.float32)
    mean_shift = jax.random.normal(key_shift, (D,), jnp.float32)
    spread_noise = jax.random.normal(key_noise, (N, D), jnp.float32)
    prec_diag = jax.random.uniform(key_prec, (D,), jnp.float32, 0.2, 1.8) / D
    fac_scale = 1.3 / D
    low_rank = (jax.random.normal(key_fac, (D, R), jnp.float32) * fac_scale).astype(jnp.bfloat16)
    coef_rows = jax.random.normal(key_cmean, (1, R), jnp.float32) + jax.random.normal(key_coef, (N, R), jnp.float32)
    span_part = jnp.dot(coef_rows, low_rank.astype(jnp.float32).T) / (fac_scale * R ** 0.5)
    particles = mean_vec[None, :] + mean_shift[None, :] + spread_noise + span_part
    return {"particles": particles, "prec_diag": prec_diag, "mean_vec": mean_vec, "low_rank": low_rank}


def svgd_step(particles, prec_diag, mean_vec, low_rank):
    centered = particles - mean_vec[None, :]
    proj_full = jnp.dot(centered.astype(jnp.bfloat16), low_rank, preferred_element_type=jnp.float32)
    low_term = jnp.dot(proj_full.astype(jnp.bfloat16), low_rank.T, preferred_element_type=jnp.float32)
    grad_log = -(centered * prec_diag[None, :] + low_term)
    part_bf = particles.astype(jnp.bfloat16)
    gram_full = jnp.dot(part_bf, part_bf.T, preferred_element_type=jnp.float32)
    gram_diag = jnp.diagonal(gram_full)
    sq_dist = jnp.maximum(gram_diag[:, None] + gram_diag[None, :] - 2.0 * gram_full, 0.0)
    kernel = jnp.exp(-sq_dist / BANDWIDTH)
    drive_term = grad_log - (2.0 / BANDWIDTH) * particles
    applied = jnp.dot(kernel.astype(jnp.bfloat16), drive_term.astype(jnp.bfloat16), preferred_element_type=jnp.float32)
    phi_dir = (applied + (2.0 / BANDWIDTH) * jnp.sum(kernel, axis=1)[:, None] * particles) / N
    return particles + STEP_SIZE * phi_dir


def reference(particles, prec_diag, mean_vec, low_rank):
    def scan_body(carry, unused):
        return svgd_step(carry, prec_diag, mean_vec, low_rank), None
    result_particles, unused_out = lax.scan(scan_body, particles, None, length=NUM_STEPS)
    return result_particles
```

```python
import functools

import jax
import jax.numpy as jnp
from jax import lax
from jax.experimental import pallas as pl
from jax.experimental.pallas import tpu as pltpu
from jax.sharding import PartitionSpec as P

NUM_STEPS = 3
BAND_SCALE = 4.0
STEP_SCALE = 0.4
FEAT_AXES = ("slab", "feat")
LEAD_AXES = ("ens", "slab", "feat")

ROWS = 2048
TILE = 128
BLK = 512
COLORS = 6
SROWS = COLORS * BLK
UNITS = (None, ((0, 1), (0, 2), (0, 3)), ((1, 2), (1, 3), (2, 3)))
OFFS = (((0, 1), (0, 2), (0, 3)), ((1, 2), (1, 3), (2, 3)))
PM_ROW = 4 * BLK
OWN = 32
MESH = pl.DeviceIdType.MESH
NT = (((1,), (1,)), ((), ()))
F32, BF16 = jnp.float32, jnp.bfloat16


def div(a, b):
    return lax.div(a, jnp.int32(b))


def rem(a, b):
    return lax.rem(a, jnp.int32(b))


def _kernel(
    bandwidth, step_size, n_part,
    theta_ref, lam_ref, mu_ref, fac_ref, out_ref,
    bfull, pml, pmr, nrow, ncol, srow, pack, r0, r1, r2, r3, kg, kfull, adrv, svec, srecv, stot, spart,
    pre_send, pre_recv, rs_send, rs_recv, x_send, x_recv, dd_send, dd_recv, s_send, s_recv, sp_send, sp_recv,
):
    width = theta_ref.shape[1]
    rep_coef = 2.0 / bandwidth
    core = lax.axis_index("slab")
    feat = lax.axis_index("feat")
    coords = (rem(feat, 4), rem(div(feat, 4), 4), div(feat, 16))
    strides = (1, 4, 16)

    def chip(dim, coord):
        return {"feat": feat + (coord - coords[dim]) * strides[dim]}

    turned = [[coords[dim]] + [rem(coords[dim] + j, 4) for j in range(1, 4)] for dim in range(3)]

    def around(dim, j):
        return turned[dim][j]

    ring = [[chip(dim, turned[dim][j]) for j in range(4)] for dim in range(3)]
    low_bit = [rem(c, 2) for c in coords]
    pair_bit = [[rem(div(t + 1, 2), 2) for t in turned[dim]] for dim in range(3)]
    high_bit = [[div(t, 2) for t in turned[dim]] for dim in range(3)]

    mate = {"slab": 1 - core}

    def al(x, m=16):
        return pl.multiple_of(x, m)

    halves = []
    for k in range(COLORS):
        steps = []
        start, length, cur = 0, BLK, coords[k % 3]
        for s in range(2):
            if (k // 3 + s) % 2 == 0:
                other, bit = cur + 1 - 2 * low_bit[k % 3], pair_bit[k % 3][0]
            else:
                other, bit = 3 - cur, high_bit[k % 3][0]
            length = length // 2
            keep, give = start + bit * length, start + (1 - bit) * length
            start = keep
            steps.append((chip(k % 3, other), length, keep, give))
        halves.append(steps)

    def dims(k):
        return k % 3, (k + 1) % 3, (k + 2) % 3

    def base(st, k):
        return st * SROWS + k * BLK

    quarters = [[base(st, k) + halves[k][1][2] for k in range(COLORS)] for st in range(3)]
    owns = [[quarters[st][k] + OWN * coords[dims(k)[1]] for k in range(COLORS)] for st in range(3)]
    pieces = [[OWN * around(dims(k)[1], j) for j in range(4)] for k in range(COLORS)]

    places = []
    for k in range(COLORS):
        one, two = (pair_bit, high_bit) if k < 3 else (high_bit, pair_bit)
        places.append([TILE * (2 * one[k % 3][j] + two[k % 3][j]) for j in range(4)])

    def quarter(st, k):
        return quarters[st][k]

    def own(st, k):
        return owns[st][k]

    barrier = pltpu.get_barrier_semaphore()
    pl.semaphore_signal(barrier, inc=1, device_id=mate, device_id_type=MESH)
    for dim in range(3):
        for j in range(1, 4):
            pl.semaphore_signal(barrier, inc=1, device_id=ring[dim][j], device_id_type=MESH)
    pl.semaphore_wait(barrier, 10)

    row_i = lax.broadcasted_iota(jnp.int32, (TILE, TILE), 0)
    col_i = lax.broadcasted_iota(jnp.int32, (TILE, TILE), 1)
    eye, upper, lower = row_i == col_i, row_i < col_i, row_i > col_i
    sub_o = lax.broadcasted_iota(jnp.int32, (OWN, TILE), 0)
    lane_o = lax.broadcasted_iota(jnp.int32, (OWN, TILE), 1)

    def remote(src, dst, ssem, rsem, where):
        return pltpu.make_async_remote_copy(src_ref=src, dst_ref=dst, send_sem=ssem, recv_sem=rsem, device_id=where, device_id_type=MESH)

    def pre_copy(ch, what):
        if what == 0:
            rows = pl.ds(ch * BLK, BLK)
            src, dst = bfull.at[rows, 0:width], bfull.at[rows, width:2 * width]
        else:
            src, dst = pml.at[pl.ds(al(ch * BLK + (1 - core) * 256), 256)], pmr.at[pl.ds(ch * 256, 256)]
        return remote(src, dst, pre_send.at[what, ch], pre_recv.at[what, ch], mate)

    def prepare(ch, th):
        rows = pl.ds(ch * BLK, BLK)
        bfull[rows, 0:width] = th.astype(BF16)
        pml[rows, :] = jnp.dot((th - mu_ref[...]).astype(BF16), fac_ref[...], preferred_element_type=F32)

    for ch in range(4):
        rows = pl.ds(ch * BLK, BLK)
        th = theta_ref[rows, :]
        out_ref[rows, :] = th
        prepare(ch, th)
        for what in range(2):
            pre_copy(ch, what).start()

    def one_step(step_index, carry):
        sends = []

        def begin(cps):
            for cp in cps:
                cp.start()
            sends.extend(cps)

        def rs_copy(st, s, k):
            peer, length, keep, give = halves[k][s]
            src = pack.at[pl.ds(al(base(st, k) + give), length)]
            return remote(src, (r0, r1)[s].at[st, k], rs_send.at[st, s, k], rs_recv.at[st, s, k], peer)

        def x_copies(st, e, k):
            d1, d2, d3 = dims(k)
            dim = (d2, d3, d2, d1)[e]
            cps = []
            for j in range(1, 4):
                if e == 0:
                    src = pack.at[pl.ds(al(quarter(st, k) + pieces[k][j]), OWN)]
                    dst = r2.at[st, k, j - 1]
                elif e == 1:
                    src = dst = r3.at[st, k, coords[dim]]
                else:
                    rng = pl.ds(al(own(st, k)), OWN) if e == 2 else pl.ds(al(quarter(st, k)), TILE)
                    src = dst = kg.at[core, rng]
                cps.append(remote(src, dst, x_send.at[st, e, k, j - 1], x_recv.at[st, e, k, j - 1], ring[dim][j]))
            return cps

        def dd_copy(st, k, j):
            if j == 0:
                begin_row = quarter(st, k)
            else:
                begin_row = base(st, k) + places[k][4 - j]
            rng = pl.ds(al(begin_row), TILE)
            return remote(kg.at[core, rng], kg.at[core, rng], dd_send.at[st, k, j], dd_recv.at[st, k, j], mate)

        def s_copies(st, ph, d):
            dim = ((d + 1) % 3, d)[ph]
            return [
                remote(svec.at[st, ph, d], srecv.at[st, ph, d, j - 1], s_send.at[st, ph, d, j - 1], s_recv.at[st, ph, d, j - 1], ring[dim][j])
                for j in range(1, 4)
            ]

        def sp_copy(st):
            return remote(stot.at[st], spart.at[st], sp_send.at[st], sp_recv.at[st], mate)

        def diag_tiles(sup):
            bb = bfull[pl.ds(sup * BLK, BLK), :]
            g = lax.dot_general(bb, bb, NT, preferred_element_type=F32)

            def tile(i, j):
                return g[i * TILE:(i + 1) * TILE, j * TILE:(j + 1) * TILE]

            rows_n, cols_n = [], []
            for i in range(4):
                d = jnp.where(eye, tile(i, i), 0.0)
                rows_n.append(jnp.broadcast_to(jnp.sum(d, axis=1, keepdims=True), (TILE, TILE)))
                cols_n.append(jnp.sum(d, axis=0, keepdims=True))
                nrow[pl.ds((4 * sup + i) * TILE, TILE), :] = rows_n[i]
                ncol[pl.ds(4 * sup + i, 1), :] = cols_n[i]

            def dist(i, j):
                return rows_n[i] + cols_n[j] - 2.0 * tile(i, j)

            for t in range(3):
                pack[pl.ds(base(0, sup) + t * TILE, TILE), :] = jnp.where(core == 0, dist(*OFFS[0][t]), dist(*OFFS[1][t]))
            one = jnp.where(core == 0, dist(0, 0), dist(2, 2))
            two = jnp.where(core == 0, dist(1, 1), dist(3, 3))
            pack[pl.ds(base(0, sup) + 3 * TILE, TILE), :] = jnp.where(upper, one, two)

        def unit_tiles(st, u):
            sup, m = UNITS[st][u]
            lhs = bfull[pl.ds(sup * BLK, BLK), :]
            rhs = bfull[pl.ds(al((2 * m + core) * 256), 256), :]
            g = lax.dot_general(lhs, rhs, NT, preferred_element_type=F32)
            for b in range(2):
                nc = ncol[pl.ds(4 * m + 2 * core + b, 1), :]
                pack[pl.ds(base(st, 2 * u + b), BLK), :] = nrow[pl.ds(sup * BLK, BLK), :] + nc - 2.0 * g[:, b * TILE:(b + 1) * TILE]

        def row_sums(st, k, kern):
            place = own(0, k) - base(0, k)
            slot, r = div(place, TILE), rem(place, TILE)

            def by_rows(vals):
                rs = jnp.sum(vals, axis=1, keepdims=True)
                return jnp.sum(jnp.where(lane_o == sub_o + r, rs, 0.0), axis=0, keepdims=True)

            def by_cols(vals):
                return jnp.sum(vals, axis=0, keepdims=True)

            if st > 0:
                sup, m = UNITS[st][k // 2]
                return [(4 * sup + slot, by_rows(kern)), (4 * m + 2 * core + k % 2, by_cols(kern))]
            both = div(slot, 3)
            i0 = (1 - both) * core * (1 + div(slot, 2)) + both * 2 * core
            j0 = (1 - both) * ((1 - core) * (slot + 1) + core * (2 + div(slot + 1, 2))) + both * 2 * core
            up = jnp.where(lane_o + 1000 * (1 - both) > sub_o + r, kern, 0.0)
            lo = jnp.where(lane_o + 1000 * (1 - both) < sub_o + r, kern, 0.0)
            nxt = 4 * k + 2 * core + 1
            return [(4 * k + i0, by_rows(up)), (4 * k + j0, by_cols(up)), (nxt, by_rows(lo)), (nxt, by_cols(lo))]

        def advance(st, s):
            parts = [[], [], []]
            for k in range(COLORS):
                mine = pl.ds(al(own(st, k)), OWN)
                if s < 2:
                    peer, length, keep, give = halves[k][s]
                    rs_copy(st, s, k).wait_recv()
                    rng = pl.ds(al(base(st, k) + keep), length)
                    pack[rng, :] += (r0, r1)[s][st, k]
                    begin([rs_copy(st, 1, k)] if s == 0 else x_copies(st, 0, k))
                elif s == 2:
                    for cp in x_copies(st, 0, k):
                        cp.wait_recv()
                    r3[st, k, coords[dims(k)[2]]] = pack[mine, :] + r2[st, k, 0] + r2[st, k, 1] + r2[st, k, 2]
                    begin(x_copies(st, 1, k))
                elif s == 3:
                    for cp in x_copies(st, 1, k):
                        cp.wait_recv()
                    full = (r3[st, k, 0] + r3[st, k, 1]) + (r3[st, k, 2] + r3[st, k, 3])
                    if st == 0 and k >= 4:
                        kern = full
                    else:
                        kern = jnp.exp(-jnp.maximum(full, 0.0) / bandwidth)
                        parts[k % 3] += row_sums(st, k, kern)
                    kg[core, mine, :] = kern.astype(BF16)
                    begin(x_copies(st, 2, k))
                elif s == 4:
                    for cp in x_copies(st, 2, k):
                        cp.wait_recv()
                    begin(x_copies(st, 3, k))
                    begin([dd_copy(st, k, 0)])
                else:
                    for j, cp in enumerate(x_copies(st, 3, k)):
                        cp.wait_recv()
                        begin([dd_copy(st, k, j + 1)])
            if s == 3:
                for d in range(3):
                    svec[st, 0, d] = jnp.zeros((16, TILE), F32)
                    for block, line in parts[d]:
                        svec[st, 0, d, pl.ds(block, 1), :] += line
                    begin(s_copies(st, 0, d))
            if s == 4:
                for d in range(3):
                    for cp in s_copies(st, 0, d):
                        cp.wait_recv()
                    svec[st, 1, d] = svec[st, 0, d] + srecv[st, 0, d, 0] + srecv[st, 0, d, 1] + srecv[st, 0, d, 2]
                    begin(s_copies(st, 1, d))
            if s == 5:
                tot = jnp.zeros((16, TILE), F32)
                for d in range(3):
                    for cp in s_copies(st, 1, d):
                        cp.wait_recv()
                    tot = tot + ((svec[st, 1, d] + srecv[st, 1, d, 0]) + (srecv[st, 1, d, 1] + srecv[st, 1, d, 2]))
                stot[st] = tot
                begin([sp_copy(st)])

        def unpack(st):
            for k in range(COLORS):
                for j in range(4):
                    dd_copy(st, k, j).wait_recv()
            for c in range(2):
                if st > 0:
                    for k in range(COLORS):
                        sup, m = UNITS[st][k // 2]
                        src = kg[c, pl.ds(base(st, k), BLK), :]
                        jcol = pl.ds((4 * m + 2 * c + k % 2) * TILE, TILE)
                        kfull[pl.ds(sup * BLK, BLK), jcol] = src
                        kfull[jcol, pl.ds(sup * BLK, BLK)] = src.T
                    continue
                for sup in range(4):
                    for t, (i, j) in enumerate(OFFS[c]):
                        src = kg[c, pl.ds(base(0, sup) + t * TILE, TILE), :]
                        ri, rj = pl.ds((4 * sup + i) * TILE, TILE), pl.ds((4 * sup + j) * TILE, TILE)
                        kfull[ri, rj] = src
                        kfull[rj, ri] = src.T
                    src = kg[c, pl.ds(base(0, sup) + 3 * TILE, TILE), :]
                    srt = src.T
                    one = jnp.ones((TILE, TILE), BF16)
                    ra, rb = pl.ds((4 * sup + 2 * c) * TILE, TILE), pl.ds((4 * sup + 2 * c + 1) * TILE, TILE)
                    kfull[ra, ra] = jnp.where(upper, src, jnp.where(lower, srt, one))
                    kfull[rb, rb] = jnp.where(lower, src, jnp.where(upper, srt, one))

        def drive():
            for q in range(8):
                rows = pl.ds(q * 256, 256)
                pm = kg[q % 2, pl.ds(PM_ROW + (q // 2) * 256, 256), :]
                low = lax.dot_general(pm, fac_ref[...], NT, preferred_element_type=F32)
                th = out_ref[rows, :]
                grad = -((th - mu_ref[...]) * lam_ref[...] + low)
                adrv[rows, :] = (grad - rep_coef * th).astype(BF16)

        def sum_rows(blocks):
            tot = stot[0] + spart[0] + stot[1] + spart[1] + 1.0
            if len(blocks) > 4:
                tot = tot + (stot[2] + spart[2])
            for blk in blocks:
                line = jnp.sum(jnp.where(eye, jnp.broadcast_to(tot[blk:blk + 1, :], (TILE, TILE)), 0.0), axis=1, keepdims=True)
                srow[pl.ds(blk * TILE, TILE), :] = jnp.broadcast_to(rep_coef * line, (TILE, TILE))

        def update(ch):
            rows = pl.ds(ch * BLK, BLK)
            acc = jnp.dot(kfull[rows, :], adrv[...], preferred_element_type=F32)
            new = []
            for t in range(width // TILE):
                cols = slice(t * TILE, (t + 1) * TILE)
                th = out_ref[rows, cols]
                phi = (acc[:, cols] + srow[rows, :] * th) / n_part
                new.append(th + step_size * phi)
            th = jnp.concatenate(new, axis=1)
            out_ref[rows, :] = th
            prepare(ch, th)

            @pl.when(step_index < NUM_STEPS - 1)
            def _():
                for what in range(2):
                    pre_copy(ch, what).start()

        for ch in range(4):
            pre_copy(ch, 1).wait_recv()
            mine = pl.ds(al(ch * BLK + core * 256), 256)
            pack[pl.ds(PM_ROW + ch * 256, 256), :] = pml[mine, :] + pmr[pl.ds(ch * 256, 256), :]
            if ch % 2 == 1:
                begin([rs_copy(0, 0, 4 + ch // 2)])
        for sup in range(4):
            pre_copy(sup, 0).wait_recv()
            diag_tiles(sup)
            begin([rs_copy(0, 0, sup)])
        for st in (1, 2):
            for u in range(3):
                unit_tiles(st, u)
                begin([rs_copy(st, 0, 2 * u), rs_copy(st, 0, 2 * u + 1)])
        for s in range(5):
            for st in range(3):
                advance(st, s)
        advance(0, 5)
        advance(1, 5)
        unpack(0)
        drive()
        advance(2, 5)
        for ch in range(4):
            for what in range(2):
                pre_copy(ch, what).wait_send()
        sp_copy(0).wait_recv()
        sp_copy(1).wait_recv()
        sum_rows(range(4))
        unpack(1)
        update(0)
        sp_copy(2).wait_recv()
        sum_rows(range(4, 16))
        unpack(2)
        for ch in range(1, 4):
            update(ch)
        for cp in sends:
            cp.wait_send()
        return carry

    lax.fori_loop(0, NUM_STEPS, one_step, 0)


def solution(mesh):
    def run_steps(particles, prec_diag, mean_vec, low_rank):
        total_rows, width = particles.shape
        n_part = total_rows // mesh.shape["ens"]
        bandwidth = BAND_SCALE * width
        step_size = STEP_SCALE * width
        loc = width // (mesh.shape["slab"] * mesh.shape["feat"])
        rank = low_rank.shape[1]
        vm, dma = pltpu.VMEM, pltpu.SemaphoreType.DMA

        def local_steps(current, prec_loc, mean_loc, fac_loc):
            spec = pl.BlockSpec(memory_space=pltpu.VMEM)
            call = pl.pallas_call(
                functools.partial(_kernel, bandwidth, step_size, n_part),
                out_shape=jax.ShapeDtypeStruct((n_part, loc), F32),
                in_specs=[spec] * 4,
                out_specs=spec,
                scratch_shapes=[
                    vm((ROWS, 2 * loc), BF16), vm((ROWS, rank), F32), vm((ROWS // 2, rank), F32),
                    vm((ROWS, TILE), F32), vm((16, TILE), F32), vm((ROWS, TILE), F32),
                    vm((3 * SROWS, TILE), F32),
                    vm((3, COLORS, BLK // 2, TILE), F32), vm((3, COLORS, BLK // 4, TILE), F32),
                    vm((3, COLORS, 3, OWN, TILE), F32), vm((3, COLORS, 4, OWN, TILE), F32),
                    vm((2, 3 * SROWS, TILE), BF16), vm((ROWS, ROWS), BF16), vm((ROWS, loc), BF16),
                    vm((3, 2, 3, 16, TILE), F32), vm((3, 2, 3, 3, 16, TILE), F32), vm((3, 16, TILE), F32), vm((3, 16, TILE), F32),
                    dma((2, 4)), dma((2, 4)), dma((3, 2, COLORS)), dma((3, 2, COLORS)), dma((3, 4, COLORS, 3)), dma((3, 4, COLORS, 3)),
                    dma((3, COLORS, 4)), dma((3, COLORS, 4)), dma((3, 2, 3, 3)), dma((3, 2, 3, 3)), dma((3,)), dma((3,)),
                ],
                compiler_params=pltpu.CompilerParams(collective_id=0, has_side_effects=True, vmem_limit_bytes=62 * 1024 * 1024),
                name="svgd",
            )
            return call(current, prec_loc.reshape(1, loc), mean_loc.reshape(1, loc), fac_loc)

        sharded = jax.shard_map(
            local_steps,
            mesh=mesh,
            in_specs=(P("ens", FEAT_AXES), P(LEAD_AXES), P(LEAD_AXES), P(LEAD_AXES, None)),
            out_specs=P("ens", FEAT_AXES),
            check_vma=False,
        )
        return sharded(particles, prec_diag, mean_vec, low_rank)

    return run_steps
```

```python
import functools

import jax
import jax.numpy as jnp
from jax import lax
from jax.experimental import pallas as pl
from jax.experimental.pallas import tpu as pltpu
from jax.sharding import PartitionSpec as P

NUM_STEPS = 3
BAND_SCALE = 4.0
STEP_SCALE = 0.4
FEAT_AXES = ("slab", "feat")
LEAD_AXES = ("ens", "slab", "feat")

ROWS = 2048
TILE = 128
BLK = 512
COLORS = 6
SROWS = COLORS * BLK
UNITS = (None, ((0, 1), (0, 2), (0, 3)), ((1, 2), (1, 3), (2, 3)))
OFFS = (((0, 1), (0, 2), (0, 3)), ((1, 2), (1, 3), (2, 3)))
PM_ROW = 4 * BLK
SENT = 1536 + 768 + 576 + 576 + 288 + 1152 + 1536 + 288 + 16
OWN = 32
MESH = pl.DeviceIdType.MESH
NT = (((1,), (1,)), ((), ()))
F32, BF16 = jnp.float32, jnp.bfloat16


def div(a, b):
    return lax.div(a, jnp.int32(b))


def rem(a, b):
    return lax.rem(a, jnp.int32(b))


def _kernel(
    bandwidth, step_size, n_part,
    theta_ref, lam_ref, mu_ref, fac_ref, out_ref,
    bfull, pml, pmr, nrow, ncol, srow, pack, r0, r1, r2, r3, kg, kfull, adrv, svec, srecv, stot, spart,
    in_sem, pre_send, pre_recv, sent, rs_recv, x_recv, far_recv, dd_recv, s_recv, sp_recv,
):
    width = out_ref.shape[1]
    rep_coef = 2.0 / bandwidth
    core = lax.axis_index("slab")
    feat = lax.axis_index("feat")
    coords = (rem(feat, 4), rem(div(feat, 4), 4), div(feat, 16))
    strides = (1, 4, 16)

    def chip(dim, coord):
        return {"feat": feat + (coord - coords[dim]) * strides[dim]}

    turned = [[coords[dim]] + [rem(coords[dim] + j, 4) for j in range(1, 4)] for dim in range(3)]

    def around(dim, j):
        return turned[dim][j]

    ring = [[chip(dim, turned[dim][j]) for j in range(4)] for dim in range(3)]
    low_bit = [rem(c, 2) for c in coords]
    pair_bit = [[rem(div(t + 1, 2), 2) for t in turned[dim]] for dim in range(3)]
    high_bit = [[div(t, 2) for t in turned[dim]] for dim in range(3)]

    mate = {"slab": 1 - core}

    def al(x, m=16):
        return pl.multiple_of(x, m)

    halves = []
    for k in range(COLORS):
        steps = []
        start, length, cur = 0, BLK, coords[k % 3]
        for s in range(2):
            if (k // 3 + s) % 2 == 0:
                other, bit = cur + 1 - 2 * low_bit[k % 3], pair_bit[k % 3][0]
            else:
                other, bit = 3 - cur, high_bit[k % 3][0]
            length = length // 2
            keep, give = start + bit * length, start + (1 - bit) * length
            start = keep
            steps.append((chip(k % 3, other), length, keep, give))
        halves.append(steps)

    def dims(k):
        return k % 3, (k + 1) % 3, (k + 2) % 3

    def base(st, k):
        return st * SROWS + k * BLK

    quarters = [[base(st, k) + halves[k][1][2] for k in range(COLORS)] for st in range(3)]
    owns = [[quarters[st][k] + OWN * coords[dims(k)[1]] for k in range(COLORS)] for st in range(3)]
    pieces = [[OWN * around(dims(k)[1], j) for j in range(4)] for k in range(COLORS)]

    places = []
    for k in range(COLORS):
        one, two = (pair_bit, high_bit) if k < 3 else (high_bit, pair_bit)
        places.append([TILE * (2 * one[k % 3][j] + two[k % 3][j]) for j in range(4)])

    def quarter(st, k):
        return quarters[st][k]

    def own(st, k):
        return owns[st][k]

    barrier = pltpu.get_barrier_semaphore()
    pl.semaphore_signal(barrier, inc=1, device_id=mate, device_id_type=MESH)
    for dim in range(3):
        for j in range(1, 4):
            pl.semaphore_signal(barrier, inc=1, device_id=ring[dim][j], device_id_type=MESH)
    loads = [pltpu.make_async_copy(theta_ref.at[pl.ds(ch * BLK, BLK)], out_ref.at[pl.ds(ch * BLK, BLK)], in_sem.at[ch]) for ch in range(4)]
    for cp in loads:
        cp.start()

    row_i = lax.broadcasted_iota(jnp.int32, (TILE, TILE), 0)
    col_i = lax.broadcasted_iota(jnp.int32, (TILE, TILE), 1)
    eye, upper, lower = row_i == col_i, row_i < col_i, row_i > col_i
    sub_o = lax.broadcasted_iota(jnp.int32, (OWN, TILE), 0)
    lane_o = lax.broadcasted_iota(jnp.int32, (OWN, TILE), 1)

    def remote(src, dst, ssem, rsem, where):
        return pltpu.make_async_remote_copy(src_ref=src, dst_ref=dst, send_sem=ssem, recv_sem=rsem, device_id=where, device_id_type=MESH)

    def pre_copy(ch, what):
        if what == 0:
            rows = pl.ds(ch * BLK, BLK)
            src, dst = bfull.at[rows, 0:width], bfull.at[rows, width:2 * width]
        else:
            src, dst = pml.at[pl.ds(al(ch * BLK + (1 - core) * 256), 256)], pmr.at[pl.ds(ch * 256, 256)]
        return remote(src, dst, pre_send, pre_recv.at[what, ch], mate)

    def prepare(start, length, th):
        rows = pl.ds(start, length)
        bfull[rows, 0:width] = th.astype(BF16)
        pml[rows, :] = jnp.dot((th - mu_ref[...]).astype(BF16), fac_ref[...], preferred_element_type=F32)

    def begin(cps):
        for cp in cps:
            cp.start()

    def arrive(ref, sem):
        remote(ref, ref, sent.at[0], sem, mate).wait_recv()

    def x_arrive(st, e, k):
        arrive((r2.at[st, k], r3.at[st, k, 0:3], kg.at[core, 0:3 * OWN])[e], x_recv.at[st, e, k])

    def rs_copy(st, s, k):
        peer, length, keep, give = halves[k][s]
        src = pack.at[pl.ds(al(base(st, k) + give), length)]
        return remote(src, (r0, r1)[s].at[st, k], sent.at[st], rs_recv.at[st, s, k], peer)

    def x_copies(st, e, k):
        d1, d2, d3 = dims(k)
        dim = (d2, d3, d2, d1)[e]
        cps = []
        for j in range(1, 4):
            if e == 0:
                src = pack.at[pl.ds(al(quarter(st, k) + pieces[k][j]), OWN)]
                dst = r2.at[st, k, j - 1]
            elif e == 1:
                src = dst = r3.at[st, k, coords[dim]]
            else:
                rng = pl.ds(al(own(st, k)), OWN) if e == 2 else pl.ds(al(quarter(st, k)), TILE)
                src = dst = kg.at[core, rng]
            arrived = far_recv.at[st, k, j - 1] if e == 3 else x_recv.at[st, e, k]
            cps.append(remote(src, dst, sent.at[st], arrived, ring[dim][j]))
        return cps

    def dd_copy(st, k, j):
        if j == 0:
            begin_row = quarter(st, k)
        else:
            begin_row = base(st, k) + places[k][4 - j]
        rng = pl.ds(al(begin_row), TILE)
        return remote(kg.at[core, rng], kg.at[core, rng], sent.at[st], dd_recv.at[st, k], mate)

    def s_copies(st, ph, d):
        dim = ((d + 1) % 3, d)[ph]
        return [
            remote(svec.at[st, ph, d], srecv.at[st, ph, d, j - 1], sent.at[st], s_recv.at[st, ph, d], ring[dim][j])
            for j in range(1, 4)
        ]

    def sp_copy(st):
        return remote(stot.at[st], spart.at[st], sent.at[st], sp_recv.at[st], mate)

    def diag_tiles(sup):
        bb = bfull[pl.ds(sup * BLK, BLK), :]
        g = lax.dot_general(bb, bb, NT, preferred_element_type=F32)

        def tile(i, j):
            return g[i * TILE:(i + 1) * TILE, j * TILE:(j + 1) * TILE]

        rows_n, cols_n = [], []
        for i in range(4):
            d = jnp.where(eye, tile(i, i), 0.0)
            rows_n.append(jnp.broadcast_to(jnp.sum(d, axis=1, keepdims=True), (TILE, TILE)))
            cols_n.append(jnp.sum(d, axis=0, keepdims=True))
            nrow[pl.ds((4 * sup + i) * TILE, TILE), :] = rows_n[i]
            ncol[pl.ds(4 * sup + i, 1), :] = cols_n[i]

        def dist(i, j):
            return rows_n[i] + cols_n[j] - 2.0 * tile(i, j)

        for t in range(3):
            pack[pl.ds(base(0, sup) + t * TILE, TILE), :] = jnp.where(core == 0, dist(*OFFS[0][t]), dist(*OFFS[1][t]))
        one = jnp.where(core == 0, dist(0, 0), dist(2, 2))
        two = jnp.where(core == 0, dist(1, 1), dist(3, 3))
        pack[pl.ds(base(0, sup) + 3 * TILE, TILE), :] = jnp.where(upper, one, two)

    def pm_tiles():
        for ch in range(4):
            pre_copy(ch, 1).wait_recv()
            mine = pl.ds(al(ch * BLK + core * 256), 256)
            pack[pl.ds(PM_ROW + ch * 256, 256), :] = pml[mine, :] + pmr[pl.ds(ch * 256, 256), :]
        begin([rs_copy(0, 0, 4), rs_copy(0, 0, 5)])

    def open_step():
        for sup in range(4):
            pre_copy(sup, 0).wait_recv()
            diag_tiles(sup)
            begin([rs_copy(0, 0, sup)])
            if sup == 2:
                pm_tiles()

    for ch in range(4):
        loads[ch].wait()
        prepare(ch * BLK, BLK, out_ref[pl.ds(ch * BLK, BLK), :])
    pl.semaphore_wait(barrier, 10)
    for ch in range(4):
        begin([pre_copy(ch, 1), pre_copy(ch, 0)])
    open_step()

    def one_step(step_index, carry):
        def unit_tiles(st, units):
            sup = UNITS[st][units[0]][0]
            blocks = [4 * UNITS[st][u][1] + 2 * core for u in units]
            lhs = jnp.concatenate([bfull[pl.ds(al(blk * TILE), 256), :] for blk in blocks], axis=0)
            g = lax.dot_general(lhs, bfull[pl.ds(sup * BLK, BLK), :], NT, preferred_element_type=F32)
            for n, u in enumerate(units):
                for b in range(2):
                    nr = nrow[pl.ds(al((blocks[n] + b) * TILE), TILE), :]
                    for a in range(4):
                        tile = g[n * 256 + b * TILE:n * 256 + (b + 1) * TILE, a * TILE:(a + 1) * TILE]
                        pack[pl.ds(base(st, 2 * u + b) + a * TILE, TILE), :] = nr + ncol[4 * sup + a:4 * sup + a + 1, :] - 2.0 * tile
                begin([rs_copy(st, 0, 2 * u), rs_copy(st, 0, 2 * u + 1)])

        def row_sums(st, k, kern):
            place = own(0, k) - base(0, k)
            slot, r = div(place, TILE), rem(place, TILE)

            def by_rows(vals):
                rs = jnp.sum(vals, axis=1, keepdims=True)
                return jnp.sum(jnp.where(lane_o == sub_o + r, rs, 0.0), axis=0, keepdims=True)

            def by_cols(vals):
                return jnp.sum(vals, axis=0, keepdims=True)

            if st > 0:
                sup, m = UNITS[st][k // 2]
                return [(4 * m + 2 * core + k % 2, by_rows(kern)), (4 * sup + slot, by_cols(kern))]
            both = div(slot, 3)
            i0 = (1 - both) * core * (1 + div(slot, 2)) + both * 2 * core
            j0 = (1 - both) * ((1 - core) * (slot + 1) + core * (2 + div(slot + 1, 2))) + both * 2 * core
            up = jnp.where(lane_o + 1000 * (1 - both) > sub_o + r, kern, 0.0)
            lo = jnp.where(lane_o + 1000 * (1 - both) < sub_o + r, kern, 0.0)
            nxt = 4 * k + 2 * core + 1
            return [(4 * k + i0, by_rows(up)), (4 * k + j0, by_cols(up)), (nxt, by_rows(lo)), (nxt, by_cols(lo))]

        def advance(st, s):
            parts = [[], [], []]
            for k in range(COLORS):
                mine = pl.ds(al(own(st, k)), OWN)
                if s < 2:
                    peer, length, keep, give = halves[k][s]
                    rs_copy(st, s, k).wait_recv()
                    rng = pl.ds(al(base(st, k) + keep), length)
                    pack[rng, :] += (r0, r1)[s][st, k]
                    begin([rs_copy(st, 1, k)] if s == 0 else x_copies(st, 0, k))
                elif s == 2:
                    x_arrive(st, 0, k)
                    r3[st, k, coords[dims(k)[2]]] = pack[mine, :] + r2[st, k, 0] + r2[st, k, 1] + r2[st, k, 2]
                    begin(x_copies(st, 1, k))
                elif s == 3:
                    x_arrive(st, 1, k)
                    full = (r3[st, k, 0] + r3[st, k, 1]) + (r3[st, k, 2] + r3[st, k, 3])
                    if st == 0 and k >= 4:
                        kern = full
                    else:
                        kern = jnp.exp(-jnp.maximum(full, 0.0) / bandwidth)
                        parts[k % 3] += row_sums(st, k, kern)
                    kg[core, mine, :] = kern.astype(BF16)
                    begin(x_copies(st, 2, k))
                elif s == 4:
                    x_arrive(st, 2, k)
                    begin(x_copies(st, 3, k))
                    begin([dd_copy(st, k, 0)])
                else:
                    for j, cp in enumerate(x_copies(st, 3, k)):
                        cp.wait_recv()
                        begin([dd_copy(st, k, j + 1)])
            if s == 3:
                for d in range(3):
                    svec[st, 0, d] = jnp.zeros((16, TILE), F32)
                    for block, line in parts[d]:
                        svec[st, 0, d, pl.ds(block, 1), :] += line
                    begin(s_copies(st, 0, d))
            if s == 4:
                for d in range(3):
                    arrive(srecv.at[st, 0, d], s_recv.at[st, 0, d])
                    svec[st, 1, d] = svec[st, 0, d] + srecv[st, 0, d, 0] + srecv[st, 0, d, 1] + srecv[st, 0, d, 2]
                    begin(s_copies(st, 1, d))
            if s == 5:
                tot = jnp.zeros((16, TILE), F32)
                for d in range(3):
                    arrive(srecv.at[st, 1, d], s_recv.at[st, 1, d])
                    tot = tot + ((svec[st, 1, d] + srecv[st, 1, d, 0]) + (srecv[st, 1, d, 1] + srecv[st, 1, d, 2]))
                stot[st] = tot
                begin([sp_copy(st)])

        def unpack(st):
            for k in range(COLORS):
                arrive(kg.at[core, 0:BLK], dd_recv.at[st, k])
            for c in range(2):
                if st > 0:
                    for k in range(COLORS):
                        sup, m = UNITS[st][k // 2]
                        jrng = pl.ds((4 * m + 2 * c + k % 2) * TILE, TILE)
                        for a in range(4):
                            src = kg[c, pl.ds(base(st, k) + a * TILE, TILE), :]
                            srng = pl.ds((4 * sup + a) * TILE, TILE)
                            kfull[jrng, srng] = src
                            kfull[srng, jrng] = src.T
                    continue
                for sup in range(4):
                    for t, (i, j) in enumerate(OFFS[c]):
                        src = kg[c, pl.ds(base(0, sup) + t * TILE, TILE), :]
                        ri, rj = pl.ds((4 * sup + i) * TILE, TILE), pl.ds((4 * sup + j) * TILE, TILE)
                        kfull[ri, rj] = src
                        kfull[rj, ri] = src.T
                    src = kg[c, pl.ds(base(0, sup) + 3 * TILE, TILE), :]
                    srt = src.T
                    one = jnp.ones((TILE, TILE), BF16)
                    ra, rb = pl.ds((4 * sup + 2 * c) * TILE, TILE), pl.ds((4 * sup + 2 * c + 1) * TILE, TILE)
                    kfull[ra, ra] = jnp.where(upper, src, jnp.where(lower, srt, one))
                    kfull[rb, rb] = jnp.where(lower, src, jnp.where(upper, srt, one))

        def drive():
            for q in range(8):
                rows = pl.ds(q * 256, 256)
                pm = kg[q % 2, pl.ds(PM_ROW + (q // 2) * 256, 256), :]
                low = lax.dot_general(pm, fac_ref[...], NT, preferred_element_type=F32)
                th = out_ref[rows, :]
                grad = -((th - mu_ref[...]) * lam_ref[...] + low)
                adrv[rows, :] = (grad - rep_coef * th).astype(BF16)

        def sum_rows(blocks):
            tot = stot[0] + spart[0] + stot[1] + spart[1] + 1.0
            if len(blocks) > 4:
                tot = tot + (stot[2] + spart[2])
            for blk in blocks:
                line = jnp.sum(jnp.where(eye, jnp.broadcast_to(tot[blk:blk + 1, :], (TILE, TILE)), 0.0), axis=1, keepdims=True)
                srow[pl.ds(blk * TILE, TILE), :] = jnp.broadcast_to(rep_coef * line, (TILE, TILE))

        def update(ch):
            for half in range(2):
                start = ch * BLK + half * 256
                rows = pl.ds(start, 256)
                acc = jnp.dot(kfull[rows, :], adrv[...], preferred_element_type=F32)
                new = []
                for t in range(width // TILE):
                    cols = slice(t * TILE, (t + 1) * TILE)
                    th = out_ref[rows, cols]
                    phi = (acc[:, cols] + srow[rows, :] * th) / n_part
                    new.append(th + step_size * phi)
                th = jnp.concatenate(new, axis=1)
                out_ref[rows, :] = th
                prepare(start, 256, th)
            begin([pre_copy(ch, 1), pre_copy(ch, 0)])

        unit_tiles(1, (0, 1, 2))
        unit_tiles(2, (0, 1))
        unit_tiles(2, (2,))
        for s in range(5):
            for st in range(3):
                advance(st, s)
        advance(0, 5)
        advance(1, 5)
        unpack(0)
        drive()
        advance(2, 5)
        remote(pack.at[0:5120], pack.at[0:5120], pre_send, sp_recv.at[0], mate).wait_send()
        for st in range(2):
            arrive(stot.at[st], sp_recv.at[st])
        sum_rows(range(4))
        unpack(1)
        update(0)
        arrive(stot.at[2], sp_recv.at[2])
        sum_rows(range(4, 16))
        unpack(2)
        for ch in range(1, 4):
            update(ch)
        for st in range(3):
            remote(pack.at[0:SENT], pack.at[0:SENT], sent.at[st], sp_recv.at[0], mate).wait_send()
        pl.when(step_index < NUM_STEPS - 1)(open_step)
        return carry

    lax.fori_loop(0, NUM_STEPS, one_step, 0)
    for ch in range(4):
        for what in range(2):
            pre_copy(ch, what).wait_recv()
    remote(pack.at[0:5120], pack.at[0:5120], pre_send, sp_recv.at[0], mate).wait_send()


def solution(mesh):
    def run_steps(particles, prec_diag, mean_vec, low_rank):
        total_rows, width = particles.shape
        n_part = total_rows // mesh.shape["ens"]
        bandwidth = BAND_SCALE * width
        step_size = STEP_SCALE * width
        loc = width // (mesh.shape["slab"] * mesh.shape["feat"])
        rank = low_rank.shape[1]
        vm, dma = pltpu.VMEM, pltpu.SemaphoreType.DMA

        def local_steps(current, prec_loc, mean_loc, fac_loc):
            spec = pl.BlockSpec(memory_space=pltpu.VMEM)
            call = pl.pallas_call(
                functools.partial(_kernel, bandwidth, step_size, n_part),
                out_shape=jax.ShapeDtypeStruct((n_part, loc), F32),
                in_specs=[pl.BlockSpec(memory_space=pltpu.HBM)] + [spec] * 3,
                out_specs=spec,
                scratch_shapes=[
                    vm((ROWS, 2 * loc), BF16), vm((ROWS, rank), F32), vm((ROWS // 2, rank), F32),
                    vm((ROWS, TILE), F32), vm((16, TILE), F32), vm((ROWS, TILE), F32),
                    vm((3 * SROWS, TILE), F32),
                    vm((3, COLORS, BLK // 2, TILE), F32), vm((3, COLORS, BLK // 4, TILE), F32),
                    vm((3, COLORS, 3, OWN, TILE), F32), vm((3, COLORS, 4, OWN, TILE), F32),
                    vm((2, 3 * SROWS, TILE), BF16), vm((ROWS, ROWS), BF16), vm((ROWS, loc), BF16),
                    vm((3, 2, 3, 16, TILE), F32), vm((3, 2, 3, 3, 16, TILE), F32), vm((3, 16, TILE), F32), vm((3, 16, TILE), F32),
                    dma((4,)), dma, dma((2, 4)), dma((3,)), dma((3, 2, COLORS)), dma((3, 3, COLORS)), dma((3, COLORS, 3)), dma((3, COLORS)),
                    dma((3, 2, 3)), dma((3,)),
                ],
                compiler_params=pltpu.CompilerParams(collective_id=0, has_side_effects=True, vmem_limit_bytes=48 * 1024 * 1024),
                name="svgd",
            )
            return call(current, prec_loc.reshape(1, loc), mean_loc.reshape(1, loc), fac_loc)

        sharded = jax.shard_map(
            local_steps,
            mesh=mesh,
            in_specs=(P("ens", FEAT_AXES), P(LEAD_AXES), P(LEAD_AXES), P(LEAD_AXES, None)),
            out_specs=P("ens", FEAT_AXES),
            check_vma=False,
        )
        return sharded(particles, prec_diag, mean_vec, low_rank)

    return run_steps
```

```python
import functools

import jax
import jax.numpy as jnp
from jax import lax
from jax.experimental import pallas as pl
from jax.experimental.pallas import tpu as pltpu
from jax.sharding import PartitionSpec as P

NUM_STEPS = 3
BAND_SCALE = 4.0
STEP_SCALE = 0.4
FEAT_AXES = ("slab", "feat")
LEAD_AXES = ("ens", "slab", "feat")

ROWS = 2048
TILE = 128
BLK = 512
COLORS = 6
SROWS = COLORS * BLK
UNITS = ((), ((0, 3), (0, 1), (0, 2)), ((1, 2), (1, 3), (2, 3)))
OFFS = (((0, 1), (2, 0), (3, 0)), ((1, 2), (1, 3), (2, 3)))
PM_ROW = 4 * BLK
SENT = 1536 + 768 + 576 + 576 + 288 + 1152 + 1536 + 288 + 16
OWN = 32
MESH = pl.DeviceIdType.MESH
NT = (((1,), (1,)), ((), ()))
F32, BF16 = jnp.float32, jnp.bfloat16


def div(a, b):
    return lax.div(a, jnp.int32(b))


def rem(a, b):
    return lax.rem(a, jnp.int32(b))


def _kernel(
    bandwidth, step_size, n_part,
    theta_ref, lam_hbm, mu_hbm, fac_hbm, out_ref,
    lam_ref, mu_ref, fac_ref,
    bfull, pml, pmr, nrow, ncol, srow, pack, r0, r1, r2, r3, kg, kfull, adrv, svec, srecv, stot, spart,
    in_sem, pre_send, pre_recv, sent, rs_recv, x_recv, far_recv, dd_recv, s_recv, sp_recv,
):
    width = out_ref.shape[1]
    rep_coef = 2.0 / bandwidth
    core = lax.axis_index("slab")
    feat = lax.axis_index("feat")
    coords = (rem(feat, 4), rem(div(feat, 4), 4), div(feat, 16))
    strides = (1, 4, 16)

    def chip(dim, coord):
        return {"feat": feat + (coord - coords[dim]) * strides[dim]}

    turned = [[coords[dim]] + [rem(coords[dim] + j, 4) for j in range(1, 4)] for dim in range(3)]

    def around(dim, j):
        return turned[dim][j]

    ring = [[chip(dim, turned[dim][j]) for j in range(4)] for dim in range(3)]
    low_bit = [rem(c, 2) for c in coords]
    pair_bit = [[rem(div(t + 1, 2), 2) for t in turned[dim]] for dim in range(3)]
    high_bit = [[div(t, 2) for t in turned[dim]] for dim in range(3)]

    mate = {"slab": 1 - core}

    def al(x, m=16):
        return pl.multiple_of(x, m)

    halves = []
    for k in range(COLORS):
        steps = []
        start, length, cur = 0, BLK, coords[k % 3]
        for s in range(2):
            if (k // 3 + s) % 2 == 0:
                other, bit = cur + 1 - 2 * low_bit[k % 3], pair_bit[k % 3][0]
            else:
                other, bit = 3 - cur, high_bit[k % 3][0]
            length = length // 2
            keep, give = start + bit * length, start + (1 - bit) * length
            start = keep
            steps.append((chip(k % 3, other), length, keep, give))
        halves.append(steps)

    def dims(k):
        return k % 3, (k + 1) % 3, (k + 2) % 3

    def base(st, k):
        return st * SROWS + k * BLK

    quarters = [[base(st, k) + halves[k][1][2] for k in range(COLORS)] for st in range(3)]
    owns = [[quarters[st][k] + OWN * coords[dims(k)[1]] for k in range(COLORS)] for st in range(3)]
    pieces = [[OWN * around(dims(k)[1], j) for j in range(4)] for k in range(COLORS)]

    places = []
    for k in range(COLORS):
        one, two = (pair_bit, high_bit) if k < 3 else (high_bit, pair_bit)
        places.append([TILE * (2 * one[k % 3][j] + two[k % 3][j]) for j in range(4)])

    def quarter(st, k):
        return quarters[st][k]

    def own(st, k):
        return owns[st][k]

    barrier = pltpu.get_barrier_semaphore()
    pl.semaphore_signal(barrier, inc=1, device_id=mate, device_id_type=MESH)
    for dim in range(3):
        for j in range(1, 4):
            pl.semaphore_signal(barrier, inc=1, device_id=ring[dim][j], device_id_type=MESH)
    loads = [pltpu.make_async_copy(theta_ref.at[pl.ds(ch * BLK, BLK)], out_ref.at[pl.ds(ch * BLK, BLK)], in_sem.at[ch]) for ch in range(4)]
    loads += [
        pltpu.make_async_copy(src, dst, in_sem.at[4 + n])
        for n, (src, dst) in enumerate(((mu_hbm, mu_ref), (fac_hbm, fac_ref), (lam_hbm, lam_ref)))
    ]
    for cp in loads[4:] + loads[:4]:
        cp.start()

    row_i = lax.broadcasted_iota(jnp.int32, (TILE, TILE), 0)
    col_i = lax.broadcasted_iota(jnp.int32, (TILE, TILE), 1)
    eye, upper, lower = row_i == col_i, row_i < col_i, row_i > col_i
    sub_o = lax.broadcasted_iota(jnp.int32, (OWN, TILE), 0)
    lane_o = lax.broadcasted_iota(jnp.int32, (OWN, TILE), 1)

    def remote(src, dst, ssem, rsem, where):
        return pltpu.make_async_remote_copy(src_ref=src, dst_ref=dst, send_sem=ssem, recv_sem=rsem, device_id=where, device_id_type=MESH)

    def pre_copy(ch, what):
        if what == 0:
            rows = pl.ds(ch * BLK, BLK)
            src, dst = bfull.at[rows, 0:width], bfull.at[rows, width:2 * width]
        else:
            src, dst = pml.at[pl.ds(al(ch * BLK + (1 - core) * 256), 256)], pmr.at[pl.ds(ch * 256, 256)]
        return remote(src, dst, pre_send, pre_recv.at[what, ch], mate)

    def prepare(start, length, th):
        rows = pl.ds(start, length)
        bfull[rows, 0:width] = th.astype(BF16)
        pml[rows, :] = jnp.dot((th - mu_ref[...]).astype(BF16), fac_ref[...], preferred_element_type=F32)

    def begin(cps):
        for cp in cps:
            cp.start()

    def arrive(ref, sem):
        remote(ref, ref, sent.at[0], sem, mate).wait_recv()

    def x_arrive(st, e, k):
        arrive((r2.at[st, k], r3.at[st, k, 0:3], kg.at[core, 0:3 * OWN])[e], x_recv.at[st, e, k])

    def rs_copy(st, s, k):
        peer, length, keep, give = halves[k][s]
        src = pack.at[pl.ds(al(base(st, k) + give), length)]
        return remote(src, (r0, r1)[s].at[st, k], sent.at[st], rs_recv.at[st, s, k], peer)

    def x_copies(st, e, k):
        d1, d2, d3 = dims(k)
        dim = (d2, d3, d2, d1)[e]
        cps = []
        for j in range(1, 4):
            if e == 0:
                src = pack.at[pl.ds(al(quarter(st, k) + pieces[k][j]), OWN)]
                dst = r2.at[st, k, j - 1]
            elif e == 1:
                src = dst = r3.at[st, k, coords[dim]]
            else:
                rng = pl.ds(al(own(st, k)), OWN) if e == 2 else pl.ds(al(quarter(st, k)), TILE)
                src = dst = kg.at[core, rng]
            arrived = far_recv.at[st, k, j - 1] if e == 3 else x_recv.at[st, e, k]
            cps.append(remote(src, dst, sent.at[st], arrived, ring[dim][j]))
        return cps

    def dd_copy(st, k, j):
        if j == 0:
            begin_row = quarter(st, k)
        else:
            begin_row = base(st, k) + places[k][4 - j]
        rng = pl.ds(al(begin_row), TILE)
        return remote(kg.at[core, rng], kg.at[core, rng], sent.at[st], dd_recv.at[st, k], mate)

    def s_copies(st, ph, d):
        dim = ((d + 1) % 3, d)[ph]
        return [
            remote(svec.at[st, ph, d], srecv.at[st, ph, d, j - 1], sent.at[st], s_recv.at[st, ph, d], ring[dim][j])
            for j in range(1, 4)
        ]

    def sp_copy(st):
        return remote(stot.at[st], spart.at[st], sent.at[st], sp_recv.at[st], mate)

    def products(m):
        mine = bfull[pl.ds(al(m * BLK + 256 * core), 256), :]
        other = bfull[pl.ds(al(m * BLK + 256 * (1 - core)), 256), :]
        g = lax.dot_general(bfull[pl.ds(0, (m + 1) * BLK), :], mine, NT, preferred_element_type=F32)
        return g, lax.dot_general(other, other, NT, preferred_element_type=F32)

    def tiles(m, g, g_other):
        def tile(i, b):
            return g[m * BLK + i * TILE:m * BLK + (i + 1) * TILE, b * TILE:(b + 1) * TILE]

        for b in range(2):
            own_diag = jnp.where(core == 0, tile(b, b), tile(2 + b, b))
            rng = slice(b * TILE, (b + 1) * TILE)
            for half, diag in ((core, own_diag), (1 - core, g_other[rng, rng])):
                d = jnp.where(eye, diag, 0.0)
                blk = 4 * m + 2 * half + b
                nrow[pl.ds(al(blk * TILE), TILE), :] = jnp.broadcast_to(jnp.sum(d, axis=1, keepdims=True), (TILE, TILE))
                ncol[pl.ds(blk, 1), :] = jnp.sum(d, axis=0, keepdims=True)

        def dist(i, j):
            return nrow[pl.ds((4 * m + i) * TILE, TILE), :] + ncol[4 * m + j:4 * m + j + 1, :] - 2.0 * tile(i, j % 2)

        for t in range(3):
            pack[pl.ds(base(0, m) + t * TILE, TILE), :] = jnp.where(core == 0, dist(*OFFS[0][t]), dist(*OFFS[1][t]))
        one = jnp.where(core == 0, dist(0, 0), dist(2, 2))
        two = jnp.where(core == 0, dist(1, 1), dist(3, 3))
        pack[pl.ds(base(0, m) + 3 * TILE, TILE), :] = jnp.where(upper, one, two)
        begin([rs_copy(0, 0, m)])
        for st in (1, 2):
            for u, (sup, col) in enumerate(UNITS[st]):
                if col != m:
                    continue
                for b in range(2):
                    nc = ncol[pl.ds(4 * m + 2 * core + b, 1), :]
                    part = g[sup * BLK:(sup + 1) * BLK, b * TILE:(b + 1) * TILE]
                    pack[pl.ds(base(st, 2 * u + b), BLK), :] = nrow[pl.ds(sup * BLK, BLK), :] + nc - 2.0 * part
                begin([rs_copy(st, 0, 2 * u), rs_copy(st, 0, 2 * u + 1)])

    def pm_tiles():
        for ch in range(4):
            pre_copy(ch, 1).wait_recv()
            mine = pl.ds(al(ch * BLK + core * 256), 256)
            pack[pl.ds(PM_ROW + ch * 256, 256), :] = pml[mine, :] + pmr[pl.ds(ch * 256, 256), :]
        begin([rs_copy(0, 0, 4), rs_copy(0, 0, 5)])

    def open_step():
        for ch in range(3):
            pre_copy(ch, 0).wait_recv()
        gs = [products(0)]
        for m in range(4):
            if m == 2:
                pm_tiles()
                pre_copy(3, 0).wait_recv()
            if m < 3:
                gs.append(products(m + 1))
            tiles(m, *gs[m])

    for cp in loads[4:]:
        cp.wait()
    for ch in range(4):
        loads[ch].wait()
        prepare(ch * BLK, BLK, out_ref[pl.ds(ch * BLK, BLK), :])
    pl.semaphore_wait(barrier, 10)
    for ch in range(4):
        begin([pre_copy(ch, 1), pre_copy(ch, 0)])
    open_step()

    def one_step(step_index, carry):
        def row_sums(st, k, kern):
            place = own(0, k) - base(0, k)
            slot, r = div(place, TILE), rem(place, TILE)

            def by_rows(vals):
                rs = jnp.sum(vals, axis=1, keepdims=True)
                return jnp.sum(jnp.where(lane_o == sub_o + r, rs, 0.0), axis=0, keepdims=True)

            def by_cols(vals):
                return jnp.sum(vals, axis=0, keepdims=True)

            if st > 0:
                sup, m = UNITS[st][k // 2]
                return [(4 * sup + slot, by_rows(kern)), (4 * m + 2 * core + k % 2, by_cols(kern))]
            both = div(slot, 3)
            up_one = div(slot + 1, 2)
            i0 = (1 - both) * ((1 - core) * (slot + up_one) + core * (1 + div(slot, 2))) + both * 2 * core
            j0 = (1 - both) * ((1 - core) * (1 - up_one) + core * (2 + up_one)) + both * 2 * core
            up = jnp.where(lane_o + 1000 * (1 - both) > sub_o + r, kern, 0.0)
            lo = jnp.where(lane_o + 1000 * (1 - both) < sub_o + r, kern, 0.0)
            nxt = 4 * k + 2 * core + 1
            return [(4 * k + i0, by_rows(up)), (4 * k + j0, by_cols(up)), (nxt, by_rows(lo)), (nxt, by_cols(lo))]

        def advance(st, s):
            parts = [[], [], []]
            for k in range(COLORS):
                mine = pl.ds(al(own(st, k)), OWN)
                if s < 2:
                    peer, length, keep, give = halves[k][s]
                    rs_copy(st, s, k).wait_recv()
                    rng = pl.ds(al(base(st, k) + keep), length)
                    pack[rng, :] += (r0, r1)[s][st, k]
                    begin([rs_copy(st, 1, k)] if s == 0 else x_copies(st, 0, k))
                elif s == 2:
                    x_arrive(st, 0, k)
                    r3[st, k, coords[dims(k)[2]]] = pack[mine, :] + r2[st, k, 0] + r2[st, k, 1] + r2[st, k, 2]
                    begin(x_copies(st, 1, k))
                elif s == 3:
                    x_arrive(st, 1, k)
                    full = (r3[st, k, 0] + r3[st, k, 1]) + (r3[st, k, 2] + r3[st, k, 3])
                    if st == 0 and k >= 4:
                        kern = full
                    else:
                        kern = jnp.exp(-jnp.maximum(full, 0.0) / bandwidth)
                        parts[k % 3] += row_sums(st, k, kern)
                    kg[core, mine, :] = kern.astype(BF16)
                    begin(x_copies(st, 2, k))
                elif s == 4:
                    x_arrive(st, 2, k)
                    begin(x_copies(st, 3, k))
                    begin([dd_copy(st, k, 0)])
                else:
                    for j, cp in enumerate(x_copies(st, 3, k)):
                        cp.wait_recv()
                        begin([dd_copy(st, k, j + 1)])
            if s == 3:
                for d in range(3):
                    svec[st, 0, d] = jnp.zeros((16, TILE), F32)
                    for block, line in parts[d]:
                        svec[st, 0, d, pl.ds(block, 1), :] += line
                    begin(s_copies(st, 0, d))
            if s == 4:
                for d in range(3):
                    arrive(srecv.at[st, 0, d], s_recv.at[st, 0, d])
                    svec[st, 1, d] = svec[st, 0, d] + srecv[st, 0, d, 0] + srecv[st, 0, d, 1] + srecv[st, 0, d, 2]
                    begin(s_copies(st, 1, d))
            if s == 5:
                tot = jnp.zeros((16, TILE), F32)
                for d in range(3):
                    arrive(srecv.at[st, 1, d], s_recv.at[st, 1, d])
                    tot = tot + ((svec[st, 1, d] + srecv[st, 1, d, 0]) + (srecv[st, 1, d, 1] + srecv[st, 1, d, 2]))
                stot[st] = tot
                begin([sp_copy(st)])

        def unpack(st):
            for k in range(COLORS):
                arrive(kg.at[core, 0:BLK], dd_recv.at[st, k])
            for c in range(2):
                if st > 0:
                    for k in range(COLORS):
                        sup, m = UNITS[st][k // 2]
                        jrng = pl.ds((4 * m + 2 * c + k % 2) * TILE, TILE)
                        for a in range(4):
                            src = kg[c, pl.ds(base(st, k) + a * TILE, TILE), :]
                            srng = pl.ds((4 * sup + a) * TILE, TILE)
                            kfull[srng, jrng] = src
                            kfull[jrng, srng] = src.T
                    continue
                for sup in range(4):
                    for t, (i, j) in enumerate(OFFS[c]):
                        src = kg[c, pl.ds(base(0, sup) + t * TILE, TILE), :]
                        ri, rj = pl.ds((4 * sup + i) * TILE, TILE), pl.ds((4 * sup + j) * TILE, TILE)
                        kfull[ri, rj] = src
                        kfull[rj, ri] = src.T
                    src = kg[c, pl.ds(base(0, sup) + 3 * TILE, TILE), :]
                    srt = src.T
                    one = jnp.ones((TILE, TILE), BF16)
                    ra, rb = pl.ds((4 * sup + 2 * c) * TILE, TILE), pl.ds((4 * sup + 2 * c + 1) * TILE, TILE)
                    kfull[ra, ra] = jnp.where(upper, src, jnp.where(lower, srt, one))
                    kfull[rb, rb] = jnp.where(lower, src, jnp.where(upper, srt, one))

        def drive():
            for q in range(8):
                rows = pl.ds(q * 256, 256)
                pm = kg[q % 2, pl.ds(PM_ROW + (q // 2) * 256, 256), :]
                low = lax.dot_general(pm, fac_ref[...], NT, preferred_element_type=F32)
                th = out_ref[rows, :]
                grad = -((th - mu_ref[...]) * lam_ref[...] + low)
                adrv[rows, :] = (grad - rep_coef * th).astype(BF16)

        def sum_rows(blocks):
            tot = stot[0] + spart[0] + stot[1] + spart[1] + 1.0
            if len(blocks) > 4:
                tot = tot + (stot[2] + spart[2])
            for blk in blocks:
                line = jnp.sum(jnp.where(eye, jnp.broadcast_to(tot[blk:blk + 1, :], (TILE, TILE)), 0.0), axis=1, keepdims=True)
                srow[pl.ds(blk * TILE, TILE), :] = jnp.broadcast_to(rep_coef * line, (TILE, TILE))

        def update(chs):
            starts = [ch * BLK + half * 256 for ch in chs for half in range(2)]

            def product(start):
                return jnp.dot(kfull[pl.ds(start, 256), :], adrv[...], preferred_element_type=F32)

            ahead = product(starts[0])
            for n, start in enumerate(starts):
                acc = ahead
                if n + 1 < len(starts):
                    ahead = product(starts[n + 1])
                rows = pl.ds(start, 256)
                new = []
                for t in range(width // TILE):
                    cols = slice(t * TILE, (t + 1) * TILE)
                    th = out_ref[rows, cols]
                    phi = (acc[:, cols] + srow[rows, :] * th) / n_part
                    new.append(th + step_size * phi)
                th = jnp.concatenate(new, axis=1)
                out_ref[rows, :] = th
                prepare(start, 256, th)
                if n % 2 == 1:
                    begin([pre_copy(chs[n // 2], 1), pre_copy(chs[n // 2], 0)])

        for s in range(5):
            for st in range(3):
                advance(st, s)
        advance(0, 5)
        advance(1, 5)
        unpack(0)
        drive()
        advance(2, 5)
        remote(pack.at[0:5120], pack.at[0:5120], pre_send, sp_recv.at[0], mate).wait_send()
        for st in range(2):
            arrive(stot.at[st], sp_recv.at[st])
        sum_rows(range(4))
        unpack(1)
        update((0,))
        arrive(stot.at[2], sp_recv.at[2])
        sum_rows(range(4, 16))
        unpack(2)
        update((1, 2, 3))
        for st in range(3):
            remote(pack.at[0:SENT], pack.at[0:SENT], sent.at[st], sp_recv.at[0], mate).wait_send()
        pl.when(step_index < NUM_STEPS - 1)(open_step)
        return carry

    lax.fori_loop(0, NUM_STEPS, one_step, 0)
    for ch in range(4):
        for what in range(2):
            pre_copy(ch, what).wait_recv()
    remote(pack.at[0:5120], pack.at[0:5120], pre_send, sp_recv.at[0], mate).wait_send()


def solution(mesh):
    def run_steps(particles, prec_diag, mean_vec, low_rank):
        total_rows, width = particles.shape
        n_part = total_rows // mesh.shape["ens"]
        bandwidth = BAND_SCALE * width
        step_size = STEP_SCALE * width
        loc = width // (mesh.shape["slab"] * mesh.shape["feat"])
        rank = low_rank.shape[1]
        vm, dma = pltpu.VMEM, pltpu.SemaphoreType.DMA

        def local_steps(current, prec_loc, mean_loc, fac_loc):
            spec = pl.BlockSpec(memory_space=pltpu.VMEM)
            call = pl.pallas_call(
                functools.partial(_kernel, bandwidth, step_size, n_part),
                out_shape=jax.ShapeDtypeStruct((n_part, loc), F32),
                in_specs=[pl.BlockSpec(memory_space=pltpu.HBM)] * 4,
                out_specs=spec,
                scratch_shapes=[
                    vm((1, loc), F32), vm((1, loc), F32), vm((loc, rank), BF16),
                    vm((ROWS, 2 * loc), BF16), vm((ROWS, rank), F32), vm((ROWS // 2, rank), F32),
                    vm((ROWS, TILE), F32), vm((16, TILE), F32), vm((ROWS, TILE), F32),
                    vm((3 * SROWS, TILE), F32),
                    vm((3, COLORS, BLK // 2, TILE), F32), vm((3, COLORS, BLK // 4, TILE), F32),
                    vm((3, COLORS, 3, OWN, TILE), F32), vm((3, COLORS, 4, OWN, TILE), F32),
                    vm((2, 3 * SROWS, TILE), BF16), vm((ROWS, ROWS), BF16), vm((ROWS, loc), BF16),
                    vm((3, 2, 3, 16, TILE), F32), vm((3, 2, 3, 3, 16, TILE), F32), vm((3, 16, TILE), F32), vm((3, 16, TILE), F32),
                    dma((7,)), dma, dma((2, 4)), dma((3,)), dma((3, 2, COLORS)), dma((3, 3, COLORS)), dma((3, COLORS, 3)), dma((3, COLORS)),
                    dma((3, 2, 3)), dma((3,)),
                ],
                compiler_params=pltpu.CompilerParams(collective_id=0, has_side_effects=True, vmem_limit_bytes=50000000),
                name="svgd",
            )
            hbm = lambda x: pltpu.with_memory_space_constraint(x, pltpu.HBM)
            return call(hbm(current), hbm(prec_loc.reshape(1, loc)), hbm(mean_loc.reshape(1, loc)), hbm(fac_loc))

        sharded = jax.shard_map(
            local_steps,
            mesh=mesh,
            in_specs=(P("ens", FEAT_AXES), P(LEAD_AXES), P(LEAD_AXES), P(LEAD_AXES, None)),
            out_specs=P("ens", FEAT_AXES),
            check_vma=False,
        )
        return sharded(particles, prec_diag, mean_vec, low_rank)

    return run_steps
```

```python
import functools

import jax
import jax.numpy as jnp
from jax import lax
from jax.experimental import pallas as pl
from jax.experimental.pallas import tpu as pltpu
from jax.sharding import PartitionSpec as P

NUM_STEPS = 3
BAND_SCALE = 4.0
STEP_SCALE = 0.4
FEAT_AXES = ("slab", "feat")
LEAD_AXES = ("ens", "slab", "feat")

ROWS = 2048
TILE = 128
BLK = 512
COLORS = 6
SROWS = COLORS * BLK
UNITS = ((), ((0, 3), (0, 1), (0, 2)), ((1, 2), (1, 3), (2, 3)))
OFFS = (((0, 1), (2, 0), (3, 0)), ((1, 2), (1, 3), (2, 3)))
PM_ROW = 4 * BLK
SENT = 1536 + 768 + 576 + 576 + 288 + 1152 + 1536
SENT_SUMS = 288 + 16
OWN = 32
MESH = pl.DeviceIdType.MESH
NT = (((1,), (1,)), ((), ()))
F32, BF16 = jnp.float32, jnp.bfloat16


def div(a, b):
    return lax.div(a, jnp.int32(b))


def rem(a, b):
    return lax.rem(a, jnp.int32(b))


def _kernel(
    bandwidth, step_size, n_part,
    theta_ref, lam_hbm, mu_hbm, fac_hbm, out_ref,
    lam_ref, mu_ref, fac_ref,
    bfull, pml, pmr, nrow, ncol, srow, pack, r0, r1, r2, r3, kg, kfull, adrv, svec, srecv, stot, spart,
    in_sem, pre_send, pre_recv, sent, rs_recv, x_recv, far_recv, dd_recv, s_recv, sp_recv,
):
    width = out_ref.shape[1]
    rep_coef = 2.0 / bandwidth
    core = lax.axis_index("slab")
    feat = lax.axis_index("feat")
    coords = (rem(feat, 4), rem(div(feat, 4), 4), div(feat, 16))
    strides = (1, 4, 16)

    def chip(dim, coord):
        return {"feat": feat + (coord - coords[dim]) * strides[dim]}

    turned = [[coords[dim]] + [rem(coords[dim] + j, 4) for j in range(1, 4)] for dim in range(3)]

    def around(dim, j):
        return turned[dim][j]

    ring = [[chip(dim, turned[dim][j]) for j in range(4)] for dim in range(3)]
    low_bit = [rem(c, 2) for c in coords]
    pair_bit = [[rem(div(t + 1, 2), 2) for t in turned[dim]] for dim in range(3)]
    high_bit = [[div(t, 2) for t in turned[dim]] for dim in range(3)]

    mate = {"slab": 1 - core}

    def al(x, m=16):
        return pl.multiple_of(x, m)

    halves = []
    for k in range(COLORS):
        steps = []
        start, length, cur = 0, BLK, coords[k % 3]
        for s in range(2):
            if (k // 3 + s) % 2 == 0:
                other, bit = cur + 1 - 2 * low_bit[k % 3], pair_bit[k % 3][0]
            else:
                other, bit = 3 - cur, high_bit[k % 3][0]
            length = length // 2
            keep, give = start + bit * length, start + (1 - bit) * length
            start = keep
            steps.append((chip(k % 3, other), length, keep, give))
        halves.append(steps)

    def dims(k):
        return k % 3, (k + 1) % 3, (k + 2) % 3

    def base(st, k):
        return st * SROWS + k * BLK

    quarters = [[base(st, k) + halves[k][1][2] for k in range(COLORS)] for st in range(3)]
    owns = [[quarters[st][k] + OWN * coords[dims(k)[1]] for k in range(COLORS)] for st in range(3)]
    pieces = [[OWN * around(dims(k)[1], j) for j in range(4)] for k in range(COLORS)]

    places = []
    for k in range(COLORS):
        one, two = (pair_bit, high_bit) if k < 3 else (high_bit, pair_bit)
        places.append([TILE * (2 * one[k % 3][j] + two[k % 3][j]) for j in range(4)])

    def quarter(st, k):
        return quarters[st][k]

    def own(st, k):
        return owns[st][k]

    barrier = pltpu.get_barrier_semaphore()
    pl.semaphore_signal(barrier, inc=1, device_id=mate, device_id_type=MESH)
    for dim in range(3):
        for j in range(1, 4):
            pl.semaphore_signal(barrier, inc=1, device_id=ring[dim][j], device_id_type=MESH)
    loads = [pltpu.make_async_copy(theta_ref.at[pl.ds(ch * BLK, BLK)], out_ref.at[pl.ds(ch * BLK, BLK)], in_sem.at[ch]) for ch in range(4)]
    loads += [
        pltpu.make_async_copy(src, dst, in_sem.at[4 + n])
        for n, (src, dst) in enumerate(((mu_hbm, mu_ref), (fac_hbm, fac_ref), (lam_hbm, lam_ref)))
    ]
    for cp in loads[4:] + loads[:4]:
        cp.start()

    row_i = lax.broadcasted_iota(jnp.int32, (TILE, TILE), 0)
    col_i = lax.broadcasted_iota(jnp.int32, (TILE, TILE), 1)
    eye, upper, lower = row_i == col_i, row_i < col_i, row_i > col_i
    sub_o = lax.broadcasted_iota(jnp.int32, (OWN, TILE), 0)
    lane_o = lax.broadcasted_iota(jnp.int32, (OWN, TILE), 1)

    def remote(src, dst, ssem, rsem, where):
        return pltpu.make_async_remote_copy(src_ref=src, dst_ref=dst, send_sem=ssem, recv_sem=rsem, device_id=where, device_id_type=MESH)

    def pre_copy(ch, what):
        if what == 0:
            rows = pl.ds(ch * BLK, BLK)
            src, dst = bfull.at[rows, 0:width], bfull.at[rows, width:2 * width]
        else:
            src, dst = pml.at[pl.ds(al(ch * BLK + (1 - core) * 256), 256)], pmr.at[pl.ds(ch * 256, 256)]
        return remote(src, dst, pre_send, pre_recv.at[what, ch], mate)

    def prepare(start, length, th):
        rows = pl.ds(start, length)
        bfull[rows, 0:width] = th.astype(BF16)
        pml[rows, :] = jnp.dot((th - mu_ref[...]).astype(BF16), fac_ref[...], preferred_element_type=F32)

    def begin(cps):
        for cp in cps:
            cp.start()

    def arrive(ref, sem):
        remote(ref, ref, sent.at[0], sem, mate).wait_recv()

    def x_arrive(st, e, k):
        arrive((r2.at[st, k], r3.at[st, k, 0:3], kg.at[core, 0:3 * OWN])[e], x_recv.at[st, e, k])

    def rs_copy(st, s, k):
        peer, length, keep, give = halves[k][s]
        src = pack.at[pl.ds(al(base(st, k) + give), length)]
        return remote(src, (r0, r1)[s].at[st, k], sent.at[st], rs_recv.at[st, s, k], peer)

    def x_copies(st, e, k):
        d1, d2, d3 = dims(k)
        dim = (d2, d3, d2, d1)[e]
        cps = []
        for j in range(1, 4):
            if e == 0:
                src = pack.at[pl.ds(al(quarter(st, k) + pieces[k][j]), OWN)]
                dst = r2.at[st, k, j - 1]
            elif e == 1:
                src = dst = r3.at[st, k, coords[dim]]
            else:
                rng = pl.ds(al(own(st, k)), OWN) if e == 2 else pl.ds(al(quarter(st, k)), TILE)
                src = dst = kg.at[core, rng]
            arrived = far_recv.at[st, k, j - 1] if e == 3 else x_recv.at[st, e, k]
            cps.append(remote(src, dst, sent.at[st], arrived, ring[dim][j]))
        return cps

    def dd_copy(st, k, j):
        if j == 0:
            begin_row = quarter(st, k)
        else:
            begin_row = base(st, k) + places[k][4 - j]
        rng = pl.ds(al(begin_row), TILE)
        return remote(kg.at[core, rng], kg.at[core, rng], sent.at[st], dd_recv.at[st, k], mate)

    def s_copies(ph, d):
        dim = ((d + 1) % 3, d)[ph]
        return [
            remote(svec.at[ph, d], srecv.at[ph, d, j - 1], sent.at[2], s_recv.at[ph, d], ring[dim][j])
            for j in range(1, 4)
        ]

    def sp_copy():
        return remote(stot, spart, sent.at[2], sp_recv, mate)

    def products(m):
        mine = bfull[pl.ds(al(m * BLK + 256 * core), 256), :]
        part = BLK if m == 3 else (m + 1) * 256
        return [lax.dot_general(bfull[pl.ds(at, part), :], mine, NT, preferred_element_type=F32) for at in range(0, (m + 1) * BLK, part)]

    def norms(m):
        for i in range(4):
            rows = pl.ds((4 * m + i) * TILE, TILE)
            wide = bfull[rows, :].astype(F32)
            n = jnp.broadcast_to(jnp.sum(wide * wide, axis=1, keepdims=True), (TILE, TILE))
            nrow[rows, :] = n
            ncol[4 * m + i:4 * m + i + 1, :] = jnp.sum(jnp.where(eye, n, 0.0), axis=0, keepdims=True)

    def tiles(m, g):
        def block(blk, b):
            n, r = divmod(blk * TILE, BLK if m == 3 else (m + 1) * 256)
            return g[n][r:r + TILE, b * TILE:(b + 1) * TILE]

        def tile(i, b):
            return block(4 * m + i, b)

        def dist(i, j):
            return nrow[pl.ds((4 * m + i) * TILE, TILE), :] + ncol[4 * m + j:4 * m + j + 1, :] - 2.0 * tile(i, j % 2)

        for t in range(3):
            pack[pl.ds(base(0, m) + t * TILE, TILE), :] = jnp.where(core == 0, dist(*OFFS[0][t]), dist(*OFFS[1][t]))
        one = jnp.where(core == 0, dist(0, 0), dist(2, 2))
        two = jnp.where(core == 0, dist(1, 1), dist(3, 3))
        pack[pl.ds(base(0, m) + 3 * TILE, TILE), :] = jnp.where(upper, one, two)
        begin([rs_copy(0, 0, m)])
        for st in (1, 2):
            for u, (sup, col) in enumerate(UNITS[st]):
                if col != m:
                    continue
                for b in range(2):
                    nc = ncol[pl.ds(4 * m + 2 * core + b, 1), :]
                    for a in range(4):
                        nr = nrow[pl.ds((4 * sup + a) * TILE, TILE), :]
                        pack[pl.ds(base(st, 2 * u + b) + a * TILE, TILE), :] = nr + nc - 2.0 * block(4 * sup + a, b)
                begin([rs_copy(st, 0, 2 * u), rs_copy(st, 0, 2 * u + 1)])

    def pm_tiles():
        for ch in range(4):
            pre_copy(ch, 1).wait_recv()
            mine = pl.ds(al(ch * BLK + core * 256), 256)
            pack[pl.ds(PM_ROW + ch * 256, 256), :] = pml[mine, :] + pmr[pl.ds(ch * 256, 256), :]
        begin([rs_copy(0, 0, 4), rs_copy(0, 0, 5)])

    def open_step():
        for ch in range(3):
            pre_copy(ch, 0).wait_recv()
        gs = [products(0)]
        norms(0)
        for m in range(4):
            if m == 2:
                pm_tiles()
                pre_copy(3, 0).wait_recv()
            if m < 3:
                gs.append(products(m + 1))
                norms(m + 1)
            tiles(m, gs[m])

    for cp in loads[4:]:
        cp.wait()
    for ch in range(4):
        loads[ch].wait()
        prepare(ch * BLK, BLK, out_ref[pl.ds(ch * BLK, BLK), :])
    pl.semaphore_wait(barrier, 10)
    for ch in range(4):
        begin([pre_copy(ch, 1), pre_copy(ch, 0)])
    open_step()

    def one_step(step_index, carry):
        def row_sums(st, k, kern):
            place = own(0, k) - base(0, k)
            slot, r = div(place, TILE), rem(place, TILE)

            def by_rows(vals):
                rs = jnp.sum(vals, axis=1, keepdims=True)
                return jnp.sum(jnp.where(lane_o == sub_o + r, rs, 0.0), axis=0, keepdims=True)

            def by_cols(vals):
                return jnp.sum(vals, axis=0, keepdims=True)

            if st > 0:
                sup, m = UNITS[st][k // 2]
                return [(4 * sup + slot, by_rows(kern)), (4 * m + 2 * core + k % 2, by_cols(kern))]
            both = div(slot, 3)
            up_one = div(slot + 1, 2)
            i0 = (1 - both) * ((1 - core) * (slot + up_one) + core * (1 + div(slot, 2))) + both * 2 * core
            j0 = (1 - both) * ((1 - core) * (1 - up_one) + core * (2 + up_one)) + both * 2 * core
            up = jnp.where(lane_o + 1000 * (1 - both) > sub_o + r, kern, 0.0)
            lo = jnp.where(lane_o + 1000 * (1 - both) < sub_o + r, kern, 0.0)
            nxt = 4 * k + 2 * core + 1
            return [(4 * k + i0, by_rows(up)), (4 * k + j0, by_cols(up)), (nxt, by_rows(lo)), (nxt, by_cols(lo))]

        def advance(st, s):
            parts = [[], [], []]
            for k in range(COLORS):
                mine = pl.ds(al(own(st, k)), OWN)
                if s < 2:
                    peer, length, keep, give = halves[k][s]
                    rs_copy(st, s, k).wait_recv()
                    rng = pl.ds(al(base(st, k) + keep), length)
                    pack[rng, :] += (r0, r1)[s][st, k]
                    begin([rs_copy(st, 1, k)] if s == 0 else x_copies(st, 0, k))
                elif s == 2:
                    x_arrive(st, 0, k)
                    r3[st, k, coords[dims(k)[2]]] = pack[mine, :] + r2[st, k, 0] + r2[st, k, 1] + r2[st, k, 2]
                    begin(x_copies(st, 1, k))
                elif s == 3:
                    x_arrive(st, 1, k)
                    full = (r3[st, k, 0] + r3[st, k, 1]) + (r3[st, k, 2] + r3[st, k, 3])
                    if st == 0 and k >= 4:
                        kern = full
                    else:
                        kern = jnp.exp(-jnp.maximum(full, 0.0) / bandwidth)
                        parts[k % 3] += row_sums(st, k, kern)
                    kg[core, mine, :] = kern.astype(BF16)
                    begin(x_copies(st, 2, k))
                elif s == 4:
                    x_arrive(st, 2, k)
                    begin(x_copies(st, 3, k))
                    begin([dd_copy(st, k, 0)])
                else:
                    for j, cp in enumerate(x_copies(st, 3, k)):
                        cp.wait_recv()
                        begin([dd_copy(st, k, j + 1)])
            if s == 3:
                for d in range(3):
                    if st == 0:
                        svec[0, d] = jnp.zeros((16, TILE), F32)
                    for block, line in parts[d]:
                        svec[0, d, pl.ds(block, 1), :] += line
                    if st == 2:
                        begin(s_copies(0, d))
            if st == 2 and s == 4:
                for d in range(3):
                    arrive(srecv.at[0, d], s_recv.at[0, d])
                    svec[1, d] = svec[0, d] + srecv[0, d, 0] + srecv[0, d, 1] + srecv[0, d, 2]
                    begin(s_copies(1, d))
            if st == 2 and s == 5:
                tot = jnp.zeros((16, TILE), F32)
                for d in range(3):
                    arrive(srecv.at[1, d], s_recv.at[1, d])
                    tot = tot + ((svec[1, d] + srecv[1, d, 0]) + (srecv[1, d, 1] + srecv[1, d, 2]))
                stot[...] = tot
                begin([sp_copy()])

        def unpack(st):
            for k in range(COLORS):
                arrive(kg.at[core, 0:BLK], dd_recv.at[st, k])
            for c in range(2):
                if st > 0:
                    for k in range(COLORS):
                        sup, m = UNITS[st][k // 2]
                        jrng = pl.ds((4 * m + 2 * c + k % 2) * TILE, TILE)
                        for a in range(4):
                            src = kg[c, pl.ds(base(st, k) + a * TILE, TILE), :]
                            srng = pl.ds((4 * sup + a) * TILE, TILE)
                            kfull[srng, jrng] = src
                            kfull[jrng, srng] = src.T
                    continue
                for sup in range(4):
                    for t, (i, j) in enumerate(OFFS[c]):
                        src = kg[c, pl.ds(base(0, sup) + t * TILE, TILE), :]
                        ri, rj = pl.ds((4 * sup + i) * TILE, TILE), pl.ds((4 * sup + j) * TILE, TILE)
                        kfull[ri, rj] = src
                        kfull[rj, ri] = src.T
                    src = kg[c, pl.ds(base(0, sup) + 3 * TILE, TILE), :]
                    srt = src.T
                    one = jnp.ones((TILE, TILE), BF16)
                    ra, rb = pl.ds((4 * sup + 2 * c) * TILE, TILE), pl.ds((4 * sup + 2 * c + 1) * TILE, TILE)
                    kfull[ra, ra] = jnp.where(upper, src, jnp.where(lower, srt, one))
                    kfull[rb, rb] = jnp.where(lower, src, jnp.where(upper, srt, one))

        def drive():
            for q in range(8):
                rows = pl.ds(q * 256, 256)
                pm = kg[q % 2, pl.ds(PM_ROW + (q // 2) * 256, 256), :]
                low = lax.dot_general(pm, fac_ref[...], NT, preferred_element_type=F32)
                th = out_ref[rows, :]
                grad = -((th - mu_ref[...]) * lam_ref[...] + low)
                adrv[rows, :] = (grad - rep_coef * th).astype(BF16)

        def sum_rows():
            tot = stot[...] + spart[...] + 1.0
            for blk in range(16):
                line = jnp.sum(jnp.where(eye, jnp.broadcast_to(tot[blk:blk + 1, :], (TILE, TILE)), 0.0), axis=1, keepdims=True)
                srow[pl.ds(blk * TILE, TILE), :] = jnp.broadcast_to(rep_coef * line, (TILE, TILE))

        def update(chs):
            starts = [ch * BLK + half * 256 for ch in chs for half in range(2)]

            def product(start):
                return jnp.dot(kfull[pl.ds(start, 256), :], adrv[...], preferred_element_type=F32)

            ahead = product(starts[0])
            for n, start in enumerate(starts):
                acc = ahead
                if n + 1 < len(starts):
                    ahead = product(starts[n + 1])
                rows = pl.ds(start, 256)
                new = []
                for t in range(width // TILE):
                    cols = slice(t * TILE, (t + 1) * TILE)
                    th = out_ref[rows, cols]
                    phi = (acc[:, cols] + srow[rows, :] * th) / n_part
                    new.append(th + step_size * phi)
                th = jnp.concatenate(new, axis=1)
                out_ref[rows, :] = th
                prepare(start, 256, th)
                if n % 2 == 1:
                    begin([pre_copy(chs[n // 2], 1), pre_copy(chs[n // 2], 0)])

        for s in range(5):
            for st in range(3):
                advance(st, s)
        advance(0, 5)
        advance(1, 5)
        unpack(0)
        drive()
        advance(2, 5)
        remote(pack.at[0:5120], pack.at[0:5120], pre_send, sp_recv, mate).wait_send()
        unpack(1)
        arrive(stot, sp_recv)
        sum_rows()
        update((0,))
        unpack(2)
        update((1, 2, 3))
        for st in range(3):
            total = pack.at[0:SENT + (SENT_SUMS if st == 2 else 0)]
            remote(total, total, sent.at[st], sp_recv, mate).wait_send()
        pl.when(step_index < NUM_STEPS - 1)(open_step)
        return carry

    lax.fori_loop(0, NUM_STEPS, one_step, 0)
    for ch in range(4):
        for what in range(2):
            pre_copy(ch, what).wait_recv()
    remote(pack.at[0:5120], pack.at[0:5120], pre_send, sp_recv, mate).wait_send()


def solution(mesh):
    def run_steps(particles, prec_diag, mean_vec, low_rank):
        total_rows, width = particles.shape
        n_part = total_rows // mesh.shape["ens"]
        bandwidth = BAND_SCALE * width
        step_size = STEP_SCALE * width
        loc = width // (mesh.shape["slab"] * mesh.shape["feat"])
        rank = low_rank.shape[1]
        vm, dma = pltpu.VMEM, pltpu.SemaphoreType.DMA

        def local_steps(current, prec_loc, mean_loc, fac_loc):
            spec = pl.BlockSpec(memory_space=pltpu.VMEM)
            call = pl.pallas_call(
                functools.partial(_kernel, bandwidth, step_size, n_part),
                out_shape=jax.ShapeDtypeStruct((n_part, loc), F32),
                in_specs=[pl.BlockSpec(memory_space=pltpu.HBM)] * 4,
                out_specs=spec,
                scratch_shapes=[
                    vm((1, loc), F32), vm((1, loc), F32), vm((loc, rank), BF16),
                    vm((ROWS, 2 * loc), BF16), vm((ROWS, rank), F32), vm((ROWS // 2, rank), F32),
                    vm((ROWS, TILE), F32), vm((16, TILE), F32), vm((ROWS, TILE), F32),
                    vm((3 * SROWS, TILE), F32),
                    vm((3, COLORS, BLK // 2, TILE), F32), vm((3, COLORS, BLK // 4, TILE), F32),
                    vm((3, COLORS, 3, OWN, TILE), F32), vm((3, COLORS, 4, OWN, TILE), F32),
                    vm((2, 3 * SROWS, TILE), BF16), vm((ROWS, ROWS), BF16), vm((ROWS, loc), BF16),
                    vm((2, 3, 16, TILE), F32), vm((2, 3, 3, 16, TILE), F32), vm((16, TILE), F32), vm((16, TILE), F32),
                    dma((7,)), dma, dma((2, 4)), dma((3,)), dma((3, 2, COLORS)), dma((3, 3, COLORS)), dma((3, COLORS, 3)), dma((3, COLORS)),
                    dma((2, 3)), dma,
                ],
                compiler_params=pltpu.CompilerParams(collective_id=0, has_side_effects=True, vmem_limit_bytes=50000000),
                name="svgd",
            )
            hbm = lambda x: pltpu.with_memory_space_constraint(x, pltpu.HBM)
            return call(hbm(current), hbm(prec_loc.reshape(1, loc)), hbm(mean_loc.reshape(1, loc)), hbm(fac_loc))

        sharded = jax.shard_map(
            local_steps,
            mesh=mesh,
            in_specs=(P("ens", FEAT_AXES), P(LEAD_AXES), P(LEAD_AXES), P(LEAD_AXES, None)),
            out_specs=P("ens", FEAT_AXES),
            check_vma=False,
        )
        return sharded(particles, prec_diag, mean_vec, low_rank)

    return run_steps
```

```python
import functools

import jax
import jax.numpy as jnp
from jax import lax
from jax.experimental import pallas as pl
from jax.experimental.pallas import tpu as pltpu
from jax.sharding import PartitionSpec as P

NUM_STEPS = 3
BAND_SCALE = 4.0
STEP_SCALE = 0.4
FEAT_AXES = ("slab", "feat")
LEAD_AXES = ("ens", "slab", "feat")

ROWS = 2048
TILE = 128
BLK = 512
COLORS = 6
SROWS = COLORS * BLK
UNITS = ((), ((0, 3), (0, 1), (0, 2)), ((1, 2), (1, 3), (2, 3)))
OFFS = (((0, 1), (2, 0), (3, 0)), ((1, 2), (1, 3), (2, 3)))
PM_ROW = 4 * BLK
SENT = 1536 + 768 + 576 + 576 + 288 + 1152 + 1536
SENT_SUMS = 288 + 16
OWN = 32
MESH = pl.DeviceIdType.MESH
NT = (((1,), (1,)), ((), ()))
F32, BF16 = jnp.float32, jnp.bfloat16


def div(a, b):
    return lax.div(a, jnp.int32(b))


def rem(a, b):
    return lax.rem(a, jnp.int32(b))


def _kernel(
    bandwidth, step_size, n_part,
    theta_ref, lam_hbm, mu_hbm, fac_hbm, out_ref,
    lam_ref, mu_ref, fac_ref,
    bfull, pml, pmr, nrow, ncol, pack, r0, r1, r2, r3, kg, kfull, adrv, svec, srecv, stot, spart,
    in_sem, pre_send, pre_recv, sent, rs_recv, x_recv, far_recv, dd_recv, s_recv, sp_recv,
):
    width = out_ref.shape[1]
    rep_coef = 2.0 / bandwidth
    core = lax.axis_index("slab")
    feat = lax.axis_index("feat")
    coords = (rem(feat, 4), rem(div(feat, 4), 4), div(feat, 16))
    strides = (1, 4, 16)

    def chip(dim, coord):
        return {"feat": feat + (coord - coords[dim]) * strides[dim]}

    turned = [[coords[dim]] + [rem(coords[dim] + j, 4) for j in range(1, 4)] for dim in range(3)]

    def around(dim, j):
        return turned[dim][j]

    ring = [[chip(dim, turned[dim][j]) for j in range(4)] for dim in range(3)]
    low_bit = [rem(c, 2) for c in coords]
    pair_bit = [[rem(div(t + 1, 2), 2) for t in turned[dim]] for dim in range(3)]
    high_bit = [[div(t, 2) for t in turned[dim]] for dim in range(3)]

    mate = {"slab": 1 - core}

    def al(x, m=16):
        return pl.multiple_of(x, m)

    halves = []
    for k in range(COLORS):
        steps = []
        start, length, cur = 0, BLK, coords[k % 3]
        for s in range(2):
            if (k // 3 + s) % 2 == 0:
                other, bit = cur + 1 - 2 * low_bit[k % 3], pair_bit[k % 3][0]
            else:
                other, bit = 3 - cur, high_bit[k % 3][0]
            length = length // 2
            keep, give = start + bit * length, start + (1 - bit) * length
            start = keep
            steps.append((chip(k % 3, other), length, keep, give))
        halves.append(steps)

    def dims(k):
        return k % 3, (k + 1) % 3, (k + 2) % 3

    def base(st, k):
        return st * SROWS + k * BLK

    quarters = [[base(st, k) + halves[k][1][2] for k in range(COLORS)] for st in range(3)]
    owns = [[quarters[st][k] + OWN * coords[dims(k)[1]] for k in range(COLORS)] for st in range(3)]
    pieces = [[OWN * around(dims(k)[1], j) for j in range(4)] for k in range(COLORS)]

    places = []
    for k in range(COLORS):
        one, two = (pair_bit, high_bit) if k < 3 else (high_bit, pair_bit)
        places.append([TILE * (2 * one[k % 3][j] + two[k % 3][j]) for j in range(4)])

    def quarter(st, k):
        return quarters[st][k]

    def own(st, k):
        return owns[st][k]

    barrier = pltpu.get_barrier_semaphore()
    pl.semaphore_signal(barrier, inc=1, device_id=mate, device_id_type=MESH)
    for dim in range(3):
        for j in range(1, 4):
            pl.semaphore_signal(barrier, inc=1, device_id=ring[dim][j], device_id_type=MESH)
    loads = [pltpu.make_async_copy(theta_ref.at[pl.ds(ch * BLK, BLK)], out_ref.at[pl.ds(ch * BLK, BLK)], in_sem.at[ch]) for ch in range(4)]
    loads += [
        pltpu.make_async_copy(src, dst, in_sem.at[4 + n])
        for n, (src, dst) in enumerate(((mu_hbm, mu_ref), (fac_hbm, fac_ref), (lam_hbm, lam_ref)))
    ]
    for cp in loads[4:] + loads[:4]:
        cp.start()

    row_i = lax.broadcasted_iota(jnp.int32, (TILE, TILE), 0)
    col_i = lax.broadcasted_iota(jnp.int32, (TILE, TILE), 1)
    eye, upper, lower = row_i == col_i, row_i < col_i, row_i > col_i
    sub_o = lax.broadcasted_iota(jnp.int32, (OWN, TILE), 0)
    lane_o = lax.broadcasted_iota(jnp.int32, (OWN, TILE), 1)

    def remote(src, dst, ssem, rsem, where):
        return pltpu.make_async_remote_copy(src_ref=src, dst_ref=dst, send_sem=ssem, recv_sem=rsem, device_id=where, device_id_type=MESH)

    def pre_copy(ch, what):
        if what == 0:
            rows = pl.ds(ch * BLK, BLK)
            src, dst = bfull.at[rows, 0:width], bfull.at[rows, width:2 * width]
        else:
            src, dst = pml.at[pl.ds(al(ch * BLK + (1 - core) * 256), 256)], pmr.at[pl.ds(ch * 256, 256)]
        return remote(src, dst, pre_send, pre_recv.at[what, ch], mate)

    def prepare(start, length, th):
        rows = pl.ds(start, length)
        bfull[rows, 0:width] = th.astype(BF16)
        pml[rows, :] = jnp.dot((th - mu_ref[...]).astype(BF16), fac_ref[...], preferred_element_type=F32)

    def begin(cps):
        for cp in cps:
            cp.start()

    def arrive(ref, sem):
        remote(ref, ref, sent.at[0], sem, mate).wait_recv()

    def x_arrive(st, e, k):
        arrive((r2.at[st, k], r3.at[st, k, 0:3], kg.at[core, 0:3 * OWN])[e], x_recv.at[st, e, k])

    def rs_copy(st, s, k):
        peer, length, keep, give = halves[k][s]
        src = pack.at[pl.ds(al(base(st, k) + give), length)]
        return remote(src, (r0, r1)[s].at[st, k], sent.at[st], rs_recv.at[st, s, k], peer)

    def x_copies(st, e, k):
        d1, d2, d3 = dims(k)
        dim = (d2, d3, d2, d1)[e]
        cps = []
        for j in range(1, 4):
            if e == 0:
                src = pack.at[pl.ds(al(quarter(st, k) + pieces[k][j]), OWN)]
                dst = r2.at[st, k, j - 1]
            elif e == 1:
                src = dst = r3.at[st, k, coords[dim]]
            else:
                rng = pl.ds(al(own(st, k)), OWN) if e == 2 else pl.ds(al(quarter(st, k)), TILE)
                src = dst = kg.at[core, rng]
            arrived = far_recv.at[st, k, j - 1] if e == 3 else x_recv.at[st, e, k]
            cps.append(remote(src, dst, sent.at[st], arrived, ring[dim][j]))
        return cps

    def dd_copy(st, k, j):
        if j == 0:
            begin_row = quarter(st, k)
        else:
            begin_row = base(st, k) + places[k][4 - j]
        rng = pl.ds(al(begin_row), TILE)
        return remote(kg.at[core, rng], kg.at[core, rng], sent.at[st], dd_recv.at[st, k], mate)

    def s_copies(ph, d):
        dim = ((d + 1) % 3, d)[ph]
        return [
            remote(svec.at[ph, d], srecv.at[ph, d, j - 1], sent.at[2], s_recv.at[ph, d], ring[dim][j])
            for j in range(1, 4)
        ]

    def sp_copy():
        return remote(stot, spart, sent.at[2], sp_recv, mate)

    def products(m):
        mine = bfull[pl.ds(al(m * BLK + 256 * core), 256), :]
        part = BLK if m == 3 else (m + 1) * 256
        return [lax.dot_general(bfull[pl.ds(at, part), :], mine, NT, preferred_element_type=F32) for at in range(0, (m + 1) * BLK, part)]

    def norms(m):
        for i in range(4):
            rows = pl.ds((4 * m + i) * TILE, TILE)
            wide = bfull[rows, :].astype(F32)
            n = jnp.broadcast_to(jnp.sum(wide * wide, axis=1, keepdims=True), (TILE, TILE))
            nrow[rows, :] = n
            ncol[4 * m + i:4 * m + i + 1, :] = jnp.sum(jnp.where(eye, n, 0.0), axis=0, keepdims=True)

    def tiles(m, g):
        def block(blk, b):
            n, r = divmod(blk * TILE, BLK if m == 3 else (m + 1) * 256)
            return g[n][r:r + TILE, b * TILE:(b + 1) * TILE]

        def tile(i, b):
            return block(4 * m + i, b)

        def dist(i, j):
            return nrow[pl.ds((4 * m + i) * TILE, TILE), :] + ncol[4 * m + j:4 * m + j + 1, :] - 2.0 * tile(i, j % 2)

        for t in range(3):
            pack[pl.ds(base(0, m) + t * TILE, TILE), :] = jnp.where(core == 0, dist(*OFFS[0][t]), dist(*OFFS[1][t]))
        one = jnp.where(core == 0, dist(0, 0), dist(2, 2))
        two = jnp.where(core == 0, dist(1, 1), dist(3, 3))
        pack[pl.ds(base(0, m) + 3 * TILE, TILE), :] = jnp.where(upper, one, two)
        begin([rs_copy(0, 0, m)])
        for st in (1, 2):
            for u, (sup, col) in enumerate(UNITS[st]):
                if col != m:
                    continue
                for b in range(2):
                    nc = ncol[pl.ds(4 * m + 2 * core + b, 1), :]
                    for a in range(4):
                        nr = nrow[pl.ds((4 * sup + a) * TILE, TILE), :]
                        pack[pl.ds(base(st, 2 * u + b) + a * TILE, TILE), :] = nr + nc - 2.0 * block(4 * sup + a, b)
                begin([rs_copy(st, 0, 2 * u), rs_copy(st, 0, 2 * u + 1)])

    def pm_tiles(half):
        for ch in (2 * half, 2 * half + 1):
            pre_copy(ch, 1).wait_recv()
            mine = pl.ds(al(ch * BLK + core * 256), 256)
            pack[pl.ds(PM_ROW + ch * 256, 256), :] = pml[mine, :] + pmr[pl.ds(ch * 256, 256), :]
        begin([rs_copy(0, 0, 4 + half)])

    def open_step():
        for half in range(2):
            pm_tiles(half)
            gs = []
            for m in (2 * half, 2 * half + 1):
                pre_copy(m, 0).wait_recv()
            for m in (2 * half, 2 * half + 1):
                gs.append(products(m))
                norms(m)
            for n in range(2):
                tiles(2 * half + n, gs[n])

    for cp in loads[4:]:
        cp.wait()
    for ch in range(4):
        loads[ch].wait()
        prepare(ch * BLK, BLK, out_ref[pl.ds(ch * BLK, BLK), :])
    pl.semaphore_wait(barrier, 10)
    for ch in range(4):
        begin([pre_copy(ch, 1), pre_copy(ch, 0)])
    open_step()

    def one_step(step_index, carry):
        def row_sums(st, k, kern):
            place = own(0, k) - base(0, k)
            slot, r = div(place, TILE), rem(place, TILE)

            def by_rows(vals):
                rs = jnp.sum(vals, axis=1, keepdims=True)
                return jnp.sum(jnp.where(lane_o == sub_o + r, rs, 0.0), axis=0, keepdims=True)

            def by_cols(vals):
                return jnp.sum(vals, axis=0, keepdims=True)

            if st > 0:
                sup, m = UNITS[st][k // 2]
                return [(4 * sup + slot, by_rows(kern)), (4 * m + 2 * core + k % 2, by_cols(kern))]
            both = div(slot, 3)
            up_one = div(slot + 1, 2)
            i0 = (1 - both) * ((1 - core) * (slot + up_one) + core * (1 + div(slot, 2))) + both * 2 * core
            j0 = (1 - both) * ((1 - core) * (1 - up_one) + core * (2 + up_one)) + both * 2 * core
            up = jnp.where(lane_o + 1000 * (1 - both) > sub_o + r, kern, 0.0)
            lo = jnp.where(lane_o + 1000 * (1 - both) < sub_o + r, kern, 0.0)
            nxt = 4 * k + 2 * core + 1
            return [(4 * k + i0, by_rows(up)), (4 * k + j0, by_cols(up)), (nxt, by_rows(lo)), (nxt, by_cols(lo))]

        def advance(st, s):
            parts = [[], [], []]
            for k in range(COLORS):
                mine = pl.ds(al(own(st, k)), OWN)
                if s < 2:
                    peer, length, keep, give = halves[k][s]
                    rs_copy(st, s, k).wait_recv()
                    rng = pl.ds(al(base(st, k) + keep), length)
                    pack[rng, :] += (r0, r1)[s][st, k]
                    begin([rs_copy(st, 1, k)] if s == 0 else x_copies(st, 0, k))
                elif s == 2:
                    x_arrive(st, 0, k)
                    r3[st, k, coords[dims(k)[2]]] = pack[mine, :] + r2[st, k, 0] + r2[st, k, 1] + r2[st, k, 2]
                    begin(x_copies(st, 1, k))
                elif s == 3:
                    x_arrive(st, 1, k)
                    full = (r3[st, k, 0] + r3[st, k, 1]) + (r3[st, k, 2] + r3[st, k, 3])
                    if st == 0 and k >= 4:
                        kern = full
                    else:
                        kern = jnp.exp(-jnp.maximum(full, 0.0) / bandwidth)
                        parts[k % 3] += row_sums(st, k, kern)
                    kg[core, mine, :] = kern.astype(BF16)
                    begin(x_copies(st, 2, k))
                elif s == 4:
                    x_arrive(st, 2, k)
                    begin(x_copies(st, 3, k))
                    begin([dd_copy(st, k, 0)])
                else:
                    for j, cp in enumerate(x_copies(st, 3, k)):
                        cp.wait_recv()
                        begin([dd_copy(st, k, j + 1)])
            if s == 3:
                for d in range(3):
                    if st == 0:
                        svec[0, d] = jnp.zeros((16, TILE), F32)
                    for block, line in parts[d]:
                        svec[0, d, pl.ds(block, 1), :] += line
                    if st == 2:
                        begin(s_copies(0, d))
            if st == 2 and s == 4:
                for d in range(3):
                    arrive(srecv.at[0, d], s_recv.at[0, d])
                    svec[1, d] = svec[0, d] + srecv[0, d, 0] + srecv[0, d, 1] + srecv[0, d, 2]
                    begin(s_copies(1, d))
            if st == 2 and s == 5:
                tot = jnp.zeros((16, TILE), F32)
                for d in range(3):
                    arrive(srecv.at[1, d], s_recv.at[1, d])
                    tot = tot + ((svec[1, d] + srecv[1, d, 0]) + (srecv[1, d, 1] + srecv[1, d, 2]))
                stot[...] = tot
                begin([sp_copy()])

        def unpack_wait(st):
            for k in range(COLORS):
                arrive(kg.at[core, 0:BLK], dd_recv.at[st, k])

        def unpack(st):
            for c in range(2):
                if st > 0:
                    for k in range(COLORS):
                        sup, m = UNITS[st][k // 2]
                        jrng = pl.ds((4 * m + 2 * c + k % 2) * TILE, TILE)
                        for a in range(4):
                            src = kg[c, pl.ds(base(st, k) + a * TILE, TILE), :]
                            srng = pl.ds((4 * sup + a) * TILE, TILE)
                            kfull[srng, jrng] = src
                            kfull[jrng, srng] = src.T
                    continue
                for sup in range(4):
                    for t, (i, j) in enumerate(OFFS[c]):
                        src = kg[c, pl.ds(base(0, sup) + t * TILE, TILE), :]
                        ri, rj = pl.ds((4 * sup + i) * TILE, TILE), pl.ds((4 * sup + j) * TILE, TILE)
                        kfull[ri, rj] = src
                        kfull[rj, ri] = src.T
                    src = kg[c, pl.ds(base(0, sup) + 3 * TILE, TILE), :]
                    srt = src.T
                    one = jnp.ones((TILE, TILE), BF16)
                    ra, rb = pl.ds((4 * sup + 2 * c) * TILE, TILE), pl.ds((4 * sup + 2 * c + 1) * TILE, TILE)
                    kfull[ra, ra] = jnp.where(upper, src, jnp.where(lower, srt, one))
                    kfull[rb, rb] = jnp.where(lower, src, jnp.where(upper, srt, one))

        def drive():
            for q in range(8):
                rows = pl.ds(q * 256, 256)
                pm = kg[q % 2, pl.ds(PM_ROW + (q // 2) * 256, 256), :]
                low = lax.dot_general(pm, fac_ref[...], NT, preferred_element_type=F32)
                th = out_ref[rows, :]
                grad = -((th - mu_ref[...]) * lam_ref[...] + low)
                adrv[rows, :] = (grad - rep_coef * th).astype(BF16)

        def product(start, cols):
            return jnp.dot(kfull[pl.ds(start, 256), cols[0]:cols[1]], adrv[cols[0]:cols[1], :], preferred_element_type=F32)

        def update(chs, early=()):
            starts = [ch * BLK + half * 256 for ch in chs for half in range(2)]
            tot = stot[...] + spart[...] + 1.0

            def whole(n):
                if n < len(early):
                    return early[n] + product(starts[n], (2 * BLK, ROWS))
                return product(starts[n], (0, ROWS))

            ahead = whole(0)
            for n, start in enumerate(starts):
                acc = ahead
                if n + 1 < len(starts):
                    ahead = whole(n + 1)
                rows = pl.ds(start, 256)
                sums = []
                for blk in (start // TILE, start // TILE + 1):
                    line = jnp.where(eye, jnp.broadcast_to(tot[blk:blk + 1, :], (TILE, TILE)), 0.0)
                    sums.append(rep_coef * jnp.sum(line, axis=1, keepdims=True))
                sums = jnp.broadcast_to(jnp.concatenate(sums, axis=0), (256, TILE))
                new = []
                for t in range(width // TILE):
                    cols = slice(t * TILE, (t + 1) * TILE)
                    th = out_ref[rows, cols]
                    phi = (acc[:, cols] + sums * th) / n_part
                    new.append(th + step_size * phi)
                th = jnp.concatenate(new, axis=1)
                out_ref[rows, :] = th
                prepare(start, 256, th)
                if n % 2 == 1:
                    begin([pre_copy(chs[n // 2], 1), pre_copy(chs[n // 2], 0)])

        for s in range(5):
            for st in range(3):
                advance(st, s)
        advance(0, 5)
        advance(1, 5)
        unpack_wait(0)
        unpack(0)
        drive()
        advance(2, 5)
        remote(pack.at[0:5120], pack.at[0:5120], pre_send, sp_recv, mate).wait_send()
        unpack_wait(1)
        unpack(1)
        arrive(stot, sp_recv)
        update((0,))
        unpack_wait(2)
        early = [product(BLK + half * 256, (0, 2 * BLK)) for half in range(2)]
        unpack(2)
        update((1, 2, 3), early)
        for st in range(3):
            total = pack.at[0:SENT + (SENT_SUMS if st == 2 else 0)]
            remote(total, total, sent.at[st], sp_recv, mate).wait_send()
        pl.when(step_index < NUM_STEPS - 1)(open_step)
        return carry

    lax.fori_loop(0, NUM_STEPS, one_step, 0)
    for ch in range(4):
        for what in range(2):
            pre_copy(ch, what).wait_recv()
    remote(pack.at[0:5120], pack.at[0:5120], pre_send, sp_recv, mate).wait_send()


def solution(mesh):
    def run_steps(particles, prec_diag, mean_vec, low_rank):
        total_rows, width = particles.shape
        n_part = total_rows // mesh.shape["ens"]
        bandwidth = BAND_SCALE * width
        step_size = STEP_SCALE * width
        loc = width // (mesh.shape["slab"] * mesh.shape["feat"])
        rank = low_rank.shape[1]
        vm, dma = pltpu.VMEM, pltpu.SemaphoreType.DMA

        def local_steps(current, prec_loc, mean_loc, fac_loc):
            spec = pl.BlockSpec(memory_space=pltpu.VMEM)
            call = pl.pallas_call(
                functools.partial(_kernel, bandwidth, step_size, n_part),
                out_shape=jax.ShapeDtypeStruct((n_part, loc), F32),
                in_specs=[pl.BlockSpec(memory_space=pltpu.HBM)] * 4,
                out_specs=spec,
                scratch_shapes=[
                    vm((1, loc), F32), vm((1, loc), F32), vm((loc, rank), BF16),
                    vm((ROWS, 2 * loc), BF16), vm((ROWS, rank), F32), vm((ROWS // 2, rank), F32),
                    vm((ROWS, TILE), F32), vm((16, TILE), F32),
                    vm((3 * SROWS, TILE), F32),
                    vm((3, COLORS, BLK // 2, TILE), F32), vm((3, COLORS, BLK // 4, TILE), F32),
                    vm((3, COLORS, 3, OWN, TILE), F32), vm((3, COLORS, 4, OWN, TILE), F32),
                    vm((2, 3 * SROWS, TILE), BF16), vm((ROWS, ROWS), BF16), vm((ROWS, loc), BF16),
                    vm((2, 3, 16, TILE), F32), vm((2, 3, 3, 16, TILE), F32), vm((16, TILE), F32), vm((16, TILE), F32),
                    dma((7,)), dma, dma((2, 4)), dma((3,)), dma((3, 2, COLORS)), dma((3, 3, COLORS)), dma((3, COLORS, 3)), dma((3, COLORS)),
                    dma((2, 3)), dma,
                ],
                compiler_params=pltpu.CompilerParams(collective_id=0, has_side_effects=True, vmem_limit_bytes=50000000),
                name="svgd",
            )
            hbm = lambda x: pltpu.with_memory_space_constraint(x, pltpu.HBM)
            return call(hbm(current), hbm(prec_loc.reshape(1, loc)), hbm(mean_loc.reshape(1, loc)), hbm(fac_loc))

        sharded = jax.shard_map(
            local_steps,
            mesh=mesh,
            in_specs=(P("ens", FEAT_AXES), P(LEAD_AXES), P(LEAD_AXES), P(LEAD_AXES, None)),
            out_specs=P("ens", FEAT_AXES),
            check_vma=False,
        )
        return sharded(particles, prec_diag, mean_vec, low_rank)

    return run_steps
```

```python
import functools

import jax
import jax.numpy as jnp
from jax import lax
from jax.experimental import pallas as pl
from jax.experimental.pallas import tpu as pltpu
from jax.sharding import PartitionSpec as P

NUM_STEPS = 3
BAND_SCALE = 4.0
STEP_SCALE = 0.4
FEAT_AXES = ("slab", "feat")
LEAD_AXES = ("ens", "slab", "feat")

ROWS = 2048
TILE = 128
BLK = 512
COLORS = 6
SROWS = COLORS * BLK
UNITS = ((), ((0, 3), (0, 1), (0, 2)), ((1, 2), (1, 3), (2, 3)))
OFFS = (((0, 1), (2, 0), (3, 0)), ((1, 2), (1, 3), (2, 3)))
PM_ROW = 4 * BLK
SENT = 1536 + 768 + 576 + 576 + 288 + 1152 + 1536
SENT_SUMS = 288 + 16
OWN = 32
MESH = pl.DeviceIdType.MESH
NT = (((1,), (1,)), ((), ()))
F32, BF16 = jnp.float32, jnp.bfloat16


def div(a, b):
    return lax.div(a, jnp.int32(b))


def rem(a, b):
    return lax.rem(a, jnp.int32(b))


def _kernel(
    bandwidth, step_size, n_part,
    theta_ref, lam_hbm, mu_hbm, fac_hbm, out_ref,
    lam_ref, mu_ref, fac_ref,
    bfull, pml, pmr, nrow, ncol, pack, r0, r1, r2, r3, kg, kfull, adrv, svec, srecv, stot, spart,
    in_sem, pre_send, pre_recv, sent, rs_recv, x_recv, far_recv, dd_recv, s_recv, sp_recv,
):
    width = out_ref.shape[1]
    rep_coef = 2.0 / bandwidth
    core = lax.axis_index("slab")
    feat = lax.axis_index("feat")
    coords = (rem(feat, 4), rem(div(feat, 4), 4), div(feat, 16))
    strides = (1, 4, 16)

    def chip(dim, coord):
        return {"feat": feat + (coord - coords[dim]) * strides[dim]}

    turned = [[coords[dim]] + [rem(coords[dim] + j, 4) for j in range(1, 4)] for dim in range(3)]

    def around(dim, j):
        return turned[dim][j]

    ring = [[chip(dim, turned[dim][j]) for j in range(4)] for dim in range(3)]
    low_bit = [rem(c, 2) for c in coords]
    pair_bit = [[rem(div(t + 1, 2), 2) for t in turned[dim]] for dim in range(3)]
    high_bit = [[div(t, 2) for t in turned[dim]] for dim in range(3)]

    mate = {"slab": 1 - core}

    def al(x, m=16):
        return pl.multiple_of(x, m)

    halves = []
    for k in range(COLORS):
        steps = []
        start, length, cur = 0, BLK, coords[k % 3]
        for s in range(2):
            if (k // 3 + s) % 2 == 0:
                other, bit = cur + 1 - 2 * low_bit[k % 3], pair_bit[k % 3][0]
            else:
                other, bit = 3 - cur, high_bit[k % 3][0]
            length = length // 2
            keep, give = start + bit * length, start + (1 - bit) * length
            start = keep
            steps.append((chip(k % 3, other), length, keep, give))
        halves.append(steps)

    def dims(k):
        return k % 3, (k + 1) % 3, (k + 2) % 3

    def base(st, k):
        return st * SROWS + k * BLK

    quarters = [[base(st, k) + halves[k][1][2] for k in range(COLORS)] for st in range(3)]
    owns = [[quarters[st][k] + OWN * coords[dims(k)[1]] for k in range(COLORS)] for st in range(3)]
    pieces = [[OWN * around(dims(k)[1], j) for j in range(4)] for k in range(COLORS)]

    places = []
    for k in range(COLORS):
        one, two = (pair_bit, high_bit) if k < 3 else (high_bit, pair_bit)
        places.append([TILE * (2 * one[k % 3][j] + two[k % 3][j]) for j in range(4)])

    def quarter(st, k):
        return quarters[st][k]

    def own(st, k):
        return owns[st][k]

    barrier = pltpu.get_barrier_semaphore()
    pl.semaphore_signal(barrier, inc=1, device_id=mate, device_id_type=MESH)
    for dim in range(3):
        for j in range(1, 4):
            pl.semaphore_signal(barrier, inc=1, device_id=ring[dim][j], device_id_type=MESH)
    loads = [pltpu.make_async_copy(theta_ref.at[pl.ds(ch * BLK, BLK)], out_ref.at[pl.ds(ch * BLK, BLK)], in_sem.at[ch]) for ch in range(4)]
    loads += [
        pltpu.make_async_copy(src, dst, in_sem.at[4 + n])
        for n, (src, dst) in enumerate(((mu_hbm, mu_ref), (fac_hbm, fac_ref), (lam_hbm, lam_ref)))
    ]
    for cp in loads[4:] + loads[:4]:
        cp.start()

    row_i = lax.broadcasted_iota(jnp.int32, (TILE, TILE), 0)
    col_i = lax.broadcasted_iota(jnp.int32, (TILE, TILE), 1)
    eye, upper, lower = row_i == col_i, row_i < col_i, row_i > col_i
    sub_o = lax.broadcasted_iota(jnp.int32, (OWN, TILE), 0)
    lane_o = lax.broadcasted_iota(jnp.int32, (OWN, TILE), 1)

    def remote(src, dst, ssem, rsem, where):
        return pltpu.make_async_remote_copy(src_ref=src, dst_ref=dst, send_sem=ssem, recv_sem=rsem, device_id=where, device_id_type=MESH)

    def pre_copy(ch, what):
        if what == 0:
            rows = pl.ds(ch * BLK, BLK)
            src, dst = bfull.at[rows, 0:width], bfull.at[rows, width:2 * width]
        else:
            src, dst = pml.at[pl.ds(al(ch * BLK + (1 - core) * 256), 256)], pmr.at[pl.ds(ch * 256, 256)]
        return remote(src, dst, pre_send, pre_recv.at[what, ch], mate)

    def prepare(start, length, th):
        rows = pl.ds(start, length)
        bfull[rows, 0:width] = th.astype(BF16)
        pml[rows, :] = jnp.dot((th - mu_ref[...]).astype(BF16), fac_ref[...], preferred_element_type=F32)

    def begin(cps):
        for cp in cps:
            cp.start()

    def arrive(ref, sem):
        remote(ref, ref, sent.at[0], sem, mate).wait_recv()

    def x_arrive(st, e, k):
        arrive((r2.at[st, k], r3.at[st, k, 0:3], kg.at[core, 0:3 * OWN])[e], x_recv.at[st, e, k])

    def rs_copy(st, s, k):
        peer, length, keep, give = halves[k][s]
        src = pack.at[pl.ds(al(base(st, k) + give), length)]
        return remote(src, (r0, r1)[s].at[st, k], sent.at[st], rs_recv.at[st, s, k], peer)

    def gathered(st, k, row, rows):
        if st == 0:
            return kg.at[core, pl.ds(al(base(0, k) + row), rows)]
        sup, m = UNITS[st][k // 2]
        return kfull.at[pl.ds(al(sup * BLK + row), rows), pl.ds(al((4 * m + 2 * core + k % 2) * TILE, TILE), TILE)]

    def x_copies(st, e, k):
        d1, d2, d3 = dims(k)
        dim = (d2, d3, d2, d1)[e]
        cps = []
        for j in range(1, 4):
            if e == 0:
                src = pack.at[pl.ds(al(quarter(st, k) + pieces[k][j]), OWN)]
                dst = r2.at[st, k, j - 1]
            elif e == 1:
                src = dst = r3.at[st, k, coords[dim]]
            else:
                start = (own if e == 2 else quarter)(0, k) - base(0, k)
                src = dst = gathered(st, k, start, OWN if e == 2 else TILE)
            arrived = far_recv.at[st, k, j - 1] if e == 3 else x_recv.at[st, e, k]
            cps.append(remote(src, dst, sent.at[st], arrived, ring[dim][j]))
        return cps

    def dd_copy(st, k, j):
        ref = gathered(st, k, halves[k][1][2] if j == 0 else places[k][4 - j], TILE)
        return remote(ref, ref, sent.at[st], dd_recv.at[st, k], mate)

    def s_copies(ph, d):
        dim = ((d + 1) % 3, d)[ph]
        return [
            remote(svec.at[ph, d], srecv.at[ph, d, j - 1], sent.at[2], s_recv.at[ph, d], ring[dim][j])
            for j in range(1, 4)
        ]

    def sp_copy():
        return remote(stot, spart, sent.at[2], sp_recv, mate)

    def products(m):
        mine = bfull[pl.ds(al(m * BLK + 256 * core), 256), :]
        part = BLK if m == 3 else (m + 1) * 256
        return [lax.dot_general(bfull[pl.ds(at, part), :], mine, NT, preferred_element_type=F32) for at in range(0, (m + 1) * BLK, part)]

    def norms(m):
        for i in range(4):
            rows = pl.ds((4 * m + i) * TILE, TILE)
            wide = bfull[rows, :].astype(F32)
            n = jnp.broadcast_to(jnp.sum(wide * wide, axis=1, keepdims=True), (TILE, TILE))
            nrow[rows, :] = n
            ncol[4 * m + i:4 * m + i + 1, :] = jnp.sum(jnp.where(eye, n, 0.0), axis=0, keepdims=True)

    def tiles(m, g):
        def block(blk, b):
            n, r = divmod(blk * TILE, BLK if m == 3 else (m + 1) * 256)
            return g[n][r:r + TILE, b * TILE:(b + 1) * TILE]

        def tile(i, b):
            return block(4 * m + i, b)

        def dist(i, j):
            return nrow[pl.ds((4 * m + i) * TILE, TILE), :] + ncol[4 * m + j:4 * m + j + 1, :] - 2.0 * tile(i, j % 2)

        for t in range(3):
            pack[pl.ds(base(0, m) + t * TILE, TILE), :] = jnp.where(core == 0, dist(*OFFS[0][t]), dist(*OFFS[1][t]))
        one = jnp.where(core == 0, dist(0, 0), dist(2, 2))
        two = jnp.where(core == 0, dist(1, 1), dist(3, 3))
        pack[pl.ds(base(0, m) + 3 * TILE, TILE), :] = jnp.where(upper, one, two)
        begin([rs_copy(0, 0, m)])
        for st in (1, 2):
            for u, (sup, col) in enumerate(UNITS[st]):
                if col != m:
                    continue
                for b in range(2):
                    nc = ncol[pl.ds(4 * m + 2 * core + b, 1), :]
                    for a in range(4):
                        nr = nrow[pl.ds((4 * sup + a) * TILE, TILE), :]
                        pack[pl.ds(base(st, 2 * u + b) + a * TILE, TILE), :] = nr + nc - 2.0 * block(4 * sup + a, b)
                begin([rs_copy(st, 0, 2 * u), rs_copy(st, 0, 2 * u + 1)])

    def pm_tiles(half):
        for ch in (2 * half, 2 * half + 1):
            pre_copy(ch, 1).wait_recv()
            mine = pl.ds(al(ch * BLK + core * 256), 256)
            pack[pl.ds(PM_ROW + ch * 256, 256), :] = pml[mine, :] + pmr[pl.ds(ch * 256, 256), :]
        begin([rs_copy(0, 0, 4 + half)])

    def open_step():
        begin([pre_copy(3, 1), pre_copy(3, 0)])
        for half in range(2):
            pm_tiles(half)
            gs = []
            for m in (2 * half, 2 * half + 1):
                pre_copy(m, 0).wait_recv()
            for m in (2 * half, 2 * half + 1):
                gs.append(products(m))
                norms(m)
            for n in range(2):
                tiles(2 * half + n, gs[n])

    for cp in loads[4:]:
        cp.wait()
    for ch in range(4):
        loads[ch].wait()
        prepare(ch * BLK, BLK, out_ref[pl.ds(ch * BLK, BLK), :])
    pl.semaphore_wait(barrier, 10)
    for ch in range(3):
        begin([pre_copy(ch, 1), pre_copy(ch, 0)])
    open_step()

    def one_step(step_index, carry):
        def row_sums(st, k, kern):
            place = own(0, k) - base(0, k)
            slot, r = div(place, TILE), rem(place, TILE)

            def by_rows(vals):
                rs = jnp.sum(vals, axis=1, keepdims=True)
                return jnp.sum(jnp.where(lane_o == sub_o + r, rs, 0.0), axis=0, keepdims=True)

            def by_cols(vals):
                return jnp.sum(vals, axis=0, keepdims=True)

            if st > 0:
                sup, m = UNITS[st][k // 2]
                return [(4 * sup + slot, by_rows(kern)), (4 * m + 2 * core + k % 2, by_cols(kern))]
            both = div(slot, 3)
            up_one = div(slot + 1, 2)
            i0 = (1 - both) * ((1 - core) * (slot + up_one) + core * (1 + div(slot, 2))) + both * 2 * core
            j0 = (1 - both) * ((1 - core) * (1 - up_one) + core * (2 + up_one)) + both * 2 * core
            up = jnp.where(lane_o + 1000 * (1 - both) > sub_o + r, kern, 0.0)
            lo = jnp.where(lane_o + 1000 * (1 - both) < sub_o + r, kern, 0.0)
            nxt = 4 * k + 2 * core + 1
            return [(4 * k + i0, by_rows(up)), (4 * k + j0, by_cols(up)), (nxt, by_rows(lo)), (nxt, by_cols(lo))]

        def advance(st, s):
            parts = [[], [], []]
            if st == 2 and s == 4:
                for d in range(3):
                    arrive(srecv.at[0, d], s_recv.at[0, d])
                    svec[1, d] = svec[0, d] + srecv[0, d, 0] + srecv[0, d, 1] + srecv[0, d, 2]
                    begin(s_copies(1, d))
            if st == 2 and s == 5:
                tot = jnp.zeros((16, TILE), F32)
                for d in range(3):
                    arrive(srecv.at[1, d], s_recv.at[1, d])
                    tot = tot + ((svec[1, d] + srecv[1, d, 0]) + (srecv[1, d, 1] + srecv[1, d, 2]))
                stot[...] = tot
                begin([sp_copy()])
            for k in range(COLORS):
                mine = pl.ds(al(own(st, k)), OWN)
                if s < 2:
                    peer, length, keep, give = halves[k][s]
                    rs_copy(st, s, k).wait_recv()
                    rng = pl.ds(al(base(st, k) + keep), length)
                    pack[rng, :] += (r0, r1)[s][st, k]
                    begin([rs_copy(st, 1, k)] if s == 0 else x_copies(st, 0, k))
                elif s == 2:
                    x_arrive(st, 0, k)
                    r3[st, k, coords[dims(k)[2]]] = pack[mine, :] + r2[st, k, 0] + r2[st, k, 1] + r2[st, k, 2]
                    begin(x_copies(st, 1, k))
                elif s == 3:
                    x_arrive(st, 1, k)
                    full = (r3[st, k, 0] + r3[st, k, 1]) + (r3[st, k, 2] + r3[st, k, 3])
                    if st == 0 and k >= 4:
                        kern = full
                    else:
                        kern = jnp.exp(-jnp.maximum(full, 0.0) / bandwidth)
                        parts[k % 3] += row_sums(st, k, kern)
                    gathered(st, k, own(0, k) - base(0, k), OWN)[...] = kern.astype(BF16)
                    begin(x_copies(st, 2, k))
                elif s == 4:
                    x_arrive(st, 2, k)
                    begin(x_copies(st, 3, k))
                    begin([dd_copy(st, k, 0)])
                else:
                    for j, cp in enumerate(x_copies(st, 3, k)):
                        cp.wait_recv()
                        begin([dd_copy(st, k, j + 1)])
            if s == 3:
                for d in range(3):
                    if st == 0:
                        svec[0, d] = jnp.zeros((16, TILE), F32)
                    for block, line in parts[d]:
                        svec[0, d, pl.ds(block, 1), :] += line
                    if st == 2:
                        begin(s_copies(0, d))
        def unpack_wait(st):
            for k in range(COLORS):
                arrive(kg.at[core, 0:BLK], dd_recv.at[st, k])

        def unpack(st):
            for c in range(2):
                if st > 0:
                    for k in range(COLORS):
                        sup, m = UNITS[st][k // 2]
                        jrng = pl.ds((4 * m + 2 * c + k % 2) * TILE, TILE)
                        for a in range(4):
                            srng = pl.ds((4 * sup + a) * TILE, TILE)
                            kfull[jrng, srng] = kfull[srng, jrng].T
                    continue
                for sup in range(4):
                    for t, (i, j) in enumerate(OFFS[c]):
                        src = kg[c, pl.ds(base(0, sup) + t * TILE, TILE), :]
                        ri, rj = pl.ds((4 * sup + i) * TILE, TILE), pl.ds((4 * sup + j) * TILE, TILE)
                        kfull[ri, rj] = src
                        kfull[rj, ri] = src.T
                    src = kg[c, pl.ds(base(0, sup) + 3 * TILE, TILE), :]
                    srt = src.T
                    one = jnp.ones((TILE, TILE), BF16)
                    ra, rb = pl.ds((4 * sup + 2 * c) * TILE, TILE), pl.ds((4 * sup + 2 * c + 1) * TILE, TILE)
                    kfull[ra, ra] = jnp.where(upper, src, jnp.where(lower, srt, one))
                    kfull[rb, rb] = jnp.where(lower, src, jnp.where(upper, srt, one))

        def drive():
            for q in range(8):
                rows = pl.ds(q * 256, 256)
                pm = kg[q % 2, pl.ds(PM_ROW + (q // 2) * 256, 256), :]
                low = lax.dot_general(pm, fac_ref[...], NT, preferred_element_type=F32)
                th = out_ref[rows, :]
                grad = -((th - mu_ref[...]) * lam_ref[...] + low)
                adrv[rows, :] = (grad - rep_coef * th).astype(BF16)

        def product(start):
            return jnp.dot(kfull[pl.ds(start, 256), :], adrv[...], preferred_element_type=F32)

        def update(chs, st):
            starts = [ch * BLK + half * 256 for ch in chs for half in range(2)]
            tot = stot[...] + spart[...] + 1.0

            ahead = product(starts[0])
            unpack(st)
            for n, start in enumerate(starts):
                acc = ahead
                if n + 1 < len(starts):
                    ahead = product(starts[n + 1])
                rows = pl.ds(start, 256)
                sums = []
                for blk in (start // TILE, start // TILE + 1):
                    line = jnp.where(eye, jnp.broadcast_to(tot[blk:blk + 1, :], (TILE, TILE)), 0.0)
                    sums.append(rep_coef * jnp.sum(line, axis=1, keepdims=True))
                sums = jnp.broadcast_to(jnp.concatenate(sums, axis=0), (256, TILE))
                new = []
                for t in range(width // TILE):
                    cols = slice(t * TILE, (t + 1) * TILE)
                    th = out_ref[rows, cols]
                    phi = (acc[:, cols] + sums * th) / n_part
                    new.append(th + step_size * phi)
                th = jnp.concatenate(new, axis=1)
                out_ref[rows, :] = th
                prepare(start, 256, th)
                if n % 2 == 1 and chs[n // 2] < 3:
                    begin([pre_copy(chs[n // 2], 1), pre_copy(chs[n // 2], 0)])

        for s in range(5):
            for st in range(3):
                advance(st, s)
        advance(0, 5)
        advance(1, 5)
        unpack_wait(0)
        unpack(0)
        drive()
        advance(2, 5)
        remote(pack.at[0:5120], pack.at[0:5120], pre_send, sp_recv, mate).wait_send()
        unpack_wait(1)
        arrive(stot, sp_recv)
        update((0,), 1)
        unpack_wait(2)
        update((1, 2, 3), 2)
        for st in range(3):
            total = pack.at[0:SENT + (SENT_SUMS if st == 2 else 0)]
            remote(total, total, sent.at[st], sp_recv, mate).wait_send()
        pl.when(step_index < NUM_STEPS - 1)(open_step)
        return carry

    lax.fori_loop(0, NUM_STEPS, one_step, 0)
    for ch in range(3):
        for what in range(2):
            pre_copy(ch, what).wait_recv()
    remote(pack.at[0:3840], pack.at[0:3840], pre_send, sp_recv, mate).wait_send()


def solution(mesh):
    def run_steps(particles, prec_diag, mean_vec, low_rank):
        total_rows, width = particles.shape
        n_part = total_rows // mesh.shape["ens"]
        bandwidth = BAND_SCALE * width
        step_size = STEP_SCALE * width
        loc = width // (mesh.shape["slab"] * mesh.shape["feat"])
        rank = low_rank.shape[1]
        vm, dma = pltpu.VMEM, pltpu.SemaphoreType.DMA

        def local_steps(current, prec_loc, mean_loc, fac_loc):
            spec = pl.BlockSpec(memory_space=pltpu.VMEM)
            call = pl.pallas_call(
                functools.partial(_kernel, bandwidth, step_size, n_part),
                out_shape=jax.ShapeDtypeStruct((n_part, loc), F32),
                in_specs=[pl.BlockSpec(memory_space=pltpu.HBM)] * 4,
                out_specs=spec,
                scratch_shapes=[
                    vm((1, loc), F32), vm((1, loc), F32), vm((loc, rank), BF16),
                    vm((ROWS, 2 * loc), BF16), vm((ROWS, rank), F32), vm((ROWS // 2, rank), F32),
                    vm((ROWS, TILE), F32), vm((16, TILE), F32),
                    vm((3 * SROWS, TILE), F32),
                    vm((3, COLORS, BLK // 2, TILE), F32), vm((3, COLORS, BLK // 4, TILE), F32),
                    vm((3, COLORS, 3, OWN, TILE), F32), vm((3, COLORS, 4, OWN, TILE), F32),
                    vm((2, SROWS, TILE), BF16), vm((ROWS, ROWS), BF16), vm((ROWS, loc), BF16),
                    vm((2, 3, 16, TILE), F32), vm((2, 3, 3, 16, TILE), F32), vm((16, TILE), F32), vm((16, TILE), F32),
                    dma((7,)), dma, dma((2, 4)), dma((3,)), dma((3, 2, COLORS)), dma((3, 3, COLORS)), dma((3, COLORS, 3)), dma((3, COLORS)),
                    dma((2, 3)), dma,
                ],
                compiler_params=pltpu.CompilerParams(collective_id=0, has_side_effects=True, vmem_limit_bytes=50000000),
                name="svgd",
            )
            hbm = lambda x: pltpu.with_memory_space_constraint(x, pltpu.HBM)
            return call(hbm(current), hbm(prec_loc.reshape(1, loc)), hbm(mean_loc.reshape(1, loc)), hbm(fac_loc))

        sharded = jax.shard_map(
            local_steps,
            mesh=mesh,
            in_specs=(P("ens", FEAT_AXES), P(LEAD_AXES), P(LEAD_AXES), P(LEAD_AXES, None)),
            out_specs=P("ens", FEAT_AXES),
            check_vma=False,
        )
        return sharded(particles, prec_diag, mean_vec, low_rank)

    return run_steps
```

```python
import functools

import jax
import jax.numpy as jnp
from jax import lax
from jax.experimental import pallas as pl
from jax.experimental.pallas import tpu as pltpu
from jax.sharding import PartitionSpec as P

NUM_STEPS = 3
BAND_SCALE = 4.0
STEP_SCALE = 0.4
FEAT_AXES = ("slab", "feat")
LEAD_AXES = ("ens", "slab", "feat")

ROWS = 2048
TILE = 128
BLK = 512
COLORS = 6
SROWS = COLORS * BLK
UNITS = ((), ((0, 3), (0, 1), (0, 2)), ((1, 2), (1, 3), (2, 3)))
OFFS = (((0, 1), (2, 0), (3, 0)), ((1, 2), (1, 3), (2, 3)))
PM_ROW = 4 * BLK
SENT = 1536 + 768 + 576 + 576 + 288 + 1152 + 1536
SENT_SUMS = 288 + 16
OWN = 32
MESH = pl.DeviceIdType.MESH
NT = (((1,), (1,)), ((), ()))
F32, BF16 = jnp.float32, jnp.bfloat16


def div(a, b):
    return lax.div(a, jnp.int32(b))


def rem(a, b):
    return lax.rem(a, jnp.int32(b))


def _kernel(
    bandwidth, step_size, n_part,
    theta_ref, lam_hbm, mu_hbm, fac_hbm, out_ref,
    lam_ref, mu_ref, fac_ref,
    bfull, pml, pmr, nrow, ncol, pack, r0, r1, r2, r3, kg, kfull, adrv, svec, srecv, stot, spart,
    in_sem, pre_send, pre_recv, sent, rs_recv, x_recv, far_recv, dd_recv, s_recv, sp_recv,
):
    width = out_ref.shape[1]
    rep_coef = 2.0 / bandwidth
    core = lax.axis_index("slab")
    feat = lax.axis_index("feat")
    coords = (rem(feat, 4), rem(div(feat, 4), 4), div(feat, 16))
    strides = (1, 4, 16)

    def chip(dim, coord):
        return {"feat": feat + (coord - coords[dim]) * strides[dim]}

    turned = [[coords[dim]] + [rem(coords[dim] + j, 4) for j in range(1, 4)] for dim in range(3)]

    def around(dim, j):
        return turned[dim][j]

    ring = [[chip(dim, turned[dim][j]) for j in range(4)] for dim in range(3)]
    low_bit = [rem(c, 2) for c in coords]
    pair_bit = [[rem(div(t + 1, 2), 2) for t in turned[dim]] for dim in range(3)]
    high_bit = [[div(t, 2) for t in turned[dim]] for dim in range(3)]

    mate = {"slab": 1 - core}

    def al(x, m=16):
        return pl.multiple_of(x, m)

    halves = []
    for k in range(COLORS):
        steps = []
        start, length, cur = 0, BLK, coords[k % 3]
        for s in range(2):
            if (k // 3 + s) % 2 == 0:
                other, bit = cur + 1 - 2 * low_bit[k % 3], pair_bit[k % 3][0]
            else:
                other, bit = 3 - cur, high_bit[k % 3][0]
            length = length // 2
            keep, give = start + bit * length, start + (1 - bit) * length
            start = keep
            steps.append((chip(k % 3, other), length, keep, give))
        halves.append(steps)

    def dims(k):
        return k % 3, (k + 1) % 3, (k + 2) % 3

    def base(st, k):
        return st * SROWS + k * BLK

    quarters = [[base(st, k) + halves[k][1][2] for k in range(COLORS)] for st in range(3)]
    owns = [[quarters[st][k] + OWN * coords[dims(k)[1]] for k in range(COLORS)] for st in range(3)]
    pieces = [[OWN * around(dims(k)[1], j) for j in range(4)] for k in range(COLORS)]

    places = []
    for k in range(COLORS):
        one, two = (pair_bit, high_bit) if k < 3 else (high_bit, pair_bit)
        places.append([TILE * (2 * one[k % 3][j] + two[k % 3][j]) for j in range(4)])

    def quarter(st, k):
        return quarters[st][k]

    def own(st, k):
        return owns[st][k]

    barrier = pltpu.get_barrier_semaphore()
    pl.semaphore_signal(barrier, inc=1, device_id=mate, device_id_type=MESH)
    for dim in range(3):
        for j in range(1, 4):
            pl.semaphore_signal(barrier, inc=1, device_id=ring[dim][j], device_id_type=MESH)
    loads = [pltpu.make_async_copy(theta_ref.at[pl.ds(ch * BLK, BLK)], out_ref.at[pl.ds(ch * BLK, BLK)], in_sem.at[ch]) for ch in range(4)]
    loads += [
        pltpu.make_async_copy(src, dst, in_sem.at[4 + n])
        for n, (src, dst) in enumerate(((mu_hbm, mu_ref), (fac_hbm, fac_ref), (lam_hbm, lam_ref)))
    ]
    for cp in loads[4:] + loads[:4]:
        cp.start()

    row_i = lax.broadcasted_iota(jnp.int32, (TILE, TILE), 0)
    col_i = lax.broadcasted_iota(jnp.int32, (TILE, TILE), 1)
    eye, upper, lower = row_i == col_i, row_i < col_i, row_i > col_i
    sub_o = lax.broadcasted_iota(jnp.int32, (OWN, TILE), 0)
    lane_o = lax.broadcasted_iota(jnp.int32, (OWN, TILE), 1)

    def remote(src, dst, ssem, rsem, where):
        return pltpu.make_async_remote_copy(src_ref=src, dst_ref=dst, send_sem=ssem, recv_sem=rsem, device_id=where, device_id_type=MESH)

    def pre_bf16(piece):
        rows = pl.ds(piece * 256, 256)
        return remote(bfull.at[rows, 0:width], bfull.at[rows, width:2 * width], pre_send, pre_recv.at[piece], mate)

    def pre_pm(ch):
        src, dst = pml.at[pl.ds(al(ch * BLK + (1 - core) * 256), 256)], pmr.at[pl.ds(ch * 256, 256)]
        return remote(src, dst, pre_send, pre_recv.at[8 + ch], mate)

    def prepare(start, length, th):
        rows = pl.ds(start, length)
        bfull[rows, 0:width] = th.astype(BF16)
        pml[rows, :] = jnp.dot((th - mu_ref[...]).astype(BF16), fac_ref[...], preferred_element_type=F32)

    def begin(cps):
        for cp in cps:
            cp.start()

    def arrive(ref, sem):
        remote(ref, ref, sent.at[0], sem, mate).wait_recv()

    def x_arrive(st, e, k):
        arrive((r2.at[st, k], r3.at[st, k, 0:3], kg.at[core, 0:3 * OWN])[e], x_recv.at[st, e, k])

    def rs_copy(st, s, k):
        peer, length, keep, give = halves[k][s]
        src = pack.at[pl.ds(al(base(st, k) + give), length)]
        return remote(src, (r0, r1)[s].at[st, k], sent.at[st], rs_recv.at[st, s, k], peer)

    def gathered(st, k, row, rows):
        if st == 0:
            return kg.at[core, pl.ds(al(base(0, k) + row), rows)]
        sup, m = UNITS[st][k // 2]
        return kfull.at[pl.ds(al(sup * BLK + row), rows), pl.ds(al((4 * m + 2 * core + k % 2) * TILE, TILE), TILE)]

    def x_copies(st, e, k):
        d1, d2, d3 = dims(k)
        dim = (d2, d3, d2, d1)[e]
        cps = []
        for j in range(1, 4):
            if e == 0:
                src = pack.at[pl.ds(al(quarter(st, k) + pieces[k][j]), OWN)]
                dst = r2.at[st, k, j - 1]
            elif e == 1:
                src = dst = r3.at[st, k, coords[dim]]
            else:
                start = (own if e == 2 else quarter)(0, k) - base(0, k)
                src = dst = gathered(st, k, start, OWN if e == 2 else TILE)
            arrived = far_recv.at[st, k, j - 1] if e == 3 else x_recv.at[st, e, k]
            cps.append(remote(src, dst, sent.at[st], arrived, ring[dim][j]))
        return cps

    def dd_copy(st, k, j):
        ref = gathered(st, k, halves[k][1][2] if j == 0 else places[k][4 - j], TILE)
        return remote(ref, ref, sent.at[st], dd_recv.at[st, k], mate)

    def s_copies(ph, d):
        dim = ((d + 1) % 3, d)[ph]
        return [
            remote(svec.at[ph, d], srecv.at[ph, d, j - 1], sent.at[2], s_recv.at[ph, d], ring[dim][j])
            for j in range(1, 4)
        ]

    def sp_copy():
        return remote(stot, spart, sent.at[2], sp_recv, mate)

    def products(m):
        mine = bfull[pl.ds(al(m * BLK + 256 * core), 256), :]
        part = BLK if m == 3 else (m + 1) * 256
        return [lax.dot_general(bfull[pl.ds(at, part), :], mine, NT, preferred_element_type=F32) for at in range(0, (m + 1) * BLK, part)]

    def norms(m):
        for i in range(4):
            rows = pl.ds((4 * m + i) * TILE, TILE)
            wide = bfull[rows, :].astype(F32)
            n = jnp.broadcast_to(jnp.sum(wide * wide, axis=1, keepdims=True), (TILE, TILE))
            nrow[rows, :] = n
            ncol[4 * m + i:4 * m + i + 1, :] = jnp.sum(jnp.where(eye, n, 0.0), axis=0, keepdims=True)

    def tiles(m, g):
        def block(blk, b):
            n, r = divmod(blk * TILE, BLK if m == 3 else (m + 1) * 256)
            return g[n][r:r + TILE, b * TILE:(b + 1) * TILE]

        def tile(i, b):
            return block(4 * m + i, b)

        def dist(i, j):
            return nrow[pl.ds((4 * m + i) * TILE, TILE), :] + ncol[4 * m + j:4 * m + j + 1, :] - 2.0 * tile(i, j % 2)

        for t in range(3):
            pack[pl.ds(base(0, m) + t * TILE, TILE), :] = jnp.where(core == 0, dist(*OFFS[0][t]), dist(*OFFS[1][t]))
        one = jnp.where(core == 0, dist(0, 0), dist(2, 2))
        two = jnp.where(core == 0, dist(1, 1), dist(3, 3))
        pack[pl.ds(base(0, m) + 3 * TILE, TILE), :] = jnp.where(upper, one, two)
        begin([rs_copy(0, 0, m)])
        for st in (1, 2):
            for u, (sup, col) in enumerate(UNITS[st]):
                if col != m:
                    continue
                for b in range(2):
                    nc = ncol[pl.ds(4 * m + 2 * core + b, 1), :]
                    for a in range(4):
                        nr = nrow[pl.ds((4 * sup + a) * TILE, TILE), :]
                        pack[pl.ds(base(st, 2 * u + b) + a * TILE, TILE), :] = nr + nc - 2.0 * block(4 * sup + a, b)
                begin([rs_copy(st, 0, 2 * u), rs_copy(st, 0, 2 * u + 1)])

    def pm_tiles(half):
        for ch in (2 * half, 2 * half + 1):
            pre_pm(ch).wait_recv()
            mine = pl.ds(al(ch * BLK + core * 256), 256)
            pack[pl.ds(PM_ROW + ch * 256, 256), :] = pml[mine, :] + pmr[pl.ds(ch * 256, 256), :]
        begin([rs_copy(0, 0, 4 + half)])

    def open_step():
        begin([pre_pm(3), pre_bf16(7)])
        pm_tiles(0)
        for piece in range(4):
            pre_bf16(piece).wait_recv()
        gs = []
        for m in range(2):
            gs.append(products(m))
            norms(m)
        for m in range(2):
            tiles(m, gs[m])
        for m in range(2, 4):
            for piece in range(2 * m, 2 * m + 2):
                pre_bf16(piece).wait_recv()
            g = products(m)
            norms(m)
            tiles(m, g)
            if m == 2:
                pm_tiles(1)

    for cp in loads[4:]:
        cp.wait()
    for ch in range(4):
        loads[ch].wait()
        prepare(ch * BLK, BLK, out_ref[pl.ds(ch * BLK, BLK), :])
        if ch == 0:
            pl.semaphore_wait(barrier, 10)
        if ch < 3:
            begin([pre_pm(ch)])
        begin([pre_bf16(piece) for piece in (2 * ch, 2 * ch + 1) if piece < 7])
    open_step()

    def one_step(step_index, carry):
        def row_sums(st, k, kern):
            place = own(0, k) - base(0, k)
            slot, r = div(place, TILE), rem(place, TILE)

            def by_rows(vals):
                rs = jnp.sum(vals, axis=1, keepdims=True)
                return jnp.sum(jnp.where(lane_o == sub_o + r, rs, 0.0), axis=0, keepdims=True)

            def by_cols(vals):
                return jnp.sum(vals, axis=0, keepdims=True)

            if st > 0:
                sup, m = UNITS[st][k // 2]
                return [(4 * sup + slot, by_rows(kern)), (4 * m + 2 * core + k % 2, by_cols(kern))]
            both = div(slot, 3)
            up_one = div(slot + 1, 2)
            i0 = (1 - both) * ((1 - core) * (slot + up_one) + core * (1 + div(slot, 2))) + both * 2 * core
            j0 = (1 - both) * ((1 - core) * (1 - up_one) + core * (2 + up_one)) + both * 2 * core
            up = jnp.where(lane_o + 1000 * (1 - both) > sub_o + r, kern, 0.0)
            lo = jnp.where(lane_o + 1000 * (1 - both) < sub_o + r, kern, 0.0)
            nxt = 4 * k + 2 * core + 1
            return [(4 * k + i0, by_rows(up)), (4 * k + j0, by_cols(up)), (nxt, by_rows(lo)), (nxt, by_cols(lo))]

        def advance(st, s):
            parts = [[], [], []]
            if st == 2 and s == 4:
                for d in range(3):
                    arrive(srecv.at[0, d], s_recv.at[0, d])
                    svec[1, d] = svec[0, d] + srecv[0, d, 0] + srecv[0, d, 1] + srecv[0, d, 2]
                    begin(s_copies(1, d))
            if st == 2 and s == 5:
                tot = jnp.zeros((16, TILE), F32)
                for d in range(3):
                    arrive(srecv.at[1, d], s_recv.at[1, d])
                    tot = tot + ((svec[1, d] + srecv[1, d, 0]) + (srecv[1, d, 1] + srecv[1, d, 2]))
                stot[...] = tot
                begin([sp_copy()])
            for k in range(COLORS):
                mine = pl.ds(al(own(st, k)), OWN)
                if s < 2:
                    peer, length, keep, give = halves[k][s]
                    rs_copy(st, s, k).wait_recv()
                    rng = pl.ds(al(base(st, k) + keep), length)
                    pack[rng, :] += (r0, r1)[s][st, k]
                    begin([rs_copy(st, 1, k)] if s == 0 else x_copies(st, 0, k))
                elif s == 2:
                    x_arrive(st, 0, k)
                    r3[st, k, coords[dims(k)[2]]] = pack[mine, :] + r2[st, k, 0] + r2[st, k, 1] + r2[st, k, 2]
                    begin(x_copies(st, 1, k))
                elif s == 3:
                    x_arrive(st, 1, k)
                    full = (r3[st, k, 0] + r3[st, k, 1]) + (r3[st, k, 2] + r3[st, k, 3])
                    if st == 0 and k >= 4:
                        kern = full
                    else:
                        kern = jnp.exp(-jnp.maximum(full, 0.0) / bandwidth)
                        parts[k % 3] += row_sums(st, k, kern)
                    gathered(st, k, own(0, k) - base(0, k), OWN)[...] = kern.astype(BF16)
                    begin(x_copies(st, 2, k))
                elif s == 4:
                    x_arrive(st, 2, k)
                    begin(x_copies(st, 3, k))
                    begin([dd_copy(st, k, 0)])
                else:
                    for j, cp in enumerate(x_copies(st, 3, k)):
                        cp.wait_recv()
                        begin([dd_copy(st, k, j + 1)])
            if s == 3:
                for d in range(3):
                    if st == 0:
                        svec[0, d] = jnp.zeros((16, TILE), F32)
                    for block, line in parts[d]:
                        svec[0, d, pl.ds(block, 1), :] += line
                    if st == 2:
                        begin(s_copies(0, d))
        def unpack_wait(st):
            for k in range(COLORS):
                arrive(kg.at[core, 0:BLK], dd_recv.at[st, k])

        def unpack(st):
            for c in range(2):
                if st > 0:
                    for k in range(COLORS):
                        sup, m = UNITS[st][k // 2]
                        jrng = pl.ds((4 * m + 2 * c + k % 2) * TILE, TILE)
                        for a in range(4):
                            srng = pl.ds((4 * sup + a) * TILE, TILE)
                            kfull[jrng, srng] = kfull[srng, jrng].T
                    continue
                for sup in range(4):
                    for t, (i, j) in enumerate(OFFS[c]):
                        src = kg[c, pl.ds(base(0, sup) + t * TILE, TILE), :]
                        ri, rj = pl.ds((4 * sup + i) * TILE, TILE), pl.ds((4 * sup + j) * TILE, TILE)
                        kfull[ri, rj] = src
                        kfull[rj, ri] = src.T
                    src = kg[c, pl.ds(base(0, sup) + 3 * TILE, TILE), :]
                    srt = src.T
                    one = jnp.ones((TILE, TILE), BF16)
                    ra, rb = pl.ds((4 * sup + 2 * c) * TILE, TILE), pl.ds((4 * sup + 2 * c + 1) * TILE, TILE)
                    kfull[ra, ra] = jnp.where(upper, src, jnp.where(lower, srt, one))
                    kfull[rb, rb] = jnp.where(lower, src, jnp.where(upper, srt, one))

        def drive():
            for q in range(8):
                rows = pl.ds(q * 256, 256)
                pm = kg[q % 2, pl.ds(PM_ROW + (q // 2) * 256, 256), :]
                low = lax.dot_general(pm, fac_ref[...], NT, preferred_element_type=F32)
                th = out_ref[rows, :]
                grad = -((th - mu_ref[...]) * lam_ref[...] + low)
                adrv[rows, :] = (grad - rep_coef * th).astype(BF16)

        def product(start):
            return jnp.dot(kfull[pl.ds(start, 256), :], adrv[...], preferred_element_type=F32)

        def finish(start, acc, tot):
            rows = pl.ds(start, 256)
            sums = []
            for blk in (start // TILE, start // TILE + 1):
                line = jnp.where(eye, jnp.broadcast_to(tot[blk:blk + 1, :], (TILE, TILE)), 0.0)
                sums.append(rep_coef * jnp.sum(line, axis=1, keepdims=True))
            sums = jnp.broadcast_to(jnp.concatenate(sums, axis=0), (256, TILE))
            new = []
            for t in range(width // TILE):
                cols = slice(t * TILE, (t + 1) * TILE)
                th = out_ref[rows, cols]
                phi = (acc[:, cols] + sums * th) / n_part
                new.append(th + step_size * phi)
            th = jnp.concatenate(new, axis=1)
            out_ref[rows, :] = th
            prepare(start, 256, th)
            piece = start // 256
            if piece == 6:
                begin([pre_bf16(6)])
            elif piece in (1, 3, 5):
                begin([pre_pm(piece // 2), pre_bf16(piece - 1), pre_bf16(piece)])

        for s in range(5):
            for st in range(3):
                advance(st, s)
        advance(0, 5)
        advance(1, 5)
        unpack_wait(0)
        unpack(0)
        drive()
        advance(2, 5)
        remote(pack.at[0:5120], pack.at[0:5120], pre_send, sp_recv, mate).wait_send()
        def update(starts, st):
            tot = stot[...] + spart[...] + 1.0
            ahead = product(starts[0])
            unpack(st)
            for n, start in enumerate(starts):
                acc = ahead
                if n + 1 < len(starts):
                    ahead = product(starts[n + 1])
                finish(start, acc, tot)

        unpack_wait(1)
        arrive(stot, sp_recv)
        update(range(0, BLK, 256), 1)
        unpack_wait(2)
        update(range(BLK, ROWS, 256), 2)
        for st in range(3):
            total = pack.at[0:SENT + (SENT_SUMS if st == 2 else 0)]
            remote(total, total, sent.at[st], sp_recv, mate).wait_send()
        pl.when(step_index < NUM_STEPS - 1)(open_step)
        return carry

    lax.fori_loop(0, NUM_STEPS, one_step, 0)
    for ch in range(3):
        pre_pm(ch).wait_recv()
    for piece in range(7):
        pre_bf16(piece).wait_recv()
    total = pack.at[0:7 * 512 + 3 * 256]
    remote(total, total, pre_send, sp_recv, mate).wait_send()


def solution(mesh):
    def run_steps(particles, prec_diag, mean_vec, low_rank):
        total_rows, width = particles.shape
        n_part = total_rows // mesh.shape["ens"]
        bandwidth = BAND_SCALE * width
        step_size = STEP_SCALE * width
        loc = width // (mesh.shape["slab"] * mesh.shape["feat"])
        rank = low_rank.shape[1]
        vm, dma = pltpu.VMEM, pltpu.SemaphoreType.DMA

        def local_steps(current, prec_loc, mean_loc, fac_loc):
            spec = pl.BlockSpec(memory_space=pltpu.VMEM)
            call = pl.pallas_call(
                functools.partial(_kernel, bandwidth, step_size, n_part),
                out_shape=jax.ShapeDtypeStruct((n_part, loc), F32),
                in_specs=[pl.BlockSpec(memory_space=pltpu.HBM)] * 4,
                out_specs=spec,
                scratch_shapes=[
                    vm((1, loc), F32), vm((1, loc), F32), vm((loc, rank), BF16),
                    vm((ROWS, 2 * loc), BF16), vm((ROWS, rank), F32), vm((ROWS // 2, rank), F32),
                    vm((ROWS, TILE), F32), vm((16, TILE), F32),
                    vm((3 * SROWS, TILE), F32),
                    vm((3, COLORS, BLK // 2, TILE), F32), vm((3, COLORS, BLK // 4, TILE), F32),
                    vm((3, COLORS, 3, OWN, TILE), F32), vm((3, COLORS, 4, OWN, TILE), F32),
                    vm((2, SROWS, TILE), BF16), vm((ROWS, ROWS), BF16), vm((ROWS, loc), BF16),
                    vm((2, 3, 16, TILE), F32), vm((2, 3, 3, 16, TILE), F32), vm((16, TILE), F32), vm((16, TILE), F32),
                    dma((7,)), dma, dma((12,)), dma((3,)), dma((3, 2, COLORS)), dma((3, 3, COLORS)), dma((3, COLORS, 3)), dma((3, COLORS)),
                    dma((2, 3)), dma,
                ],
                compiler_params=pltpu.CompilerParams(collective_id=0, has_side_effects=True, vmem_limit_bytes=50000000),
                name="svgd",
            )
            hbm = lambda x: pltpu.with_memory_space_constraint(x, pltpu.HBM)
            return call(hbm(current), hbm(prec_loc.reshape(1, loc)), hbm(mean_loc.reshape(1, loc)), hbm(fac_loc))

        sharded = jax.shard_map(
            local_steps,
            mesh=mesh,
            in_specs=(P("ens", FEAT_AXES), P(LEAD_AXES), P(LEAD_AXES), P(LEAD_AXES, None)),
            out_specs=P("ens", FEAT_AXES),
            check_vma=False,
        )
        return sharded(particles, prec_diag, mean_vec, low_rank)

    return run_steps
```

```python
import functools

import jax
import jax.numpy as jnp
from jax import lax
from jax.experimental import pallas as pl
from jax.experimental.pallas import tpu as pltpu
from jax.sharding import PartitionSpec as P

NUM_STEPS = 3
BAND_SCALE = 4.0
STEP_SCALE = 0.4
FEAT_AXES = ("slab", "feat")
LEAD_AXES = ("ens", "slab", "feat")

ROWS = 2048
TILE = 128
BLK = 512
COLORS = 6
SROWS = COLORS * BLK
UNITS = ((), ((0, 3), (0, 1), (0, 2)), ((1, 2), (1, 3), (2, 3)))
OFFS = (((0, 1), (2, 0), (3, 0)), ((1, 2), (1, 3), (2, 3)))
PM_ROW = 4 * BLK
SENT = 1536 + 768 + 576 + 576 + 576 + 864 + 1536
SENT_SUMS = 288 + 16
OWN = 32
MESH = pl.DeviceIdType.MESH
NT = (((1,), (1,)), ((), ()))
F32, BF16 = jnp.float32, jnp.bfloat16


def div(a, b):
    return lax.div(a, jnp.int32(b))


def rem(a, b):
    return lax.rem(a, jnp.int32(b))


def _kernel(
    bandwidth, step_size, n_part,
    theta_ref, lam_hbm, mu_hbm, fac_hbm, out_ref,
    lam_ref, mu_ref, fac_ref,
    bfull, pml, pmr, nrow, ncol, pack, r0, r1, r2, r3, kg, kfull, adrv, svec, srecv, stot, spart,
    in_sem, pre_send, pre_recv, sent, rs_recv, x_recv, near_recv, far_recv, dd_recv, s_recv, sp_recv,
):
    width = out_ref.shape[1]
    rep_coef = 2.0 / bandwidth
    core = lax.axis_index("slab")
    feat = lax.axis_index("feat")
    coords = (rem(feat, 4), rem(div(feat, 4), 4), div(feat, 16))
    strides = (1, 4, 16)

    def chip(dim, coord):
        return {"feat": feat + (coord - coords[dim]) * strides[dim]}

    turned = [[coords[dim]] + [rem(coords[dim] + j, 4) for j in range(1, 4)] for dim in range(3)]

    def around(dim, j):
        return turned[dim][j]

    ring = [[chip(dim, turned[dim][j]) for j in range(4)] for dim in range(3)]
    low_bit = [rem(c, 2) for c in coords]
    pair_bit = [[rem(div(t + 1, 2), 2) for t in turned[dim]] for dim in range(3)]
    high_bit = [[div(t, 2) for t in turned[dim]] for dim in range(3)]

    mate = {"slab": 1 - core}

    def al(x, m=16):
        return pl.multiple_of(x, m)

    halves = []
    for k in range(COLORS):
        steps = []
        start, length, cur = 0, BLK, coords[k % 3]
        for s in range(2):
            if (k // 3 + s) % 2 == 0:
                other, bit = cur + 1 - 2 * low_bit[k % 3], pair_bit[k % 3][0]
            else:
                other, bit = 3 - cur, high_bit[k % 3][0]
            length = length // 2
            keep, give = start + bit * length, start + (1 - bit) * length
            start = keep
            steps.append((chip(k % 3, other), length, keep, give))
        halves.append(steps)

    def dims(k):
        return k % 3, (k + 1) % 3, (k + 2) % 3

    def base(st, k):
        return st * SROWS + k * BLK

    quarters = [[base(st, k) + halves[k][1][2] for k in range(COLORS)] for st in range(3)]
    owns = [[quarters[st][k] + OWN * coords[dims(k)[1]] for k in range(COLORS)] for st in range(3)]
    pieces = [[OWN * around(dims(k)[1], j) for j in range(4)] for k in range(COLORS)]

    places = []
    for k in range(COLORS):
        one, two = (pair_bit, high_bit) if k < 3 else (high_bit, pair_bit)
        places.append([TILE * (2 * one[k % 3][j] + two[k % 3][j]) for j in range(4)])

    def quarter(st, k):
        return quarters[st][k]

    def own(st, k):
        return owns[st][k]

    barrier = pltpu.get_barrier_semaphore()
    pl.semaphore_signal(barrier, inc=1, device_id=mate, device_id_type=MESH)
    for dim in range(3):
        for j in range(1, 4):
            pl.semaphore_signal(barrier, inc=1, device_id=ring[dim][j], device_id_type=MESH)
    loads = [pltpu.make_async_copy(theta_ref.at[pl.ds(ch * BLK, BLK)], out_ref.at[pl.ds(ch * BLK, BLK)], in_sem.at[ch]) for ch in range(4)]
    loads += [
        pltpu.make_async_copy(src, dst, in_sem.at[4 + n])
        for n, (src, dst) in enumerate(((mu_hbm, mu_ref), (fac_hbm, fac_ref), (lam_hbm, lam_ref)))
    ]
    for cp in loads[4:] + loads[:4]:
        cp.start()

    row_i = lax.broadcasted_iota(jnp.int32, (TILE, TILE), 0)
    col_i = lax.broadcasted_iota(jnp.int32, (TILE, TILE), 1)
    eye, upper, lower = row_i == col_i, row_i < col_i, row_i > col_i
    sub_o = lax.broadcasted_iota(jnp.int32, (OWN, TILE), 0)
    lane_o = lax.broadcasted_iota(jnp.int32, (OWN, TILE), 1)

    def remote(src, dst, ssem, rsem, where):
        return pltpu.make_async_remote_copy(src_ref=src, dst_ref=dst, send_sem=ssem, recv_sem=rsem, device_id=where, device_id_type=MESH)

    def pre_bf16(piece):
        rows = pl.ds(piece * 256, 256)
        return remote(bfull.at[rows, 0:width], bfull.at[rows, width:2 * width], pre_send, pre_recv.at[piece], mate)

    def pre_pm(ch):
        src, dst = pml.at[pl.ds(al(ch * BLK + (1 - core) * 256), 256)], pmr.at[pl.ds(ch * 256, 256)]
        return remote(src, dst, pre_send, pre_recv.at[8 + ch], mate)

    def prepare(start, length, th):
        rows = pl.ds(start, length)
        bfull[rows, 0:width] = th.astype(BF16)
        pml[rows, :] = jnp.dot((th - mu_ref[...]).astype(BF16), fac_ref[...], preferred_element_type=F32)

    def begin(cps):
        for cp in cps:
            cp.start()

    def arrive(ref, sem):
        remote(ref, ref, sent.at[0], sem, mate).wait_recv()

    def x_arrive(st, e, k):
        arrive((r2.at[st, k], r3.at[st, k, 0:3])[e], x_recv.at[st, e, k])

    def rs_copy(st, s, k):
        peer, length, keep, give = halves[k][s]
        src = pack.at[pl.ds(al(base(st, k) + give), length)]
        return remote(src, (r0, r1)[s].at[st, k], sent.at[st], rs_recv.at[st, s, k], peer)

    def gathered(st, k, row, rows):
        if st == 0:
            return kg.at[core, pl.ds(al(base(0, k) + row), rows)]
        sup, m = UNITS[st][k // 2]
        return kfull.at[pl.ds(al(sup * BLK + row), rows), pl.ds(al((4 * m + 2 * core + k % 2) * TILE, TILE), TILE)]

    def x_copies(st, e, k):
        d1, d2, d3 = dims(k)
        dim = (d2, d3)[e]
        cps = []
        for j in range(1, 4):
            if e == 0:
                src = pack.at[pl.ds(al(quarter(st, k) + pieces[k][j]), OWN)]
                dst = r2.at[st, k, j - 1]
            else:
                src = dst = r3.at[st, k, coords[dim]]
            cps.append(remote(src, dst, sent.at[st], x_recv.at[st, e, k], ring[dim][j]))
        return cps

    def gather_copies(st, k, j):
        d1, d2, d3 = dims(k)
        ref = gathered(st, k, halves[k][1][2] + pieces[k][(4 - j) % 4], OWN)
        cps = [remote(ref, ref, sent.at[st], far_recv.at[st, k, i - 1], ring[d1][i]) for i in range(1, 4)]
        if j == 0:
            cps = [remote(ref, ref, sent.at[st], near_recv.at[st, k, i - 1], ring[d2][i]) for i in range(1, 4)] + cps
        return cps

    def dd_copy(st, k, j):
        ref = gathered(st, k, halves[k][1][2] if j == 0 else places[k][4 - j], TILE)
        return remote(ref, ref, sent.at[st], dd_recv.at[st, k], mate)

    def s_copies(ph, d):
        dim = ((d + 1) % 3, d)[ph]
        return [
            remote(svec.at[ph, d], srecv.at[ph, d, j - 1], sent.at[2], s_recv.at[ph, d], ring[dim][j])
            for j in range(1, 4)
        ]

    def sp_copy():
        return remote(stot, spart, sent.at[2], sp_recv, mate)

    def products(m):
        mine = bfull[pl.ds(al(m * BLK + 256 * core), 256), :]
        part = BLK if m == 3 else (m + 1) * 256
        return [lax.dot_general(bfull[pl.ds(at, part), :], mine, NT, preferred_element_type=F32) for at in range(0, (m + 1) * BLK, part)]

    def norms(m):
        for i in range(4):
            rows = pl.ds((4 * m + i) * TILE, TILE)
            wide = bfull[rows, :].astype(F32)
            n = jnp.broadcast_to(jnp.sum(wide * wide, axis=1, keepdims=True), (TILE, TILE))
            nrow[rows, :] = n
            ncol[4 * m + i:4 * m + i + 1, :] = jnp.sum(jnp.where(eye, n, 0.0), axis=0, keepdims=True)

    def tiles(m, g):
        def block(blk, b):
            n, r = divmod(blk * TILE, BLK if m == 3 else (m + 1) * 256)
            return g[n][r:r + TILE, b * TILE:(b + 1) * TILE]

        def tile(i, b):
            return block(4 * m + i, b)

        def dist(i, j):
            return nrow[pl.ds((4 * m + i) * TILE, TILE), :] + ncol[4 * m + j:4 * m + j + 1, :] - 2.0 * tile(i, j % 2)

        for t in range(3):
            pack[pl.ds(base(0, m) + t * TILE, TILE), :] = jnp.where(core == 0, dist(*OFFS[0][t]), dist(*OFFS[1][t]))
        one = jnp.where(core == 0, dist(0, 0), dist(2, 2))
        two = jnp.where(core == 0, dist(1, 1), dist(3, 3))
        pack[pl.ds(base(0, m) + 3 * TILE, TILE), :] = jnp.where(upper, one, two)
        begin([rs_copy(0, 0, m)])
        for st in (1, 2):
            for u, (sup, col) in enumerate(UNITS[st]):
                if col != m:
                    continue
                for b in range(2):
                    nc = ncol[pl.ds(4 * m + 2 * core + b, 1), :]
                    for a in range(4):
                        nr = nrow[pl.ds((4 * sup + a) * TILE, TILE), :]
                        pack[pl.ds(base(st, 2 * u + b) + a * TILE, TILE), :] = nr + nc - 2.0 * block(4 * sup + a, b)
                begin([rs_copy(st, 0, 2 * u), rs_copy(st, 0, 2 * u + 1)])

    def pm_tiles(half):
        for ch in (2 * half, 2 * half + 1):
            pre_pm(ch).wait_recv()
            mine = pl.ds(al(ch * BLK + core * 256), 256)
            pack[pl.ds(PM_ROW + ch * 256, 256), :] = pml[mine, :] + pmr[pl.ds(ch * 256, 256), :]
        begin([rs_copy(0, 0, 4 + half)])

    def open_step():
        begin([pre_pm(3), pre_bf16(7)])
        pm_tiles(0)
        for piece in range(4):
            pre_bf16(piece).wait_recv()
        gs = []
        for m in range(2):
            gs.append(products(m))
            norms(m)
        for m in range(2):
            tiles(m, gs[m])
        pm_tiles(1)
        for m in range(2, 4):
            for piece in range(2 * m, 2 * m + 2):
                pre_bf16(piece).wait_recv()
            g = products(m)
            norms(m)
            tiles(m, g)

    for cp in loads[4:]:
        cp.wait()
    for ch in range(4):
        loads[ch].wait()
        prepare(ch * BLK, BLK, out_ref[pl.ds(ch * BLK, BLK), :])
        if ch == 0:
            pl.semaphore_wait(barrier, 10)
        if ch < 3:
            begin([pre_pm(ch)])
        begin([pre_bf16(piece) for piece in (2 * ch, 2 * ch + 1) if piece < 7])
    open_step()

    def one_step(step_index, carry):
        def row_sums(st, k, kern):
            place = own(0, k) - base(0, k)
            slot, r = div(place, TILE), rem(place, TILE)

            def by_rows(vals):
                rs = jnp.sum(vals, axis=1, keepdims=True)
                return jnp.sum(jnp.where(lane_o == sub_o + r, rs, 0.0), axis=0, keepdims=True)

            def by_cols(vals):
                return jnp.sum(vals, axis=0, keepdims=True)

            if st > 0:
                sup, m = UNITS[st][k // 2]
                return [(4 * sup + slot, by_rows(kern)), (4 * m + 2 * core + k % 2, by_cols(kern))]
            both = div(slot, 3)
            up_one = div(slot + 1, 2)
            i0 = (1 - both) * ((1 - core) * (slot + up_one) + core * (1 + div(slot, 2))) + both * 2 * core
            j0 = (1 - both) * ((1 - core) * (1 - up_one) + core * (2 + up_one)) + both * 2 * core
            up = jnp.where(lane_o + 1000 * (1 - both) > sub_o + r, kern, 0.0)
            lo = jnp.where(lane_o + 1000 * (1 - both) < sub_o + r, kern, 0.0)
            nxt = 4 * k + 2 * core + 1
            return [(4 * k + i0, by_rows(up)), (4 * k + j0, by_cols(up)), (nxt, by_rows(lo)), (nxt, by_cols(lo))]

        def advance(st, s):
            parts = [[], [], []]
            if st == 2 and s == 4:
                for d in range(3):
                    arrive(srecv.at[0, d], s_recv.at[0, d])
                    svec[1, d] = svec[0, d] + srecv[0, d, 0] + srecv[0, d, 1] + srecv[0, d, 2]
                    begin(s_copies(1, d))
            if st == 2 and s == 5:
                tot = jnp.zeros((16, TILE), F32)
                for d in range(3):
                    arrive(srecv.at[1, d], s_recv.at[1, d])
                    tot = tot + ((svec[1, d] + srecv[1, d, 0]) + (srecv[1, d, 1] + srecv[1, d, 2]))
                stot[...] = tot
                begin([sp_copy()])
            for k in range(COLORS):
                mine = pl.ds(al(own(st, k)), OWN)
                if s < 2:
                    peer, length, keep, give = halves[k][s]
                    rs_copy(st, s, k).wait_recv()
                    rng = pl.ds(al(base(st, k) + keep), length)
                    pack[rng, :] += (r0, r1)[s][st, k]
                    begin([rs_copy(st, 1, k)] if s == 0 else x_copies(st, 0, k))
                elif s == 2:
                    x_arrive(st, 0, k)
                    r3[st, k, coords[dims(k)[2]]] = pack[mine, :] + r2[st, k, 0] + r2[st, k, 1] + r2[st, k, 2]
                    begin(x_copies(st, 1, k))
                elif s == 3:
                    x_arrive(st, 1, k)
                    full = (r3[st, k, 0] + r3[st, k, 1]) + (r3[st, k, 2] + r3[st, k, 3])
                    if st == 0 and k >= 4:
                        kern = full
                    else:
                        kern = jnp.exp(-jnp.maximum(full, 0.0) / bandwidth)
                        parts[k % 3] += row_sums(st, k, kern)
                    gathered(st, k, own(0, k) - base(0, k), OWN)[...] = kern.astype(BF16)
                    begin(gather_copies(st, k, 0))
                elif s == 4:
                    for j in range(1, 4):
                        arrive(kg.at[core, 0:OWN], near_recv.at[st, k, j - 1])
                        begin(gather_copies(st, k, j))
                    begin([dd_copy(st, k, 0)])
                else:
                    for j in range(1, 4):
                        arrive(kg.at[core, 0:TILE], far_recv.at[st, k, j - 1])
                        begin([dd_copy(st, k, j)])
            if s == 3:
                for d in range(3):
                    if st == 0:
                        svec[0, d] = jnp.zeros((16, TILE), F32)
                    for block, line in parts[d]:
                        svec[0, d, pl.ds(block, 1), :] += line
                    if st == 2:
                        begin(s_copies(0, d))
        def unpack_wait(st):
            for k in range(COLORS):
                arrive(kg.at[core, 0:BLK], dd_recv.at[st, k])

        def unpack(st):
            for c in range(2):
                if st > 0:
                    for k in range(COLORS):
                        sup, m = UNITS[st][k // 2]
                        jrng = pl.ds((4 * m + 2 * c + k % 2) * TILE, TILE)
                        for a in range(4):
                            srng = pl.ds((4 * sup + a) * TILE, TILE)
                            kfull[jrng, srng] = kfull[srng, jrng].T
                    continue
                for sup in range(4):
                    for t, (i, j) in enumerate(OFFS[c]):
                        src = kg[c, pl.ds(base(0, sup) + t * TILE, TILE), :]
                        ri, rj = pl.ds((4 * sup + i) * TILE, TILE), pl.ds((4 * sup + j) * TILE, TILE)
                        kfull[ri, rj] = src
                        kfull[rj, ri] = src.T
                    src = kg[c, pl.ds(base(0, sup) + 3 * TILE, TILE), :]
                    srt = src.T
                    one = jnp.ones((TILE, TILE), BF16)
                    ra, rb = pl.ds((4 * sup + 2 * c) * TILE, TILE), pl.ds((4 * sup + 2 * c + 1) * TILE, TILE)
                    kfull[ra, ra] = jnp.where(upper, src, jnp.where(lower, srt, one))
                    kfull[rb, rb] = jnp.where(lower, src, jnp.where(upper, srt, one))

        def drive():
            for q in range(8):
                rows = pl.ds(q * 256, 256)
                pm = kg[q % 2, pl.ds(PM_ROW + (q // 2) * 256, 256), :]
                low = lax.dot_general(pm, fac_ref[...], NT, preferred_element_type=F32)
                th = out_ref[rows, :]
                grad = -((th - mu_ref[...]) * lam_ref[...] + low)
                adrv[rows, :] = (grad - rep_coef * th).astype(BF16)

        def product(start):
            return jnp.dot(kfull[pl.ds(start, 256), :], adrv[...], preferred_element_type=F32)

        def finish(start, acc, tot):
            rows = pl.ds(start, 256)
            sums = []
            for blk in (start // TILE, start // TILE + 1):
                line = jnp.where(eye, jnp.broadcast_to(tot[blk:blk + 1, :], (TILE, TILE)), 0.0)
                sums.append(rep_coef * jnp.sum(line, axis=1, keepdims=True))
            sums = jnp.broadcast_to(jnp.concatenate(sums, axis=0), (256, TILE))
            new = []
            for t in range(width // TILE):
                cols = slice(t * TILE, (t + 1) * TILE)
                th = out_ref[rows, cols]
                phi = (acc[:, cols] + sums * th) / n_part
                new.append(th + step_size * phi)
            th = jnp.concatenate(new, axis=1)
            out_ref[rows, :] = th
            prepare(start, 256, th)
            piece = start // 256
            if piece == 6:
                begin([pre_bf16(6)])
            elif piece in (1, 3, 5):
                begin([pre_pm(piece // 2), pre_bf16(piece - 1), pre_bf16(piece)])

        for s in range(5):
            for st in range(3):
                advance(st, s)
        advance(0, 5)
        advance(1, 5)
        unpack_wait(0)
        unpack(0)
        drive()
        advance(2, 5)
        remote(pack.at[0:5120], pack.at[0:5120], pre_send, sp_recv, mate).wait_send()
        def update(starts, st):
            tot = stot[...] + spart[...] + 1.0
            ahead = product(starts[0])
            unpack(st)
            for n, start in enumerate(starts):
                acc = ahead
                if n + 1 < len(starts):
                    ahead = product(starts[n + 1])
                finish(start, acc, tot)

        unpack_wait(1)
        arrive(stot, sp_recv)
        update(range(0, BLK, 256), 1)
        unpack_wait(2)
        update(range(BLK, ROWS, 256), 2)
        for st in range(3):
            total = pack.at[0:SENT + (SENT_SUMS if st == 2 else 0)]
            remote(total, total, sent.at[st], sp_recv, mate).wait_send()
        pl.when(step_index < NUM_STEPS - 1)(open_step)
        return carry

    lax.fori_loop(0, NUM_STEPS, one_step, 0)
    for ch in range(3):
        pre_pm(ch).wait_recv()
    for piece in range(7):
        pre_bf16(piece).wait_recv()
    total = pack.at[0:7 * 512 + 3 * 256]
    remote(total, total, pre_send, sp_recv, mate).wait_send()


def solution(mesh):
    def run_steps(particles, prec_diag, mean_vec, low_rank):
        total_rows, width = particles.shape
        n_part = total_rows // mesh.shape["ens"]
        bandwidth = BAND_SCALE * width
        step_size = STEP_SCALE * width
        loc = width // (mesh.shape["slab"] * mesh.shape["feat"])
        rank = low_rank.shape[1]
        vm, dma = pltpu.VMEM, pltpu.SemaphoreType.DMA

        def local_steps(current, prec_loc, mean_loc, fac_loc):
            spec = pl.BlockSpec(memory_space=pltpu.VMEM)
            call = pl.pallas_call(
                functools.partial(_kernel, bandwidth, step_size, n_part),
                out_shape=jax.ShapeDtypeStruct((n_part, loc), F32),
                in_specs=[pl.BlockSpec(memory_space=pltpu.HBM)] * 4,
                out_specs=spec,
                scratch_shapes=[
                    vm((1, loc), F32), vm((1, loc), F32), vm((loc, rank), BF16),
                    vm((ROWS, 2 * loc), BF16), vm((ROWS, rank), F32), vm((ROWS // 2, rank), F32),
                    vm((ROWS, TILE), F32), vm((16, TILE), F32),
                    vm((3 * SROWS, TILE), F32),
                    vm((3, COLORS, BLK // 2, TILE), F32), vm((3, COLORS, BLK // 4, TILE), F32),
                    vm((3, COLORS, 3, OWN, TILE), F32), vm((3, COLORS, 4, OWN, TILE), F32),
                    vm((2, SROWS, TILE), BF16), vm((ROWS, ROWS), BF16), vm((ROWS, loc), BF16),
                    vm((2, 3, 16, TILE), F32), vm((2, 3, 3, 16, TILE), F32), vm((16, TILE), F32), vm((16, TILE), F32),
                    dma((7,)), dma, dma((12,)), dma((3,)), dma((3, 2, COLORS)), dma((3, 2, COLORS)), dma((3, COLORS, 3)), dma((3, COLORS, 3)), dma((3, COLORS)),
                    dma((2, 3)), dma,
                ],
                compiler_params=pltpu.CompilerParams(collective_id=0, has_side_effects=True, vmem_limit_bytes=50000000),
                name="svgd",
            )
            hbm = lambda x: pltpu.with_memory_space_constraint(x, pltpu.HBM)
            return call(hbm(current), hbm(prec_loc.reshape(1, loc)), hbm(mean_loc.reshape(1, loc)), hbm(fac_loc))

        sharded = jax.shard_map(
            local_steps,
            mesh=mesh,
            in_specs=(P("ens", FEAT_AXES), P(LEAD_AXES), P(LEAD_AXES), P(LEAD_AXES, None)),
            out_specs=P("ens", FEAT_AXES),
            check_vma=False,
        )
        return sharded(particles, prec_diag, mean_vec, low_rank)

    return run_steps
```

```python
import functools

import jax
import jax.numpy as jnp
from jax import lax
from jax.experimental import pallas as pl
from jax.experimental.pallas import tpu as pltpu
from jax.sharding import PartitionSpec as P

NUM_STEPS = 3
BAND_SCALE = 4.0
STEP_SCALE = 0.4
FEAT_AXES = ("slab", "feat")
LEAD_AXES = ("ens", "slab", "feat")

ROWS = 2048
TILE = 128
HALF = 256
BLK = 2 * HALF
COLORS = 6
SROWS = COLORS * BLK
UNITS = ((), ((0, 3), (0, 1), (0, 2)), ((1, 2), (1, 3), (2, 3)))
OFFS = (((0, 1), (2, 0), (3, 0)), ((1, 2), (1, 3), (2, 3)))
PM_ROW = 4 * BLK
SENT = 6432
SENT_SUMS = 304
OWN = 32
PEERS = range(1, 4)
MESH = pl.DeviceIdType.MESH
NT = (((1,), (1,)), ((), ()))
F32, BF16 = jnp.float32, jnp.bfloat16


def div(a, b):
    return lax.div(a, jnp.int32(b))


def rem(a, b):
    return lax.rem(a, jnp.int32(b))


def _kernel(
    bandwidth, step_size, n_part,
    theta_ref, lam_hbm, mu_hbm, fac_hbm, out_ref,
    lam_ref, mu_ref, fac_ref,
    bfull, pml, pmr, nrow, ncol, pulled, scaled, pack, r0, r1, r2, r3, kg, kfull, adrv, svec, srecv, stot, spart,
    in_sem, pre_send, pre_recv, sent, rs_recv, x_recv, near_recv, far_recv, dd_recv, s_recv, sp_recv,
):
    width = out_ref.shape[1]
    rep_coef = 2.0 / bandwidth
    core = lax.axis_index("slab")
    feat = lax.axis_index("feat")
    coords = (rem(feat, 4), rem(div(feat, 4), 4), div(feat, 16))
    strides = (1, 4, 16)

    def chip(dim, coord):
        return {"feat": feat + (coord - coords[dim]) * strides[dim]}

    turned = [[coords[dim]] + [rem(coords[dim] + j, 4) for j in PEERS] for dim in range(3)]

    def around(dim, j):
        return turned[dim][j]

    ring = [[chip(dim, turned[dim][j]) for j in range(4)] for dim in range(3)]
    low_bit = [rem(c, 2) for c in coords]
    pair_bit = [[rem(div(t + 1, 2), 2) for t in turned[dim]] for dim in range(3)]
    high_bit = [[div(t, 2) for t in turned[dim]] for dim in range(3)]

    mate = {"slab": 1 - core}

    def al(x, m=16):
        return pl.multiple_of(x, m)

    halves = []
    for k in range(COLORS):
        steps = []
        start, length, cur = 0, BLK, coords[k % 3]
        for s in range(2):
            if (k // 3 + s) % 2 == 0:
                other, bit = cur + 1 - 2 * low_bit[k % 3], pair_bit[k % 3][0]
            else:
                other, bit = 3 - cur, high_bit[k % 3][0]
            length = length // 2
            keep, give = start + bit * length, start + (1 - bit) * length
            start = keep
            steps.append((chip(k % 3, other), length, keep, give))
        halves.append(steps)

    def dims(k):
        return k % 3, (k + 1) % 3, (k + 2) % 3

    def base(st, k):
        return st * SROWS + k * BLK

    quarters = [[base(st, k) + halves[k][1][2] for k in range(COLORS)] for st in range(3)]
    owns = [[quarters[st][k] + OWN * coords[dims(k)[1]] for k in range(COLORS)] for st in range(3)]
    pieces = [[OWN * around(dims(k)[1], j) for j in range(4)] for k in range(COLORS)]

    places = []
    for k in range(COLORS):
        one, two = (pair_bit, high_bit) if k < 3 else (high_bit, pair_bit)
        places.append([TILE * (2 * one[k % 3][j] + two[k % 3][j]) for j in range(4)])

    def quarter(st, k):
        return quarters[st][k]

    def own(st, k):
        return owns[st][k]

    barrier = pltpu.get_barrier_semaphore()
    pl.semaphore_signal(barrier, inc=1, device_id=mate, device_id_type=MESH)
    for dim in range(3):
        for j in PEERS:
            pl.semaphore_signal(barrier, inc=1, device_id=ring[dim][j], device_id_type=MESH)
    loads = [pltpu.make_async_copy(theta_ref.at[pl.ds(ch * BLK, BLK)], out_ref.at[pl.ds(ch * BLK, BLK)], in_sem.at[ch]) for ch in range(4)]
    loads += [
        pltpu.make_async_copy(src, dst, in_sem.at[4 + n])
        for n, (src, dst) in enumerate(((mu_hbm, mu_ref), (fac_hbm, fac_ref), (lam_hbm, lam_ref)))
    ]
    for cp in loads[4:] + loads[:4]:
        cp.start()

    row_i = lax.broadcasted_iota(jnp.int32, (TILE, TILE), 0)
    col_i = lax.broadcasted_iota(jnp.int32, (TILE, TILE), 1)
    eye, upper, lower = row_i == col_i, row_i < col_i, row_i > col_i
    sub_o = lax.broadcasted_iota(jnp.int32, (OWN, TILE), 0)
    lane_o = lax.broadcasted_iota(jnp.int32, (OWN, TILE), 1)

    def remote(src, dst, ssem, rsem, where):
        return pltpu.make_async_remote_copy(src_ref=src, dst_ref=dst, send_sem=ssem, recv_sem=rsem, device_id=where, device_id_type=MESH)

    def pre_bf16(piece):
        rows = pl.ds(piece * HALF, HALF)
        return remote(bfull.at[rows, 0:width], bfull.at[rows, width:2 * width], pre_send, pre_recv.at[piece], mate)

    def pre_pm(ch):
        src, dst = pml.at[pl.ds(al(ch * BLK + (1 - core) * HALF), HALF)], pmr.at[pl.ds(ch * HALF, HALF)]
        return remote(src, dst, pre_send, pre_recv.at[8 + ch], mate)

    def prepare(start, th):
        bfull[pl.ds(start, HALF), 0:width] = th.astype(BF16)
        return (th - mu_ref[...]).astype(BF16)

    def partial_pm(start, centered):
        for n, rows in enumerate(centered):
            pml[pl.ds(start + HALF * n, HALF), :] = jnp.dot(rows, fac_ref[...], preferred_element_type=F32)

    def begin(cps):
        for cp in cps:
            cp.start()

    def arrive(ref, sem):
        remote(ref, ref, sent.at[0], sem, mate).wait_recv()

    def x_arrive(st, e, k):
        arrive((r2.at[st, k], r3.at[st, k, 0:3])[e], x_recv.at[st, e, k])

    def rs_copy(st, s, k):
        peer, length, keep, give = halves[k][s]
        src = pack.at[pl.ds(al(base(st, k) + give), length)]
        return remote(src, (r0, r1)[s].at[st, k], sent.at[st], rs_recv.at[st, s, k], peer)

    def gathered(st, k, row, rows):
        if st == 0:
            return kg.at[core, pl.ds(al(base(0, k) + row), rows)]
        sup, m = UNITS[st][k // 2]
        return kfull.at[pl.ds(al(sup * BLK + row), rows), pl.ds(al((4 * m + 2 * core + k % 2) * TILE, TILE), TILE)]

    def x_copies(st, e, k):
        d1, d2, d3 = dims(k)
        dim = (d2, d3)[e]
        cps = []
        for j in PEERS:
            if e == 0:
                src = pack.at[pl.ds(al(quarter(st, k) + pieces[k][j]), OWN)]
                dst = r2.at[st, k, j - 1]
            else:
                src = dst = r3.at[st, k, coords[dim]]
            cps.append(remote(src, dst, sent.at[st], x_recv.at[st, e, k], ring[dim][j]))
        return cps

    def gather_copies(st, k, j):
        d1, d2, d3 = dims(k)
        ref = gathered(st, k, halves[k][1][2] + pieces[k][(4 - j) % 4], OWN)
        cps = [remote(ref, ref, sent.at[st], far_recv.at[st, k, i - 1], ring[d1][i]) for i in PEERS]
        if j == 0:
            cps = [remote(ref, ref, sent.at[st], near_recv.at[st, k, i - 1], ring[d2][i]) for i in PEERS] + cps
        return cps

    def dd_copy(st, k, j):
        ref = gathered(st, k, halves[k][1][2] if j == 0 else places[k][4 - j], TILE)
        return remote(ref, ref, sent.at[st], dd_recv.at[st, k], mate)

    def s_copies(ph, d):
        dim = ((d + 1) % 3, d)[ph]
        return [
            remote(svec.at[ph, d], srecv.at[ph, d, j - 1], sent.at[2], s_recv.at[ph, d], ring[dim][j])
            for j in PEERS
        ]

    def sp_copy():
        return remote(stot, spart, sent.at[2], sp_recv, mate)

    def products(m):
        mine = bfull[pl.ds(al(m * BLK + HALF * core), HALF), :]
        part = BLK if m == 3 else (m + 1) * HALF
        return [lax.dot_general(bfull[pl.ds(at, part), :], mine, NT, preferred_element_type=F32) for at in range(0, (m + 1) * BLK, part)]

    def norms(m):
        for i in range(4):
            rows = pl.ds((4 * m + i) * TILE, TILE)
            wide = bfull[rows, :].astype(F32)
            n = jnp.broadcast_to(jnp.sum(wide * wide, axis=1, keepdims=True), (TILE, TILE))
            nrow[rows, :] = n
            ncol[4 * m + i:4 * m + i + 1, :] = jnp.sum(jnp.where(eye, n, 0.0), axis=0, keepdims=True)

    def tiles(m, g):
        def block(blk, b):
            n, r = divmod(blk * TILE, BLK if m == 3 else (m + 1) * HALF)
            return g[n][r:r + TILE, b * TILE:(b + 1) * TILE]

        def tile(i, b):
            return block(4 * m + i, b)

        def dist(i, j):
            return nrow[pl.ds((4 * m + i) * TILE, TILE), :] + ncol[4 * m + j:4 * m + j + 1, :] - 2.0 * tile(i, j % 2)

        for t in range(3):
            pack[pl.ds(base(0, m) + t * TILE, TILE), :] = jnp.where(core == 0, dist(*OFFS[0][t]), dist(*OFFS[1][t]))
        one = jnp.where(core == 0, dist(0, 0), dist(2, 2))
        two = jnp.where(core == 0, dist(1, 1), dist(3, 3))
        pack[pl.ds(base(0, m) + 3 * TILE, TILE), :] = jnp.where(upper, one, two)
        begin([rs_copy(0, 0, m)])
        for st in (1, 2):
            for u, (sup, col) in enumerate(UNITS[st]):
                if col != m:
                    continue
                for b in range(2):
                    nc = ncol[pl.ds(4 * m + 2 * core + b, 1), :]
                    for a in range(4):
                        nr = nrow[pl.ds((4 * sup + a) * TILE, TILE), :]
                        pack[pl.ds(base(st, 2 * u + b) + a * TILE, TILE), :] = nr + nc - 2.0 * block(4 * sup + a, b)
                begin([rs_copy(st, 0, 2 * u), rs_copy(st, 0, 2 * u + 1)])

    def pm_tiles(half):
        for ch in (2 * half, 2 * half + 1):
            pre_pm(ch).wait_recv()
            mine = pl.ds(al(ch * BLK + core * HALF), HALF)
            pack[pl.ds(PM_ROW + ch * HALF, HALF), :] = pml[mine, :] + pmr[pl.ds(ch * HALF, HALF), :]
        begin([rs_copy(0, 0, 4 + half)])

    def open_step():
        begin([pre_pm(3), pre_bf16(7)])
        pm_tiles(0)
        for piece in range(4):
            pre_bf16(piece).wait_recv()
        gs = []
        for m in range(2):
            gs.append(products(m))
            norms(m)
        for m in range(2):
            tiles(m, gs[m])
        pm_tiles(1)
        for m in range(2, 4):
            for piece in range(2 * m, 2 * m + 2):
                pre_bf16(piece).wait_recv()
            g = products(m)
            norms(m)
            tiles(m, g)

    for cp in loads[4:]:
        cp.wait()
    for ch in range(4):
        loads[ch].wait()
        starts = (ch * BLK, ch * BLK + HALF)
        partial_pm(ch * BLK, [prepare(start, out_ref[pl.ds(start, HALF), :]) for start in starts])
        if ch == 0:
            pl.semaphore_wait(barrier, 10)
        if ch < 3:
            begin([pre_pm(ch)])
        begin([pre_bf16(piece) for piece in (2 * ch, 2 * ch + 1) if piece < 7])
    open_step()

    def one_step(step_index, carry):
        def row_sums(st, k, kern):
            place = own(0, k) - base(0, k)
            slot, r = div(place, TILE), rem(place, TILE)

            def by_rows(vals):
                rs = jnp.sum(vals, axis=1, keepdims=True)
                return jnp.sum(jnp.where(lane_o == sub_o + r, rs, 0.0), axis=0, keepdims=True)

            def by_cols(vals):
                return jnp.sum(vals, axis=0, keepdims=True)

            if st > 0:
                sup, m = UNITS[st][k // 2]
                return [(4 * sup + slot, by_rows(kern)), (4 * m + 2 * core + k % 2, by_cols(kern))]
            both = div(slot, 3)
            up_one = div(slot + 1, 2)
            i0 = (1 - both) * ((1 - core) * (slot + up_one) + core * (1 + div(slot, 2))) + both * 2 * core
            j0 = (1 - both) * ((1 - core) * (1 - up_one) + core * (2 + up_one)) + both * 2 * core
            up = jnp.where(lane_o + 1000 * (1 - both) > sub_o + r, kern, 0.0)
            lo = jnp.where(lane_o + 1000 * (1 - both) < sub_o + r, kern, 0.0)
            nxt = 4 * k + 2 * core + 1
            return [(4 * k + i0, by_rows(up)), (4 * k + j0, by_cols(up)), (nxt, by_rows(lo)), (nxt, by_cols(lo))]

        def advance(st, s):
            parts = [[], [], []]
            if st == 2 and s == 4:
                for d in range(3):
                    arrive(srecv.at[0, d], s_recv.at[0, d])
                    svec[1, d] = svec[0, d] + srecv[0, d, 0] + srecv[0, d, 1] + srecv[0, d, 2]
                    begin(s_copies(1, d))
            if st == 2 and s == 5:
                tot = jnp.zeros((16, TILE), F32)
                for d in range(3):
                    arrive(srecv.at[1, d], s_recv.at[1, d])
                    tot = tot + ((svec[1, d] + srecv[1, d, 0]) + (srecv[1, d, 1] + srecv[1, d, 2]))
                stot[...] = tot
                begin([sp_copy()])
            for k in range(COLORS):
                mine = pl.ds(al(own(st, k)), OWN)
                if s < 2:
                    peer, length, keep, give = halves[k][s]
                    rs_copy(st, s, k).wait_recv()
                    rng = pl.ds(al(base(st, k) + keep), length)
                    pack[rng, :] += (r0, r1)[s][st, k]
                    begin([rs_copy(st, 1, k)] if s == 0 else x_copies(st, 0, k))
                elif s == 2:
                    x_arrive(st, 0, k)
                    r3[st, k, coords[dims(k)[2]]] = pack[mine, :] + r2[st, k, 0] + r2[st, k, 1] + r2[st, k, 2]
                    begin(x_copies(st, 1, k))
                elif s == 3:
                    x_arrive(st, 1, k)
                    full = (r3[st, k, 0] + r3[st, k, 1]) + (r3[st, k, 2] + r3[st, k, 3])
                    if st == 0 and k >= 4:
                        kern = full
                    else:
                        kern = jnp.exp(-jnp.maximum(full, 0.0) / bandwidth)
                        parts[k % 3] += row_sums(st, k, kern)
                    gathered(st, k, own(0, k) - base(0, k), OWN)[...] = kern.astype(BF16)
                    begin(gather_copies(st, k, 0))
                elif s == 4:
                    for j in PEERS:
                        arrive(kg.at[core, 0:OWN], near_recv.at[st, k, j - 1])
                        begin(gather_copies(st, k, j))
                    begin([dd_copy(st, k, 0)])
                else:
                    for j in PEERS:
                        arrive(kg.at[core, 0:TILE], far_recv.at[st, k, j - 1])
                        begin([dd_copy(st, k, j)])
            if s == 3:
                for d in range(3):
                    if st == 0:
                        svec[0, d] = jnp.zeros((16, TILE), F32)
                    for block, line in parts[d]:
                        svec[0, d, pl.ds(block, 1), :] += line
                    if st == 2:
                        begin(s_copies(0, d))
        def unpack_wait(st):
            for k in range(COLORS):
                arrive(kg.at[core, 0:BLK], dd_recv.at[st, k])

        def unpack(st):
            for c in range(2):
                if st > 0:
                    for k in range(COLORS):
                        sup, m = UNITS[st][k // 2]
                        jrng = pl.ds((4 * m + 2 * c + k % 2) * TILE, TILE)
                        for a in range(4):
                            srng = pl.ds((4 * sup + a) * TILE, TILE)
                            kfull[jrng, srng] = kfull[srng, jrng].T
                    continue
                for sup in range(4):
                    for t, (i, j) in enumerate(OFFS[c]):
                        src = kg[c, pl.ds(base(0, sup) + t * TILE, TILE), :]
                        ri, rj = pl.ds((4 * sup + i) * TILE, TILE), pl.ds((4 * sup + j) * TILE, TILE)
                        kfull[ri, rj] = src
                        kfull[rj, ri] = src.T
                    src = kg[c, pl.ds(base(0, sup) + 3 * TILE, TILE), :]
                    srt = src.T
                    one = jnp.ones((TILE, TILE), BF16)
                    ra, rb = pl.ds((4 * sup + 2 * c) * TILE, TILE), pl.ds((4 * sup + 2 * c + 1) * TILE, TILE)
                    kfull[ra, ra] = jnp.where(upper, src, jnp.where(lower, srt, one))
                    kfull[rb, rb] = jnp.where(lower, src, jnp.where(upper, srt, one))

        def drive_parts():
            for q in range(8):
                rows = pl.ds(q * HALF, HALF)
                th = out_ref[rows, :]
                pulled[rows, :] = (th - mu_ref[...]) * lam_ref[...]
                scaled[rows, :] = rep_coef * th

        def drive():
            for q in range(8):
                rows = pl.ds(q * HALF, HALF)
                pm = kg[q % 2, pl.ds(PM_ROW + (q // 2) * HALF, HALF), :]
                low = lax.dot_general(pm, fac_ref[...], NT, preferred_element_type=F32)
                adrv[rows, :] = ((pulled[rows, :] + low) + scaled[rows, :]).astype(BF16)

        def product(start):
            return jnp.dot(kfull[pl.ds(start, HALF), :], adrv[...], preferred_element_type=F32)

        def finish(start, acc, tot, held):
            rows = pl.ds(start, HALF)
            sums = []
            for blk in (start // TILE, start // TILE + 1):
                line = jnp.where(eye, jnp.broadcast_to(tot[blk:blk + 1, :], (TILE, TILE)), 0.0)
                sums.append(rep_coef * jnp.sum(line, axis=1, keepdims=True))
            sums = jnp.broadcast_to(jnp.concatenate(sums, axis=0), (HALF, TILE))
            new = []
            for t in range(width // TILE):
                cols = slice(t * TILE, (t + 1) * TILE)
                th = out_ref[rows, cols]
                phi = (sums * th - acc[:, cols]) / n_part
                new.append(th + step_size * phi)
            th = jnp.concatenate(new, axis=1)
            out_ref[rows, :] = th
            held.append(prepare(start, th))
            if start % BLK:
                partial_pm(start - HALF, held[-2:])

        def share(start):
            if start % BLK and start + HALF < ROWS:
                begin([pre_pm(start // BLK), pre_bf16(start // HALF - 1), pre_bf16(start // HALF)])
            elif start + BLK == ROWS:
                begin([pre_bf16(start // HALF)])

        drive_parts()
        for s in range(5):
            for st in range(3):
                advance(st, s)
        advance(0, 5)
        advance(1, 5)
        unpack_wait(0)
        unpack(0)
        drive()
        advance(2, 5)
        remote(pack.at[0:5120], pack.at[0:5120], pre_send, sp_recv, mate).wait_send()
        def update(starts, st):
            tot = stot[...] + spart[...] + 1.0
            ahead = product(starts[0])
            unpack(st)
            held = []
            for n, start in enumerate(starts):
                acc = ahead
                if n + 1 < len(starts):
                    ahead = product(starts[n + 1])
                if n:
                    share(starts[n - 1])
                finish(start, acc, tot, held)
            share(starts[-1])

        unpack_wait(1)
        arrive(stot, sp_recv)
        update(range(0, BLK, HALF), 1)
        unpack_wait(2)
        update(range(BLK, ROWS, HALF), 2)
        for st in range(3):
            total = pack.at[0:SENT + (SENT_SUMS if st == 2 else 0)]
            remote(total, total, sent.at[st], sp_recv, mate).wait_send()
        pl.when(step_index < NUM_STEPS - 1)(open_step)
        return carry

    lax.fori_loop(0, NUM_STEPS, one_step, 0)
    for ch in range(3):
        pre_pm(ch).wait_recv()
    for piece in range(7):
        pre_bf16(piece).wait_recv()
    total = pack.at[0:7 * 512 + 3 * HALF]
    remote(total, total, pre_send, sp_recv, mate).wait_send()


def solution(mesh):
    def run_steps(particles, prec_diag, mean_vec, low_rank):
        total_rows, width = particles.shape
        n_part = total_rows // mesh.shape["ens"]
        bandwidth = BAND_SCALE * width
        step_size = STEP_SCALE * width
        loc = width // (mesh.shape["slab"] * mesh.shape["feat"])
        rank = low_rank.shape[1]
        vm, dma = pltpu.VMEM, pltpu.SemaphoreType.DMA

        def local_steps(current, prec_loc, mean_loc, fac_loc):
            spec = pl.BlockSpec(memory_space=pltpu.VMEM)
            call = pl.pallas_call(
                functools.partial(_kernel, bandwidth, step_size, n_part),
                out_shape=jax.ShapeDtypeStruct((n_part, loc), F32),
                in_specs=[pl.BlockSpec(memory_space=pltpu.HBM)] * 4,
                out_specs=spec,
                scratch_shapes=[
                    vm((1, loc), F32), vm((1, loc), F32), vm((loc, rank), BF16),
                    vm((ROWS, 2 * loc), BF16), vm((ROWS, rank), F32), vm((ROWS // 2, rank), F32),
                    vm((ROWS, TILE), F32), vm((16, TILE), F32), vm((ROWS, loc), F32), vm((ROWS, loc), F32),
                    vm((3 * SROWS, TILE), F32),
                    vm((3, COLORS, BLK // 2, TILE), F32), vm((3, COLORS, BLK // 4, TILE), F32),
                    vm((3, COLORS, 3, OWN, TILE), F32), vm((3, COLORS, 4, OWN, TILE), F32),
                    vm((2, SROWS, TILE), BF16), vm((ROWS, ROWS), BF16), vm((ROWS, loc), BF16),
                    vm((2, 3, 16, TILE), F32), vm((2, 3, 3, 16, TILE), F32), vm((16, TILE), F32), vm((16, TILE), F32),
                    dma((7,)), dma, dma((12,)), dma((3,)), dma((3, 2, COLORS)), dma((3, 2, COLORS)), dma((3, COLORS, 3)), dma((3, COLORS, 3)), dma((3, COLORS)),
                    dma((2, 3)), dma,
                ],
                compiler_params=pltpu.CompilerParams(collective_id=0, has_side_effects=True, vmem_limit_bytes=50000000),
                name="svgd",
            )
            hbm = lambda x: pltpu.with_memory_space_constraint(x, pltpu.HBM)
            return call(hbm(current), hbm(prec_loc.reshape(1, loc)), hbm(mean_loc.reshape(1, loc)), hbm(fac_loc))

        sharded = jax.shard_map(
            local_steps,
            mesh=mesh,
            in_specs=(P("ens", FEAT_AXES), P(LEAD_AXES), P(LEAD_AXES), P(LEAD_AXES, None)),
            out_specs=P("ens", FEAT_AXES),
            check_vma=False,
        )
        return sharded(particles, prec_diag, mean_vec, low_rank)

    return run_steps
```

```python
import functools

import jax
import jax.numpy as jnp
from jax import lax
from jax.experimental import pallas as pl
from jax.experimental.pallas import tpu as pltpu
from jax.sharding import PartitionSpec as P

NUM_STEPS = 3
BAND_SCALE = 4.0
STEP_SCALE = 0.4
FEAT_AXES = ("slab", "feat")
LEAD_AXES = ("ens", "slab", "feat")

ROWS = 2048
TILE = 128
HALF = 256
BLK = 2 * HALF
COLORS = 6
SROWS = COLORS * BLK
STREAMS = 6
QUARTER = HALF // 4
UNITS = ((), ((0, 3), (0, 1), (0, 2)), ((1, 2), (1, 3), (2, 3)))
OFFS = (((0, 1), (2, 0), (3, 0)), ((1, 2), (1, 3), (2, 3)))
SENT = 3216
SENT_SUMS = 304
OWN = QUARTER // 4
PEERS = (2, 1, 3)
NEAR_FIRST = (1, 3, 2)
MESH = pl.DeviceIdType.MESH
NT = (((1,), (1,)), ((), ()))
F32, BF16 = jnp.float32, jnp.bfloat16


def div(a, b):
    return lax.div(a, jnp.int32(b))


def rem(a, b):
    return lax.rem(a, jnp.int32(b))


def _kernel(
    bandwidth, step_size, n_part,
    theta_ref, lam_hbm, mu_hbm, fac_hbm, out_ref,
    lam_ref, mu_ref, fac_ref,
    bfull, pml, pmr, nrow, ncol, pulled, scaled, pack, r0, r1, r2, r3, kg, kfull, adrv, svec, srecv, stot, spart,
    in_sem, pre_send, pre_recv, sent, rs_recv, x_recv, near_recv, far_recv, dd_recv, s_recv, sp_recv,
):
    width = out_ref.shape[1]
    rep_coef = 2.0 / bandwidth
    core = lax.axis_index("slab")
    feat = lax.axis_index("feat")
    coords = (rem(feat, 4), rem(div(feat, 4), 4), div(feat, 16))
    strides = (1, 4, 16)

    def chip(dim, coord):
        return {"feat": feat + (coord - coords[dim]) * strides[dim]}

    turned = [[coords[dim]] + [rem(coords[dim] + j, 4) for j in sorted(PEERS)] for dim in range(3)]

    def around(dim, j):
        return turned[dim][j]

    ring = [[chip(dim, turned[dim][j]) for j in range(4)] for dim in range(3)]
    low_bit = [rem(c, 2) for c in coords]
    pair_bit = [[rem(div(t + 1, 2), 2) for t in turned[dim]] for dim in range(3)]
    high_bit = [[div(t, 2) for t in turned[dim]] for dim in range(3)]

    mate = {"slab": 1 - core}

    def al(x, m=16):
        return pl.multiple_of(x, m)

    halves = []
    for k in range(COLORS):
        steps = []
        start, length, cur = 0, HALF, coords[k % 3]
        for s in range(2):
            if (k // 3 + s) % 2 == 0:
                other, bit = cur + 1 - 2 * low_bit[k % 3], pair_bit[k % 3][0]
            else:
                other, bit = 3 - cur, high_bit[k % 3][0]
            length = length // 2
            keep, give = start + bit * length, start + (1 - bit) * length
            start = keep
            steps.append((chip(k % 3, other), length, keep, give))
        halves.append(steps)

    def dims(k):
        return k % 3, (k + 1) % 3, (k + 2) % 3

    def base(st, k):
        return (st * COLORS + k) * HALF

    def tile_row(kind, k, a):
        return base(2 * kind + a // 2, k) + a % 2 * TILE

    keeps = [[al(step[2]) for step in steps] for steps in halves]
    gives = [[al(step[3]) for step in steps] for steps in halves]
    pieces = [[al(halves[k][1][2] + OWN * around(dims(k)[1], j)) for j in range(4)] for k in range(COLORS)]
    places = []
    for k in range(COLORS):
        one, two = (pair_bit, high_bit) if k < 3 else (high_bit, pair_bit)
        places.append([al(QUARTER * (2 * one[k % 3][j] + two[k % 3][j])) for j in range(4)])

    columns = [[al(m * BLK + (2 * core + n) * TILE, TILE) for n in range(2)] for m in range(4)]

    def packed(st, k, row, rows):
        return pack.at[pl.ds(al(base(st, k) + row), rows)]

    barrier = pltpu.get_barrier_semaphore()
    pl.semaphore_signal(barrier, inc=1, device_id=mate, device_id_type=MESH)
    for dim in range(3):
        for j in PEERS:
            pl.semaphore_signal(barrier, inc=1, device_id=ring[dim][j], device_id_type=MESH)
    loads = [pltpu.make_async_copy(theta_ref.at[pl.ds(ch * BLK, BLK)], out_ref.at[pl.ds(ch * BLK, BLK)], in_sem.at[ch]) for ch in range(4)]
    loads += [
        pltpu.make_async_copy(src, dst, in_sem.at[4 + n])
        for n, (src, dst) in enumerate(((mu_hbm, mu_ref), (fac_hbm, fac_ref), (lam_hbm, lam_ref)))
    ]
    for cp in loads[4:] + loads[:4]:
        cp.start()

    row_i = lax.broadcasted_iota(jnp.int32, (TILE, TILE), 0)
    col_i = lax.broadcasted_iota(jnp.int32, (TILE, TILE), 1)
    eye, upper, lower = row_i == col_i, row_i < col_i, row_i > col_i
    sub_o = lax.broadcasted_iota(jnp.int32, (OWN, TILE), 0)
    lane_o = lax.broadcasted_iota(jnp.int32, (OWN, TILE), 1)

    def remote(src, dst, ssem, rsem, where):
        return pltpu.make_async_remote_copy(src_ref=src, dst_ref=dst, send_sem=ssem, recv_sem=rsem, device_id=where, device_id_type=MESH)

    def pre_bf16(piece):
        rows = pl.ds(piece * HALF, HALF)
        return remote(bfull.at[rows, 0:width], bfull.at[rows, width:2 * width], pre_send, pre_recv.at[piece], mate)

    def pre_pm(ch):
        src, dst = pml.at[pl.ds(al(ch * BLK + (1 - core) * HALF), HALF)], pmr.at[pl.ds(ch * HALF, HALF)]
        return remote(src, dst, pre_send, pre_recv.at[8 + ch], mate)

    def prepare(start, th):
        bfull[pl.ds(start, HALF), 0:width] = th.astype(BF16)
        return (th - mu_ref[...]).astype(BF16)

    def partial_pm(start, centered):
        for n, rows in enumerate(centered):
            pml[pl.ds(start + HALF * n, HALF), :] = jnp.dot(rows, fac_ref[...], preferred_element_type=F32)

    def begin(cps):
        for cp in cps:
            cp.start()

    def arrive(ref, sem):
        remote(ref, ref, sent.at[0], sem, mate).wait_recv()

    def x_arrive(st, e, k):
        arrive((r2.at[st, k], r3.at[st, k, 0:3])[e], x_recv.at[st, e, k])

    def rs_copy(st, s, k):
        peer, length, keep, give = halves[k][s]
        src = packed(st, k, gives[k][s], length)
        return remote(src, (r0, r1)[s].at[st, k], sent.at[st], rs_recv.at[st, s, k], peer)

    def gathered(st, k, row, rows):
        if st < 2:
            return kg.at[core, pl.ds(base(st, k) + row, rows)]
        sup, m = UNITS[st // 2][k // 2]
        return kfull.at[pl.ds(sup * BLK + st % 2 * HALF + row, rows), pl.ds(columns[m][k % 2], TILE)]

    def x_copies(st, e, k):
        d1, d2, d3 = dims(k)
        dim = (d2, d3)[e]
        cps = []
        for j in PEERS:
            if e == 0:
                src = packed(st, k, pieces[k][j], OWN)
                dst = r2.at[st, k, j - 1]
            else:
                src = dst = r3.at[st, k, coords[dim]]
            cps.append(remote(src, dst, sent.at[st], x_recv.at[st, e, k], ring[dim][j]))
        return cps

    def gather_copies(st, k, j):
        d1, d2, d3 = dims(k)
        ref = gathered(st, k, pieces[k][(4 - j) % 4], OWN)
        cps = [remote(ref, ref, sent.at[st], far_recv.at[st, k, i - 1], ring[d1][i]) for i in PEERS]
        if j == 0:
            cps = [remote(ref, ref, sent.at[st], near_recv.at[st, k, i - 1], ring[d2][i]) for i in PEERS] + cps
        return cps

    def dd_copy(st, k, j):
        ref = gathered(st, k, keeps[k][1] if j == 0 else places[k][4 - j], QUARTER)
        return remote(ref, ref, sent.at[st], dd_recv.at[st, k], mate)

    def s_copies(ph, d):
        dim = ((d + 1) % 3, d)[ph]
        return [
            remote(svec.at[ph, d], srecv.at[ph, d, j - 1], sent.at[STREAMS - 1], s_recv.at[ph, d], ring[dim][j])
            for j in PEERS
        ]

    def sp_copy():
        return remote(stot, spart, sent.at[STREAMS - 1], sp_recv, mate)

    def products(m):
        mine = bfull[pl.ds(al(m * BLK + HALF * core), HALF), :]
        part = BLK if m == 3 else (m + 1) * HALF
        return [lax.dot_general(bfull[pl.ds(at, part), :], mine, NT, preferred_element_type=F32) for at in range(0, (m + 1) * BLK, part)]

    def norms(m):
        for i in range(4):
            rows = pl.ds((4 * m + i) * TILE, TILE)
            wide = bfull[rows, :].astype(F32)
            n = jnp.broadcast_to(jnp.sum(wide * wide, axis=1, keepdims=True), (TILE, TILE))
            nrow[rows, :] = n
            ncol[4 * m + i:4 * m + i + 1, :] = jnp.sum(jnp.where(eye, n, 0.0), axis=0, keepdims=True)

    def tiles(m, g):
        def block(blk, b):
            n, r = divmod(blk * TILE, BLK if m == 3 else (m + 1) * HALF)
            return g[n][r:r + TILE, b * TILE:(b + 1) * TILE]

        def tile(i, b):
            return block(4 * m + i, b)

        def dist(i, j):
            return nrow[pl.ds((4 * m + i) * TILE, TILE), :] + ncol[4 * m + j:4 * m + j + 1, :] - 2.0 * tile(i, j % 2)

        for t in range(3):
            pack[pl.ds(tile_row(0, m, t), TILE), :] = jnp.where(core == 0, dist(*OFFS[0][t]), dist(*OFFS[1][t]))
        one = jnp.where(core == 0, dist(0, 0), dist(2, 2))
        two = jnp.where(core == 0, dist(1, 1), dist(3, 3))
        pack[pl.ds(tile_row(0, m, 3), TILE), :] = jnp.where(upper, one, two)
        begin([rs_copy(0, 0, m), rs_copy(1, 0, m)])
        for kind in (1, 2):
            for u, (sup, col) in enumerate(UNITS[kind]):
                if col != m:
                    continue
                for b in range(2):
                    nc = ncol[pl.ds(4 * m + 2 * core + b, 1), :]
                    for a in range(4):
                        nr = nrow[pl.ds((4 * sup + a) * TILE, TILE), :]
                        pack[pl.ds(tile_row(kind, 2 * u + b, a), TILE), :] = nr + nc - 2.0 * block(4 * sup + a, b)
                begin([rs_copy(st, 0, 2 * u + b) for st in (2 * kind, 2 * kind + 1) for b in range(2)])

    def pm_tiles(half):
        for ch in (2 * half, 2 * half + 1):
            pre_pm(ch).wait_recv()
            mine = pl.ds(al(ch * BLK + core * HALF), HALF)
            pack[pl.ds(base(ch % 2, 4 + half), HALF), :] = pml[mine, :] + pmr[pl.ds(ch * HALF, HALF), :]
            begin([rs_copy(ch % 2, 0, 4 + half)])

    def open_step():
        begin([pre_pm(3), pre_bf16(7)])
        pm_tiles(0)
        for piece in range(4):
            pre_bf16(piece).wait_recv()
        gs = []
        for m in range(2):
            gs.append(products(m))
            norms(m)
        for m in range(2):
            tiles(m, gs[m])
        pm_tiles(1)
        for m in range(2, 4):
            for piece in range(2 * m, 2 * m + 2):
                pre_bf16(piece).wait_recv()
            g = products(m)
            norms(m)
            tiles(m, g)

    for cp in loads[4:]:
        cp.wait()
    for ch in range(4):
        loads[ch].wait()
        starts = (ch * BLK, ch * BLK + HALF)
        partial_pm(ch * BLK, [prepare(start, out_ref[pl.ds(start, HALF), :]) for start in starts])
        if ch == 0:
            pl.semaphore_wait(barrier, 10)
        if ch < 3:
            begin([pre_pm(ch)])
        begin([pre_bf16(piece) for piece in (2 * ch, 2 * ch + 1) if piece < 7])
    open_step()

    def one_step(step_index, carry):
        def row_sums(st, k, kern):
            place = pieces[k][0] + st % 2 * HALF
            slot, r = div(place, TILE), rem(place, TILE)

            def by_rows(vals):
                rs = jnp.sum(vals, axis=1, keepdims=True)
                return jnp.sum(jnp.where(lane_o == sub_o + r, rs, 0.0), axis=0, keepdims=True)

            def by_cols(vals):
                return jnp.sum(vals, axis=0, keepdims=True)

            if st > 1:
                sup, m = UNITS[st // 2][k // 2]
                return [(4 * sup + slot, by_rows(kern)), (4 * m + 2 * core + k % 2, by_cols(kern))]
            both = div(slot, 3)
            up_one = div(slot + 1, 2)
            i0 = (1 - both) * ((1 - core) * (slot + up_one) + core * (1 + div(slot, 2))) + both * 2 * core
            j0 = (1 - both) * ((1 - core) * (1 - up_one) + core * (2 + up_one)) + both * 2 * core
            up = jnp.where(lane_o + 1000 * (1 - both) > sub_o + r, kern, 0.0)
            lo = jnp.where(lane_o + 1000 * (1 - both) < sub_o + r, kern, 0.0)
            nxt = 4 * k + 2 * core + 1
            return [(4 * k + i0, by_rows(up)), (4 * k + j0, by_cols(up)), (nxt, by_rows(lo)), (nxt, by_cols(lo))]

        def advance(st, s):
            parts = [[], [], []]
            if s == 4 and st == STREAMS - 1:
                for d in range(3):
                    arrive(srecv.at[0, d], s_recv.at[0, d])
                    svec[1, d] = svec[0, d] + srecv[0, d, 0] + srecv[0, d, 1] + srecv[0, d, 2]
                    begin(s_copies(1, d))
            if s == 5 and st == STREAMS - 1:
                tot = jnp.zeros((16, TILE), F32)
                for d in range(3):
                    arrive(srecv.at[1, d], s_recv.at[1, d])
                    tot = tot + ((svec[1, d] + srecv[1, d, 0]) + (srecv[1, d, 1] + srecv[1, d, 2]))
                stot[...] = tot
                begin([sp_copy()])
            kerns = []
            for k in range(COLORS if s < 4 else 0):
                if s < 2:
                    peer, length, keep, give = halves[k][s]
                    rs_copy(st, s, k).wait_recv()
                    packed(st, k, keeps[k][s], length)[...] += (r0, r1)[s][st, k]
                    begin([rs_copy(st, 1, k)] if s == 0 else x_copies(st, 0, k))
                elif s == 2:
                    x_arrive(st, 0, k)
                    r3[st, k, coords[dims(k)[2]]] = packed(st, k, pieces[k][0], OWN)[...] + r2[st, k, 0] + r2[st, k, 1] + r2[st, k, 2]
                    begin(x_copies(st, 1, k))
                else:
                    x_arrive(st, 1, k)
                    full = (r3[st, k, 0] + r3[st, k, 1]) + (r3[st, k, 2] + r3[st, k, 3])
                    kern = full if st < 2 and k >= 4 else jnp.exp(-jnp.maximum(full, 0.0) / bandwidth)
                    gathered(st, k, pieces[k][0], OWN)[...] = kern.astype(BF16)
                    begin(gather_copies(st, k, 0))
                    kerns.append(kern)
            for j in NEAR_FIRST if s >= 4 else ():
                for k in range(COLORS):
                    if s == 4:
                        arrive(kg.at[core, 0:OWN], near_recv.at[st, k, j - 1])
                        begin(gather_copies(st, k, j))
                        if j == NEAR_FIRST[-1]:
                            begin([dd_copy(st, k, 0)])
                    else:
                        arrive(kg.at[core, 0:QUARTER], far_recv.at[st, k, j - 1])
                        begin([dd_copy(st, k, j)])
            if s == 3:
                for k, kern in enumerate(kerns):
                    if st > 1 or k < 4:
                        parts[k % 3] += row_sums(st, k, kern)
                for d in range(3):
                    if st == 0:
                        svec[0, d] = jnp.zeros((16, TILE), F32)
                    for block, line in parts[d]:
                        svec[0, d, pl.ds(block, 1), :] += line
                    if st == STREAMS - 1:
                        begin(s_copies(0, d))
        def unpack_wait(kind):
            for st in (2 * kind, 2 * kind + 1):
                for k in range(COLORS):
                    arrive(kg.at[core, 0:HALF], dd_recv.at[st, k])

        def unpack(kind):
            for c in range(2):
                if kind > 0:
                    for k in range(COLORS):
                        sup, m = UNITS[kind][k // 2]
                        jrng = pl.ds((4 * m + 2 * c + k % 2) * TILE, TILE)
                        for a in range(4):
                            srng = pl.ds((4 * sup + a) * TILE, TILE)
                            kfull[jrng, srng] = kfull[srng, jrng].T
                    continue
                for sup in range(4):
                    for t, (i, j) in enumerate(OFFS[c]):
                        src = kg[c, pl.ds(tile_row(0, sup, t), TILE), :]
                        ri, rj = pl.ds((4 * sup + i) * TILE, TILE), pl.ds((4 * sup + j) * TILE, TILE)
                        kfull[ri, rj] = src
                        kfull[rj, ri] = src.T
                    src = kg[c, pl.ds(tile_row(0, sup, 3), TILE), :]
                    srt = src.T
                    one = jnp.ones((TILE, TILE), BF16)
                    ra, rb = pl.ds((4 * sup + 2 * c) * TILE, TILE), pl.ds((4 * sup + 2 * c + 1) * TILE, TILE)
                    kfull[ra, ra] = jnp.where(upper, src, jnp.where(lower, srt, one))
                    kfull[rb, rb] = jnp.where(lower, src, jnp.where(upper, srt, one))

        def drive_parts():
            for q in range(8):
                rows = pl.ds(q * HALF, HALF)
                th = out_ref[rows, :]
                pulled[rows, :] = (th - mu_ref[...]) * lam_ref[...]
                scaled[rows, :] = rep_coef * th

        def drive():
            for q in range(8):
                rows = pl.ds(q * HALF, HALF)
                ch = q // 2
                pm = kg[q % 2, pl.ds(base(ch % 2, 4 + ch // 2), HALF), :]
                low = lax.dot_general(pm, fac_ref[...], NT, preferred_element_type=F32)
                adrv[rows, :] = ((pulled[rows, :] + low) + scaled[rows, :]).astype(BF16)

        def product(start):
            return jnp.dot(kfull[pl.ds(start, HALF), :], adrv[...], preferred_element_type=F32)

        def finish(start, acc, tot, held):
            rows = pl.ds(start, HALF)
            sums = []
            for blk in (start // TILE, start // TILE + 1):
                line = jnp.where(eye, jnp.broadcast_to(tot[blk:blk + 1, :], (TILE, TILE)), 0.0)
                sums.append(rep_coef * jnp.sum(line, axis=1, keepdims=True))
            sums = jnp.broadcast_to(jnp.concatenate(sums, axis=0), (HALF, TILE))
            new = []
            for t in range(width // TILE):
                cols = slice(t * TILE, (t + 1) * TILE)
                th = out_ref[rows, cols]
                phi = (sums * th - acc[:, cols]) / n_part
                new.append(th + step_size * phi)
            th = jnp.concatenate(new, axis=1)
            out_ref[rows, :] = th
            held.append(prepare(start, th))
            if start % BLK:
                partial_pm(start - HALF, held[-2:])

        def share(start):
            if start % BLK and start + HALF < ROWS:
                begin([pre_pm(start // BLK), pre_bf16(start // HALF - 1), pre_bf16(start // HALF)])
            elif start + BLK == ROWS:
                begin([pre_bf16(start // HALF)])

        drive_parts()
        def early_rounds(s):
            def one(st, c):
                advance(st, s)
                return c

            lax.fori_loop(0, STREAMS, one, 0)

        for s in range(3):
            early_rounds(s)
        for s in range(3, 6):
            for st in range(STREAMS):
                if s == 5 and st == STREAMS - 2:
                    unpack_wait(0)
                    unpack(0)
                    drive()
                advance(st, s)
        remote(pack.at[0:5120], pack.at[0:5120], pre_send, sp_recv, mate).wait_send()
        def update(starts, kind):
            tot = stot[...] + spart[...] + 1.0
            ahead = product(starts[0])
            unpack(kind)
            held = []
            for n, start in enumerate(starts):
                acc = ahead
                if n + 1 < len(starts):
                    ahead = product(starts[n + 1])
                if n:
                    share(starts[n - 1])
                finish(start, acc, tot, held)
            share(starts[-1])

        unpack_wait(1)
        arrive(stot, sp_recv)
        update(range(0, BLK, HALF), 1)
        unpack_wait(2)
        update(range(BLK, ROWS, HALF), 2)
        for st in range(STREAMS):
            total = pack.at[0:SENT + (SENT_SUMS if st == STREAMS - 1 else 0)]
            remote(total, total, sent.at[st], sp_recv, mate).wait_send()
        pl.when(step_index < NUM_STEPS - 1)(open_step)
        return carry

    lax.fori_loop(0, NUM_STEPS, one_step, 0)
    for ch in range(3):
        pre_pm(ch).wait_recv()
    for piece in range(7):
        pre_bf16(piece).wait_recv()
    total = pack.at[0:7 * 512 + 3 * HALF]
    remote(total, total, pre_send, sp_recv, mate).wait_send()


def solution(mesh):
    def run_steps(particles, prec_diag, mean_vec, low_rank):
        total_rows, width = particles.shape
        n_part = total_rows // mesh.shape["ens"]
        bandwidth = BAND_SCALE * width
        step_size = STEP_SCALE * width
        loc = width // (mesh.shape["slab"] * mesh.shape["feat"])
        rank = low_rank.shape[1]
        vm, dma = pltpu.VMEM, pltpu.SemaphoreType.DMA

        def local_steps(current, prec_loc, mean_loc, fac_loc):
            spec = pl.BlockSpec(memory_space=pltpu.VMEM)
            call = pl.pallas_call(
                functools.partial(_kernel, bandwidth, step_size, n_part),
                out_shape=jax.ShapeDtypeStruct((n_part, loc), F32),
                in_specs=[pl.BlockSpec(memory_space=pltpu.HBM)] * 4,
                out_specs=spec,
                scratch_shapes=[
                    vm((1, loc), F32), vm((1, loc), F32), vm((loc, rank), BF16),
                    vm((ROWS, 2 * loc), BF16), vm((ROWS, rank), F32), vm((ROWS // 2, rank), F32),
                    vm((ROWS, TILE), F32), vm((16, TILE), F32), vm((ROWS, loc), F32), vm((ROWS, loc), F32),
                    vm((3 * SROWS, TILE), F32),
                    vm((STREAMS, COLORS, HALF // 2, TILE), F32), vm((STREAMS, COLORS, QUARTER, TILE), F32),
                    vm((STREAMS, COLORS, 3, OWN, TILE), F32), vm((STREAMS, COLORS, 4, OWN, TILE), F32),
                    vm((2, SROWS, TILE), BF16), vm((ROWS, ROWS), BF16), vm((ROWS, loc), BF16),
                    vm((2, 3, 16, TILE), F32), vm((2, 3, 3, 16, TILE), F32), vm((16, TILE), F32), vm((16, TILE), F32),
                    dma((7,)), dma, dma((12,)), dma((STREAMS,)), dma((STREAMS, 2, COLORS)), dma((STREAMS, 2, COLORS)),
                    dma((STREAMS, COLORS, 3)), dma((STREAMS, COLORS, 3)), dma((STREAMS, COLORS)),
                    dma((2, 3)), dma,
                ],
                compiler_params=pltpu.CompilerParams(collective_id=0, has_side_effects=True, vmem_limit_bytes=50000000),
                name="svgd",
            )
            hbm = lambda x: pltpu.with_memory_space_constraint(x, pltpu.HBM)
            return call(hbm(current), hbm(prec_loc.reshape(1, loc)), hbm(mean_loc.reshape(1, loc)), hbm(fac_loc))

        sharded = jax.shard_map(
            local_steps,
            mesh=mesh,
            in_specs=(P("ens", FEAT_AXES), P(LEAD_AXES), P(LEAD_AXES), P(LEAD_AXES, None)),
            out_specs=P("ens", FEAT_AXES),
            check_vma=False,
        )
        return sharded(particles, prec_diag, mean_vec, low_rank)

    return run_steps
```

```python
import functools

import jax
import jax.numpy as jnp
from jax import lax
from jax.experimental import pallas as pl
from jax.experimental.pallas import tpu as pltpu
from jax.sharding import PartitionSpec as P

NUM_STEPS = 3
BAND_SCALE = 4.0
STEP_SCALE = 0.4
FEAT_AXES = ("slab", "feat")
LEAD_AXES = ("ens", "slab", "feat")

ROWS = 2048
TILE = 128
HALF = 256
BLK = 2 * HALF
COLORS = 6
SROWS = COLORS * BLK
STREAMS = 6
QUARTER = HALF // 4
UNITS = ((), ((0, 3), (0, 1), (0, 2)), ((1, 2), (1, 3), (2, 3)))
OFFS = (((0, 1), (2, 0), (3, 0)), ((1, 2), (1, 3), (2, 3)))
SENT = 3216
SENT_SUMS = 304
OWN = QUARTER // 4
PEERS = (2, 1, 3)
NEAR_FIRST = (1, 3, 2)
MESH = pl.DeviceIdType.MESH
NT = (((1,), (1,)), ((), ()))
F32, BF16 = jnp.float32, jnp.bfloat16


def div(a, b):
    return lax.div(a, jnp.int32(b))


def rem(a, b):
    return lax.rem(a, jnp.int32(b))


def _kernel(
    bandwidth, step_size, n_part,
    theta_ref, lam_hbm, mu_hbm, fac_hbm, out_ref,
    lam_ref, mu_ref, fac_ref,
    bfull, pml, pmr, nrow, ncol, pulled, scaled, pack, r0, r1, r2, r3, kg, kfull, adrv, svec, srecv, stot, spart,
    in_sem, pre_send, pre_recv, sent, rs_recv, x_recv, near_recv, far_recv, dd_recv, s_recv, sp_recv,
):
    width = out_ref.shape[1]
    rep_coef = 2.0 / bandwidth
    core = lax.axis_index("slab")
    feat = lax.axis_index("feat")
    coords = (rem(feat, 4), rem(div(feat, 4), 4), div(feat, 16))
    strides = (1, 4, 16)

    def chip(dim, coord):
        return {"feat": feat + (coord - coords[dim]) * strides[dim]}

    turned = [[coords[dim]] + [rem(coords[dim] + j, 4) for j in sorted(PEERS)] for dim in range(3)]

    def around(dim, j):
        return turned[dim][j]

    ring = [[chip(dim, turned[dim][j]) for j in range(4)] for dim in range(3)]
    low_bit = [rem(c, 2) for c in coords]
    pair_bit = [[rem(div(t + 1, 2), 2) for t in turned[dim]] for dim in range(3)]
    high_bit = [[div(t, 2) for t in turned[dim]] for dim in range(3)]

    mate = {"slab": 1 - core}

    def al(x, m=16):
        return pl.multiple_of(x, m)

    halves = []
    for k in range(COLORS):
        steps = []
        start, length, cur = 0, HALF, coords[k % 3]
        for s in range(2):
            if (k // 3 + s) % 2 == 0:
                other, bit = cur + 1 - 2 * low_bit[k % 3], pair_bit[k % 3][0]
            else:
                other, bit = 3 - cur, high_bit[k % 3][0]
            length = length // 2
            keep, give = start + bit * length, start + (1 - bit) * length
            start = keep
            steps.append((chip(k % 3, other), length, keep, give))
        halves.append(steps)

    def dims(k):
        return k % 3, (k + 1) % 3, (k + 2) % 3

    def base(st, k):
        return (st * COLORS + k) * HALF

    def tile_row(kind, k, a):
        return base(2 * kind + a // 2, k) + a % 2 * TILE

    keeps = [[al(step[2]) for step in steps] for steps in halves]
    gives = [[al(step[3]) for step in steps] for steps in halves]
    pieces = [[al(halves[k][1][2] + OWN * around(dims(k)[1], j)) for j in range(4)] for k in range(COLORS)]
    places = []
    for k in range(COLORS):
        one, two = (pair_bit, high_bit) if k < 3 else (high_bit, pair_bit)
        places.append([al(QUARTER * (2 * one[k % 3][j] + two[k % 3][j])) for j in range(4)])

    columns = [[al(m * BLK + (2 * core + n) * TILE, TILE) for n in range(2)] for m in range(4)]

    def packed(st, k, row, rows):
        return pack.at[pl.ds(al(base(st, k) + row), rows)]

    loads = [pltpu.make_async_copy(theta_ref.at[pl.ds(ch * BLK, BLK)], out_ref.at[pl.ds(ch * BLK, BLK)], in_sem.at[ch]) for ch in range(4)]
    loads += [
        pltpu.make_async_copy(src, dst, in_sem.at[4 + n])
        for n, (src, dst) in enumerate(((mu_hbm, mu_ref), (fac_hbm, fac_ref), (lam_hbm, lam_ref)))
    ]
    for cp in loads[4:] + loads[:1]:
        cp.start()
    barrier = pltpu.get_barrier_semaphore()
    pl.semaphore_signal(barrier, inc=1, device_id=mate, device_id_type=MESH)
    for dim in range(3):
        for j in PEERS:
            pl.semaphore_signal(barrier, inc=1, device_id=ring[dim][j], device_id_type=MESH)
    for cp in loads[1:4]:
        cp.start()

    row_i = lax.broadcasted_iota(jnp.int32, (TILE, TILE), 0)
    col_i = lax.broadcasted_iota(jnp.int32, (TILE, TILE), 1)
    eye, upper, lower = row_i == col_i, row_i < col_i, row_i > col_i
    sub_o = lax.broadcasted_iota(jnp.int32, (OWN, TILE), 0)
    lane_o = lax.broadcasted_iota(jnp.int32, (OWN, TILE), 1)

    def remote(src, dst, ssem, rsem, where):
        return pltpu.make_async_remote_copy(src_ref=src, dst_ref=dst, send_sem=ssem, recv_sem=rsem, device_id=where, device_id_type=MESH)

    def pre_bf16(piece):
        rows = pl.ds(piece * HALF, HALF)
        return remote(bfull.at[rows, 0:width], bfull.at[rows, width:2 * width], pre_send, pre_recv.at[piece], mate)

    def pre_pm(ch):
        src, dst = pml.at[pl.ds(al(ch * BLK + (1 - core) * HALF), HALF)], pmr.at[pl.ds(ch * HALF, HALF)]
        return remote(src, dst, pre_send, pre_recv.at[8 + ch], mate)

    def prepare(start, th):
        bfull[pl.ds(start, HALF), 0:width] = th.astype(BF16)
        return (th - mu_ref[...]).astype(BF16)

    def partial_pm(start, centered):
        for n, rows in enumerate(centered):
            pml[pl.ds(start + HALF * n, HALF), :] = jnp.dot(rows, fac_ref[...], preferred_element_type=F32)

    def begin(cps):
        for cp in cps:
            cp.start()

    def arrive(ref, sem):
        remote(ref, ref, sent.at[0], sem, mate).wait_recv()

    def pair_arrive(rows, sem):
        arrive(pack.at[0:6 * rows], sem)

    def rs_copy(st, s, k):
        peer, length, keep, give = halves[k][s]
        src = packed(st, k, gives[k][s], length)
        return remote(src, (r0, r1)[s].at[st, k], sent.at[st], rs_recv.at[st, s, k], peer)

    def gathered(st, k, row, rows):
        if st < 2:
            return kg.at[core, pl.ds(base(st, k) + row, rows)]
        sup, m = UNITS[st // 2][k // 2]
        return kfull.at[pl.ds(sup * BLK + st % 2 * HALF + row, rows), pl.ds(columns[m][k % 2], TILE)]

    def x_copies(st, e, k):
        d1, d2, d3 = dims(k)
        dim = (d2, d3)[e]
        cps = []
        for j in PEERS:
            if e == 0:
                src = packed(st, k, pieces[k][j], OWN)
                dst = r2.at[st, k, j - 1]
            else:
                src = dst = r3.at[st, k, coords[dim]]
            cps.append(remote(src, dst, sent.at[st], x_recv.at[st, e, k % 3], ring[dim][j]))
        return cps

    def gather_copies(st, k, j):
        d1, d2, d3 = dims(k)
        ref = gathered(st, k, pieces[k][(4 - j) % 4], OWN)
        cps = [remote(ref, ref, sent.at[st], far_recv.at[st, k % 3], ring[d1][i]) for i in PEERS]
        if j == 0:
            cps = [remote(ref, ref, sent.at[st], near_recv.at[st, k % 3], ring[d2][i]) for i in PEERS] + cps
        return cps

    def dd_copy(st, k, j):
        ref = gathered(st, k, keeps[k][1] if j == 0 else places[k][4 - j], QUARTER)
        return remote(ref, ref, sent.at[st], dd_recv.at[st], mate)

    def s_copies(ph, d):
        dim = ((d + 1) % 3, d)[ph]
        return [
            remote(svec.at[ph, d], srecv.at[ph, d, j - 1], sent.at[STREAMS - 1], s_recv.at[ph, d], ring[dim][j])
            for j in PEERS
        ]

    def sp_copy():
        return remote(stot, spart, sent.at[STREAMS - 1], sp_recv, mate)

    def products(m):
        mine = bfull[pl.ds(al(m * BLK + HALF * core), HALF), :]
        part = BLK if m == 3 else (m + 1) * HALF
        return [lax.dot_general(bfull[pl.ds(at, part), :], mine, NT, preferred_element_type=F32) for at in range(0, (m + 1) * BLK, part)]

    def norms(m):
        for i in range(4):
            rows = pl.ds((4 * m + i) * TILE, TILE)
            wide = bfull[rows, :].astype(F32)
            n = jnp.broadcast_to(jnp.sum(wide * wide, axis=1, keepdims=True), (TILE, TILE))
            nrow[rows, :] = n
            ncol[4 * m + i:4 * m + i + 1, :] = jnp.sum(jnp.where(eye, n, 0.0), axis=0, keepdims=True)

    def tiles(m, g):
        def block(blk, b):
            n, r = divmod(blk * TILE, BLK if m == 3 else (m + 1) * HALF)
            return g[n][r:r + TILE, b * TILE:(b + 1) * TILE]

        def tile(i, b):
            return block(4 * m + i, b)

        def dist(i, j):
            return nrow[pl.ds((4 * m + i) * TILE, TILE), :] + ncol[4 * m + j:4 * m + j + 1, :] - 2.0 * tile(i, j % 2)

        for t in range(3):
            pack[pl.ds(tile_row(0, m, t), TILE), :] = jnp.where(core == 0, dist(*OFFS[0][t]), dist(*OFFS[1][t]))
        one = jnp.where(core == 0, dist(0, 0), dist(2, 2))
        two = jnp.where(core == 0, dist(1, 1), dist(3, 3))
        pack[pl.ds(tile_row(0, m, 3), TILE), :] = jnp.where(upper, one, two)
        begin([rs_copy(0, 0, m), rs_copy(1, 0, m)])
        for kind in (1, 2):
            for u, (sup, col) in enumerate(UNITS[kind]):
                if col != m:
                    continue
                for b in range(2):
                    nc = ncol[pl.ds(4 * m + 2 * core + b, 1), :]
                    for a in range(4):
                        nr = nrow[pl.ds((4 * sup + a) * TILE, TILE), :]
                        pack[pl.ds(tile_row(kind, 2 * u + b, a), TILE), :] = nr + nc - 2.0 * block(4 * sup + a, b)
                begin([rs_copy(st, 0, 2 * u + b) for st in (2 * kind, 2 * kind + 1) for b in range(2)])

    def pm_tiles(half):
        for ch in (2 * half, 2 * half + 1):
            pre_pm(ch).wait_recv()
            mine = pl.ds(al(ch * BLK + core * HALF), HALF)
            pack[pl.ds(base(ch % 2, 4 + half), HALF), :] = pml[mine, :] + pmr[pl.ds(ch * HALF, HALF), :]
            begin([rs_copy(ch % 2, 0, 4 + half)])

    def open_step(finish_last):
        pm_tiles(0)
        for piece in range(4):
            pre_bf16(piece).wait_recv()
        gs = [products(m) for m in range(2)]
        finish_last()
        for m in range(2):
            norms(m)
        begin([pre_pm(3), pre_bf16(7)])
        for m in range(2):
            tiles(m, gs[m])
        pm_tiles(1)
        for m in range(2, 4):
            for piece in range(2 * m, 2 * m + 2):
                pre_bf16(piece).wait_recv()
            g = products(m)
            norms(m)
            tiles(m, g)

    for cp in loads[4:]:
        cp.wait()
    for ch in range(4):
        loads[ch].wait()
        starts = (ch * BLK, ch * BLK + HALF)
        partial_pm(ch * BLK, [prepare(start, out_ref[pl.ds(start, HALF), :]) for start in starts])
        if ch == 0:
            pl.semaphore_wait(barrier, 10)
        if ch < 3:
            begin([pre_pm(ch)])
        begin([pre_bf16(piece) for piece in (2 * ch, 2 * ch + 1) if piece < 7])
    open_step(lambda: None)

    def one_step(step_index, carry):
        def row_sums(st, k, kern):
            place = pieces[k][0] + st % 2 * HALF
            slot, r = div(place, TILE), rem(place, TILE)

            def by_rows(vals):
                rs = jnp.sum(vals, axis=1, keepdims=True)
                return jnp.sum(jnp.where(lane_o == sub_o + r, rs, 0.0), axis=0, keepdims=True)

            def by_cols(vals):
                return jnp.sum(vals, axis=0, keepdims=True)

            if st > 1:
                sup, m = UNITS[st // 2][k // 2]
                return [(4 * sup + slot, by_rows(kern)), (4 * m + 2 * core + k % 2, by_cols(kern))]
            both = div(slot, 3)
            up_one = div(slot + 1, 2)
            i0 = (1 - both) * ((1 - core) * (slot + up_one) + core * (1 + div(slot, 2))) + both * 2 * core
            j0 = (1 - both) * ((1 - core) * (1 - up_one) + core * (2 + up_one)) + both * 2 * core
            up = jnp.where(lane_o + 1000 * (1 - both) > sub_o + r, kern, 0.0)
            lo = jnp.where(lane_o + 1000 * (1 - both) < sub_o + r, kern, 0.0)
            nxt = 4 * k + 2 * core + 1
            return [(4 * k + i0, by_rows(up)), (4 * k + j0, by_cols(up)), (nxt, by_rows(lo)), (nxt, by_cols(lo))]

        def advance(st, s):
            parts = [[], [], []]
            if s == 4 and st == STREAMS - 1:
                for d in range(3):
                    arrive(srecv.at[0, d], s_recv.at[0, d])
                    svec[1, d] = svec[0, d] + srecv[0, d, 0] + srecv[0, d, 1] + srecv[0, d, 2]
                    begin(s_copies(1, d))
            if s == 5 and st == STREAMS - 1:
                tot = jnp.zeros((16, TILE), F32)
                for d in range(3):
                    arrive(srecv.at[1, d], s_recv.at[1, d])
                    tot = tot + ((svec[1, d] + srecv[1, d, 0]) + (srecv[1, d, 1] + srecv[1, d, 2]))
                stot[...] = tot
                begin([sp_copy()])
            kerns = {}
            for k in (range(COLORS) if s < 2 else (0, 3, 1, 4, 2, 5)):
                if s < 2:
                    peer, length, keep, give = halves[k][s]
                    rs_copy(st, s, k).wait_recv()
                    packed(st, k, keeps[k][s], length)[...] += (r0, r1)[s][st, k]
                    begin([rs_copy(st, 1, k)] if s == 0 else x_copies(st, 0, k))
                    continue
                if k < 3:
                    sem = x_recv.at[st, s - 2, k] if s < 4 else (near_recv, far_recv)[s - 4].at[st, k]
                    pair_arrive((OWN, OWN, OWN // 2, QUARTER // 2)[s - 2], sem)
                if s == 2:
                    r3[st, k, coords[dims(k)[2]]] = packed(st, k, pieces[k][0], OWN)[...] + r2[st, k, 0] + r2[st, k, 1] + r2[st, k, 2]
                    begin(x_copies(st, 1, k))
                elif s == 3:
                    full = (r3[st, k, 0] + r3[st, k, 1]) + (r3[st, k, 2] + r3[st, k, 3])
                    kern = full if st < 2 and k >= 4 else jnp.exp(-jnp.maximum(full, 0.0) / bandwidth)
                    gathered(st, k, pieces[k][0], OWN)[...] = kern.astype(BF16)
                    begin(gather_copies(st, k, 0))
                    kerns[k] = kern
                elif s == 4:
                    begin([dd_copy(st, k, 0)])
                    for j in NEAR_FIRST:
                        begin(gather_copies(st, k, j))
                else:
                    begin([dd_copy(st, k, j) for j in NEAR_FIRST])
            if s == 3:
                for k, kern in kerns.items():
                    if st > 1 or k < 4:
                        parts[k % 3] += row_sums(st, k, kern)
                for d in range(3):
                    if st == 0:
                        svec[0, d] = jnp.zeros((16, TILE), F32)
                    for block, line in parts[d]:
                        svec[0, d, pl.ds(block, 1), :] += line
                    if st == STREAMS - 1:
                        begin(s_copies(0, d))
        def unpack_wait(kind):
            for st in (2 * kind, 2 * kind + 1):
                arrive(kg.at[core, 0:COLORS * HALF], dd_recv.at[st])

        def unpack(kind):
            for c in range(2):
                if kind > 0:
                    for k in range(COLORS):
                        sup, m = UNITS[kind][k // 2]
                        jrng = pl.ds((4 * m + 2 * c + k % 2) * TILE, TILE)
                        for a in range(4):
                            srng = pl.ds((4 * sup + a) * TILE, TILE)
                            kfull[jrng, srng] = kfull[srng, jrng].T
                    continue
                for sup in range(4):
                    for t, (i, j) in enumerate(OFFS[c]):
                        src = kg[c, pl.ds(tile_row(0, sup, t), TILE), :]
                        ri, rj = pl.ds((4 * sup + i) * TILE, TILE), pl.ds((4 * sup + j) * TILE, TILE)
                        kfull[ri, rj] = src
                        kfull[rj, ri] = src.T
                    src = kg[c, pl.ds(tile_row(0, sup, 3), TILE), :]
                    srt = src.T
                    one = jnp.ones((TILE, TILE), BF16)
                    ra, rb = pl.ds((4 * sup + 2 * c) * TILE, TILE), pl.ds((4 * sup + 2 * c + 1) * TILE, TILE)
                    kfull[ra, ra] = jnp.where(upper, src, jnp.where(lower, srt, one))
                    kfull[rb, rb] = jnp.where(lower, src, jnp.where(upper, srt, one))

        def drive_parts():
            for q in range(8):
                rows = pl.ds(q * HALF, HALF)
                th = out_ref[rows, :]
                pulled[rows, :] = (th - mu_ref[...]) * lam_ref[...]
                scaled[rows, :] = rep_coef * th

        def drive():
            for q in range(8):
                rows = pl.ds(q * HALF, HALF)
                ch = q // 2
                pm = kg[q % 2, pl.ds(base(ch % 2, 4 + ch // 2), HALF), :]
                low = lax.dot_general(pm, fac_ref[...], NT, preferred_element_type=F32)
                adrv[rows, :] = ((pulled[rows, :] + low) + scaled[rows, :]).astype(BF16)

        def product(start):
            return jnp.dot(kfull[pl.ds(start, HALF), :], adrv[...], preferred_element_type=F32)

        def finish(start, acc, tot, held):
            rows = pl.ds(start, HALF)
            sums = []
            for blk in (start // TILE, start // TILE + 1):
                line = jnp.where(eye, jnp.broadcast_to(tot[blk:blk + 1, :], (TILE, TILE)), 0.0)
                sums.append(rep_coef * jnp.sum(line, axis=1, keepdims=True))
            sums = jnp.broadcast_to(jnp.concatenate(sums, axis=0), (HALF, TILE))
            new = []
            for t in range(width // TILE):
                cols = slice(t * TILE, (t + 1) * TILE)
                th = out_ref[rows, cols]
                phi = (sums * th - acc[:, cols]) / n_part
                new.append(th + step_size * phi)
            th = jnp.concatenate(new, axis=1)
            out_ref[rows, :] = th
            held.append(prepare(start, th))
            if start % BLK:
                partial_pm(start - HALF, held[-2:])

        def share(start):
            if start % BLK and start + HALF < ROWS:
                begin([pre_pm(start // BLK), pre_bf16(start // HALF - 1), pre_bf16(start // HALF)])
            elif start + BLK == ROWS:
                begin([pre_bf16(start // HALF)])

        drive_parts()
        def early_rounds(s):
            def one(st, c):
                advance(st, s)
                return c

            lax.fori_loop(0, STREAMS, one, 0)

        for s in range(3):
            early_rounds(s)
        for s in range(3, 6):
            for st in range(STREAMS):
                if s == 5 and st == STREAMS - 2:
                    unpack_wait(0)
                    unpack(0)
                    drive()
                advance(st, s)
        remote(pack.at[0:5120], pack.at[0:5120], pre_send, sp_recv, mate).wait_send()
        def update(starts, kind):
            tot = stot[...] + spart[...] + 1.0
            ahead = product(starts[0])
            unpack(kind)
            held = []
            for n, start in enumerate(starts):
                acc = ahead
                if n + 1 < len(starts):
                    ahead = product(starts[n + 1])
                if n:
                    share(starts[n - 1])
                if start + HALF == ROWS:
                    return lambda: finish(start, acc, tot, list(held))
                finish(start, acc, tot, held)
            share(starts[-1])

        unpack_wait(1)
        arrive(stot, sp_recv)
        update(range(0, BLK, HALF), 1)
        unpack_wait(2)
        finish_last = update(range(BLK, ROWS, HALF), 2)
        for st in range(STREAMS):
            total = pack.at[0:SENT + (SENT_SUMS if st == STREAMS - 1 else 0)]
            remote(total, total, sent.at[st], sp_recv, mate).wait_send()
        pl.when(step_index < NUM_STEPS - 1)(lambda: open_step(finish_last))
        pl.when(step_index == NUM_STEPS - 1)(finish_last)
        return carry

    lax.fori_loop(0, NUM_STEPS, one_step, 0)
    for ch in range(3):
        pre_pm(ch).wait_recv()
    for piece in range(7):
        pre_bf16(piece).wait_recv()
    total = pack.at[0:7 * 512 + 3 * HALF]
    remote(total, total, pre_send, sp_recv, mate).wait_send()


def solution(mesh):
    def run_steps(particles, prec_diag, mean_vec, low_rank):
        total_rows, width = particles.shape
        n_part = total_rows // mesh.shape["ens"]
        bandwidth = BAND_SCALE * width
        step_size = STEP_SCALE * width
        loc = width // (mesh.shape["slab"] * mesh.shape["feat"])
        rank = low_rank.shape[1]
        vm, dma = pltpu.VMEM, pltpu.SemaphoreType.DMA

        def local_steps(current, prec_loc, mean_loc, fac_loc):
            spec = pl.BlockSpec(memory_space=pltpu.VMEM)
            call = pl.pallas_call(
                functools.partial(_kernel, bandwidth, step_size, n_part),
                out_shape=jax.ShapeDtypeStruct((n_part, loc), F32),
                in_specs=[pl.BlockSpec(memory_space=pltpu.HBM)] * 4,
                out_specs=spec,
                scratch_shapes=[
                    vm((1, loc), F32), vm((1, loc), F32), vm((loc, rank), BF16),
                    vm((ROWS, 2 * loc), BF16), vm((ROWS, rank), F32), vm((ROWS // 2, rank), F32),
                    vm((ROWS, TILE), F32), vm((16, TILE), F32), vm((ROWS, loc), F32), vm((ROWS, loc), F32),
                    vm((3 * SROWS, TILE), F32),
                    vm((STREAMS, COLORS, HALF // 2, TILE), F32), vm((STREAMS, COLORS, QUARTER, TILE), F32),
                    vm((STREAMS, COLORS, 3, OWN, TILE), F32), vm((STREAMS, COLORS, 4, OWN, TILE), F32),
                    vm((2, SROWS, TILE), BF16), vm((ROWS, ROWS), BF16), vm((ROWS, loc), BF16),
                    vm((2, 3, 16, TILE), F32), vm((2, 3, 3, 16, TILE), F32), vm((16, TILE), F32), vm((16, TILE), F32),
                    dma((7,)), dma, dma((12,)), dma((STREAMS,)), dma((STREAMS, 2, COLORS)), dma((STREAMS, 2, 3)),
                    dma((STREAMS, 3)), dma((STREAMS, 3)), dma((STREAMS,)),
                    dma((2, 3)), dma,
                ],
                compiler_params=pltpu.CompilerParams(collective_id=0, has_side_effects=True, vmem_limit_bytes=50000000),
                name="svgd",
            )
            hbm = lambda x: pltpu.with_memory_space_constraint(x, pltpu.HBM)
            return call(hbm(current), hbm(prec_loc.reshape(1, loc)), hbm(mean_loc.reshape(1, loc)), hbm(fac_loc))

        sharded = jax.shard_map(
            local_steps,
            mesh=mesh,
            in_specs=(P("ens", FEAT_AXES), P(LEAD_AXES), P(LEAD_AXES), P(LEAD_AXES, None)),
            out_specs=P("ens", FEAT_AXES),
            check_vma=False,
        )
        return sharded(particles, prec_diag, mean_vec, low_rank)

    return run_steps
```

```python
import functools

import jax
import jax.numpy as jnp
from jax import lax
from jax.experimental import pallas as pl
from jax.experimental.pallas import tpu as pltpu
from jax.sharding import PartitionSpec as P

NUM_STEPS = 3
BAND_SCALE = 4.0
STEP_SCALE = 0.4
FEAT_AXES = ("slab", "feat")
LEAD_AXES = ("ens", "slab", "feat")

ROWS = 2048
TILE = 128
HALF = 256
BLK = 2 * HALF
COLORS = 6
SROWS = COLORS * BLK
STREAMS = 6
QUARTER = HALF // 4
UNITS = ((), ((0, 3), (0, 1), (0, 2)), ((1, 2), (1, 3), (2, 3)))
OFFS = (((0, 1), (2, 0), (3, 0)), ((1, 2), (1, 3), (2, 3)))
SENT = 3216
SENT_SUMS = 304
OWN = QUARTER // 4
PEERS = (2, 1, 3)
NEAR_FIRST = (1, 3, 2)
MESH = pl.DeviceIdType.MESH
NT = (((1,), (1,)), ((), ()))
F32, BF16 = jnp.float32, jnp.bfloat16


def div(a, b):
    return lax.div(a, jnp.int32(b))


def rem(a, b):
    return lax.rem(a, jnp.int32(b))


def _kernel(
    bandwidth, step_size, n_part,
    theta_ref, lam_hbm, mu_hbm, fac_hbm, out_ref,
    lam_ref, mu_ref, fac_ref,
    bfull, pml, pmr, nrow, ncol, pulled, scaled, pack, r0, r1, r2, r3, kg, kfull, adrv, svec, srecv, stot, spart,
    in_sem, pre_send, pre_recv, sent, rs_recv, x_recv, near_recv, far_recv, dd_recv, s_recv, sp_recv,
):
    width = out_ref.shape[1]
    rep_coef = 2.0 / bandwidth
    core = lax.axis_index("slab")
    feat = lax.axis_index("feat")
    coords = (rem(feat, 4), rem(div(feat, 4), 4), div(feat, 16))
    strides = (1, 4, 16)

    def chip(dim, coord):
        return {"feat": feat + (coord - coords[dim]) * strides[dim]}

    turned = [[coords[dim]] + [rem(coords[dim] + j, 4) for j in sorted(PEERS)] for dim in range(3)]

    def around(dim, j):
        return turned[dim][j]

    ring = [[chip(dim, turned[dim][j]) for j in range(4)] for dim in range(3)]
    low_bit = [rem(c, 2) for c in coords]
    pair_bit = [[rem(div(t + 1, 2), 2) for t in turned[dim]] for dim in range(3)]
    high_bit = [[div(t, 2) for t in turned[dim]] for dim in range(3)]

    mate = {"slab": 1 - core}

    def al(x, m=16):
        return pl.multiple_of(x, m)

    halves = []
    for k in range(COLORS):
        steps = []
        start, length, cur = 0, HALF, coords[k % 3]
        for s in range(2):
            if (k // 3 + s) % 2 == 0:
                other, bit = cur + 1 - 2 * low_bit[k % 3], pair_bit[k % 3][0]
            else:
                other, bit = 3 - cur, high_bit[k % 3][0]
            length = length // 2
            keep, give = start + bit * length, start + (1 - bit) * length
            start = keep
            steps.append((chip(k % 3, other), length, keep, give))
        halves.append(steps)

    def dims(k):
        return k % 3, (k + 1) % 3, (k + 2) % 3

    def base(st, k):
        return (st * COLORS + k) * HALF

    def tile_row(kind, k, a):
        return base(2 * kind + a // 2, k) + a % 2 * TILE

    keeps = [[al(step[2]) for step in steps] for steps in halves]
    gives = [[al(step[3]) for step in steps] for steps in halves]
    pieces = [[al(halves[k][1][2] + OWN * around(dims(k)[1], j)) for j in range(4)] for k in range(COLORS)]
    places = []
    for k in range(COLORS):
        one, two = (pair_bit, high_bit) if k < 3 else (high_bit, pair_bit)
        places.append([al(QUARTER * (2 * one[k % 3][j] + two[k % 3][j])) for j in range(4)])

    columns = [[al(m * BLK + (2 * core + n) * TILE, TILE) for n in range(2)] for m in range(4)]

    def packed(st, k, row, rows):
        return pack.at[pl.ds(al(base(st, k) + row), rows)]

    loads = [pltpu.make_async_copy(theta_ref.at[pl.ds(ch * BLK, BLK)], out_ref.at[pl.ds(ch * BLK, BLK)], in_sem.at[ch]) for ch in range(4)]
    loads += [
        pltpu.make_async_copy(src, dst, in_sem.at[4 + n])
        for n, (src, dst) in enumerate(((mu_hbm, mu_ref), (fac_hbm, fac_ref), (lam_hbm, lam_ref)))
    ]
    for cp in loads[4:] + loads[:1]:
        cp.start()
    barrier = pltpu.get_barrier_semaphore()
    pl.semaphore_signal(barrier, inc=1, device_id=mate, device_id_type=MESH)
    for dim in range(3):
        for j in PEERS:
            pl.semaphore_signal(barrier, inc=1, device_id=ring[dim][j], device_id_type=MESH)
    for cp in loads[1:4]:
        cp.start()

    row_i = lax.broadcasted_iota(jnp.int32, (TILE, TILE), 0)
    col_i = lax.broadcasted_iota(jnp.int32, (TILE, TILE), 1)
    eye, upper, lower = row_i == col_i, row_i < col_i, row_i > col_i
    sub_o = lax.broadcasted_iota(jnp.int32, (OWN, TILE), 0)
    lane_o = lax.broadcasted_iota(jnp.int32, (OWN, TILE), 1)

    def remote(src, dst, ssem, rsem, where):
        return pltpu.make_async_remote_copy(src_ref=src, dst_ref=dst, send_sem=ssem, recv_sem=rsem, device_id=where, device_id_type=MESH)

    def pre_bf16(piece):
        rows = pl.ds(piece * HALF, HALF)
        return remote(bfull.at[rows, 0:width], bfull.at[rows, width:2 * width], pre_send, pre_recv.at[piece], mate)

    def pre_pm(ch):
        src, dst = pml.at[pl.ds(al(ch * BLK + (1 - core) * HALF), HALF)], pmr.at[pl.ds(ch * HALF, HALF)]
        return remote(src, dst, pre_send, pre_recv.at[8 + ch], mate)

    def prepare(start, th):
        bfull[pl.ds(start, HALF), 0:width] = th.astype(BF16)
        return (th - mu_ref[...]).astype(BF16)

    def partial_pm(start, centered):
        for n, rows in enumerate(centered):
            pml[pl.ds(start + HALF * n, HALF), :] = jnp.dot(rows, fac_ref[...], preferred_element_type=F32)

    def begin(cps):
        for cp in cps:
            cp.start()

    def arrive(ref, sem):
        remote(ref, ref, sent.at[0], sem, mate).wait_recv()

    def pair_arrive(rows, sem):
        arrive(pack.at[0:6 * rows], sem)

    def rs_copy(st, s, k):
        peer, length, keep, give = halves[k][s]
        src = packed(st, k, gives[k][s], length)
        return remote(src, (r0, r1)[s].at[st, k], sent.at[st], rs_recv.at[st, s, k], peer)

    def gathered(st, k, row, rows):
        if st < 2:
            return kg.at[core, pl.ds(base(st, k) + row, rows)]
        sup, m = UNITS[st // 2][k // 2]
        return kfull.at[pl.ds(sup * BLK + st % 2 * HALF + row, rows), pl.ds(columns[m][k % 2], TILE)]

    def x_copies(st, e, k):
        d1, d2, d3 = dims(k)
        dim = (d2, d3)[e]
        cps = []
        for j in PEERS:
            if e == 0:
                src = packed(st, k, pieces[k][j], OWN)
                dst = r2.at[st, k, j - 1]
            else:
                src = dst = r3.at[st, k, coords[dim]]
            cps.append(remote(src, dst, sent.at[st], x_recv.at[st, e, k % 3], ring[dim][j]))
        return cps

    def gather_copies(st, k, j):
        d1, d2, d3 = dims(k)
        ref = gathered(st, k, pieces[k][(4 - j) % 4], OWN)
        cps = [remote(ref, ref, sent.at[st], far_recv.at[st, k % 3], ring[d1][i]) for i in PEERS]
        if j == 0:
            cps = [remote(ref, ref, sent.at[st], near_recv.at[st, k % 3], ring[d2][i]) for i in PEERS] + cps
        return cps

    def dd_copy(st, k, j):
        ref = gathered(st, k, keeps[k][1] if j == 0 else places[k][4 - j], QUARTER)
        return remote(ref, ref, sent.at[st], dd_recv.at[st], mate)

    def s_copies(ph, d):
        dim = ((d + 1) % 3, d)[ph]
        return [
            remote(svec.at[ph, d], srecv.at[ph, d, j - 1], sent.at[STREAMS - 1], s_recv.at[ph, d], ring[dim][j])
            for j in PEERS
        ]

    def sp_copy():
        return remote(stot, spart, sent.at[STREAMS - 1], sp_recv, mate)

    def products(m):
        mine = bfull[pl.ds(al(m * BLK + HALF * core), HALF), :]
        part = BLK if m == 3 else (m + 1) * HALF
        return [lax.dot_general(bfull[pl.ds(at, part), :], mine, NT, preferred_element_type=F32) for at in range(0, (m + 1) * BLK, part)]

    def norms(m):
        for i in range(4):
            rows = pl.ds((4 * m + i) * TILE, TILE)
            wide = bfull[rows, :].astype(F32)
            n = jnp.broadcast_to(jnp.sum(wide * wide, axis=1, keepdims=True), (TILE, TILE))
            nrow[rows, :] = n
            ncol[4 * m + i:4 * m + i + 1, :] = jnp.sum(jnp.where(eye, n, 0.0), axis=0, keepdims=True)

    def tiles(m, g):
        def block(blk, b):
            n, r = divmod(blk * TILE, BLK if m == 3 else (m + 1) * HALF)
            return g[n][r:r + TILE, b * TILE:(b + 1) * TILE]

        def tile(i, b):
            return block(4 * m + i, b)

        def dist(i, j):
            return nrow[pl.ds((4 * m + i) * TILE, TILE), :] + ncol[4 * m + j:4 * m + j + 1, :] - 2.0 * tile(i, j % 2)

        for t in range(3):
            pack[pl.ds(tile_row(0, m, t), TILE), :] = jnp.where(core == 0, dist(*OFFS[0][t]), dist(*OFFS[1][t]))
        one = jnp.where(core == 0, dist(0, 0), dist(2, 2))
        two = jnp.where(core == 0, dist(1, 1), dist(3, 3))
        pack[pl.ds(tile_row(0, m, 3), TILE), :] = jnp.where(upper, one, two)
        begin([rs_copy(0, 0, m), rs_copy(1, 0, m)])
        for kind in (1, 2):
            for u, (sup, col) in enumerate(UNITS[kind]):
                if col != m:
                    continue
                for b in range(2):
                    nc = ncol[pl.ds(4 * m + 2 * core + b, 1), :]
                    for a in range(4):
                        nr = nrow[pl.ds((4 * sup + a) * TILE, TILE), :]
                        pack[pl.ds(tile_row(kind, 2 * u + b, a), TILE), :] = nr + nc - 2.0 * block(4 * sup + a, b)
                begin([rs_copy(st, 0, 2 * u + b) for st in (2 * kind, 2 * kind + 1) for b in range(2)])

    def pm_tiles(half):
        for ch in (2 * half, 2 * half + 1):
            pre_pm(ch).wait_recv()
            mine = pl.ds(al(ch * BLK + core * HALF), HALF)
            pack[pl.ds(base(ch % 2, 4 + half), HALF), :] = pml[mine, :] + pmr[pl.ds(ch * HALF, HALF), :]
            begin([rs_copy(ch % 2, 0, 4 + half)])

    def open_step(finish_last):
        pm_tiles(0)
        for piece in range(4):
            pre_bf16(piece).wait_recv()
        finish_last()
        gs = []
        for m in range(2):
            gs.append(products(m))
            norms(m)
        begin([pre_pm(3), pre_bf16(7)])
        for m in range(2):
            tiles(m, gs[m])
        pm_tiles(1)
        for m in range(2, 4):
            for piece in range(2 * m, 2 * m + 2):
                pre_bf16(piece).wait_recv()
            g = products(m)
            norms(m)
            tiles(m, g)

    for cp in loads[4:]:
        cp.wait()
    for ch in range(4):
        loads[ch].wait()
        starts = (ch * BLK, ch * BLK + HALF)
        partial_pm(ch * BLK, [prepare(start, out_ref[pl.ds(start, HALF), :]) for start in starts])
        if ch == 0:
            pl.semaphore_wait(barrier, 10)
        if ch < 3:
            begin([pre_pm(ch)])
        begin([pre_bf16(piece) for piece in (2 * ch, 2 * ch + 1) if piece < 7])
    open_step(lambda: None)

    def one_step(step_index, carry):
        def row_sums(st, k, kern):
            place = pieces[k][0] + st % 2 * HALF
            slot, r = div(place, TILE), rem(place, TILE)

            def by_rows(vals):
                rs = jnp.sum(vals, axis=1, keepdims=True)
                return jnp.sum(jnp.where(lane_o == sub_o + r, rs, 0.0), axis=0, keepdims=True)

            def by_cols(vals):
                return jnp.sum(vals, axis=0, keepdims=True)

            if st > 1:
                sup, m = UNITS[st // 2][k // 2]
                return [(4 * sup + slot, by_rows(kern)), (4 * m + 2 * core + k % 2, by_cols(kern))]
            both = div(slot, 3)
            up_one = div(slot + 1, 2)
            i0 = (1 - both) * ((1 - core) * (slot + up_one) + core * (1 + div(slot, 2))) + both * 2 * core
            j0 = (1 - both) * ((1 - core) * (1 - up_one) + core * (2 + up_one)) + both * 2 * core
            up = jnp.where(lane_o + 1000 * (1 - both) > sub_o + r, kern, 0.0)
            lo = jnp.where(lane_o + 1000 * (1 - both) < sub_o + r, kern, 0.0)
            nxt = 4 * k + 2 * core + 1
            return [(4 * k + i0, by_rows(up)), (4 * k + j0, by_cols(up)), (nxt, by_rows(lo)), (nxt, by_cols(lo))]

        def advance(st, s):
            parts = [[], [], []]
            if s == 4 and st == STREAMS - 1:
                for d in range(3):
                    arrive(srecv.at[0, d], s_recv.at[0, d])
                    svec[1, d] = svec[0, d] + srecv[0, d, 0] + srecv[0, d, 1] + srecv[0, d, 2]
                    begin(s_copies(1, d))
            if s == 5 and st == STREAMS - 1:
                tot = jnp.zeros((16, TILE), F32)
                for d in range(3):
                    arrive(srecv.at[1, d], s_recv.at[1, d])
                    tot = tot + ((svec[1, d] + srecv[1, d, 0]) + (srecv[1, d, 1] + srecv[1, d, 2]))
                stot[...] = tot
                begin([sp_copy()])
            kerns = {}
            for k in (range(COLORS) if s < 2 else (0, 3, 1, 4, 2, 5)):
                if s < 2:
                    peer, length, keep, give = halves[k][s]
                    rs_copy(st, s, k).wait_recv()
                    packed(st, k, keeps[k][s], length)[...] += (r0, r1)[s][st, k]
                    begin([rs_copy(st, 1, k)] if s == 0 else x_copies(st, 0, k))
                    continue
                if k < 3:
                    sem = x_recv.at[st, s - 2, k] if s < 4 else (near_recv, far_recv)[s - 4].at[st, k]
                    pair_arrive((OWN, OWN, OWN // 2, QUARTER // 2)[s - 2], sem)
                if s == 2:
                    r3[st, k, coords[dims(k)[2]]] = packed(st, k, pieces[k][0], OWN)[...] + r2[st, k, 0] + r2[st, k, 1] + r2[st, k, 2]
                    begin(x_copies(st, 1, k))
                elif s == 3:
                    full = (r3[st, k, 0] + r3[st, k, 1]) + (r3[st, k, 2] + r3[st, k, 3])
                    kern = full if st < 2 and k >= 4 else jnp.exp(-jnp.maximum(full, 0.0) / bandwidth)
                    gathered(st, k, pieces[k][0], OWN)[...] = kern.astype(BF16)
                    begin(gather_copies(st, k, 0))
                    kerns[k] = kern
                elif s == 4:
                    begin([dd_copy(st, k, 0)])
                    for j in NEAR_FIRST:
                        begin(gather_copies(st, k, j))
                else:
                    begin([dd_copy(st, k, j) for j in NEAR_FIRST])
            if s == 3:
                for k, kern in kerns.items():
                    if st > 1 or k < 4:
                        parts[k % 3] += row_sums(st, k, kern)
                for d in range(3):
                    if st == 0:
                        svec[0, d] = jnp.zeros((16, TILE), F32)
                    for block, line in parts[d]:
                        svec[0, d, pl.ds(block, 1), :] += line
                    if st == STREAMS - 1:
                        begin(s_copies(0, d))
        def unpack_wait(kind):
            for st in (2 * kind, 2 * kind + 1):
                arrive(kg.at[core, 0:COLORS * HALF], dd_recv.at[st])

        def unpack(kind):
            for c in range(2):
                if kind > 0:
                    for k in range(COLORS):
                        sup, m = UNITS[kind][k // 2]
                        jrng = pl.ds((4 * m + 2 * c + k % 2) * TILE, TILE)
                        for a in range(4):
                            srng = pl.ds((4 * sup + a) * TILE, TILE)
                            kfull[jrng, srng] = kfull[srng, jrng].T
                    continue
                for sup in range(4):
                    for t, (i, j) in enumerate(OFFS[c]):
                        src = kg[c, pl.ds(tile_row(0, sup, t), TILE), :]
                        ri, rj = pl.ds((4 * sup + i) * TILE, TILE), pl.ds((4 * sup + j) * TILE, TILE)
                        kfull[ri, rj] = src
                        kfull[rj, ri] = src.T
                    src = kg[c, pl.ds(tile_row(0, sup, 3), TILE), :]
                    srt = src.T
                    one = jnp.ones((TILE, TILE), BF16)
                    ra, rb = pl.ds((4 * sup + 2 * c) * TILE, TILE), pl.ds((4 * sup + 2 * c + 1) * TILE, TILE)
                    kfull[ra, ra] = jnp.where(upper, src, jnp.where(lower, srt, one))
                    kfull[rb, rb] = jnp.where(lower, src, jnp.where(upper, srt, one))

        def drive_parts():
            for q in range(8):
                rows = pl.ds(q * HALF, HALF)
                th = out_ref[rows, :]
                pulled[rows, :] = (th - mu_ref[...]) * lam_ref[...]
                scaled[rows, :] = rep_coef * th

        def drive():
            for q in range(8):
                rows = pl.ds(q * HALF, HALF)
                ch = q // 2
                pm = kg[q % 2, pl.ds(base(ch % 2, 4 + ch // 2), HALF), :]
                low = lax.dot_general(pm, fac_ref[...], NT, preferred_element_type=F32)
                adrv[rows, :] = ((pulled[rows, :] + low) + scaled[rows, :]).astype(BF16)

        def product(start):
            return jnp.dot(kfull[pl.ds(start, HALF), :], adrv[...], preferred_element_type=F32)

        def finish(start, acc, tot, held):
            rows = pl.ds(start, HALF)
            sums = []
            for blk in (start // TILE, start // TILE + 1):
                line = jnp.where(eye, jnp.broadcast_to(tot[blk:blk + 1, :], (TILE, TILE)), 0.0)
                sums.append(rep_coef * jnp.sum(line, axis=1, keepdims=True))
            sums = jnp.broadcast_to(jnp.concatenate(sums, axis=0), (HALF, TILE))
            new = []
            for t in range(width // TILE):
                cols = slice(t * TILE, (t + 1) * TILE)
                th = out_ref[rows, cols]
                phi = (sums * th - acc[:, cols]) / n_part
                new.append(th + step_size * phi)
            th = jnp.concatenate(new, axis=1)
            out_ref[rows, :] = th
            held.append(prepare(start, th))
            if start % BLK:
                partial_pm(start - HALF, held[-2:])

        def share(start):
            if start % BLK and start + HALF < ROWS:
                begin([pre_pm(start // BLK), pre_bf16(start // HALF - 1), pre_bf16(start // HALF)])
            elif start + BLK == ROWS:
                begin([pre_bf16(start // HALF)])

        drive_parts()
        def early_rounds(s):
            def one(st, c):
                advance(st, s)
                return c

            lax.fori_loop(0, STREAMS, one, 0)

        for s in range(3):
            early_rounds(s)
        for s in range(3, 6):
            for st in range(STREAMS):
                if s == 5 and st == STREAMS - 2:
                    unpack_wait(0)
                    unpack(0)
                    drive()
                advance(st, s)
        remote(pack.at[0:5120], pack.at[0:5120], pre_send, sp_recv, mate).wait_send()
        def update(starts, kind):
            tot = stot[...] + spart[...] + 1.0
            ahead = product(starts[0])
            unpack(kind)
            held = []
            for n, start in enumerate(starts):
                acc = ahead
                if n + 1 < len(starts):
                    ahead = product(starts[n + 1])
                if n:
                    share(starts[n - 1])
                if start + HALF == ROWS:
                    return lambda: finish(start, acc, tot, list(held))
                finish(start, acc, tot, held)
            share(starts[-1])

        unpack_wait(1)
        arrive(stot, sp_recv)
        update(range(0, BLK, HALF), 1)
        unpack_wait(2)
        finish_last = update(range(BLK, ROWS, HALF), 2)
        for st in range(STREAMS):
            total = pack.at[0:SENT + (SENT_SUMS if st == STREAMS - 1 else 0)]
            remote(total, total, sent.at[st], sp_recv, mate).wait_send()
        pl.when(step_index < NUM_STEPS - 1)(lambda: open_step(finish_last))
        pl.when(step_index == NUM_STEPS - 1)(finish_last)
        return carry

    lax.fori_loop(0, NUM_STEPS, one_step, 0)
    for ch in range(3):
        pre_pm(ch).wait_recv()
    for piece in range(7):
        pre_bf16(piece).wait_recv()
    total = pack.at[0:7 * 512 + 3 * HALF]
    remote(total, total, pre_send, sp_recv, mate).wait_send()


def solution(mesh):
    def run_steps(particles, prec_diag, mean_vec, low_rank):
        total_rows, width = particles.shape
        n_part = total_rows // mesh.shape["ens"]
        bandwidth = BAND_SCALE * width
        step_size = STEP_SCALE * width
        loc = width // (mesh.shape["slab"] * mesh.shape["feat"])
        rank = low_rank.shape[1]
        vm, dma = pltpu.VMEM, pltpu.SemaphoreType.DMA

        def local_steps(current, prec_loc, mean_loc, fac_loc):
            spec = pl.BlockSpec(memory_space=pltpu.VMEM)
            call = pl.pallas_call(
                functools.partial(_kernel, bandwidth, step_size, n_part),
                out_shape=jax.ShapeDtypeStruct((n_part, loc), F32),
                in_specs=[pl.BlockSpec(memory_space=pltpu.HBM)] * 4,
                out_specs=spec,
                scratch_shapes=[
                    vm((1, loc), F32), vm((1, loc), F32), vm((loc, rank), BF16),
                    vm((ROWS, 2 * loc), BF16), vm((ROWS, rank), F32), vm((ROWS // 2, rank), F32),
                    vm((ROWS, TILE), F32), vm((16, TILE), F32), vm((ROWS, loc), F32), vm((ROWS, loc), F32),
                    vm((3 * SROWS, TILE), F32),
                    vm((STREAMS, COLORS, HALF // 2, TILE), F32), vm((STREAMS, COLORS, QUARTER, TILE), F32),
                    vm((STREAMS, COLORS, 3, OWN, TILE), F32), vm((STREAMS, COLORS, 4, OWN, TILE), F32),
                    vm((2, SROWS, TILE), BF16), vm((ROWS, ROWS), BF16), vm((ROWS, loc), BF16),
                    vm((2, 3, 16, TILE), F32), vm((2, 3, 3, 16, TILE), F32), vm((16, TILE), F32), vm((16, TILE), F32),
                    dma((7,)), dma, dma((12,)), dma((STREAMS,)), dma((STREAMS, 2, COLORS)), dma((STREAMS, 2, 3)),
                    dma((STREAMS, 3)), dma((STREAMS, 3)), dma((STREAMS,)),
                    dma((2, 3)), dma,
                ],
                compiler_params=pltpu.CompilerParams(collective_id=0, has_side_effects=True, vmem_limit_bytes=50000000),
                name="svgd",
            )
            hbm = lambda x: pltpu.with_memory_space_constraint(x, pltpu.HBM)
            return call(hbm(current), hbm(prec_loc.reshape(1, loc)), hbm(mean_loc.reshape(1, loc)), hbm(fac_loc))

        sharded = jax.shard_map(
            local_steps,
            mesh=mesh,
            in_specs=(P("ens", FEAT_AXES), P(LEAD_AXES), P(LEAD_AXES), P(LEAD_AXES, None)),
            out_specs=P("ens", FEAT_AXES),
            check_vma=False,
        )
        return sharded(particles, prec_diag, mean_vec, low_rank)

    return run_steps
```

```python
import functools

import jax
import jax.numpy as jnp
from jax import lax
from jax.experimental import pallas as pl
from jax.experimental.pallas import tpu as pltpu
from jax.sharding import PartitionSpec as P

NUM_STEPS = 3
BAND_SCALE = 4.0
STEP_SCALE = 0.4
FEAT_AXES = ("slab", "feat")
LEAD_AXES = ("ens", "slab", "feat")

ROWS = 2048
TILE = 128
HALF = 256
BLK = 2 * HALF
COLORS = 6
SROWS = COLORS * BLK
PM_AT = ((0, 4), (1, 3), (0, 5), (1, 5))
STREAMS = 6
QUARTER = HALF // 4
UNITS = ((), ((0, 3), (0, 1), (0, 2)), ((1, 2), (1, 3), (2, 3)))
OFFS = (((0, 1), (2, 0), (3, 0)), ((1, 2), (1, 3), (2, 3)))
SENT = 3216
SENT_SUMS = 304
OWN = QUARTER // 4
PEERS = (2, 1, 3)
NEAR_FIRST = (1, 3, 2)
MESH = pl.DeviceIdType.MESH
NT = (((1,), (1,)), ((), ()))
F32, BF16 = jnp.float32, jnp.bfloat16


def div(a, b):
    return lax.div(a, jnp.int32(b))


def rem(a, b):
    return lax.rem(a, jnp.int32(b))


def _kernel(
    bandwidth, step_size, n_part,
    theta_ref, lam_hbm, mu_hbm, fac_hbm, out_ref,
    lam_ref, mu_ref, fac_ref,
    bfull, pml, pmr, nrow, ncol, pulled, scaled, pack, r0, r1, r2, r3, kg, kfull, adrv, svec, srecv, stot, spart,
    in_sem, pre_send, pre_recv, sent, rs_recv, x_recv, near_recv, far_recv, dd_recv, s_recv, sp_recv,
):
    width = out_ref.shape[1]
    rep_coef = 2.0 / bandwidth
    core = lax.axis_index("slab")
    feat = lax.axis_index("feat")
    coords = (rem(feat, 4), rem(div(feat, 4), 4), div(feat, 16))
    strides = (1, 4, 16)

    def chip(dim, coord):
        return {"feat": feat + (coord - coords[dim]) * strides[dim]}

    turned = [[coords[dim]] + [rem(coords[dim] + j, 4) for j in sorted(PEERS)] for dim in range(3)]

    def around(dim, j):
        return turned[dim][j]

    ring = [[chip(dim, turned[dim][j]) for j in range(4)] for dim in range(3)]
    low_bit = [rem(c, 2) for c in coords]
    pair_bit = [[rem(div(t + 1, 2), 2) for t in turned[dim]] for dim in range(3)]
    high_bit = [[div(t, 2) for t in turned[dim]] for dim in range(3)]

    mate = {"slab": 1 - core}

    def al(x, m=16):
        return pl.multiple_of(x, m)

    halves = []
    for k in range(COLORS):
        steps = []
        start, length, cur = 0, HALF, coords[k % 3]
        for s in range(2):
            if (k // 3 + s) % 2 == 0:
                other, bit = cur + 1 - 2 * low_bit[k % 3], pair_bit[k % 3][0]
            else:
                other, bit = 3 - cur, high_bit[k % 3][0]
            length = length // 2
            keep, give = start + bit * length, start + (1 - bit) * length
            start = keep
            steps.append((chip(k % 3, other), length, keep, give))
        halves.append(steps)

    def dims(k):
        return k % 3, (k + 1) % 3, (k + 2) % 3

    def moved(m, part):
        return 4 if m == 3 and part == 1 else m

    def base(st, k):
        return (st * COLORS + k) * HALF

    def tile_row(kind, k, a):
        return base(2 * kind + a // 2, moved(k, a // 2) if kind == 0 else k) + a % 2 * TILE

    keeps = [[al(step[2]) for step in steps] for steps in halves]
    gives = [[al(step[3]) for step in steps] for steps in halves]
    pieces = [[al(halves[k][1][2] + OWN * around(dims(k)[1], j)) for j in range(4)] for k in range(COLORS)]
    places = []
    for k in range(COLORS):
        one, two = (pair_bit, high_bit) if k < 3 else (high_bit, pair_bit)
        places.append([al(QUARTER * (2 * one[k % 3][j] + two[k % 3][j])) for j in range(4)])

    columns = [[al(m * BLK + (2 * core + n) * TILE, TILE) for n in range(2)] for m in range(4)]

    def packed(st, k, row, rows):
        return pack.at[pl.ds(al(base(st, k) + row), rows)]

    loads = [pltpu.make_async_copy(theta_ref.at[pl.ds(ch * BLK, BLK)], out_ref.at[pl.ds(ch * BLK, BLK)], in_sem.at[ch]) for ch in range(4)]
    loads += [
        pltpu.make_async_copy(src, dst, in_sem.at[4 + n])
        for n, (src, dst) in enumerate(((mu_hbm, mu_ref), (fac_hbm, fac_ref), (lam_hbm, lam_ref)))
    ]
    for cp in loads[4:] + loads[:1]:
        cp.start()
    barrier = pltpu.get_barrier_semaphore()
    pl.semaphore_signal(barrier, inc=1, device_id=mate, device_id_type=MESH)
    for dim in range(3):
        for j in PEERS:
            pl.semaphore_signal(barrier, inc=1, device_id=ring[dim][j], device_id_type=MESH)
    for cp in loads[1:4]:
        cp.start()

    row_i = lax.broadcasted_iota(jnp.int32, (TILE, TILE), 0)
    col_i = lax.broadcasted_iota(jnp.int32, (TILE, TILE), 1)
    eye, upper, lower = row_i == col_i, row_i < col_i, row_i > col_i
    sub_o = lax.broadcasted_iota(jnp.int32, (OWN, TILE), 0)
    lane_o = lax.broadcasted_iota(jnp.int32, (OWN, TILE), 1)

    def remote(src, dst, ssem, rsem, where):
        return pltpu.make_async_remote_copy(src_ref=src, dst_ref=dst, send_sem=ssem, recv_sem=rsem, device_id=where, device_id_type=MESH)

    def pre_bf16(piece):
        rows = pl.ds(piece * HALF, HALF)
        return remote(bfull.at[rows, 0:width], bfull.at[rows, width:2 * width], pre_send, pre_recv.at[piece], mate)

    def pre_pm(ch):
        src, dst = pml.at[pl.ds(al(ch * BLK + (1 - core) * HALF), HALF)], pmr.at[pl.ds(ch * HALF, HALF)]
        return remote(src, dst, pre_send, pre_recv.at[8 + ch], mate)

    def prepare(start, th):
        bfull[pl.ds(start, HALF), 0:width] = th.astype(BF16)
        return (th - mu_ref[...]).astype(BF16)

    def partial_pm(start, centered):
        for n, rows in enumerate(centered):
            pml[pl.ds(start + HALF * n, HALF), :] = jnp.dot(rows, fac_ref[...], preferred_element_type=F32)

    def begin(cps):
        for cp in cps:
            cp.start()

    def arrive(ref, sem):
        remote(ref, ref, sent.at[0], sem, mate).wait_recv()

    def pair_arrive(rows, sem):
        arrive(pack.at[0:6 * rows], sem)

    def rs_copy(st, s, k):
        peer, length, keep, give = halves[k][s]
        src = packed(st, k, gives[k][s], length)
        return remote(src, (r0, r1)[s].at[st, k], sent.at[st], rs_recv.at[st, s, k], peer)

    def gathered(st, k, row, rows):
        if st < 2:
            return kg.at[core, pl.ds(base(st, k) + row, rows)]
        sup, m = UNITS[st // 2][k // 2]
        return kfull.at[pl.ds(sup * BLK + st % 2 * HALF + row, rows), pl.ds(columns[m][k % 2], TILE)]

    def x_copies(st, e, k):
        d1, d2, d3 = dims(k)
        dim = (d2, d3)[e]
        cps = []
        for j in PEERS:
            if e == 0:
                src = packed(st, k, pieces[k][j], OWN)
                dst = r2.at[st, k, j - 1]
            else:
                src = dst = r3.at[st, k, coords[dim]]
            cps.append(remote(src, dst, sent.at[st], x_recv.at[st, e, k % 3], ring[dim][j]))
        return cps

    def gather_copies(st, k, j):
        d1, d2, d3 = dims(k)
        ref = gathered(st, k, pieces[k][(4 - j) % 4], OWN)
        cps = [remote(ref, ref, sent.at[st], far_recv.at[st, k % 3], ring[d1][i]) for i in PEERS]
        if j == 0:
            cps = [remote(ref, ref, sent.at[st], near_recv.at[st, k % 3], ring[d2][i]) for i in PEERS] + cps
        return cps

    def dd_copy(st, k, j):
        ref = gathered(st, k, keeps[k][1] if j == 0 else places[k][4 - j], QUARTER)
        return remote(ref, ref, sent.at[st], dd_recv.at[st], mate)

    def s_copies(ph, d):
        dim = ((d + 1) % 3, d)[ph]
        return [
            remote(svec.at[ph, d], srecv.at[ph, d, j - 1], sent.at[STREAMS - 1], s_recv.at[ph, d], ring[dim][j])
            for j in PEERS
        ]

    def sp_copy():
        return remote(stot, spart, sent.at[STREAMS - 1], sp_recv, mate)

    def products(m):
        mine = bfull[pl.ds(al(m * BLK + HALF * core), HALF), :]
        part = BLK if m == 3 else (m + 1) * HALF
        return [lax.dot_general(bfull[pl.ds(at, part), :], mine, NT, preferred_element_type=F32) for at in range(0, (m + 1) * BLK, part)]

    def norms(m):
        for i in range(4):
            rows = pl.ds((4 * m + i) * TILE, TILE)
            wide = bfull[rows, :].astype(F32)
            n = jnp.broadcast_to(jnp.sum(wide * wide, axis=1, keepdims=True), (TILE, TILE))
            nrow[rows, :] = n
            ncol[4 * m + i:4 * m + i + 1, :] = jnp.sum(jnp.where(eye, n, 0.0), axis=0, keepdims=True)

    def tiles(m, g):
        def block(blk, b):
            n, r = divmod(blk * TILE, BLK if m == 3 else (m + 1) * HALF)
            return g[n][r:r + TILE, b * TILE:(b + 1) * TILE]

        def tile(i, b):
            return block(4 * m + i, b)

        def dist(i, j):
            return nrow[pl.ds((4 * m + i) * TILE, TILE), :] + ncol[4 * m + j:4 * m + j + 1, :] - 2.0 * tile(i, j % 2)

        for t in range(3):
            pack[pl.ds(tile_row(0, m, t), TILE), :] = jnp.where(core == 0, dist(*OFFS[0][t]), dist(*OFFS[1][t]))
        one = jnp.where(core == 0, dist(0, 0), dist(2, 2))
        two = jnp.where(core == 0, dist(1, 1), dist(3, 3))
        pack[pl.ds(tile_row(0, m, 3), TILE), :] = jnp.where(upper, one, two)
        begin([rs_copy(part, 0, moved(m, part)) for part in range(2)])
        for kind in (1, 2):
            for u, (sup, col) in enumerate(UNITS[kind]):
                if col != m:
                    continue
                for b in range(2):
                    nc = ncol[pl.ds(4 * m + 2 * core + b, 1), :]
                    for a in range(4):
                        nr = nrow[pl.ds((4 * sup + a) * TILE, TILE), :]
                        pack[pl.ds(tile_row(kind, 2 * u + b, a), TILE), :] = nr + nc - 2.0 * block(4 * sup + a, b)
                begin([rs_copy(st, 0, 2 * u + b) for st in (2 * kind, 2 * kind + 1) for b in range(2)])

    def pm_tiles(chs):
        for ch in chs:
            pre_pm(ch).wait_recv()
            mine = pl.ds(al(ch * BLK + core * HALF), HALF)
            pack[pl.ds(base(*PM_AT[ch]), HALF), :] = pml[mine, :] + pmr[pl.ds(ch * HALF, HALF), :]
            begin([rs_copy(PM_AT[ch][0], 0, PM_AT[ch][1])])

    def open_step(finish_last):
        pm_tiles(range(3))
        for piece in range(4):
            pre_bf16(piece).wait_recv()
        finish_last()
        gs = []
        for m in range(2):
            gs.append(products(m))
            norms(m)
        begin([pre_pm(3), pre_bf16(7)])
        for m in range(2):
            tiles(m, gs[m])
        pm_tiles((3,))
        for m in range(2, 4):
            for piece in range(2 * m, 2 * m + 2):
                pre_bf16(piece).wait_recv()
            g = products(m)
            norms(m)
            tiles(m, g)

    for cp in loads[4:]:
        cp.wait()
    for ch in range(4):
        loads[ch].wait()
        starts = (ch * BLK, ch * BLK + HALF)
        partial_pm(ch * BLK, [prepare(start, out_ref[pl.ds(start, HALF), :]) for start in starts])
        if ch == 0:
            pl.semaphore_wait(barrier, 10)
        if ch < 3:
            begin([pre_pm(ch)])
        begin([pre_bf16(piece) for piece in (2 * ch, 2 * ch + 1) if piece < 7])
    open_step(lambda: None)

    def one_step(step_index, carry):
        def row_sums(st, k, kern):
            place = pieces[k][0] + st % 2 * HALF
            slot, r = div(place, TILE), rem(place, TILE)

            def by_rows(vals):
                rs = jnp.sum(vals, axis=1, keepdims=True)
                return jnp.sum(jnp.where(lane_o == sub_o + r, rs, 0.0), axis=0, keepdims=True)

            def by_cols(vals):
                return jnp.sum(vals, axis=0, keepdims=True)

            if st > 1:
                sup, m = UNITS[st // 2][k // 2]
                return [(4 * sup + slot, by_rows(kern)), (4 * m + 2 * core + k % 2, by_cols(kern))]
            m = min(k, 3)
            both = div(slot, 3)
            up_one = div(slot + 1, 2)
            i0 = (1 - both) * ((1 - core) * (slot + up_one) + core * (1 + div(slot, 2))) + both * 2 * core
            j0 = (1 - both) * ((1 - core) * (1 - up_one) + core * (2 + up_one)) + both * 2 * core
            up = jnp.where(lane_o + 1000 * (1 - both) > sub_o + r, kern, 0.0)
            lo = jnp.where(lane_o + 1000 * (1 - both) < sub_o + r, kern, 0.0)
            nxt = 4 * m + 2 * core + 1
            return [(4 * m + i0, by_rows(up)), (4 * m + j0, by_cols(up)), (nxt, by_rows(lo)), (nxt, by_cols(lo))]

        def advance(st, s):
            parts = [[], [], []]
            if s == 4 and st == STREAMS - 1:
                for d in range(3):
                    arrive(srecv.at[0, d], s_recv.at[0, d])
                    svec[1, d] = svec[0, d] + srecv[0, d, 0] + srecv[0, d, 1] + srecv[0, d, 2]
                    begin(s_copies(1, d))
            if s == 5 and st == STREAMS - 1:
                tot = jnp.zeros((16, TILE), F32)
                for d in range(3):
                    arrive(srecv.at[1, d], s_recv.at[1, d])
                    tot = tot + ((svec[1, d] + srecv[1, d, 0]) + (srecv[1, d, 1] + srecv[1, d, 2]))
                stot[...] = tot
                begin([sp_copy()])
            kerns = {}
            for k in (range(COLORS) if s < 2 else (0, 3, 1, 4, 2, 5)):
                if s < 2:
                    peer, length, keep, give = halves[k][s]
                    rs_copy(st, s, k).wait_recv()
                    packed(st, k, keeps[k][s], length)[...] += (r0, r1)[s][st, k]
                    begin([rs_copy(st, 1, k)] if s == 0 else x_copies(st, 0, k))
                    continue
                if k < 3:
                    sem = x_recv.at[st, s - 2, k] if s < 4 else (near_recv, far_recv)[s - 4].at[st, k]
                    pair_arrive((OWN, OWN, OWN // 2, QUARTER // 2)[s - 2], sem)
                if s == 2:
                    r3[st, k, coords[dims(k)[2]]] = packed(st, k, pieces[k][0], OWN)[...] + r2[st, k, 0] + r2[st, k, 1] + r2[st, k, 2]
                    begin(x_copies(st, 1, k))
                elif s == 3:
                    full = (r3[st, k, 0] + r3[st, k, 1]) + (r3[st, k, 2] + r3[st, k, 3])
                    kern = full if (st, k) in PM_AT else jnp.exp(-jnp.maximum(full, 0.0) / bandwidth)
                    gathered(st, k, pieces[k][0], OWN)[...] = kern.astype(BF16)
                    begin(gather_copies(st, k, 0))
                    kerns[k] = kern
                elif s == 4:
                    begin([dd_copy(st, k, 0)])
                    for j in NEAR_FIRST:
                        begin(gather_copies(st, k, j))
                else:
                    begin([dd_copy(st, k, j) for j in NEAR_FIRST])
            if s == 3:
                for k, kern in kerns.items():
                    if (st, k) not in PM_AT:
                        parts[k % 3] += row_sums(st, k, kern)
                for d in range(3):
                    if st == 0:
                        svec[0, d] = jnp.zeros((16, TILE), F32)
                    for block, line in parts[d]:
                        svec[0, d, pl.ds(block, 1), :] += line
                    if st == STREAMS - 1:
                        begin(s_copies(0, d))
        def unpack_wait(kind):
            for st in (2 * kind, 2 * kind + 1):
                arrive(kg.at[core, 0:COLORS * HALF], dd_recv.at[st])

        def unpack(kind):
            for c in range(2):
                if kind > 0:
                    for k in range(COLORS):
                        sup, m = UNITS[kind][k // 2]
                        jrng = pl.ds((4 * m + 2 * c + k % 2) * TILE, TILE)
                        for a in range(4):
                            srng = pl.ds((4 * sup + a) * TILE, TILE)
                            kfull[jrng, srng] = kfull[srng, jrng].T
                    continue
                for sup in range(4):
                    for t, (i, j) in enumerate(OFFS[c]):
                        src = kg[c, pl.ds(tile_row(0, sup, t), TILE), :]
                        ri, rj = pl.ds((4 * sup + i) * TILE, TILE), pl.ds((4 * sup + j) * TILE, TILE)
                        kfull[ri, rj] = src
                        kfull[rj, ri] = src.T
                    src = kg[c, pl.ds(tile_row(0, sup, 3), TILE), :]
                    srt = src.T
                    one = jnp.ones((TILE, TILE), BF16)
                    ra, rb = pl.ds((4 * sup + 2 * c) * TILE, TILE), pl.ds((4 * sup + 2 * c + 1) * TILE, TILE)
                    kfull[ra, ra] = jnp.where(upper, src, jnp.where(lower, srt, one))
                    kfull[rb, rb] = jnp.where(lower, src, jnp.where(upper, srt, one))

        def drive_parts():
            for q in range(8):
                rows = pl.ds(q * HALF, HALF)
                th = out_ref[rows, :]
                pulled[rows, :] = (th - mu_ref[...]) * lam_ref[...]
                scaled[rows, :] = rep_coef * th

        def drive():
            for q in range(8):
                rows = pl.ds(q * HALF, HALF)
                ch = q // 2
                pm = kg[q % 2, pl.ds(base(*PM_AT[ch]), HALF), :]
                low = lax.dot_general(pm, fac_ref[...], NT, preferred_element_type=F32)
                adrv[rows, :] = ((pulled[rows, :] + low) + scaled[rows, :]).astype(BF16)

        def product(start):
            return jnp.dot(kfull[pl.ds(start, HALF), :], adrv[...], preferred_element_type=F32)

        def finish(start, acc, tot, held):
            rows = pl.ds(start, HALF)
            sums = []
            for blk in (start // TILE, start // TILE + 1):
                line = jnp.where(eye, jnp.broadcast_to(tot[blk:blk + 1, :], (TILE, TILE)), 0.0)
                sums.append(rep_coef * jnp.sum(line, axis=1, keepdims=True))
            sums = jnp.broadcast_to(jnp.concatenate(sums, axis=0), (HALF, TILE))
            new = []
            for t in range(width // TILE):
                cols = slice(t * TILE, (t + 1) * TILE)
                th = out_ref[rows, cols]
                phi = (sums * th - acc[:, cols]) / n_part
                new.append(th + step_size * phi)
            th = jnp.concatenate(new, axis=1)
            out_ref[rows, :] = th
            held.append(prepare(start, th))
            if start % BLK:
                partial_pm(start - HALF, held[-2:])

        def share(start):
            if start % BLK and start + HALF < ROWS:
                begin([pre_pm(start // BLK), pre_bf16(start // HALF - 1), pre_bf16(start // HALF)])
            elif start + BLK == ROWS:
                begin([pre_bf16(start // HALF)])

        drive_parts()
        def early_rounds(s):
            def one(st, c):
                advance(st, s)
                return c

            lax.fori_loop(0, STREAMS, one, 0)

        for s in range(3):
            early_rounds(s)
        for s in range(3, 6):
            for st in range(STREAMS):
                if s == 5 and st == STREAMS - 2:
                    unpack_wait(0)
                    unpack(0)
                    drive()
                advance(st, s)
        remote(pack.at[0:5120], pack.at[0:5120], pre_send, sp_recv, mate).wait_send()
        def update(starts, kind):
            tot = stot[...] + spart[...] + 1.0
            ahead = product(starts[0])
            unpack(kind)
            held = []
            for n, start in enumerate(starts):
                acc = ahead
                if n + 1 < len(starts):
                    ahead = product(starts[n + 1])
                if n:
                    share(starts[n - 1])
                if start + HALF == ROWS:
                    return lambda: finish(start, acc, tot, list(held))
                finish(start, acc, tot, held)
            share(starts[-1])

        unpack_wait(1)
        arrive(stot, sp_recv)
        update(range(0, BLK, HALF), 1)
        unpack_wait(2)
        finish_last = update(range(BLK, ROWS, HALF), 2)
        for st in range(STREAMS):
            total = pack.at[0:SENT + (SENT_SUMS if st == STREAMS - 1 else 0)]
            remote(total, total, sent.at[st], sp_recv, mate).wait_send()
        pl.when(step_index < NUM_STEPS - 1)(lambda: open_step(finish_last))
        pl.when(step_index == NUM_STEPS - 1)(finish_last)
        return carry

    lax.fori_loop(0, NUM_STEPS, one_step, 0)
    for ch in range(3):
        pre_pm(ch).wait_recv()
    for piece in range(7):
        pre_bf16(piece).wait_recv()
    total = pack.at[0:7 * 512 + 3 * HALF]
    remote(total, total, pre_send, sp_recv, mate).wait_send()


def solution(mesh):
    def run_steps(particles, prec_diag, mean_vec, low_rank):
        total_rows, width = particles.shape
        n_part = total_rows // mesh.shape["ens"]
        bandwidth = BAND_SCALE * width
        step_size = STEP_SCALE * width
        loc = width // (mesh.shape["slab"] * mesh.shape["feat"])
        rank = low_rank.shape[1]
        vm, dma = pltpu.VMEM, pltpu.SemaphoreType.DMA

        def local_steps(current, prec_loc, mean_loc, fac_loc):
            spec = pl.BlockSpec(memory_space=pltpu.VMEM)
            call = pl.pallas_call(
                functools.partial(_kernel, bandwidth, step_size, n_part),
                out_shape=jax.ShapeDtypeStruct((n_part, loc), F32),
                in_specs=[pl.BlockSpec(memory_space=pltpu.HBM)] * 4,
                out_specs=spec,
                scratch_shapes=[
                    vm((1, loc), F32), vm((1, loc), F32), vm((loc, rank), BF16),
                    vm((ROWS, 2 * loc), BF16), vm((ROWS, rank), F32), vm((ROWS // 2, rank), F32),
                    vm((ROWS, TILE), F32), vm((16, TILE), F32), vm((ROWS, loc), F32), vm((ROWS, loc), F32),
                    vm((3 * SROWS, TILE), F32),
                    vm((STREAMS, COLORS, HALF // 2, TILE), F32), vm((STREAMS, COLORS, QUARTER, TILE), F32),
                    vm((STREAMS, COLORS, 3, OWN, TILE), F32), vm((STREAMS, COLORS, 4, OWN, TILE), F32),
                    vm((2, SROWS, TILE), BF16), vm((ROWS, ROWS), BF16), vm((ROWS, loc), BF16),
                    vm((2, 3, 16, TILE), F32), vm((2, 3, 3, 16, TILE), F32), vm((16, TILE), F32), vm((16, TILE), F32),
                    dma((7,)), dma, dma((12,)), dma((STREAMS,)), dma((STREAMS, 2, COLORS)), dma((STREAMS, 2, 3)),
                    dma((STREAMS, 3)), dma((STREAMS, 3)), dma((STREAMS,)),
                    dma((2, 3)), dma,
                ],
                compiler_params=pltpu.CompilerParams(collective_id=0, has_side_effects=True, vmem_limit_bytes=50000000),
                name="svgd",
            )
            hbm = lambda x: pltpu.with_memory_space_constraint(x, pltpu.HBM)
            return call(hbm(current), hbm(prec_loc.reshape(1, loc)), hbm(mean_loc.reshape(1, loc)), hbm(fac_loc))

        sharded = jax.shard_map(
            local_steps,
            mesh=mesh,
            in_specs=(P("ens", FEAT_AXES), P(LEAD_AXES), P(LEAD_AXES), P(LEAD_AXES, None)),
            out_specs=P("ens", FEAT_AXES),
            check_vma=False,
        )
        return sharded(particles, prec_diag, mean_vec, low_rank)

    return run_steps
```

```python
import functools

import jax
import jax.numpy as jnp
from jax import lax
from jax.experimental import pallas as pl
from jax.experimental.pallas import tpu as pltpu
from jax.sharding import PartitionSpec as P

NUM_STEPS = 3
BAND_SCALE = 4.0
STEP_SCALE = 0.4
FEAT_AXES = ("slab", "feat")
LEAD_AXES = ("ens", "slab", "feat")

ROWS = 2048
TILE = 128
HALF = 256
BLK = 2 * HALF
COLORS = 6
SROWS = COLORS * BLK
PM_AT = ((0, 0), (0, 1), (0, 5), (1, 5))
DIAG_AT = (((1, 0), (1, 1)), ((0, 4), (1, 4)), ((0, 2), (0, 3)), ((1, 2), (1, 3)))
STREAMS = 6
QUARTER = HALF // 4
UNITS = ((), ((0, 3), (0, 1), (0, 2)), ((1, 2), (1, 3), (2, 3)))
OFFS = (((0, 1), (2, 0), (3, 0)), ((1, 2), (1, 3), (2, 3)))
SENT = 3216
SENT_SUMS = 304
OWN = QUARTER // 4
PEERS = (2, 1, 3)
NEAR_FIRST = (1, 3, 2)
MESH = pl.DeviceIdType.MESH
NT = (((1,), (1,)), ((), ()))
F32, BF16 = jnp.float32, jnp.bfloat16


def div(a, b):
    return lax.div(a, jnp.int32(b))


def rem(a, b):
    return lax.rem(a, jnp.int32(b))


def _kernel(
    bandwidth, step_size, n_part,
    theta_ref, lam_hbm, mu_hbm, fac_hbm, out_ref,
    lam_ref, mu_ref, fac_ref,
    bfull, pml, pmr, nrow, ncol, pulled, scaled, pack, r0, r1, r2, r3, kg, kfull, adrv, svec, srecv, stot, spart,
    in_sem, pre_send, pre_recv, sent, rs_recv, x_recv, near_recv, far_recv, dd_recv, s_recv, sp_recv,
):
    width = out_ref.shape[1]
    rep_coef = 2.0 / bandwidth
    core = lax.axis_index("slab")
    feat = lax.axis_index("feat")
    coords = (rem(feat, 4), rem(div(feat, 4), 4), div(feat, 16))
    strides = (1, 4, 16)

    def chip(dim, coord):
        return {"feat": feat + (coord - coords[dim]) * strides[dim]}

    turned = [[coords[dim]] + [rem(coords[dim] + j, 4) for j in sorted(PEERS)] for dim in range(3)]

    def around(dim, j):
        return turned[dim][j]

    ring = [[chip(dim, turned[dim][j]) for j in range(4)] for dim in range(3)]
    low_bit = [rem(c, 2) for c in coords]
    pair_bit = [[rem(div(t + 1, 2), 2) for t in turned[dim]] for dim in range(3)]
    high_bit = [[div(t, 2) for t in turned[dim]] for dim in range(3)]

    mate = {"slab": 1 - core}

    def al(x, m=16):
        return pl.multiple_of(x, m)

    halves = []
    for k in range(COLORS):
        steps = []
        start, length, cur = 0, HALF, coords[k % 3]
        for s in range(2):
            if (k // 3 + s) % 2 == 0:
                other, bit = cur + 1 - 2 * low_bit[k % 3], pair_bit[k % 3][0]
            else:
                other, bit = 3 - cur, high_bit[k % 3][0]
            length = length // 2
            keep, give = start + bit * length, start + (1 - bit) * length
            start = keep
            steps.append((chip(k % 3, other), length, keep, give))
        halves.append(steps)

    def dims(k):
        return k % 3, (k + 1) % 3, (k + 2) % 3

    def base(st, k):
        return (st * COLORS + k) * HALF

    def tile_row(kind, k, a):
        st, k = DIAG_AT[k][a // 2] if kind == 0 else (2 * kind + a // 2, k)
        return base(st, k) + a % 2 * TILE

    keeps = [[al(step[2]) for step in steps] for steps in halves]
    gives = [[al(step[3]) for step in steps] for steps in halves]
    pieces = [[al(halves[k][1][2] + OWN * around(dims(k)[1], j)) for j in range(4)] for k in range(COLORS)]
    places = []
    for k in range(COLORS):
        one, two = (pair_bit, high_bit) if k < 3 else (high_bit, pair_bit)
        places.append([al(QUARTER * (2 * one[k % 3][j] + two[k % 3][j])) for j in range(4)])

    columns = [[al(m * BLK + (2 * core + n) * TILE, TILE) for n in range(2)] for m in range(4)]

    def packed(st, k, row, rows):
        return pack.at[pl.ds(al(base(st, k) + row), rows)]

    loads = [pltpu.make_async_copy(theta_ref.at[pl.ds(ch * BLK, BLK)], out_ref.at[pl.ds(ch * BLK, BLK)], in_sem.at[ch]) for ch in range(4)]
    loads += [
        pltpu.make_async_copy(src, dst, in_sem.at[4 + n])
        for n, (src, dst) in enumerate(((mu_hbm, mu_ref), (fac_hbm, fac_ref), (lam_hbm, lam_ref)))
    ]
    for cp in loads[4:] + loads[:1]:
        cp.start()
    barrier = pltpu.get_barrier_semaphore()
    pl.semaphore_signal(barrier, inc=1, device_id=mate, device_id_type=MESH)
    for dim in range(3):
        for j in PEERS:
            pl.semaphore_signal(barrier, inc=1, device_id=ring[dim][j], device_id_type=MESH)
    for cp in loads[1:4]:
        cp.start()

    row_i = lax.broadcasted_iota(jnp.int32, (TILE, TILE), 0)
    col_i = lax.broadcasted_iota(jnp.int32, (TILE, TILE), 1)
    eye, upper, lower = row_i == col_i, row_i < col_i, row_i > col_i
    sub_o = lax.broadcasted_iota(jnp.int32, (OWN, TILE), 0)
    lane_o = lax.broadcasted_iota(jnp.int32, (OWN, TILE), 1)

    def remote(src, dst, ssem, rsem, where):
        return pltpu.make_async_remote_copy(src_ref=src, dst_ref=dst, send_sem=ssem, recv_sem=rsem, device_id=where, device_id_type=MESH)

    def pre_bf16(piece):
        rows = pl.ds(piece * HALF, HALF)
        return remote(bfull.at[rows, 0:width], bfull.at[rows, width:2 * width], pre_send, pre_recv.at[piece], mate)

    def pre_pm(ch):
        src, dst = pml.at[pl.ds(al(ch * BLK + (1 - core) * HALF), HALF)], pmr.at[pl.ds(ch * HALF, HALF)]
        return remote(src, dst, pre_send, pre_recv.at[8 + ch], mate)

    def prepare(start, th):
        bfull[pl.ds(start, HALF), 0:width] = th.astype(BF16)
        return (th - mu_ref[...]).astype(BF16)

    def partial_pm(start, centered):
        for n, rows in enumerate(centered):
            pml[pl.ds(start + HALF * n, HALF), :] = jnp.dot(rows, fac_ref[...], preferred_element_type=F32)

    def begin(cps):
        for cp in cps:
            cp.start()

    def arrive(ref, sem):
        remote(ref, ref, sent.at[0], sem, mate).wait_recv()

    def pair_arrive(rows, sem):
        arrive(pack.at[0:6 * rows], sem)

    def rs_copy(st, s, k):
        peer, length, keep, give = halves[k][s]
        src = packed(st, k, gives[k][s], length)
        return remote(src, (r0, r1)[s].at[st, k], sent.at[st], rs_recv.at[st, s, k], peer)

    def gathered(st, k, row, rows):
        if st < 2:
            return kg.at[core, pl.ds(base(st, k) + row, rows)]
        sup, m = UNITS[st // 2][k // 2]
        return kfull.at[pl.ds(sup * BLK + st % 2 * HALF + row, rows), pl.ds(columns[m][k % 2], TILE)]

    def x_copies(st, e, k):
        d1, d2, d3 = dims(k)
        dim = (d2, d3)[e]
        cps = []
        for j in PEERS:
            if e == 0:
                src = packed(st, k, pieces[k][j], OWN)
                dst = r2.at[st, k, j - 1]
            else:
                src = dst = r3.at[st, k, coords[dim]]
            cps.append(remote(src, dst, sent.at[st], x_recv.at[st, e, k % 3], ring[dim][j]))
        return cps

    def gather_copies(st, k, j):
        d1, d2, d3 = dims(k)
        ref = gathered(st, k, pieces[k][(4 - j) % 4], OWN)
        cps = [remote(ref, ref, sent.at[st], far_recv.at[st, k % 3], ring[d1][i]) for i in PEERS]
        if j == 0:
            cps = [remote(ref, ref, sent.at[st], near_recv.at[st, k % 3], ring[d2][i]) for i in PEERS] + cps
        return cps

    def dd_copy(st, k, j):
        ref = gathered(st, k, keeps[k][1] if j == 0 else places[k][4 - j], QUARTER)
        return remote(ref, ref, sent.at[st], dd_recv.at[st], mate)

    def s_copies(ph, d):
        dim = ((d + 1) % 3, d)[ph]
        return [
            remote(svec.at[ph, d], srecv.at[ph, d, j - 1], sent.at[STREAMS - 1], s_recv.at[ph, d], ring[dim][j])
            for j in PEERS
        ]

    def sp_copy():
        return remote(stot, spart, sent.at[STREAMS - 1], sp_recv, mate)

    def products(m):
        mine = bfull[pl.ds(al(m * BLK + HALF * core), HALF), :]
        part = BLK if m == 3 else (m + 1) * HALF
        return [lax.dot_general(bfull[pl.ds(at, part), :], mine, NT, preferred_element_type=F32) for at in range(0, (m + 1) * BLK, part)]

    def norms(m):
        for i in range(4):
            rows = pl.ds((4 * m + i) * TILE, TILE)
            wide = bfull[rows, :].astype(F32)
            n = jnp.broadcast_to(jnp.sum(wide * wide, axis=1, keepdims=True), (TILE, TILE))
            nrow[rows, :] = n
            ncol[4 * m + i:4 * m + i + 1, :] = jnp.sum(jnp.where(eye, n, 0.0), axis=0, keepdims=True)

    def tiles(m, g):
        def block(blk, b):
            n, r = divmod(blk * TILE, BLK if m == 3 else (m + 1) * HALF)
            return g[n][r:r + TILE, b * TILE:(b + 1) * TILE]

        def tile(i, b):
            return block(4 * m + i, b)

        def dist(i, j):
            return nrow[pl.ds((4 * m + i) * TILE, TILE), :] + ncol[4 * m + j:4 * m + j + 1, :] - 2.0 * tile(i, j % 2)

        for t in range(3):
            pack[pl.ds(tile_row(0, m, t), TILE), :] = jnp.where(core == 0, dist(*OFFS[0][t]), dist(*OFFS[1][t]))
        one = jnp.where(core == 0, dist(0, 0), dist(2, 2))
        two = jnp.where(core == 0, dist(1, 1), dist(3, 3))
        pack[pl.ds(tile_row(0, m, 3), TILE), :] = jnp.where(upper, one, two)
        begin([rs_copy(st, 0, k) for st, k in DIAG_AT[m]])
        for kind in (1, 2):
            for u, (sup, col) in enumerate(UNITS[kind]):
                if col != m:
                    continue
                for b in range(2):
                    nc = ncol[pl.ds(4 * m + 2 * core + b, 1), :]
                    for a in range(4):
                        nr = nrow[pl.ds((4 * sup + a) * TILE, TILE), :]
                        pack[pl.ds(tile_row(kind, 2 * u + b, a), TILE), :] = nr + nc - 2.0 * block(4 * sup + a, b)
                begin([rs_copy(st, 0, 2 * u + b) for st in (2 * kind, 2 * kind + 1) for b in range(2)])

    def pm_tiles(chs):
        for ch in chs:
            pre_pm(ch).wait_recv()
            mine = pl.ds(al(ch * BLK + core * HALF), HALF)
            pack[pl.ds(base(*PM_AT[ch]), HALF), :] = pml[mine, :] + pmr[pl.ds(ch * HALF, HALF), :]
            begin([rs_copy(PM_AT[ch][0], 0, PM_AT[ch][1])])

    def open_step(finish_last):
        pm_tiles(range(3))
        for piece in range(4):
            pre_bf16(piece).wait_recv()
        finish_last()
        one, zero = products(1), products(0)
        for m in range(2):
            norms(m)
        begin([pre_pm(3), pre_bf16(7)])
        tiles(1, one)
        tiles(0, zero)
        pm_tiles((3,))
        for m in range(2, 4):
            for piece in range(2 * m, 2 * m + 2):
                pre_bf16(piece).wait_recv()
            g = products(m)
            norms(m)
            tiles(m, g)

    for cp in loads[4:]:
        cp.wait()
    for ch in range(4):
        loads[ch].wait()
        starts = (ch * BLK, ch * BLK + HALF)
        partial_pm(ch * BLK, [prepare(start, out_ref[pl.ds(start, HALF), :]) for start in starts])
        if ch == 0:
            pl.semaphore_wait(barrier, 10)
        if ch < 3:
            begin([pre_pm(ch)])
        begin([pre_bf16(piece) for piece in (2 * ch, 2 * ch + 1) if piece < 7])
    open_step(lambda: None)

    def one_step(step_index, carry):
        def row_sums(st, k, kern):
            m, part = (0, st % 2) if st > 1 else [(m, part) for m in range(4) for part in range(2) if DIAG_AT[m][part] == (st, k)][0]
            place = pieces[k][0] + part * HALF
            slot, r = div(place, TILE), rem(place, TILE)

            def by_rows(vals):
                rs = jnp.sum(vals, axis=1, keepdims=True)
                return jnp.sum(jnp.where(lane_o == sub_o + r, rs, 0.0), axis=0, keepdims=True)

            def by_cols(vals):
                return jnp.sum(vals, axis=0, keepdims=True)

            if st > 1:
                sup, m = UNITS[st // 2][k // 2]
                return [(4 * sup + slot, by_rows(kern)), (4 * m + 2 * core + k % 2, by_cols(kern))]
            both = div(slot, 3)
            up_one = div(slot + 1, 2)
            i0 = (1 - both) * ((1 - core) * (slot + up_one) + core * (1 + div(slot, 2))) + both * 2 * core
            j0 = (1 - both) * ((1 - core) * (1 - up_one) + core * (2 + up_one)) + both * 2 * core
            up = jnp.where(lane_o + 1000 * (1 - both) > sub_o + r, kern, 0.0)
            lo = jnp.where(lane_o + 1000 * (1 - both) < sub_o + r, kern, 0.0)
            nxt = 4 * m + 2 * core + 1
            return [(4 * m + i0, by_rows(up)), (4 * m + j0, by_cols(up)), (nxt, by_rows(lo)), (nxt, by_cols(lo))]

        def advance(st, s):
            parts = [[], [], []]
            if s == 4 and st == STREAMS - 1:
                for d in range(3):
                    arrive(srecv.at[0, d], s_recv.at[0, d])
                    svec[1, d] = svec[0, d] + srecv[0, d, 0] + srecv[0, d, 1] + srecv[0, d, 2]
                    begin(s_copies(1, d))
            if s == 5 and st == STREAMS - 1:
                tot = jnp.zeros((16, TILE), F32)
                for d in range(3):
                    arrive(srecv.at[1, d], s_recv.at[1, d])
                    tot = tot + ((svec[1, d] + srecv[1, d, 0]) + (srecv[1, d, 1] + srecv[1, d, 2]))
                stot[...] = tot
                begin([sp_copy()])
            kerns = {}
            for k in (range(COLORS) if s < 2 else (0, 3, 1, 4, 2, 5)):
                if s < 2:
                    peer, length, keep, give = halves[k][s]
                    rs_copy(st, s, k).wait_recv()
                    packed(st, k, keeps[k][s], length)[...] += (r0, r1)[s][st, k]
                    begin([rs_copy(st, 1, k)] if s == 0 else x_copies(st, 0, k))
                    continue
                if k < 3:
                    sem = x_recv.at[st, s - 2, k] if s < 4 else (near_recv, far_recv)[s - 4].at[st, k]
                    pair_arrive((OWN, OWN, OWN // 2, QUARTER // 2)[s - 2], sem)
                if s == 2:
                    r3[st, k, coords[dims(k)[2]]] = packed(st, k, pieces[k][0], OWN)[...] + r2[st, k, 0] + r2[st, k, 1] + r2[st, k, 2]
                    begin(x_copies(st, 1, k))
                elif s == 3:
                    full = (r3[st, k, 0] + r3[st, k, 1]) + (r3[st, k, 2] + r3[st, k, 3])
                    kern = full if (st, k) in PM_AT else jnp.exp(-jnp.maximum(full, 0.0) / bandwidth)
                    gathered(st, k, pieces[k][0], OWN)[...] = kern.astype(BF16)
                    begin(gather_copies(st, k, 0))
                    kerns[k] = kern
                elif s == 4:
                    begin([dd_copy(st, k, 0)])
                    for j in NEAR_FIRST:
                        begin(gather_copies(st, k, j))
                else:
                    begin([dd_copy(st, k, j) for j in NEAR_FIRST])
            if s == 3:
                for k, kern in kerns.items():
                    if (st, k) not in PM_AT:
                        parts[k % 3] += row_sums(st, k, kern)
                for d in range(3):
                    if st == 0:
                        svec[0, d] = jnp.zeros((16, TILE), F32)
                    for block, line in parts[d]:
                        svec[0, d, pl.ds(block, 1), :] += line
                    if st == STREAMS - 1:
                        begin(s_copies(0, d))
        def unpack_wait(kind):
            for st in (2 * kind, 2 * kind + 1):
                arrive(kg.at[core, 0:COLORS * HALF], dd_recv.at[st])

        def unpack(kind):
            for c in range(2):
                if kind > 0:
                    for k in range(COLORS):
                        sup, m = UNITS[kind][k // 2]
                        jrng = pl.ds((4 * m + 2 * c + k % 2) * TILE, TILE)
                        for a in range(4):
                            srng = pl.ds((4 * sup + a) * TILE, TILE)
                            kfull[jrng, srng] = kfull[srng, jrng].T
                    continue
                for sup in range(4):
                    for t, (i, j) in enumerate(OFFS[c]):
                        src = kg[c, pl.ds(tile_row(0, sup, t), TILE), :]
                        ri, rj = pl.ds((4 * sup + i) * TILE, TILE), pl.ds((4 * sup + j) * TILE, TILE)
                        kfull[ri, rj] = src
                        kfull[rj, ri] = src.T
                    src = kg[c, pl.ds(tile_row(0, sup, 3), TILE), :]
                    srt = src.T
                    one = jnp.ones((TILE, TILE), BF16)
                    ra, rb = pl.ds((4 * sup + 2 * c) * TILE, TILE), pl.ds((4 * sup + 2 * c + 1) * TILE, TILE)
                    kfull[ra, ra] = jnp.where(upper, src, jnp.where(lower, srt, one))
                    kfull[rb, rb] = jnp.where(lower, src, jnp.where(upper, srt, one))

        def drive_parts():
            for q in range(8):
                rows = pl.ds(q * HALF, HALF)
                th = out_ref[rows, :]
                pulled[rows, :] = (th - mu_ref[...]) * lam_ref[...]
                scaled[rows, :] = rep_coef * th

        def drive():
            for q in range(8):
                rows = pl.ds(q * HALF, HALF)
                ch = q // 2
                pm = kg[q % 2, pl.ds(base(*PM_AT[ch]), HALF), :]
                low = lax.dot_general(pm, fac_ref[...], NT, preferred_element_type=F32)
                adrv[rows, :] = ((pulled[rows, :] + low) + scaled[rows, :]).astype(BF16)

        def product(start):
            return jnp.dot(kfull[pl.ds(start, HALF), :], adrv[...], preferred_element_type=F32)

        def finish(start, acc, tot, held):
            rows = pl.ds(start, HALF)
            sums = []
            for blk in (start // TILE, start // TILE + 1):
                line = jnp.where(eye, jnp.broadcast_to(tot[blk:blk + 1, :], (TILE, TILE)), 0.0)
                sums.append(rep_coef * jnp.sum(line, axis=1, keepdims=True))
            sums = jnp.broadcast_to(jnp.concatenate(sums, axis=0), (HALF, TILE))
            new = []
            for t in range(width // TILE):
                cols = slice(t * TILE, (t + 1) * TILE)
                th = out_ref[rows, cols]
                phi = (sums * th - acc[:, cols]) / n_part
                new.append(th + step_size * phi)
            th = jnp.concatenate(new, axis=1)
            out_ref[rows, :] = th
            held.append(prepare(start, th))
            if start % BLK:
                partial_pm(start - HALF, held[-2:])

        def share(start):
            if start % BLK and start + HALF < ROWS:
                begin([pre_pm(start // BLK), pre_bf16(start // HALF - 1), pre_bf16(start // HALF)])
            elif start + BLK == ROWS:
                begin([pre_bf16(start // HALF)])

        drive_parts()
        def early_rounds(s):
            def one(st, c):
                advance(st, s)
                return c

            lax.fori_loop(0, STREAMS, one, 0)

        for s in range(3):
            early_rounds(s)
        for s in range(3, 6):
            for st in range(STREAMS):
                if s == 5 and st == STREAMS - 2:
                    unpack_wait(0)
                    unpack(0)
                    drive()
                advance(st, s)
        remote(pack.at[0:5120], pack.at[0:5120], pre_send, sp_recv, mate).wait_send()
        def update(starts, kind):
            tot = stot[...] + spart[...] + 1.0
            ahead = product(starts[0])
            unpack(kind)
            held = []
            for n, start in enumerate(starts):
                acc = ahead
                if n + 1 < len(starts):
                    ahead = product(starts[n + 1])
                if n:
                    share(starts[n - 1])
                if start + HALF == ROWS:
                    return lambda: finish(start, acc, tot, list(held))
                finish(start, acc, tot, held)
            share(starts[-1])

        unpack_wait(1)
        arrive(stot, sp_recv)
        update(range(0, BLK, HALF), 1)
        unpack_wait(2)
        finish_last = update(range(BLK, ROWS, HALF), 2)
        for st in range(STREAMS):
            total = pack.at[0:SENT + (SENT_SUMS if st == STREAMS - 1 else 0)]
            remote(total, total, sent.at[st], sp_recv, mate).wait_send()
        pl.when(step_index < NUM_STEPS - 1)(lambda: open_step(finish_last))
        pl.when(step_index == NUM_STEPS - 1)(finish_last)
        return carry

    lax.fori_loop(0, NUM_STEPS, one_step, 0)
    for ch in range(3):
        pre_pm(ch).wait_recv()
    for piece in range(7):
        pre_bf16(piece).wait_recv()
    total = pack.at[0:7 * 512 + 3 * HALF]
    remote(total, total, pre_send, sp_recv, mate).wait_send()


def solution(mesh):
    def run_steps(particles, prec_diag, mean_vec, low_rank):
        total_rows, width = particles.shape
        n_part = total_rows // mesh.shape["ens"]
        bandwidth = BAND_SCALE * width
        step_size = STEP_SCALE * width
        loc = width // (mesh.shape["slab"] * mesh.shape["feat"])
        rank = low_rank.shape[1]
        vm, dma = pltpu.VMEM, pltpu.SemaphoreType.DMA

        def local_steps(current, prec_loc, mean_loc, fac_loc):
            spec = pl.BlockSpec(memory_space=pltpu.VMEM)
            call = pl.pallas_call(
                functools.partial(_kernel, bandwidth, step_size, n_part),
                out_shape=jax.ShapeDtypeStruct((n_part, loc), F32),
                in_specs=[pl.BlockSpec(memory_space=pltpu.HBM)] * 4,
                out_specs=spec,
                scratch_shapes=[
                    vm((1, loc), F32), vm((1, loc), F32), vm((loc, rank), BF16),
                    vm((ROWS, 2 * loc), BF16), vm((ROWS, rank), F32), vm((ROWS // 2, rank), F32),
                    vm((ROWS, TILE), F32), vm((16, TILE), F32), vm((ROWS, loc), F32), vm((ROWS, loc), F32),
                    vm((3 * SROWS, TILE), F32),
                    vm((STREAMS, COLORS, HALF // 2, TILE), F32), vm((STREAMS, COLORS, QUARTER, TILE), F32),
                    vm((STREAMS, COLORS, 3, OWN, TILE), F32), vm((STREAMS, COLORS, 4, OWN, TILE), F32),
                    vm((2, SROWS, TILE), BF16), vm((ROWS, ROWS), BF16), vm((ROWS, loc), BF16),
                    vm((2, 3, 16, TILE), F32), vm((2, 3, 3, 16, TILE), F32), vm((16, TILE), F32), vm((16, TILE), F32),
                    dma((7,)), dma, dma((12,)), dma((STREAMS,)), dma((STREAMS, 2, COLORS)), dma((STREAMS, 2, 3)),
                    dma((STREAMS, 3)), dma((STREAMS, 3)), dma((STREAMS,)),
                    dma((2, 3)), dma,
                ],
                compiler_params=pltpu.CompilerParams(collective_id=0, has_side_effects=True, vmem_limit_bytes=50000000),
                name="svgd",
            )
            hbm = lambda x: pltpu.with_memory_space_constraint(x, pltpu.HBM)
            return call(hbm(current), hbm(prec_loc.reshape(1, loc)), hbm(mean_loc.reshape(1, loc)), hbm(fac_loc))

        sharded = jax.shard_map(
            local_steps,
            mesh=mesh,
            in_specs=(P("ens", FEAT_AXES), P(LEAD_AXES), P(LEAD_AXES), P(LEAD_AXES, None)),
            out_specs=P("ens", FEAT_AXES),
            check_vma=False,
        )
        return sharded(particles, prec_diag, mean_vec, low_rank)

    return run_steps
```

```python
import functools

import jax
import jax.numpy as jnp
from jax import lax
from jax.experimental import pallas as pl
from jax.experimental.pallas import tpu as pltpu
from jax.sharding import PartitionSpec as P

NUM_STEPS = 3
BAND_SCALE = 4.0
STEP_SCALE = 0.4
FEAT_AXES = ("slab", "feat")
LEAD_AXES = ("ens", "slab", "feat")

ROWS = 2048
TILE = 128
HALF = 256
BLK = 2 * HALF
COLORS = 6
SROWS = COLORS * BLK
PM_AT = ((0, 0), (0, 1), (0, 5), (1, 5))
DIAG_AT = (((1, 0), (1, 1)), ((0, 4), (1, 4)), ((0, 2), (0, 3)), ((1, 2), (1, 3)))
STREAMS = 6
QUARTER = HALF // 4
UNITS = ((), ((0, 3), (0, 1), (0, 2)), ((1, 2), (1, 3), (2, 3)))
OFFS = (((0, 1), (2, 0), (3, 0)), ((1, 2), (1, 3), (2, 3)))
SENT = 3216
SENT_SUMS = 304
OWN = QUARTER // 4
PEERS = (2, 1, 3)
NEAR_FIRST = (1, 3, 2)
MESH = pl.DeviceIdType.MESH
NT = (((1,), (1,)), ((), ()))
F32, BF16 = jnp.float32, jnp.bfloat16


def div(a, b):
    return lax.div(a, jnp.int32(b))


def rem(a, b):
    return lax.rem(a, jnp.int32(b))


def _kernel(
    bandwidth, step_size, n_part,
    theta_ref, lam_hbm, mu_hbm, fac_hbm, out_ref,
    lam_ref, mu_ref, fac_ref,
    bfull, pml, pmr, nrow, ncol, pulled, scaled, pack, r0, r1, r2, r3, kg, kfull, adrv, svec, srecv, stot, spart,
    in_sem, pre_send, pre_recv, sent, rs_recv, x_recv, near_recv, far_recv, dd_recv, s_recv, sp_recv,
):
    width = out_ref.shape[1]
    rep_coef = 2.0 / bandwidth
    core = lax.axis_index("slab")
    feat = lax.axis_index("feat")
    coords = (rem(feat, 4), rem(div(feat, 4), 4), div(feat, 16))
    strides = (1, 4, 16)

    def chip(dim, coord):
        return {"feat": feat + (coord - coords[dim]) * strides[dim]}

    turned = [[coords[dim]] + [rem(coords[dim] + j, 4) for j in sorted(PEERS)] for dim in range(3)]

    def around(dim, j):
        return turned[dim][j]

    ring = [[chip(dim, turned[dim][j]) for j in range(4)] for dim in range(3)]
    low_bit = [rem(c, 2) for c in coords]
    pair_bit = [[rem(div(t + 1, 2), 2) for t in turned[dim]] for dim in range(3)]
    high_bit = [[div(t, 2) for t in turned[dim]] for dim in range(3)]

    mate = {"slab": 1 - core}

    def al(x, m=16):
        return pl.multiple_of(x, m)

    halves = []
    for k in range(COLORS):
        steps = []
        start, length, cur = 0, HALF, coords[k % 3]
        for s in range(2):
            if (k // 3 + s) % 2 == 0:
                other, bit = cur + 1 - 2 * low_bit[k % 3], pair_bit[k % 3][0]
            else:
                other, bit = 3 - cur, high_bit[k % 3][0]
            length = length // 2
            keep, give = start + bit * length, start + (1 - bit) * length
            start = keep
            steps.append((chip(k % 3, other), length, keep, give))
        halves.append(steps)

    def dims(k):
        return k % 3, (k + 1) % 3, (k + 2) % 3

    def base(st, k):
        return (st * COLORS + k) * HALF

    def tile_row(kind, k, a):
        st, k = DIAG_AT[k][a // 2] if kind == 0 else (2 * kind + a // 2, k)
        return base(st, k) + a % 2 * TILE

    keeps = [[al(step[2]) for step in steps] for steps in halves]
    gives = [[al(step[3]) for step in steps] for steps in halves]
    pieces = [[al(halves[k][1][2] + OWN * around(dims(k)[1], j)) for j in range(4)] for k in range(COLORS)]
    places = []
    for k in range(COLORS):
        one, two = (pair_bit, high_bit) if k < 3 else (high_bit, pair_bit)
        places.append([al(QUARTER * (2 * one[k % 3][j] + two[k % 3][j])) for j in range(4)])

    columns = [[al(m * BLK + (2 * core + n) * TILE, TILE) for n in range(2)] for m in range(4)]

    def packed(st, k, row, rows):
        return pack.at[pl.ds(al(base(st, k) + row), rows)]

    loads = [pltpu.make_async_copy(theta_ref.at[pl.ds(ch * BLK, BLK)], out_ref.at[pl.ds(ch * BLK, BLK)], in_sem.at[ch]) for ch in range(4)]
    loads += [
        pltpu.make_async_copy(src, dst, in_sem.at[4 + n])
        for n, (src, dst) in enumerate(((mu_hbm, mu_ref), (fac_hbm, fac_ref), (lam_hbm, lam_ref)))
    ]
    for cp in loads[4:] + loads[:1]:
        cp.start()
    barrier = pltpu.get_barrier_semaphore()
    pl.semaphore_signal(barrier, inc=1, device_id=mate, device_id_type=MESH)
    for dim in range(3):
        for j in PEERS:
            pl.semaphore_signal(barrier, inc=1, device_id=ring[dim][j], device_id_type=MESH)
    for cp in loads[1:4]:
        cp.start()

    row_i = lax.broadcasted_iota(jnp.int32, (TILE, TILE), 0)
    col_i = lax.broadcasted_iota(jnp.int32, (TILE, TILE), 1)
    eye, upper, lower = row_i == col_i, row_i < col_i, row_i > col_i
    sub_o = lax.broadcasted_iota(jnp.int32, (OWN, TILE), 0)
    lane_o = lax.broadcasted_iota(jnp.int32, (OWN, TILE), 1)

    def remote(src, dst, ssem, rsem, where):
        return pltpu.make_async_remote_copy(src_ref=src, dst_ref=dst, send_sem=ssem, recv_sem=rsem, device_id=where, device_id_type=MESH)

    def pre_bf16(piece):
        rows = pl.ds(piece * HALF, HALF)
        return remote(bfull.at[rows, 0:width], bfull.at[rows, width:2 * width], pre_send, pre_recv.at[piece], mate)

    def pre_pm(ch):
        src, dst = pml.at[pl.ds(al(ch * BLK + (1 - core) * HALF), HALF)], pmr.at[pl.ds(ch * HALF, HALF)]
        return remote(src, dst, pre_send, pre_recv.at[8 + ch], mate)

    def prepare(start, th):
        bfull[pl.ds(start, HALF), 0:width] = th.astype(BF16)
        return (th - mu_ref[...]).astype(BF16)

    def partial_pm(start, centered):
        for n, rows in enumerate(centered):
            pml[pl.ds(start + HALF * n, HALF), :] = jnp.dot(rows, fac_ref[...], preferred_element_type=F32)

    def begin(cps):
        for cp in cps:
            cp.start()

    def arrive(ref, sem):
        remote(ref, ref, sent.at[0], sem, mate).wait_recv()

    def pair_arrive(rows, sem):
        arrive(pack.at[0:6 * rows], sem)

    def rs_copy(st, s, k):
        peer, length, keep, give = halves[k][s]
        src = packed(st, k, gives[k][s], length)
        return remote(src, (r0, r1)[s].at[st, k], sent.at[st], rs_recv.at[st, s, k], peer)

    def gathered(st, k, row, rows):
        if st < 2:
            return kg.at[core, pl.ds(base(st, k) + row, rows)]
        sup, m = UNITS[st // 2][k // 2]
        return kfull.at[pl.ds(sup * BLK + st % 2 * HALF + row, rows), pl.ds(columns[m][k % 2], TILE)]

    def x_copies(st, e, k):
        d1, d2, d3 = dims(k)
        dim = (d2, d3)[e]
        cps = []
        for j in PEERS:
            if e == 0:
                src = packed(st, k, pieces[k][j], OWN)
                dst = r2.at[st, k, j - 1]
            else:
                src = dst = r3.at[st, k, coords[dim]]
            cps.append(remote(src, dst, sent.at[st], x_recv.at[st, e, k % 3], ring[dim][j]))
        return cps

    def gather_copies(st, k, j):
        d1, d2, d3 = dims(k)
        ref = gathered(st, k, pieces[k][(4 - j) % 4], OWN)
        cps = [remote(ref, ref, sent.at[st], far_recv.at[st, k % 3], ring[d1][i]) for i in PEERS]
        if j == 0:
            cps = [remote(ref, ref, sent.at[st], near_recv.at[st, k % 3], ring[d2][i]) for i in PEERS] + cps
        return cps

    def dd_copy(st, k, j):
        ref = gathered(st, k, keeps[k][1] if j == 0 else places[k][4 - j], QUARTER)
        return remote(ref, ref, sent.at[st], dd_recv.at[st], mate)

    def s_copies(ph, d):
        dim = ((d + 1) % 3, d)[ph]
        return [
            remote(svec.at[ph, d], srecv.at[ph, d, j - 1], sent.at[STREAMS - 1], s_recv.at[ph, d], ring[dim][j])
            for j in PEERS
        ]

    def sp_copy():
        return remote(stot, spart, sent.at[STREAMS - 1], sp_recv, mate)

    def products(m):
        mine = bfull[pl.ds(al(m * BLK + HALF * core), HALF), :]
        part = BLK if m == 3 else (m + 1) * HALF
        return [lax.dot_general(bfull[pl.ds(at, part), :], mine, NT, preferred_element_type=F32) for at in range(0, (m + 1) * BLK, part)]

    def norms(m):
        for i in range(4):
            rows = pl.ds((4 * m + i) * TILE, TILE)
            wide = bfull[rows, :].astype(F32)
            n = jnp.broadcast_to(jnp.sum(wide * wide, axis=1, keepdims=True), (TILE, TILE))
            nrow[rows, :] = n
            ncol[4 * m + i:4 * m + i + 1, :] = jnp.sum(jnp.where(eye, n, 0.0), axis=0, keepdims=True)

    def tiles(m, g):
        def block(blk, b):
            n, r = divmod(blk * TILE, BLK if m == 3 else (m + 1) * HALF)
            return g[n][r:r + TILE, b * TILE:(b + 1) * TILE]

        def tile(i, b):
            return block(4 * m + i, b)

        def dist(i, j):
            return nrow[pl.ds((4 * m + i) * TILE, TILE), :] + ncol[4 * m + j:4 * m + j + 1, :] - 2.0 * tile(i, j % 2)

        for t in range(3):
            pack[pl.ds(tile_row(0, m, t), TILE), :] = jnp.where(core == 0, dist(*OFFS[0][t]), dist(*OFFS[1][t]))
        one = jnp.where(core == 0, dist(0, 0), dist(2, 2))
        two = jnp.where(core == 0, dist(1, 1), dist(3, 3))
        pack[pl.ds(tile_row(0, m, 3), TILE), :] = jnp.where(upper, one, two)
        begin([rs_copy(st, 0, k) for st, k in DIAG_AT[m]])
        for kind in (1, 2):
            for u, (sup, col) in enumerate(UNITS[kind]):
                if col != m:
                    continue
                for b in range(2):
                    nc = ncol[pl.ds(4 * m + 2 * core + b, 1), :]
                    for a in range(4):
                        nr = nrow[pl.ds((4 * sup + a) * TILE, TILE), :]
                        pack[pl.ds(tile_row(kind, 2 * u + b, a), TILE), :] = nr + nc - 2.0 * block(4 * sup + a, b)
                begin([rs_copy(st, 0, 2 * u + b) for st in (2 * kind, 2 * kind + 1) for b in range(2)])

    def pm_tiles(chs):
        for ch in chs:
            pre_pm(ch).wait_recv()
            mine = pl.ds(al(ch * BLK + core * HALF), HALF)
            pack[pl.ds(base(*PM_AT[ch]), HALF), :] = pml[mine, :] + pmr[pl.ds(ch * HALF, HALF), :]
            begin([rs_copy(PM_AT[ch][0], 0, PM_AT[ch][1])])

    def open_step(finish_last):
        pm_tiles(range(3))
        for piece in range(4):
            pre_bf16(piece).wait_recv()
        one = products(1)
        for m in range(2):
            norms(m)
        zero = products(0)
        tiles(1, one)
        finish_last()
        begin([pre_pm(3), pre_bf16(7)])
        tiles(0, zero)
        for m in range(2, 4):
            for piece in range(2 * m, 2 * m + 2):
                pre_bf16(piece).wait_recv()
            g = products(m)
            norms(m)
            tiles(m, g)
            if m == 2:
                pm_tiles((3,))

    for cp in loads[4:]:
        cp.wait()
    for ch in range(4):
        loads[ch].wait()
        starts = (ch * BLK, ch * BLK + HALF)
        partial_pm(ch * BLK, [prepare(start, out_ref[pl.ds(start, HALF), :]) for start in starts])
        if ch == 0:
            pl.semaphore_wait(barrier, 10)
        if ch < 3:
            begin([pre_pm(ch)])
        begin([pre_bf16(piece) for piece in (2 * ch, 2 * ch + 1) if piece < 7])
    open_step(lambda: None)

    def one_step(step_index, carry):
        def row_sums(st, k, kern):
            m, part = (0, st % 2) if st > 1 else [(m, part) for m in range(4) for part in range(2) if DIAG_AT[m][part] == (st, k)][0]
            place = pieces[k][0] + part * HALF
            slot, r = div(place, TILE), rem(place, TILE)

            def by_rows(vals):
                rs = jnp.sum(vals, axis=1, keepdims=True)
                return jnp.sum(jnp.where(lane_o == sub_o + r, rs, 0.0), axis=0, keepdims=True)

            def by_cols(vals):
                return jnp.sum(vals, axis=0, keepdims=True)

            if st > 1:
                sup, m = UNITS[st // 2][k // 2]
                return [(4 * sup + slot, by_rows(kern)), (4 * m + 2 * core + k % 2, by_cols(kern))]
            both = div(slot, 3)
            up_one = div(slot + 1, 2)
            i0 = (1 - both) * ((1 - core) * (slot + up_one) + core * (1 + div(slot, 2))) + both * 2 * core
            j0 = (1 - both) * ((1 - core) * (1 - up_one) + core * (2 + up_one)) + both * 2 * core
            up = jnp.where(lane_o + 1000 * (1 - both) > sub_o + r, kern, 0.0)
            lo = jnp.where(lane_o + 1000 * (1 - both) < sub_o + r, kern, 0.0)
            nxt = 4 * m + 2 * core + 1
            return [(4 * m + i0, by_rows(up)), (4 * m + j0, by_cols(up)), (nxt, by_rows(lo)), (nxt, by_cols(lo))]

        def advance(st, s):
            parts = [[], [], []]
            if s == 4 and st == STREAMS - 1:
                for d in range(3):
                    arrive(srecv.at[0, d], s_recv.at[0, d])
                    svec[1, d] = svec[0, d] + srecv[0, d, 0] + srecv[0, d, 1] + srecv[0, d, 2]
                    begin(s_copies(1, d))
            if s == 5 and st == STREAMS - 1:
                tot = jnp.zeros((16, TILE), F32)
                for d in range(3):
                    arrive(srecv.at[1, d], s_recv.at[1, d])
                    tot = tot + ((svec[1, d] + srecv[1, d, 0]) + (srecv[1, d, 1] + srecv[1, d, 2]))
                stot[...] = tot
                begin([sp_copy()])
            kerns = {}
            for k in (range(COLORS) if s < 2 else (0, 3, 1, 4, 2, 5)):
                if s < 2:
                    peer, length, keep, give = halves[k][s]
                    rs_copy(st, s, k).wait_recv()
                    packed(st, k, keeps[k][s], length)[...] += (r0, r1)[s][st, k]
                    begin([rs_copy(st, 1, k)] if s == 0 else x_copies(st, 0, k))
                    continue
                if k < 3:
                    sem = x_recv.at[st, s - 2, k] if s < 4 else (near_recv, far_recv)[s - 4].at[st, k]
                    pair_arrive((OWN, OWN, OWN // 2, QUARTER // 2)[s - 2], sem)
                if s == 2:
                    r3[st, k, coords[dims(k)[2]]] = packed(st, k, pieces[k][0], OWN)[...] + r2[st, k, 0] + r2[st, k, 1] + r2[st, k, 2]
                    begin(x_copies(st, 1, k))
                elif s == 3:
                    full = (r3[st, k, 0] + r3[st, k, 1]) + (r3[st, k, 2] + r3[st, k, 3])
                    kern = full if (st, k) in PM_AT else jnp.exp(-jnp.maximum(full, 0.0) / bandwidth)
                    gathered(st, k, pieces[k][0], OWN)[...] = kern.astype(BF16)
                    begin(gather_copies(st, k, 0))
                    kerns[k] = kern
                elif s == 4:
                    begin([dd_copy(st, k, 0)])
                    for j in NEAR_FIRST:
                        begin(gather_copies(st, k, j))
                else:
                    begin([dd_copy(st, k, j) for j in NEAR_FIRST])
            if s == 3:
                for k, kern in kerns.items():
                    if (st, k) not in PM_AT:
                        parts[k % 3] += row_sums(st, k, kern)
                for d in range(3):
                    if st == 0:
                        svec[0, d] = jnp.zeros((16, TILE), F32)
                    for block, line in parts[d]:
                        svec[0, d, pl.ds(block, 1), :] += line
                    if st == STREAMS - 1:
                        begin(s_copies(0, d))
        def unpack_wait(kind):
            for st in (2 * kind, 2 * kind + 1):
                arrive(kg.at[core, 0:COLORS * HALF], dd_recv.at[st])

        def unpack(kind):
            for c in range(2):
                if kind > 0:
                    for k in range(COLORS):
                        sup, m = UNITS[kind][k // 2]
                        jrng = pl.ds((4 * m + 2 * c + k % 2) * TILE, TILE)
                        for a in range(4):
                            srng = pl.ds((4 * sup + a) * TILE, TILE)
                            kfull[jrng, srng] = kfull[srng, jrng].T
                    continue
                for sup in range(4):
                    for t, (i, j) in enumerate(OFFS[c]):
                        src = kg[c, pl.ds(tile_row(0, sup, t), TILE), :]
                        ri, rj = pl.ds((4 * sup + i) * TILE, TILE), pl.ds((4 * sup + j) * TILE, TILE)
                        kfull[ri, rj] = src
                        kfull[rj, ri] = src.T
                    src = kg[c, pl.ds(tile_row(0, sup, 3), TILE), :]
                    srt = src.T
                    one = jnp.ones((TILE, TILE), BF16)
                    ra, rb = pl.ds((4 * sup + 2 * c) * TILE, TILE), pl.ds((4 * sup + 2 * c + 1) * TILE, TILE)
                    kfull[ra, ra] = jnp.where(upper, src, jnp.where(lower, srt, one))
                    kfull[rb, rb] = jnp.where(lower, src, jnp.where(upper, srt, one))

        def drive_parts():
            for q in range(8):
                rows = pl.ds(q * HALF, HALF)
                th = out_ref[rows, :]
                pulled[rows, :] = (th - mu_ref[...]) * lam_ref[...]
                scaled[rows, :] = rep_coef * th

        def drive():
            for q in range(8):
                rows = pl.ds(q * HALF, HALF)
                ch = q // 2
                pm = kg[q % 2, pl.ds(base(*PM_AT[ch]), HALF), :]
                low = lax.dot_general(pm, fac_ref[...], NT, preferred_element_type=F32)
                adrv[rows, :] = ((pulled[rows, :] + low) + scaled[rows, :]).astype(BF16)

        def product(start):
            return jnp.dot(kfull[pl.ds(start, HALF), :], adrv[...], preferred_element_type=F32)

        def finish(start, acc, tot, held):
            rows = pl.ds(start, HALF)
            sums = []
            for blk in (start // TILE, start // TILE + 1):
                line = jnp.where(eye, jnp.broadcast_to(tot[blk:blk + 1, :], (TILE, TILE)), 0.0)
                sums.append(rep_coef * jnp.sum(line, axis=1, keepdims=True))
            sums = jnp.broadcast_to(jnp.concatenate(sums, axis=0), (HALF, TILE))
            new = []
            for t in range(width // TILE):
                cols = slice(t * TILE, (t + 1) * TILE)
                th = out_ref[rows, cols]
                phi = (sums * th - acc[:, cols]) / n_part
                new.append(th + step_size * phi)
            th = jnp.concatenate(new, axis=1)
            out_ref[rows, :] = th
            held.append(prepare(start, th))
            if start % BLK:
                partial_pm(start - HALF, held[-2:])

        def share(start):
            if start % BLK and start + HALF < ROWS:
                begin([pre_pm(start // BLK), pre_bf16(start // HALF - 1), pre_bf16(start // HALF)])
            elif start + BLK == ROWS:
                begin([pre_bf16(start // HALF)])

        drive_parts()
        def early_rounds(s):
            def one(st, c):
                advance(st, s)
                return c

            lax.fori_loop(0, STREAMS, one, 0)

        for s in range(3):
            early_rounds(s)
        for s in range(3, 6):
            for st in range(STREAMS):
                if s == 5 and st == STREAMS - 2:
                    unpack_wait(0)
                    unpack(0)
                    drive()
                advance(st, s)
        remote(pack.at[0:5120], pack.at[0:5120], pre_send, sp_recv, mate).wait_send()
        def update(starts, kind):
            tot = stot[...] + spart[...] + 1.0
            ahead = product(starts[0])
            unpack(kind)
            held = []
            for n, start in enumerate(starts):
                acc = ahead
                if n + 1 < len(starts):
                    ahead = product(starts[n + 1])
                if n:
                    share(starts[n - 1])
                if start + HALF == ROWS:
                    return lambda: finish(start, acc, tot, list(held))
                finish(start, acc, tot, held)
            share(starts[-1])

        unpack_wait(1)
        arrive(stot, sp_recv)
        update(range(0, BLK, HALF), 1)
        unpack_wait(2)
        finish_last = update(range(BLK, ROWS, HALF), 2)
        for st in range(STREAMS):
            total = pack.at[0:SENT + (SENT_SUMS if st == STREAMS - 1 else 0)]
            remote(total, total, sent.at[st], sp_recv, mate).wait_send()
        pl.when(step_index < NUM_STEPS - 1)(lambda: open_step(finish_last))
        pl.when(step_index == NUM_STEPS - 1)(finish_last)
        return carry

    lax.fori_loop(0, NUM_STEPS, one_step, 0)
    for ch in range(3):
        pre_pm(ch).wait_recv()
    for piece in range(7):
        pre_bf16(piece).wait_recv()
    total = pack.at[0:7 * 512 + 3 * HALF]
    remote(total, total, pre_send, sp_recv, mate).wait_send()


def solution(mesh):
    def run_steps(particles, prec_diag, mean_vec, low_rank):
        total_rows, width = particles.shape
        n_part = total_rows // mesh.shape["ens"]
        bandwidth = BAND_SCALE * width
        step_size = STEP_SCALE * width
        loc = width // (mesh.shape["slab"] * mesh.shape["feat"])
        rank = low_rank.shape[1]
        vm, dma = pltpu.VMEM, pltpu.SemaphoreType.DMA

        def local_steps(current, prec_loc, mean_loc, fac_loc):
            spec = pl.BlockSpec(memory_space=pltpu.VMEM)
            call = pl.pallas_call(
                functools.partial(_kernel, bandwidth, step_size, n_part),
                out_shape=jax.ShapeDtypeStruct((n_part, loc), F32),
                in_specs=[pl.BlockSpec(memory_space=pltpu.HBM)] * 4,
                out_specs=spec,
                scratch_shapes=[
                    vm((1, loc), F32), vm((1, loc), F32), vm((loc, rank), BF16),
                    vm((ROWS, 2 * loc), BF16), vm((ROWS, rank), F32), vm((ROWS // 2, rank), F32),
                    vm((ROWS, TILE), F32), vm((16, TILE), F32), vm((ROWS, loc), F32), vm((ROWS, loc), F32),
                    vm((3 * SROWS, TILE), F32),
                    vm((STREAMS, COLORS, HALF // 2, TILE), F32), vm((STREAMS, COLORS, QUARTER, TILE), F32),
                    vm((STREAMS, COLORS, 3, OWN, TILE), F32), vm((STREAMS, COLORS, 4, OWN, TILE), F32),
                    vm((2, SROWS, TILE), BF16), vm((ROWS, ROWS), BF16), vm((ROWS, loc), BF16),
                    vm((2, 3, 16, TILE), F32), vm((2, 3, 3, 16, TILE), F32), vm((16, TILE), F32), vm((16, TILE), F32),
                    dma((7,)), dma, dma((12,)), dma((STREAMS,)), dma((STREAMS, 2, COLORS)), dma((STREAMS, 2, 3)),
                    dma((STREAMS, 3)), dma((STREAMS, 3)), dma((STREAMS,)),
                    dma((2, 3)), dma,
                ],
                compiler_params=pltpu.CompilerParams(collective_id=0, has_side_effects=True, vmem_limit_bytes=50000000),
                name="svgd",
            )
            hbm = lambda x: pltpu.with_memory_space_constraint(x, pltpu.HBM)
            return call(hbm(current), hbm(prec_loc.reshape(1, loc)), hbm(mean_loc.reshape(1, loc)), hbm(fac_loc))

        sharded = jax.shard_map(
            local_steps,
            mesh=mesh,
            in_specs=(P("ens", FEAT_AXES), P(LEAD_AXES), P(LEAD_AXES), P(LEAD_AXES, None)),
            out_specs=P("ens", FEAT_AXES),
            check_vma=False,
        )
        return sharded(particles, prec_diag, mean_vec, low_rank)

    return run_steps
```

```python
import functools

import jax
import jax.numpy as jnp
from jax import lax
from jax.experimental import pallas as pl
from jax.experimental.pallas import tpu as pltpu
from jax.sharding import PartitionSpec as P

NUM_STEPS = 3
BAND_SCALE = 4.0
STEP_SCALE = 0.4
FEAT_AXES = ("slab", "feat")
LEAD_AXES = ("ens", "slab", "feat")

ROWS = 2048
TILE = 128
HALF = 256
BLK = 2 * HALF
COLORS = 6
SROWS = COLORS * BLK
PM_AT = ((0, 0), (0, 1), (0, 5), (1, 5))
DIAG_AT = (((1, 0), (1, 1)), ((0, 4), (1, 4)), ((0, 2), (0, 3)), ((1, 2), (1, 3)))
STREAMS = 6
QUARTER = HALF // 4
UNITS = ((), ((0, 3), (0, 1), (0, 2)), ((1, 2), (1, 3), (2, 3)))
OFFS = (((0, 1), (2, 0), (3, 0)), ((1, 2), (1, 3), (2, 3)))
SENT = 3216
SENT_SUMS = 304
OWN = QUARTER // 4
PEERS = (2, 1, 3)
NEAR_FIRST = (1, 3, 2)
MESH = pl.DeviceIdType.MESH
NT = (((1,), (1,)), ((), ()))
F32, BF16 = jnp.float32, jnp.bfloat16


def div(a, b):
    return lax.div(a, jnp.int32(b))


def rem(a, b):
    return lax.rem(a, jnp.int32(b))


def _kernel(
    bandwidth, step_size, n_part,
    theta_ref, lam_hbm, mu_hbm, fac_hbm, out_ref,
    lam_ref, mu_ref, fac_ref,
    bfull, pml, pmr, nown, nrow, ncol, pulled, scaled, pack, r0, r1, r2, r3, kg, kfull, adrv, svec, srecv, stot, spart,
    in_sem, pre_send, pre_recv, sent, rs_recv, x_recv, near_recv, far_recv, dd_recv, s_recv, sp_recv,
):
    width = out_ref.shape[1]
    rep_coef = 2.0 / bandwidth
    core = lax.axis_index("slab")
    feat = lax.axis_index("feat")
    coords = (rem(feat, 4), rem(div(feat, 4), 4), div(feat, 16))
    strides = (1, 4, 16)

    def chip(dim, coord):
        return {"feat": feat + (coord - coords[dim]) * strides[dim]}

    turned = [[coords[dim]] + [rem(coords[dim] + j, 4) for j in sorted(PEERS)] for dim in range(3)]

    def around(dim, j):
        return turned[dim][j]

    ring = [[chip(dim, turned[dim][j]) for j in range(4)] for dim in range(3)]
    low_bit = [rem(c, 2) for c in coords]
    pair_bit = [[rem(div(t + 1, 2), 2) for t in turned[dim]] for dim in range(3)]
    high_bit = [[div(t, 2) for t in turned[dim]] for dim in range(3)]

    mate = {"slab": 1 - core}

    def al(x, m=16):
        return pl.multiple_of(x, m)

    halves = []
    for k in range(COLORS):
        steps = []
        start, length, cur = 0, HALF, coords[k % 3]
        for s in range(2):
            if (k // 3 + s) % 2 == 0:
                other, bit = cur + 1 - 2 * low_bit[k % 3], pair_bit[k % 3][0]
            else:
                other, bit = 3 - cur, high_bit[k % 3][0]
            length = length // 2
            keep, give = start + bit * length, start + (1 - bit) * length
            start = keep
            steps.append((chip(k % 3, other), length, keep, give))
        halves.append(steps)

    def dims(k):
        return k % 3, (k + 1) % 3, (k + 2) % 3

    def base(st, k):
        return (st * COLORS + k) * HALF

    def tile_row(kind, k, a):
        st, k = DIAG_AT[k][a // 2] if kind == 0 else (2 * kind + a // 2, k)
        return base(st, k) + a % 2 * TILE

    keeps = [[al(step[2]) for step in steps] for steps in halves]
    gives = [[al(step[3]) for step in steps] for steps in halves]
    pieces = [[al(halves[k][1][2] + OWN * around(dims(k)[1], j)) for j in range(4)] for k in range(COLORS)]
    places = []
    for k in range(COLORS):
        one, two = (pair_bit, high_bit) if k < 3 else (high_bit, pair_bit)
        places.append([al(QUARTER * (2 * one[k % 3][j] + two[k % 3][j])) for j in range(4)])

    columns = [[al(m * BLK + (2 * core + n) * TILE, TILE) for n in range(2)] for m in range(4)]

    def packed(st, k, row, rows):
        return pack.at[pl.ds(al(base(st, k) + row), rows)]

    loads = [pltpu.make_async_copy(theta_ref.at[pl.ds(ch * BLK, BLK)], out_ref.at[pl.ds(ch * BLK, BLK)], in_sem.at[ch]) for ch in range(4)]
    loads += [
        pltpu.make_async_copy(src, dst, in_sem.at[4 + n])
        for n, (src, dst) in enumerate(((mu_hbm, mu_ref), (fac_hbm, fac_ref), (lam_hbm, lam_ref)))
    ]
    for cp in loads[4:] + loads[:1]:
        cp.start()
    barrier = pltpu.get_barrier_semaphore()
    pl.semaphore_signal(barrier, inc=1, device_id=mate, device_id_type=MESH)
    for dim in range(3):
        for j in PEERS:
            pl.semaphore_signal(barrier, inc=1, device_id=ring[dim][j], device_id_type=MESH)
    for cp in loads[1:4]:
        cp.start()

    row_i = lax.broadcasted_iota(jnp.int32, (TILE, TILE), 0)
    col_i = lax.broadcasted_iota(jnp.int32, (TILE, TILE), 1)
    eye, upper, lower = row_i == col_i, row_i < col_i, row_i > col_i
    sub_o = lax.broadcasted_iota(jnp.int32, (OWN, TILE), 0)
    lane_o = lax.broadcasted_iota(jnp.int32, (OWN, TILE), 1)

    def remote(src, dst, ssem, rsem, where):
        return pltpu.make_async_remote_copy(src_ref=src, dst_ref=dst, send_sem=ssem, recv_sem=rsem, device_id=where, device_id_type=MESH)

    def pre_bf16(piece):
        rows = pl.ds(piece * HALF, HALF)
        return remote(bfull.at[rows, 0:width], bfull.at[rows, width:2 * width], pre_send, pre_recv.at[piece], mate)

    def pre_pm(ch):
        src, dst = pml.at[pl.ds(al(ch * BLK + (1 - core) * HALF), HALF)], pmr.at[pl.ds(ch * HALF, HALF)]
        return remote(src, dst, pre_send, pre_recv.at[8 + ch], mate)

    def prepare(start, th):
        rounded = th.astype(BF16)
        bfull[pl.ds(start, HALF), 0:width] = rounded
        wide = rounded.astype(F32)
        nown[pl.ds(start, HALF), :] = jnp.broadcast_to(jnp.sum(wide * wide, axis=1, keepdims=True), (HALF, TILE))
        return (th - mu_ref[...]).astype(BF16)

    def partial_pm(start, centered):
        for n, rows in enumerate(centered):
            pml[pl.ds(start + HALF * n, HALF), :] = jnp.dot(rows, fac_ref[...], preferred_element_type=F32)

    def begin(cps):
        for cp in cps:
            cp.start()

    def arrive(ref, sem):
        remote(ref, ref, sent.at[0], sem, mate).wait_recv()

    def pair_arrive(rows, sem):
        arrive(pack.at[0:6 * rows], sem)

    def rs_copy(st, s, k):
        peer, length, keep, give = halves[k][s]
        src = packed(st, k, gives[k][s], length)
        return remote(src, (r0, r1)[s].at[st, k], sent.at[st], rs_recv.at[st, s, k], peer)

    def gathered(st, k, row, rows):
        if st < 2:
            return kg.at[core, pl.ds(base(st, k) + row, rows)]
        sup, m = UNITS[st // 2][k // 2]
        return kfull.at[pl.ds(sup * BLK + st % 2 * HALF + row, rows), pl.ds(columns[m][k % 2], TILE)]

    def x_copies(st, e, k):
        d1, d2, d3 = dims(k)
        dim = (d2, d3)[e]
        cps = []
        for j in PEERS:
            if e == 0:
                src = packed(st, k, pieces[k][j], OWN)
                dst = r2.at[st, k, j - 1]
            else:
                src = dst = r3.at[st, k, coords[dim]]
            cps.append(remote(src, dst, sent.at[st], x_recv.at[st, e, k % 3], ring[dim][j]))
        return cps

    def gather_copies(st, k, j):
        d1, d2, d3 = dims(k)
        ref = gathered(st, k, pieces[k][(4 - j) % 4], OWN)
        cps = [remote(ref, ref, sent.at[st], far_recv.at[st, k % 3], ring[d1][i]) for i in PEERS]
        if j == 0:
            cps = [remote(ref, ref, sent.at[st], near_recv.at[st, k % 3], ring[d2][i]) for i in PEERS] + cps
        return cps

    def dd_copy(st, k, j):
        ref = gathered(st, k, keeps[k][1] if j == 0 else places[k][4 - j], QUARTER)
        return remote(ref, ref, sent.at[st], dd_recv.at[st], mate)

    def s_copies(ph, d):
        dim = ((d + 1) % 3, d)[ph]
        return [
            remote(svec.at[ph, d], srecv.at[ph, d, j - 1], sent.at[STREAMS - 1], s_recv.at[ph, d], ring[dim][j])
            for j in PEERS
        ]

    def sp_copy():
        return remote(stot, spart, sent.at[STREAMS - 1], sp_recv, mate)

    def products(m):
        mine = bfull[pl.ds(al(m * BLK + HALF * core), HALF), :]
        part = BLK if m == 3 else (m + 1) * HALF
        return [lax.dot_general(bfull[pl.ds(at, part), :], mine, NT, preferred_element_type=F32) for at in range(0, (m + 1) * BLK, part)]

    def norms(m):
        for i in range(4):
            rows = pl.ds((4 * m + i) * TILE, TILE)
            wide = bfull[rows, width:2 * width].astype(F32)
            n = nown[rows, :] + jnp.sum(wide * wide, axis=1, keepdims=True)
            nrow[rows, :] = n
            ncol[4 * m + i:4 * m + i + 1, :] = jnp.sum(jnp.where(eye, n, 0.0), axis=0, keepdims=True)

    def tiles(m, g):
        def block(blk, b):
            n, r = divmod(blk * TILE, BLK if m == 3 else (m + 1) * HALF)
            return g[n][r:r + TILE, b * TILE:(b + 1) * TILE]

        def tile(i, b):
            return block(4 * m + i, b)

        def dist(i, j):
            return nrow[pl.ds((4 * m + i) * TILE, TILE), :] + ncol[4 * m + j:4 * m + j + 1, :] - 2.0 * tile(i, j % 2)

        for t in range(3):
            pack[pl.ds(tile_row(0, m, t), TILE), :] = jnp.where(core == 0, dist(*OFFS[0][t]), dist(*OFFS[1][t]))
        one = jnp.where(core == 0, dist(0, 0), dist(2, 2))
        two = jnp.where(core == 0, dist(1, 1), dist(3, 3))
        pack[pl.ds(tile_row(0, m, 3), TILE), :] = jnp.where(upper, one, two)
        begin([rs_copy(st, 0, k) for st, k in DIAG_AT[m]])
        for kind in (1, 2):
            for u, (sup, col) in enumerate(UNITS[kind]):
                if col != m:
                    continue
                for b in range(2):
                    nc = ncol[pl.ds(4 * m + 2 * core + b, 1), :]
                    for a in range(4):
                        nr = nrow[pl.ds((4 * sup + a) * TILE, TILE), :]
                        pack[pl.ds(tile_row(kind, 2 * u + b, a), TILE), :] = nr + nc - 2.0 * block(4 * sup + a, b)
                begin([rs_copy(st, 0, 2 * u + b) for st in (2 * kind, 2 * kind + 1) for b in range(2)])

    def pm_tiles(chs):
        for ch in chs:
            pre_pm(ch).wait_recv()
            mine = pl.ds(al(ch * BLK + core * HALF), HALF)
            pack[pl.ds(base(*PM_AT[ch]), HALF), :] = pml[mine, :] + pmr[pl.ds(ch * HALF, HALF), :]
            begin([rs_copy(PM_AT[ch][0], 0, PM_AT[ch][1])])

    def open_step(finish_last):
        pm_tiles(range(3))
        for piece in range(4):
            pre_bf16(piece).wait_recv()
        finish_last()
        one, zero = products(1), products(0)
        for m in range(2):
            norms(m)
        begin([pre_pm(3), pre_bf16(7)])
        tiles(1, one)
        tiles(0, zero)
        pm_tiles((3,))
        for m in range(2, 4):
            for piece in range(2 * m, 2 * m + 2):
                pre_bf16(piece).wait_recv()
            g = products(m)
            norms(m)
            tiles(m, g)

    for cp in loads[4:]:
        cp.wait()
    for ch in range(4):
        loads[ch].wait()
        starts = (ch * BLK, ch * BLK + HALF)
        partial_pm(ch * BLK, [prepare(start, out_ref[pl.ds(start, HALF), :]) for start in starts])
        if ch == 0:
            pl.semaphore_wait(barrier, 10)
        if ch < 3:
            begin([pre_pm(ch)])
        begin([pre_bf16(piece) for piece in (2 * ch, 2 * ch + 1) if piece < 7])
    open_step(lambda: None)

    def one_step(step_index, carry):
        def row_sums(st, k, kern):
            m, part = (0, st % 2) if st > 1 else [(m, part) for m in range(4) for part in range(2) if DIAG_AT[m][part] == (st, k)][0]
            place = pieces[k][0] + part * HALF
            slot, r = div(place, TILE), rem(place, TILE)

            def by_rows(vals):
                rs = jnp.sum(vals, axis=1, keepdims=True)
                return jnp.sum(jnp.where(lane_o == sub_o + r, rs, 0.0), axis=0, keepdims=True)

            def by_cols(vals):
                return jnp.sum(vals, axis=0, keepdims=True)

            if st > 1:
                sup, m = UNITS[st // 2][k // 2]
                return [(4 * sup + slot, by_rows(kern)), (4 * m + 2 * core + k % 2, by_cols(kern))]
            both = div(slot, 3)
            up_one = div(slot + 1, 2)
            i0 = (1 - both) * ((1 - core) * (slot + up_one) + core * (1 + div(slot, 2))) + both * 2 * core
            j0 = (1 - both) * ((1 - core) * (1 - up_one) + core * (2 + up_one)) + both * 2 * core
            up = jnp.where(lane_o + 1000 * (1 - both) > sub_o + r, kern, 0.0)
            lo = jnp.where(lane_o + 1000 * (1 - both) < sub_o + r, kern, 0.0)
            nxt = 4 * m + 2 * core + 1
            return [(4 * m + i0, by_rows(up)), (4 * m + j0, by_cols(up)), (nxt, by_rows(lo)), (nxt, by_cols(lo))]

        def advance(st, s):
            parts = [[], [], []]
            if s == 4 and st == STREAMS - 1:
                for d in range(3):
                    arrive(srecv.at[0, d], s_recv.at[0, d])
                    svec[1, d] = svec[0, d] + srecv[0, d, 0] + srecv[0, d, 1] + srecv[0, d, 2]
                    begin(s_copies(1, d))
            if s == 5 and st == STREAMS - 1:
                tot = jnp.zeros((16, TILE), F32)
                for d in range(3):
                    arrive(srecv.at[1, d], s_recv.at[1, d])
                    tot = tot + ((svec[1, d] + srecv[1, d, 0]) + (srecv[1, d, 1] + srecv[1, d, 2]))
                stot[...] = tot
                begin([sp_copy()])
            kerns = {}
            for k in (range(COLORS) if s < 2 else (0, 3, 1, 4, 2, 5)):
                if s < 2:
                    peer, length, keep, give = halves[k][s]
                    rs_copy(st, s, k).wait_recv()
                    packed(st, k, keeps[k][s], length)[...] += (r0, r1)[s][st, k]
                    begin([rs_copy(st, 1, k)] if s == 0 else x_copies(st, 0, k))
                    continue
                if k < 3:
                    sem = x_recv.at[st, s - 2, k] if s < 4 else (near_recv, far_recv)[s - 4].at[st, k]
                    pair_arrive((OWN, OWN, OWN // 2, QUARTER // 2)[s - 2], sem)
                if s == 2:
                    r3[st, k, coords[dims(k)[2]]] = packed(st, k, pieces[k][0], OWN)[...] + r2[st, k, 0] + r2[st, k, 1] + r2[st, k, 2]
                    begin(x_copies(st, 1, k))
                elif s == 3:
                    full = (r3[st, k, 0] + r3[st, k, 1]) + (r3[st, k, 2] + r3[st, k, 3])
                    kern = full if (st, k) in PM_AT else jnp.exp(-jnp.maximum(full, 0.0) / bandwidth)
                    gathered(st, k, pieces[k][0], OWN)[...] = kern.astype(BF16)
                    begin(gather_copies(st, k, 0))
                    kerns[k] = kern
                elif s == 4:
                    begin([dd_copy(st, k, 0)])
                    for j in NEAR_FIRST:
                        begin(gather_copies(st, k, j))
                else:
                    begin([dd_copy(st, k, j) for j in NEAR_FIRST])
            if s == 3:
                for k, kern in kerns.items():
                    if (st, k) not in PM_AT:
                        parts[k % 3] += row_sums(st, k, kern)
                for d in range(3):
                    if st == 0:
                        svec[0, d] = jnp.zeros((16, TILE), F32)
                    for block, line in parts[d]:
                        svec[0, d, pl.ds(block, 1), :] += line
                    if st == STREAMS - 1:
                        begin(s_copies(0, d))
        def unpack_wait(kind):
            for st in (2 * kind, 2 * kind + 1):
                arrive(kg.at[core, 0:COLORS * HALF], dd_recv.at[st])

        def unpack(kind):
            for c in range(2):
                if kind > 0:
                    for k in range(COLORS):
                        sup, m = UNITS[kind][k // 2]
                        jrng = pl.ds((4 * m + 2 * c + k % 2) * TILE, TILE)
                        for a in range(4):
                            srng = pl.ds((4 * sup + a) * TILE, TILE)
                            kfull[jrng, srng] = kfull[srng, jrng].T
                    continue
                for sup in range(4):
                    for t, (i, j) in enumerate(OFFS[c]):
                        src = kg[c, pl.ds(tile_row(0, sup, t), TILE), :]
                        ri, rj = pl.ds((4 * sup + i) * TILE, TILE), pl.ds((4 * sup + j) * TILE, TILE)
                        kfull[ri, rj] = src
                        kfull[rj, ri] = src.T
                    src = kg[c, pl.ds(tile_row(0, sup, 3), TILE), :]
                    srt = src.T
                    one = jnp.ones((TILE, TILE), BF16)
                    ra, rb = pl.ds((4 * sup + 2 * c) * TILE, TILE), pl.ds((4 * sup + 2 * c + 1) * TILE, TILE)
                    kfull[ra, ra] = jnp.where(upper, src, jnp.where(lower, srt, one))
                    kfull[rb, rb] = jnp.where(lower, src, jnp.where(upper, srt, one))

        def drive_parts():
            for q in range(8):
                rows = pl.ds(q * HALF, HALF)
                th = out_ref[rows, :]
                pulled[rows, :] = (th - mu_ref[...]) * lam_ref[...]
                scaled[rows, :] = rep_coef * th

        def drive():
            for q in range(8):
                rows = pl.ds(q * HALF, HALF)
                ch = q // 2
                pm = kg[q % 2, pl.ds(base(*PM_AT[ch]), HALF), :]
                low = lax.dot_general(pm, fac_ref[...], NT, preferred_element_type=F32)
                adrv[rows, :] = ((pulled[rows, :] + low) + scaled[rows, :]).astype(BF16)

        def product(start):
            return jnp.dot(kfull[pl.ds(start, HALF), :], adrv[...], preferred_element_type=F32)

        def finish(start, acc, tot, held):
            rows = pl.ds(start, HALF)
            sums = []
            for blk in (start // TILE, start // TILE + 1):
                line = jnp.where(eye, jnp.broadcast_to(tot[blk:blk + 1, :], (TILE, TILE)), 0.0)
                sums.append(rep_coef * jnp.sum(line, axis=1, keepdims=True))
            sums = jnp.broadcast_to(jnp.concatenate(sums, axis=0), (HALF, TILE))
            new = []
            for t in range(width // TILE):
                cols = slice(t * TILE, (t + 1) * TILE)
                th = out_ref[rows, cols]
                phi = (sums * th - acc[:, cols]) / n_part
                new.append(th + step_size * phi)
            th = jnp.concatenate(new, axis=1)
            out_ref[rows, :] = th
            held.append(prepare(start, th))
            if start % BLK:
                partial_pm(start - HALF, held[-2:])

        def share(start):
            if start % BLK and start + HALF < ROWS:
                begin([pre_pm(start // BLK), pre_bf16(start // HALF - 1), pre_bf16(start // HALF)])
            elif start + BLK == ROWS:
                begin([pre_bf16(start // HALF)])

        drive_parts()
        def early_rounds(s):
            def one(st, c):
                advance(st, s)
                return c

            lax.fori_loop(0, STREAMS, one, 0)

        for s in range(3):
            early_rounds(s)
        for s in range(3, 6):
            for st in range(STREAMS):
                if s == 5 and st == STREAMS - 2:
                    unpack_wait(0)
                    unpack(0)
                    drive()
                advance(st, s)
        remote(pack.at[0:5120], pack.at[0:5120], pre_send, sp_recv, mate).wait_send()
        def update(starts, kind):
            tot = stot[...] + spart[...] + 1.0
            ahead = product(starts[0])
            unpack(kind)
            held = []
            for n, start in enumerate(starts):
                acc = ahead
                if n + 1 < len(starts):
                    ahead = product(starts[n + 1])
                if n:
                    share(starts[n - 1])
                if start + HALF == ROWS:
                    return lambda: finish(start, acc, tot, list(held))
                finish(start, acc, tot, held)
            share(starts[-1])

        unpack_wait(1)
        arrive(stot, sp_recv)
        update(range(0, BLK, HALF), 1)
        unpack_wait(2)
        finish_last = update(range(BLK, ROWS, HALF), 2)
        for st in range(STREAMS):
            total = pack.at[0:SENT + (SENT_SUMS if st == STREAMS - 1 else 0)]
            remote(total, total, sent.at[st], sp_recv, mate).wait_send()
        pl.when(step_index < NUM_STEPS - 1)(lambda: open_step(finish_last))
        pl.when(step_index == NUM_STEPS - 1)(finish_last)
        return carry

    lax.fori_loop(0, NUM_STEPS, one_step, 0)
    for ch in range(3):
        pre_pm(ch).wait_recv()
    for piece in range(7):
        pre_bf16(piece).wait_recv()
    total = pack.at[0:7 * 512 + 3 * HALF]
    remote(total, total, pre_send, sp_recv, mate).wait_send()


def solution(mesh):
    def run_steps(particles, prec_diag, mean_vec, low_rank):
        total_rows, width = particles.shape
        n_part = total_rows // mesh.shape["ens"]
        bandwidth = BAND_SCALE * width
        step_size = STEP_SCALE * width
        loc = width // (mesh.shape["slab"] * mesh.shape["feat"])
        rank = low_rank.shape[1]
        vm, dma = pltpu.VMEM, pltpu.SemaphoreType.DMA

        def local_steps(current, prec_loc, mean_loc, fac_loc):
            spec = pl.BlockSpec(memory_space=pltpu.VMEM)
            call = pl.pallas_call(
                functools.partial(_kernel, bandwidth, step_size, n_part),
                out_shape=jax.ShapeDtypeStruct((n_part, loc), F32),
                in_specs=[pl.BlockSpec(memory_space=pltpu.HBM)] * 4,
                out_specs=spec,
                scratch_shapes=[
                    vm((1, loc), F32), vm((1, loc), F32), vm((loc, rank), BF16),
                    vm((ROWS, 2 * loc), BF16), vm((ROWS, rank), F32), vm((ROWS // 2, rank), F32), vm((ROWS, TILE), F32),
                    vm((ROWS, TILE), F32), vm((16, TILE), F32), vm((ROWS, loc), F32), vm((ROWS, loc), F32),
                    vm((3 * SROWS, TILE), F32),
                    vm((STREAMS, COLORS, HALF // 2, TILE), F32), vm((STREAMS, COLORS, QUARTER, TILE), F32),
                    vm((STREAMS, COLORS, 3, OWN, TILE), F32), vm((STREAMS, COLORS, 4, OWN, TILE), F32),
                    vm((2, SROWS, TILE), BF16), vm((ROWS, ROWS), BF16), vm((ROWS, loc), BF16),
                    vm((2, 3, 16, TILE), F32), vm((2, 3, 3, 16, TILE), F32), vm((16, TILE), F32), vm((16, TILE), F32),
                    dma((7,)), dma, dma((12,)), dma((STREAMS,)), dma((STREAMS, 2, COLORS)), dma((STREAMS, 2, 3)),
                    dma((STREAMS, 3)), dma((STREAMS, 3)), dma((STREAMS,)),
                    dma((2, 3)), dma,
                ],
                compiler_params=pltpu.CompilerParams(collective_id=0, has_side_effects=True, vmem_limit_bytes=50000000),
                name="svgd",
            )
            hbm = lambda x: pltpu.with_memory_space_constraint(x, pltpu.HBM)
            return call(hbm(current), hbm(prec_loc.reshape(1, loc)), hbm(mean_loc.reshape(1, loc)), hbm(fac_loc))

        sharded = jax.shard_map(
            local_steps,
            mesh=mesh,
            in_specs=(P("ens", FEAT_AXES), P(LEAD_AXES), P(LEAD_AXES), P(LEAD_AXES, None)),
            out_specs=P("ens", FEAT_AXES),
            check_vma=False,
        )
        return sharded(particles, prec_diag, mean_vec, low_rank)

    return run_steps
```

```python
import functools

import jax
import jax.numpy as jnp
from jax import lax
from jax.experimental import pallas as pl
from jax.experimental.pallas import tpu as pltpu
from jax.sharding import PartitionSpec as P

NUM_STEPS = 3
BAND_SCALE = 4.0
STEP_SCALE = 0.4
FEAT_AXES = ("slab", "feat")
LEAD_AXES = ("ens", "slab", "feat")

ROWS = 2048
TILE = 128
HALF = 256
BLK = 2 * HALF
COLORS = 6
SROWS = COLORS * BLK
PM_AT = ((0, 0), (0, 1), (0, 5), (1, 5))
DIAG_AT = (((1, 0), (1, 1)), ((0, 4), (1, 4)), ((0, 2), (0, 3)), ((1, 2), (1, 3)))
STREAMS = 6
QUARTER = HALF // 4
UNITS = ((), ((0, 3), (0, 1), (0, 2)), ((1, 2), (1, 3), (2, 3)))
OFFS = (((0, 1), (2, 0), (3, 0)), ((1, 2), (1, 3), (2, 3)))
SENT = 3216
SENT_SUMS = 304
OWN = QUARTER // 4
PEERS = (2, 1, 3)
NEAR_FIRST = (1, 3, 2)
MESH = pl.DeviceIdType.MESH
NT = (((1,), (1,)), ((), ()))
F32, BF16 = jnp.float32, jnp.bfloat16


def div(a, b):
    return lax.div(a, jnp.int32(b))


def rem(a, b):
    return lax.rem(a, jnp.int32(b))


def _kernel(
    bandwidth, step_size, n_part,
    theta_ref, lam_hbm, mu_hbm, fac_hbm, out_ref,
    lam_ref, mu_ref, fac_ref,
    bfull, pml, pmr, nrow, ncol, pulled, scaled, pack, r0, r1, r2, r3, kg, kfull, adrv, svec, srecv, stot, spart,
    in_sem, pre_send, pre_recv, sent, rs_recv, x_recv, near_recv, far_recv, dd_recv, s_recv, sp_recv,
):
    width = out_ref.shape[1]
    rep_coef = 2.0 / bandwidth
    core = lax.axis_index("slab")
    feat = lax.axis_index("feat")
    coords = (rem(feat, 4), rem(div(feat, 4), 4), div(feat, 16))
    strides = (1, 4, 16)

    def chip(dim, coord):
        return {"feat": feat + (coord - coords[dim]) * strides[dim]}

    turned = [[coords[dim]] + [rem(coords[dim] + j, 4) for j in sorted(PEERS)] for dim in range(3)]

    def around(dim, j):
        return turned[dim][j]

    ring = [[chip(dim, turned[dim][j]) for j in range(4)] for dim in range(3)]
    low_bit = [rem(c, 2) for c in coords]
    pair_bit = [[rem(div(t + 1, 2), 2) for t in turned[dim]] for dim in range(3)]
    high_bit = [[div(t, 2) for t in turned[dim]] for dim in range(3)]

    mate = {"slab": 1 - core}

    def al(x, m=16):
        return pl.multiple_of(x, m)

    halves = []
    for k in range(COLORS):
        steps = []
        start, length, cur = 0, HALF, coords[k % 3]
        for s in range(2):
            if (k // 3 + s) % 2 == 0:
                other, bit = cur + 1 - 2 * low_bit[k % 3], pair_bit[k % 3][0]
            else:
                other, bit = 3 - cur, high_bit[k % 3][0]
            length = length // 2
            keep, give = start + bit * length, start + (1 - bit) * length
            start = keep
            steps.append((chip(k % 3, other), length, keep, give))
        halves.append(steps)

    def dims(k):
        return k % 3, (k + 1) % 3, (k + 2) % 3

    def base(st, k):
        return (st * COLORS + k) * HALF

    def tile_row(kind, k, a):
        st, k = DIAG_AT[k][a // 2] if kind == 0 else (2 * kind + a // 2, k)
        return base(st, k) + a % 2 * TILE

    keeps = [[al(step[2]) for step in steps] for steps in halves]
    gives = [[al(step[3]) for step in steps] for steps in halves]
    pieces = [[al(halves[k][1][2] + OWN * around(dims(k)[1], j)) for j in range(4)] for k in range(COLORS)]
    places = []
    for k in range(COLORS):
        one, two = (pair_bit, high_bit) if k < 3 else (high_bit, pair_bit)
        places.append([al(QUARTER * (2 * one[k % 3][j] + two[k % 3][j])) for j in range(4)])

    columns = [[al(m * BLK + (2 * core + n) * TILE, TILE) for n in range(2)] for m in range(4)]

    def packed(st, k, row, rows):
        return pack.at[pl.ds(al(base(st, k) + row), rows)]

    loads = [pltpu.make_async_copy(theta_ref.at[pl.ds(ch * BLK, BLK)], out_ref.at[pl.ds(ch * BLK, BLK)], in_sem.at[ch]) for ch in range(4)]
    loads += [
        pltpu.make_async_copy(src, dst, in_sem.at[4 + n])
        for n, (src, dst) in enumerate(((mu_hbm, mu_ref), (fac_hbm, fac_ref), (lam_hbm, lam_ref)))
    ]
    for cp in loads[4:] + loads[:1]:
        cp.start()
    barrier = pltpu.get_barrier_semaphore()
    pl.semaphore_signal(barrier, inc=1, device_id=mate, device_id_type=MESH)
    for dim in range(3):
        for j in PEERS:
            pl.semaphore_signal(barrier, inc=1, device_id=ring[dim][j], device_id_type=MESH)
    for cp in loads[1:4]:
        cp.start()

    row_i = lax.broadcasted_iota(jnp.int32, (TILE, TILE), 0)
    col_i = lax.broadcasted_iota(jnp.int32, (TILE, TILE), 1)
    eye, upper, lower = row_i == col_i, row_i < col_i, row_i > col_i
    sub_o = lax.broadcasted_iota(jnp.int32, (OWN, TILE), 0)
    lane_o = lax.broadcasted_iota(jnp.int32, (OWN, TILE), 1)

    def remote(src, dst, ssem, rsem, where):
        return pltpu.make_async_remote_copy(src_ref=src, dst_ref=dst, send_sem=ssem, recv_sem=rsem, device_id=where, device_id_type=MESH)

    def pre_bf16(piece):
        rows = pl.ds(piece * HALF, HALF)
        return remote(bfull.at[rows, 0:width], bfull.at[rows, width:2 * width], pre_send, pre_recv.at[piece], mate)

    def pre_pm(ch):
        src, dst = pml.at[pl.ds(al(ch * BLK + (1 - core) * HALF), HALF)], pmr.at[pl.ds(ch * HALF, HALF)]
        return remote(src, dst, pre_send, pre_recv.at[8 + ch], mate)

    def prepare(start, th):
        bfull[pl.ds(start, HALF), 0:width] = th.astype(BF16)
        return (th - mu_ref[...]).astype(BF16)

    def partial_pm(start, centered):
        for n, rows in enumerate(centered):
            pml[pl.ds(start + HALF * n, HALF), :] = jnp.dot(rows, fac_ref[...], preferred_element_type=F32)

    def begin(cps):
        for cp in cps:
            cp.start()

    def arrive(ref, sem):
        remote(ref, ref, sent.at[0], sem, mate).wait_recv()

    def pair_arrive(rows, sem):
        arrive(pack.at[0:6 * rows], sem)

    def rs_copy(st, s, k):
        peer, length, keep, give = halves[k][s]
        src = packed(st, k, gives[k][s], length)
        return remote(src, (r0, r1)[s].at[st, k], sent.at[st], rs_recv.at[st, s, k], peer)

    def gathered(st, k, row, rows):
        if st < 2:
            return kg.at[core, pl.ds(base(st, k) + row, rows)]
        sup, m = UNITS[st // 2][k // 2]
        return kfull.at[pl.ds(sup * BLK + st % 2 * HALF + row, rows), pl.ds(columns[m][k % 2], TILE)]

    def x_copies(st, e, k):
        d1, d2, d3 = dims(k)
        dim = (d2, d3)[e]
        cps = []
        for j in PEERS:
            if e == 0:
                src = packed(st, k, pieces[k][j], OWN)
                dst = r2.at[st, k, j - 1]
            else:
                src = dst = r3.at[st, k, coords[dim]]
            cps.append(remote(src, dst, sent.at[st], x_recv.at[st, e, k % 3], ring[dim][j]))
        return cps

    def gather_copies(st, k, j):
        d1, d2, d3 = dims(k)
        ref = gathered(st, k, pieces[k][(4 - j) % 4], OWN)
        cps = [remote(ref, ref, sent.at[st], far_recv.at[st, k % 3], ring[d1][i]) for i in PEERS]
        if j == 0:
            cps = [remote(ref, ref, sent.at[st], near_recv.at[st, k % 3], ring[d2][i]) for i in PEERS] + cps
        return cps

    def dd_copy(st, k, j):
        ref = gathered(st, k, keeps[k][1] if j == 0 else places[k][4 - j], QUARTER)
        return remote(ref, ref, sent.at[st], dd_recv.at[st], mate)

    def s_copies(ph, d):
        dim = ((d + 1) % 3, d)[ph]
        return [
            remote(svec.at[ph, d], srecv.at[ph, d, j - 1], sent.at[STREAMS - 1], s_recv.at[ph, d], ring[dim][j])
            for j in PEERS
        ]

    def sp_copy():
        return remote(stot, spart, sent.at[STREAMS - 1], sp_recv, mate)

    def products(m):
        mine = bfull[pl.ds(al(m * BLK + HALF * core), HALF), :]
        part = BLK if m == 3 else (m + 1) * HALF
        return [lax.dot_general(bfull[pl.ds(at, part), :], mine, NT, preferred_element_type=F32) for at in range(0, (m + 1) * BLK, part)]

    def norms(m):
        for i in range(4):
            rows = pl.ds((4 * m + i) * TILE, TILE)
            wide = bfull[rows, :].astype(F32)
            n = jnp.broadcast_to(jnp.sum(wide * wide, axis=1, keepdims=True), (TILE, TILE))
            nrow[rows, :] = n
            ncol[4 * m + i:4 * m + i + 1, :] = jnp.sum(jnp.where(eye, n, 0.0), axis=0, keepdims=True)

    def tiles(m, g):
        def block(blk, b):
            n, r = divmod(blk * TILE, BLK if m == 3 else (m + 1) * HALF)
            return g[n][r:r + TILE, b * TILE:(b + 1) * TILE]

        def tile(i, b):
            return block(4 * m + i, b)

        def dist(i, j):
            return nrow[pl.ds((4 * m + i) * TILE, TILE), :] + ncol[4 * m + j:4 * m + j + 1, :] - 2.0 * tile(i, j % 2)

        for t in range(3):
            pack[pl.ds(tile_row(0, m, t), TILE), :] = jnp.where(core == 0, dist(*OFFS[0][t]), dist(*OFFS[1][t]))
        one = jnp.where(core == 0, dist(0, 0), dist(2, 2))
        two = jnp.where(core == 0, dist(1, 1), dist(3, 3))
        pack[pl.ds(tile_row(0, m, 3), TILE), :] = jnp.where(upper, one, two)
        begin([rs_copy(st, 0, k) for st, k in DIAG_AT[m]])
        for kind in (1, 2):
            for u, (sup, col) in enumerate(UNITS[kind]):
                if col != m:
                    continue
                for b in range(2):
                    nc = ncol[pl.ds(4 * m + 2 * core + b, 1), :]
                    for a in range(4):
                        nr = nrow[pl.ds((4 * sup + a) * TILE, TILE), :]
                        pack[pl.ds(tile_row(kind, 2 * u + b, a), TILE), :] = nr + nc - 2.0 * block(4 * sup + a, b)
                begin([rs_copy(st, 0, 2 * u + b) for st in (2 * kind, 2 * kind + 1) for b in range(2)])

    def pm_tiles(chs):
        for ch in chs:
            pre_pm(ch).wait_recv()
            mine = pl.ds(al(ch * BLK + core * HALF), HALF)
            pack[pl.ds(base(*PM_AT[ch]), HALF), :] = pml[mine, :] + pmr[pl.ds(ch * HALF, HALF), :]
            begin([rs_copy(PM_AT[ch][0], 0, PM_AT[ch][1])])

    def open_step(finish_last):
        pm_tiles(range(3))
        for piece in range(4):
            pre_bf16(piece).wait_recv()
        finish_last()
        one, zero = products(1), products(0)
        for m in range(2):
            norms(m)
        begin([pre_pm(3), pre_bf16(7)])
        tiles(1, one)
        tiles(0, zero)
        pm_tiles((3,))
        for m in range(2, 4):
            for piece in range(2 * m, 2 * m + 2):
                pre_bf16(piece).wait_recv()
            g = products(m)
            norms(m)
            tiles(m, g)

    for cp in loads[4:]:
        cp.wait()
    for ch in range(4):
        loads[ch].wait()
        starts = (ch * BLK, ch * BLK + HALF)
        partial_pm(ch * BLK, [prepare(start, out_ref[pl.ds(start, HALF), :]) for start in starts])
        if ch == 0:
            pl.semaphore_wait(barrier, 10)
        if ch < 3:
            begin([pre_pm(ch)])
        begin([pre_bf16(piece) for piece in (2 * ch, 2 * ch + 1) if piece < 7])
    open_step(lambda: None)

    def one_step(step_index, carry):
        def row_sums(st, k, kern):
            m, part = (0, st % 2) if st > 1 else [(m, part) for m in range(4) for part in range(2) if DIAG_AT[m][part] == (st, k)][0]
            place = pieces[k][0] + part * HALF
            slot, r = div(place, TILE), rem(place, TILE)

            def by_rows(vals):
                rs = jnp.sum(vals, axis=1, keepdims=True)
                return jnp.sum(jnp.where(lane_o == sub_o + r, rs, 0.0), axis=0, keepdims=True)

            def by_cols(vals):
                return jnp.sum(vals, axis=0, keepdims=True)

            if st > 1:
                sup, m = UNITS[st // 2][k // 2]
                return [(4 * sup + slot, by_rows(kern)), (4 * m + 2 * core + k % 2, by_cols(kern))]
            both = div(slot, 3)
            up_one = div(slot + 1, 2)
            i0 = (1 - both) * ((1 - core) * (slot + up_one) + core * (1 + div(slot, 2))) + both * 2 * core
            j0 = (1 - both) * ((1 - core) * (1 - up_one) + core * (2 + up_one)) + both * 2 * core
            up = jnp.where(lane_o + 1000 * (1 - both) > sub_o + r, kern, 0.0)
            lo = jnp.where(lane_o + 1000 * (1 - both) < sub_o + r, kern, 0.0)
            nxt = 4 * m + 2 * core + 1
            return [(4 * m + i0, by_rows(up)), (4 * m + j0, by_cols(up)), (nxt, by_rows(lo)), (nxt, by_cols(lo))]

        def advance(st, s):
            parts = [[], [], []]
            if s == 4 and st == STREAMS - 1:
                for d in range(3):
                    arrive(srecv.at[0, d], s_recv.at[0, d])
                    svec[1, d] = svec[0, d] + srecv[0, d, 0] + srecv[0, d, 1] + srecv[0, d, 2]
                    begin(s_copies(1, d))
            if s == 5 and st == STREAMS - 1:
                tot = jnp.zeros((16, TILE), F32)
                for d in range(3):
                    arrive(srecv.at[1, d], s_recv.at[1, d])
                    tot = tot + ((svec[1, d] + srecv[1, d, 0]) + (srecv[1, d, 1] + srecv[1, d, 2]))
                stot[...] = tot
                begin([sp_copy()])
            kerns = {}
            for k in ((0, 1, 5, 4, 2, 3) if s < 1 else range(COLORS) if s < 2 else (0, 3, 1, 4, 2, 5)):
                if s < 2:
                    peer, length, keep, give = halves[k][s]
                    rs_copy(st, s, k).wait_recv()
                    packed(st, k, keeps[k][s], length)[...] += (r0, r1)[s][st, k]
                    begin([rs_copy(st, 1, k)] if s == 0 else x_copies(st, 0, k))
                    continue
                if k < 3:
                    sem = x_recv.at[st, s - 2, k] if s < 4 else (near_recv, far_recv)[s - 4].at[st, k]
                    pair_arrive((OWN, OWN, OWN // 2, QUARTER // 2)[s - 2], sem)
                if s == 2:
                    r3[st, k, coords[dims(k)[2]]] = packed(st, k, pieces[k][0], OWN)[...] + r2[st, k, 0] + r2[st, k, 1] + r2[st, k, 2]
                    begin(x_copies(st, 1, k))
                elif s == 3:
                    full = (r3[st, k, 0] + r3[st, k, 1]) + (r3[st, k, 2] + r3[st, k, 3])
                    kern = full if (st, k) in PM_AT else jnp.exp(-jnp.maximum(full, 0.0) / bandwidth)
                    gathered(st, k, pieces[k][0], OWN)[...] = kern.astype(BF16)
                    begin(gather_copies(st, k, 0))
                    kerns[k] = kern
                elif s == 4:
                    begin([dd_copy(st, k, 0)])
                    for j in NEAR_FIRST:
                        begin(gather_copies(st, k, j))
                else:
                    begin([dd_copy(st, k, j) for j in NEAR_FIRST])
            if s == 3:
                for k, kern in kerns.items():
                    if (st, k) not in PM_AT:
                        parts[k % 3] += row_sums(st, k, kern)
                for d in range(3):
                    if st == 0:
                        svec[0, d] = jnp.zeros((16, TILE), F32)
                    for block, line in parts[d]:
                        svec[0, d, pl.ds(block, 1), :] += line
                    if st == STREAMS - 1:
                        begin(s_copies(0, d))
        def unpack_wait(kind):
            for st in (2 * kind, 2 * kind + 1):
                arrive(kg.at[core, 0:COLORS * HALF], dd_recv.at[st])

        def unpack(kind):
            for c in range(2):
                if kind > 0:
                    for k in range(COLORS):
                        sup, m = UNITS[kind][k // 2]
                        jrng = pl.ds((4 * m + 2 * c + k % 2) * TILE, TILE)
                        for a in range(4):
                            srng = pl.ds((4 * sup + a) * TILE, TILE)
                            kfull[jrng, srng] = kfull[srng, jrng].T
                    continue
                for sup in range(4):
                    for t, (i, j) in enumerate(OFFS[c]):
                        src = kg[c, pl.ds(tile_row(0, sup, t), TILE), :]
                        ri, rj = pl.ds((4 * sup + i) * TILE, TILE), pl.ds((4 * sup + j) * TILE, TILE)
                        kfull[ri, rj] = src
                        kfull[rj, ri] = src.T
                    src = kg[c, pl.ds(tile_row(0, sup, 3), TILE), :]
                    srt = src.T
                    one = jnp.ones((TILE, TILE), BF16)
                    ra, rb = pl.ds((4 * sup + 2 * c) * TILE, TILE), pl.ds((4 * sup + 2 * c + 1) * TILE, TILE)
                    kfull[ra, ra] = jnp.where(upper, src, jnp.where(lower, srt, one))
                    kfull[rb, rb] = jnp.where(lower, src, jnp.where(upper, srt, one))

        def drive_parts():
            for q in range(8):
                rows = pl.ds(q * HALF, HALF)
                th = out_ref[rows, :]
                pulled[rows, :] = (th - mu_ref[...]) * lam_ref[...]
                scaled[rows, :] = rep_coef * th

        def drive():
            for q in range(8):
                rows = pl.ds(q * HALF, HALF)
                ch = q // 2
                pm = kg[q % 2, pl.ds(base(*PM_AT[ch]), HALF), :]
                low = lax.dot_general(pm, fac_ref[...], NT, preferred_element_type=F32)
                adrv[rows, :] = ((pulled[rows, :] + low) + scaled[rows, :]).astype(BF16)

        def product(start):
            return jnp.dot(kfull[pl.ds(start, HALF), :], adrv[...], preferred_element_type=F32)

        def finish(start, acc, tot, held):
            rows = pl.ds(start, HALF)
            sums = []
            for blk in (start // TILE, start // TILE + 1):
                line = jnp.where(eye, jnp.broadcast_to(tot[blk:blk + 1, :], (TILE, TILE)), 0.0)
                sums.append(rep_coef * jnp.sum(line, axis=1, keepdims=True))
            sums = jnp.broadcast_to(jnp.concatenate(sums, axis=0), (HALF, TILE))
            new = []
            for t in range(width // TILE):
                cols = slice(t * TILE, (t + 1) * TILE)
                th = out_ref[rows, cols]
                phi = (sums * th - acc[:, cols]) / n_part
                new.append(th + step_size * phi)
            th = jnp.concatenate(new, axis=1)
            out_ref[rows, :] = th
            held.append(prepare(start, th))
            if start % BLK:
                partial_pm(start - HALF, held[-2:])

        def share(start):
            if start % BLK and start + HALF < ROWS:
                begin([pre_pm(start // BLK), pre_bf16(start // HALF - 1), pre_bf16(start // HALF)])
            elif start + BLK == ROWS:
                begin([pre_bf16(start // HALF)])

        drive_parts()
        def early_rounds(s):
            def one(st, c):
                advance(st, s)
                return c

            lax.fori_loop(0, STREAMS, one, 0)

        for s in range(3):
            early_rounds(s)
        for s in range(3, 6):
            for st in range(STREAMS):
                if s == 5 and st == STREAMS - 2:
                    unpack_wait(0)
                    unpack(0)
                    drive()
                advance(st, s)
        remote(pack.at[0:5120], pack.at[0:5120], pre_send, sp_recv, mate).wait_send()
        def update(starts, kind):
            tot = stot[...] + spart[...] + 1.0
            ahead = product(starts[0])
            unpack(kind)
            held = []
            for n, start in enumerate(starts):
                acc = ahead
                if n + 1 < len(starts):
                    ahead = product(starts[n + 1])
                if n:
                    share(starts[n - 1])
                if start + HALF == ROWS:
                    return lambda: finish(start, acc, tot, list(held))
                finish(start, acc, tot, held)
            share(starts[-1])

        unpack_wait(1)
        arrive(stot, sp_recv)
        update(range(0, BLK, HALF), 1)
        unpack_wait(2)
        finish_last = update(range(BLK, ROWS, HALF), 2)
        for st in range(STREAMS):
            total = pack.at[0:SENT + (SENT_SUMS if st == STREAMS - 1 else 0)]
            remote(total, total, sent.at[st], sp_recv, mate).wait_send()
        pl.when(step_index < NUM_STEPS - 1)(lambda: open_step(finish_last))
        pl.when(step_index == NUM_STEPS - 1)(finish_last)
        return carry

    lax.fori_loop(0, NUM_STEPS, one_step, 0)
    for ch in range(3):
        pre_pm(ch).wait_recv()
    for piece in range(7):
        pre_bf16(piece).wait_recv()
    total = pack.at[0:7 * 512 + 3 * HALF]
    remote(total, total, pre_send, sp_recv, mate).wait_send()


def solution(mesh):
    def run_steps(particles, prec_diag, mean_vec, low_rank):
        total_rows, width = particles.shape
        n_part = total_rows // mesh.shape["ens"]
        bandwidth = BAND_SCALE * width
        step_size = STEP_SCALE * width
        loc = width // (mesh.shape["slab"] * mesh.shape["feat"])
        rank = low_rank.shape[1]
        vm, dma = pltpu.VMEM, pltpu.SemaphoreType.DMA

        def local_steps(current, prec_loc, mean_loc, fac_loc):
            spec = pl.BlockSpec(memory_space=pltpu.VMEM)
            call = pl.pallas_call(
                functools.partial(_kernel, bandwidth, step_size, n_part),
                out_shape=jax.ShapeDtypeStruct((n_part, loc), F32),
                in_specs=[pl.BlockSpec(memory_space=pltpu.HBM)] * 4,
                out_specs=spec,
                scratch_shapes=[
                    vm((1, loc), F32), vm((1, loc), F32), vm((loc, rank), BF16),
                    vm((ROWS, 2 * loc), BF16), vm((ROWS, rank), F32), vm((ROWS // 2, rank), F32),
                    vm((ROWS, TILE), F32), vm((16, TILE), F32), vm((ROWS, loc), F32), vm((ROWS, loc), F32),
                    vm((3 * SROWS, TILE), F32),
                    vm((STREAMS, COLORS, HALF // 2, TILE), F32), vm((STREAMS, COLORS, QUARTER, TILE), F32),
                    vm((STREAMS, COLORS, 3, OWN, TILE), F32), vm((STREAMS, COLORS, 4, OWN, TILE), F32),
                    vm((2, SROWS, TILE), BF16), vm((ROWS, ROWS), BF16), vm((ROWS, loc), BF16),
                    vm((2, 3, 16, TILE), F32), vm((2, 3, 3, 16, TILE), F32), vm((16, TILE), F32), vm((16, TILE), F32),
                    dma((7,)), dma, dma((12,)), dma((STREAMS,)), dma((STREAMS, 2, COLORS)), dma((STREAMS, 2, 3)),
                    dma((STREAMS, 3)), dma((STREAMS, 3)), dma((STREAMS,)),
                    dma((2, 3)), dma,
                ],
                compiler_params=pltpu.CompilerParams(collective_id=0, has_side_effects=True, vmem_limit_bytes=50000000),
                name="svgd",
            )
            hbm = lambda x: pltpu.with_memory_space_constraint(x, pltpu.HBM)
            return call(hbm(current), hbm(prec_loc.reshape(1, loc)), hbm(mean_loc.reshape(1, loc)), hbm(fac_loc))

        sharded = jax.shard_map(
            local_steps,
            mesh=mesh,
            in_specs=(P("ens", FEAT_AXES), P(LEAD_AXES), P(LEAD_AXES), P(LEAD_AXES, None)),
            out_specs=P("ens", FEAT_AXES),
            check_vma=False,
        )
        return sharded(particles, prec_diag, mean_vec, low_rank)

    return run_steps
```
